32 devices in a mesh: dp: 2 (over x), tp: 4 (over z), cp: 4 (over y, core).
Axes of the slice: x: 2, y: 2, z: 4, core: 2. Of those that a mesh axis runs over, the one named last changes fastest.
Arguments:
- hidden_in: bfloat16 [8, 1024, 2048], P('dp'), parts along dimension 0
- lengths: int32 [8], P('dp'), parts along dimension 0
- k_cache: bfloat16 [8, 16, 4096, 128], P('dp', 'tp', 'cp'), parts along dimension 0
- v_cache: bfloat16 [8, 16, 4096, 128], P('dp', 'tp', 'cp'), parts along dimension 0
- ln1_gain: float32 [2048], replicated
- ln1_bias: float32 [2048], replicated
- ln2_gain: float32 [2048], replicated
- ln2_bias: float32 [2048], replicated
- w_qkv: bfloat16 [2048, 6144], P(None, 'tp')
- b_qkv: bfloat16 [6144], P('tp')
- w_out: bfloat16 [2048, 2048], P('tp')
- b_out: bfloat16 [2048], replicated
- w_up: bfloat16 [2048, 8192], P(None, 'tp')
- b_up: bfloat16 [8192], P('tp')
- w_down: bfloat16 [8192, 2048], P('tp')
- b_down: bfloat16 [2048], replicated
Outputs:
- output 1: bfloat16 [8, 1024, 2048], P('dp'), parts along dimension 0
- output 2: bfloat16 [8, 16, 1024, 128], P('dp', 'tp'), parts along dimension 0
- output 3: bfloat16 [8, 16, 1024, 128], P('dp', 'tp'), parts along dimension 0
There are 2 independent parts. The reference program is written for one: setup_inputs(seed, part) draws one part's arguments, and reference() takes and returns one part's arrays. A program takes and returns all parts, laid end to end along the dimension named above; an argument that names none is the same for every part.
All inputs are finite; a program needn't handle non-finite values.
Results may differ from the reference program's by a relative error of at most 0.00418695.
Values sent between devices are 32-bit elements.
A program may use at most 1 GiB of HBM per device.

```python
import math
import jax
import jax.numpy as jnp
from jax import lax

D_MODEL = 2048
NUM_HEADS = 16
HEAD_DIM = 128
FF_DIM = 8192
NUM_ROWS = 4
CHUNK_LEN = 1024
CACHE_LEN = 4096
ROT_DIM = HEAD_DIM // 4
SCORE_SCALE = HEAD_DIM ** -0.5
Q_SCALE = math.sqrt(math.log(CACHE_LEN / 4.0))
NEG_BIG = -1e30
EPSILON = 1e-5
ROPE_BASE = 10000.0


def draw_lengths(len_key):
    draw_keys = jax.random.split(len_key, 2)
    drawn = jax.random.randint(draw_keys[0], (NUM_ROWS,), 1, CACHE_LEN + 1, dtype=jnp.int32)
    full_row = jax.random.randint(draw_keys[1], (), 0, NUM_ROWS, dtype=jnp.int32)
    row_ids = jnp.arange(NUM_ROWS, dtype=jnp.int32)
    drawn = jnp.where(row_ids == full_row, CACHE_LEN, drawn)
    return jnp.where(row_ids == (full_row + 1) % NUM_ROWS, 1, drawn).astype(jnp.int32)


def draw_cache(cache_key):
    row_keys = jax.random.split(cache_key, NUM_ROWS)
    return lax.map(lambda row_key: jax.random.normal(row_key, (NUM_HEADS, CACHE_LEN, HEAD_DIM), jnp.float32).astype(jnp.bfloat16), row_keys)


def setup_inputs(seed: int = 0, part: int = 0) -> dict:
    shared = jax.random.split(jax.random.key(seed), 12)
    part_keys = jax.random.split(jax.random.fold_in(jax.random.key(seed + 1), part), 4)
    qkv_gain = jnp.array([Q_SCALE, 1.0, 1.0], jnp.float32).reshape(1, 3, 1)
    hidden_in = 0.5 * jax.random.normal(part_keys[0], (NUM_ROWS, CHUNK_LEN, D_MODEL), jnp.float32)
    w_qkv = jax.random.normal(shared[0], (D_MODEL, NUM_HEADS, 3, HEAD_DIM), jnp.float32) * qkv_gain * D_MODEL ** -0.5
    b_qkv = 0.5 * jax.random.normal(shared[1], (NUM_HEADS, 3, HEAD_DIM), jnp.float32) * qkv_gain
    return {
        "hidden_in": hidden_in.astype(jnp.bfloat16),
        "lengths": draw_lengths(part_keys[1]),
        "k_cache": draw_cache(part_keys[2]),
        "v_cache": draw_cache(part_keys[3]),
        "ln1_gain": 1.0 + 0.2 * jax.random.normal(shared[2], (D_MODEL,), jnp.float32),
        "ln1_bias": 0.2 * jax.random.normal(shared[3], (D_MODEL,), jnp.float32),
        "ln2_gain": 1.0 + 0.2 * jax.random.normal(shared[4], (D_MODEL,), jnp.float32),
        "ln2_bias": 0.2 * jax.random.normal(shared[5], (D_MODEL,), jnp.float32),
        "w_qkv": w_qkv.reshape(D_MODEL, NUM_HEADS * 3 * HEAD_DIM).astype(jnp.bfloat16),
        "b_qkv": b_qkv.reshape(NUM_HEADS * 3 * HEAD_DIM).astype(jnp.bfloat16),
        "w_out": (1.5 * D_MODEL ** -0.5 * jax.random.normal(shared[6], (D_MODEL, D_MODEL), jnp.float32)).astype(jnp.bfloat16),
        "b_out": (0.5 * jax.random.normal(shared[7], (D_MODEL,), jnp.float32)).astype(jnp.bfloat16),
        "w_up": (D_MODEL ** -0.5 * jax.random.normal(shared[8], (D_MODEL, FF_DIM), jnp.float32)).astype(jnp.bfloat16),
        "b_up": (0.5 * jax.random.normal(shared[9], (FF_DIM,), jnp.float32)).astype(jnp.bfloat16),
        "w_down": (FF_DIM ** -0.5 * jax.random.normal(shared[10], (FF_DIM, D_MODEL), jnp.float32)).astype(jnp.bfloat16),
        "b_down": (0.5 * jax.random.normal(shared[11], (D_MODEL,), jnp.float32)).astype(jnp.bfloat16),
    }


def layer_norm(values_in, gain_vec, bias_vec):
    x_f32 = values_in.astype(jnp.float32)
    row_mean = jnp.mean(x_f32, axis=-1, keepdims=True)
    centered = x_f32 - row_mean
    variance = jnp.mean(centered * centered, axis=-1, keepdims=True)
    return (centered * lax.rsqrt(variance + EPSILON) * gain_vec + bias_vec).astype(jnp.bfloat16)


def rotary(values_in, positions):
    half_rot = ROT_DIM // 2
    inv_freq = ROPE_BASE ** (-2.0 * jnp.arange(half_rot, dtype=jnp.float32) / ROT_DIM)
    angles = positions.astype(jnp.float32)[..., None] * inv_freq
    cos_tab = jnp.cos(angles)[..., None, :]
    sin_tab = jnp.sin(angles)[..., None, :]
    rot_first = values_in[..., :half_rot].astype(jnp.float32)
    rot_second = values_in[..., half_rot:ROT_DIM].astype(jnp.float32)
    new_first = rot_first * cos_tab - rot_second * sin_tab
    new_second = rot_second * cos_tab + rot_first * sin_tab
    return jnp.concatenate([new_first.astype(jnp.bfloat16), new_second.astype(jnp.bfloat16), values_in[..., ROT_DIM:]], axis=-1)


def attend_row(operands):
    q_row, kn_row, vn_row, kc_row, vc_row, row_len = operands
    cache_valid = (jnp.arange(CACHE_LEN) < row_len)[None, :]
    causal = jnp.arange(CHUNK_LEN)[:, None] >= jnp.arange(CHUNK_LEN)[None, :]

    def attend_head(head_ops):
        q_head, kn_head, vn_head, kc_head, vc_head = head_ops
        s_cache = jnp.where(cache_valid, jnp.dot(q_head, kc_head.T, preferred_element_type=jnp.float32) * SCORE_SCALE, NEG_BIG)
        s_self = jnp.where(causal, jnp.dot(q_head, kn_head.T, preferred_element_type=jnp.float32) * SCORE_SCALE, NEG_BIG)
        row_max = jnp.maximum(s_cache.max(axis=1), s_self.max(axis=1))[:, None]
        p_cache = jnp.where(cache_valid, jnp.exp(s_cache - row_max), 0.0)
        p_self = jnp.where(causal, jnp.exp(s_self - row_max), 0.0)
        prob_sum = p_cache.sum(axis=1) + p_self.sum(axis=1)
        weighted = jnp.dot(p_cache.astype(jnp.bfloat16), vc_head, preferred_element_type=jnp.float32) + jnp.dot(p_self.astype(jnp.bfloat16), vn_head, preferred_element_type=jnp.float32)
        return (weighted / prob_sum[:, None]).astype(jnp.bfloat16)

    return lax.map(attend_head, (q_row, kn_row, vn_row, kc_row, vc_row))


def reference(hidden_in, lengths, k_cache, v_cache, ln1_gain, ln1_bias, ln2_gain, ln2_bias, w_qkv, b_qkv, w_out, b_out, w_up, b_up, w_down, b_down):
    flat_in = hidden_in.reshape(NUM_ROWS * CHUNK_LEN, D_MODEL)
    normed_attn = layer_norm(flat_in, ln1_gain, ln1_bias)
    normed_mlp = layer_norm(flat_in, ln2_gain, ln2_bias)
    qkv_all = (jnp.dot(normed_attn, w_qkv, preferred_element_type=jnp.float32) + b_qkv.astype(jnp.float32)).astype(jnp.bfloat16)
    qkv_all = qkv_all.reshape(NUM_ROWS, CHUNK_LEN, NUM_HEADS, 3, HEAD_DIM)
    positions = lengths[:, None] + jnp.arange(CHUNK_LEN, dtype=jnp.int32)[None, :]
    q_rot = jnp.swapaxes(rotary(qkv_all[:, :, :, 0], positions), 1, 2)
    k_new = jnp.swapaxes(rotary(qkv_all[:, :, :, 1], positions), 1, 2)
    v_new = jnp.swapaxes(qkv_all[:, :, :, 2], 1, 2)
    context = lax.map(attend_row, (q_rot, k_new, v_new, k_cache, v_cache, lengths))
    context = jnp.swapaxes(context, 1, 2).reshape(NUM_ROWS * CHUNK_LEN, D_MODEL)
    attn_out = jnp.dot(context, w_out, preferred_element_type=jnp.float32)
    hidden = jax.nn.gelu(jnp.dot(normed_mlp, w_up, preferred_element_type=jnp.float32) + b_up.astype(jnp.float32), approximate=False).astype(jnp.bfloat16)
    mlp_out = jnp.dot(hidden, w_down, preferred_element_type=jnp.float32)
    out_sum = flat_in.astype(jnp.float32) + attn_out + b_out.astype(jnp.float32) + mlp_out + b_down.astype(jnp.float32)
    hidden_out = out_sum.astype(jnp.bfloat16).reshape(NUM_ROWS, CHUNK_LEN, D_MODEL)
    return (hidden_out, k_new, v_new)
```

```python
import functools
import math

import jax
import jax.numpy as jnp
from jax import lax
from jax.experimental import pallas as pl
from jax.experimental.pallas import tpu as pltpu
from jax.sharding import PartitionSpec as P

EPSILON = 1e-5
NEG_BIG = -1e30
ROTARY_SHARE = 4
ROPE_BASE = 10000.0
LOG2E = math.log2(math.e)
MESH = pl.DeviceIdType.MESH
F32 = jnp.float32
BF16 = jnp.bfloat16
VMEM_LIMIT = 60 * 1024 * 1024
CHUNKS = 64
STAGES = 4
LAG_BACK = 2
LAG_CORE = 3
LAG_Y = 6
LAG_LAST = 7


def layer_norm(values_in, gain_vec, bias_vec):
    x_f32 = values_in.astype(F32)
    row_mean = jnp.mean(x_f32, axis=-1, keepdims=True)
    centered = x_f32 - row_mean
    variance = jnp.mean(centered * centered, axis=-1, keepdims=True)
    return (centered * lax.rsqrt(variance + EPSILON) * gain_vec + bias_vec).astype(BF16)


def rope_table(lengths, chunk_len, head_dim):
    rot_dim = head_dim // ROTARY_SHARE
    half_rot = rot_dim // 2
    positions = lengths[:, None] + jnp.arange(chunk_len, dtype=jnp.int32)[None, :]
    inv_freq = ROPE_BASE ** (-2.0 * jnp.arange(half_rot, dtype=F32) / rot_dim)
    angles = positions.astype(F32)[..., None] * inv_freq
    cos_tab = jnp.cos(angles)
    sin_tab = jnp.sin(angles)
    pad = jnp.zeros(angles.shape[:-1] + (head_dim - 2 * rot_dim,), F32)
    return jnp.concatenate([cos_tab, cos_tab, -sin_tab, sin_tab, pad], axis=-1)


def qkv_kernel(heads, head_dim, x_ref, gain_ref, bias_ref, w_ref, wb_ref, tab_ref, q_ref, k_ref, v_ref):
    rot_dim = head_dim // ROTARY_SHARE
    half_rot = rot_dim // 2
    normed = layer_norm(x_ref[0], gain_ref[...], bias_ref[...])
    tab = tab_ref[0]
    lane = lax.broadcasted_iota(jnp.int32, tab.shape, 1)
    cos_tab = jnp.where(lane < rot_dim, tab, 1.0)
    sin_tab = jnp.where(lane < rot_dim, pltpu.roll(tab, head_dim - rot_dim, 1), 0.0)

    def rotate(values):
        wide = values.astype(F32)
        other = jnp.where(lane < half_rot, pltpu.roll(wide, head_dim - half_rot, 1), pltpu.roll(wide, half_rot, 1))
        return (wide * cos_tab + other * sin_tab).astype(BF16)

    pair = 2 * 3 * head_dim
    for first in range(0, heads, 2):
        cols = slice(first // 2 * pair, first // 2 * pair + pair)
        both = (jnp.dot(normed, w_ref[:, cols], preferred_element_type=F32) + wb_ref[:, cols]).astype(BF16)
        for h in (first, first + 1):
            base = (h - first) * 3 * head_dim
            q_ref[0, h] = rotate(both[:, base:base + head_dim])
            k_ref[0, h] = rotate(both[:, base + head_dim:base + 2 * head_dim])
            v_ref[0, h] = both[:, base + 2 * head_dim:base + 3 * head_dim]


def project_qkv(hidden_in, gain, bias, w_qkv, b_qkv, table, heads, head_dim):
    rows, chunk_len, d_model = hidden_in.shape
    tile = chunk_len // 4
    width = w_qkv.shape[1]
    out = jax.ShapeDtypeStruct((rows, heads, chunk_len, head_dim), BF16)
    head_spec = pl.BlockSpec((1, heads, tile, head_dim), lambda b, t: (b, 0, t, 0))
    once = dict(pipeline_mode=pl.Buffered(1))
    return pl.pallas_call(
        functools.partial(qkv_kernel, heads, head_dim),
        grid=(rows, chunk_len // tile),
        in_specs=[
            pl.BlockSpec((1, tile, d_model), lambda b, t: (b, t, 0)),
            pl.BlockSpec((1, d_model), lambda b, t: (0, 0), **once),
            pl.BlockSpec((1, d_model), lambda b, t: (0, 0), **once),
            pl.BlockSpec((d_model, width), lambda b, t: (0, 0), **once),
            pl.BlockSpec((1, width), lambda b, t: (0, 0), **once),
            pl.BlockSpec((1, tile, head_dim), lambda b, t: (b, t, 0)),
        ],
        out_specs=[head_spec] * 3,
        out_shape=[out] * 3,
        compiler_params=pltpu.CompilerParams(vmem_limit_bytes=VMEM_LIMIT),
        cost_estimate=pl.CostEstimate(
            flops=2 * rows * chunk_len * d_model * width,
            bytes_accessed=2 * (rows * chunk_len * (d_model + width) + d_model * width),
            transcendentals=0,
        ),
        name="qkv_rope",
    )(hidden_in, gain[None], bias[None], w_qkv, b_qkv.astype(F32)[None], table)


def block_step(heads, scale, q_of, k_of, v_of, m_scr, l_scr, o_scr, mask):
    for h in range(heads):
        scores = lax.dot_general(q_of(h), k_of(h), (((1,), (1,)), ((), ())), preferred_element_type=F32) * scale
        if mask is not None:
            scores = jnp.where(mask, scores, NEG_BIG)
        m_old = m_scr[h]
        m_new = jnp.maximum(m_old, jnp.max(scores, axis=1, keepdims=True))
        probs = jnp.exp2(scores - m_new[:, :1])
        shrink = jnp.exp2(m_old - m_new)
        l_scr[h] = l_scr[h] * shrink + jnp.sum(probs, axis=1, keepdims=True)
        m_scr[h] = m_new
        o_scr[h] = o_scr[h] * shrink + jnp.dot(probs.astype(BF16), v_of(h), preferred_element_type=F32)


def attn_kernel(heads, head_dim, q_tile, key_block, with_self, meta, q_ref, k_ref, v_ref, *rest):
    if with_self:
        kn_ref, vn_ref, *rest = rest
    os_ref, ss_ref, ok_ref, sk_ref, m_scr, l_scr, o_scr = rest
    slot = pl.program_id(0)
    tile = pl.program_id(1)
    valid = meta[2 + slot]
    scale = head_dim ** -0.5 * LOG2E
    m_scr[...] = jnp.full(m_scr.shape, NEG_BIG, F32)
    l_scr[...] = jnp.zeros(l_scr.shape, F32)
    o_scr[...] = jnp.zeros(o_scr.shape, F32)

    def query(h):
        return q_ref[0, h]

    def cache_block(block, mask):
        start = pl.multiple_of(block * key_block, key_block)
        block_step(
            heads, scale, query,
            lambda h: k_ref[0, h, pl.ds(start, key_block), :],
            lambda h: v_ref[0, h, pl.ds(start, key_block), :],
            m_scr, l_scr, o_scr, mask,
        )

    whole = lax.div(valid, key_block)

    @pl.loop(0, whole)
    def _(block):
        cache_block(block, None)

    @pl.when(lax.rem(valid, key_block) > 0)
    def _():
        keys = whole * key_block + lax.broadcasted_iota(jnp.int32, (q_tile, key_block), 1)
        cache_block(whole, keys < valid)

    if with_self:
        def own_block(block, mask):
            start = pl.multiple_of(block * q_tile, q_tile)
            block_step(
                heads, scale, query,
                lambda h: kn_ref[0, h, pl.ds(start, q_tile), :],
                lambda h: vn_ref[0, h, pl.ds(start, q_tile), :],
                m_scr, l_scr, o_scr, mask,
            )

        @pl.when(slot == 1)
        def _():
            @pl.loop(0, tile)
            def _(block):
                own_block(block, None)

            shape = (q_tile, q_tile)
            own_block(tile, lax.broadcasted_iota(jnp.int32, shape, 0) >= lax.broadcasted_iota(jnp.int32, shape, 1))

    lane = lax.broadcasted_iota(jnp.int32, (q_tile, head_dim), 1)
    stats = jnp.zeros((q_tile, head_dim), F32)
    for h in range(heads):
        stats = jnp.where(lane == h, m_scr[h], stats)
        stats = jnp.where(lane == heads + h, l_scr[h], stats)
    stats = stats.T[:8]

    @pl.when(slot == 0)
    def _():
        os_ref[...] = o_scr[...]
        ss_ref[...] = stats

    @pl.when(slot == 1)
    def _():
        ok_ref[...] = o_scr[...]
        sk_ref[...] = stats


def attend(rows, lengths, block_start, q_all, k_block, v_block, k_new=None, v_new=None):
    heads, chunk_len, head_dim = q_all.shape[1:]
    block_len = k_block.shape[2]
    q_tile = chunk_len // 4
    key_block = block_len // 2
    tiles = chunk_len // q_tile
    valid = jnp.clip(lengths[rows] - block_start, 0, block_len)
    meta = jnp.concatenate([rows, valid]).astype(jnp.int32)
    with_self = k_new is not None
    keys = pl.BlockSpec((1, heads, block_len, head_dim), lambda s, t, meta: (meta[s], 0, 0, 0))
    own = pl.BlockSpec((1, heads, chunk_len, head_dim), lambda s, t, meta: (meta[1], 0, 0, 0))
    sent = lambda s, t: jnp.where(s == 0, t, tiles - 1)
    kept = lambda s, t: jnp.where(s == 0, 0, t)
    o_shape = jax.ShapeDtypeStruct((heads, chunk_len, head_dim), F32)
    s_shape = jax.ShapeDtypeStruct((8, chunk_len), F32)
    return pl.pallas_call(
        functools.partial(attn_kernel, heads, head_dim, q_tile, key_block, with_self),
        grid_spec=pltpu.PrefetchScalarGridSpec(
            num_scalar_prefetch=1,
            grid=(2, tiles),
            in_specs=[pl.BlockSpec((1, heads, q_tile, head_dim), lambda s, t, meta: (meta[s], 0, t, 0)), keys, keys]
            + ([own, own] if with_self else []),
            out_specs=[
                pl.BlockSpec((heads, q_tile, head_dim), lambda s, t, meta: (0, sent(s, t), 0)),
                pl.BlockSpec((8, q_tile), lambda s, t, meta: (0, sent(s, t))),
                pl.BlockSpec((heads, q_tile, head_dim), lambda s, t, meta: (0, kept(s, t), 0)),
                pl.BlockSpec((8, q_tile), lambda s, t, meta: (0, kept(s, t))),
            ],
            scratch_shapes=[pltpu.VMEM((heads, q_tile, head_dim), F32)] * 3,
        ),
        out_shape=[o_shape, s_shape, o_shape, s_shape],
        compiler_params=pltpu.CompilerParams(vmem_limit_bytes=VMEM_LIMIT),
        cost_estimate=pl.CostEstimate(
            flops=16 * heads * chunk_len * (block_len + (chunk_len // 4 if with_self else 0)) * head_dim,
            bytes_accessed=2 * heads * (block_len + 2 * chunk_len) * head_dim * 4,
            transcendentals=2 * heads * chunk_len * block_len,
        ),
        name="attend_own" if with_self else "attend",
    )(meta, q_all, k_block, v_block, *((k_new, v_new) if with_self else ()))


def merge(heads, pieces):
    peak = functools.reduce(jnp.maximum, [s[:heads] for _, s in pieces])
    weights = [jnp.exp2(s[:heads] - peak) for _, s in pieces]
    total = functools.reduce(jnp.add, [s[heads:2 * heads] * w for (_, s), w in zip(pieces, weights)])
    out = functools.reduce(jnp.add, [o * w[..., None] for (o, _), w in zip(pieces, weights)])
    return out, peak, total


def share_kernel(tp_size, part, out_ref, acc, from_left, from_right, from_y, from_core, from_last, stage,
                 in_sem, left_sem, right_sem, y_sem, core_sem, last_sem, send_sem, stage_sem):
    z = lax.axis_index("tp")
    j = lax.axis_index("cp")
    y, c = lax.div(j, 2), lax.rem(j, 2)
    across, mate, corner = (1 - y) * 2 + c, y * 2 + (1 - c), (1 - y) * 2 + (1 - c)
    tokens = part.shape[0] // CHUNKS
    pairs = CHUNKS // 2
    last = tp_size - 1
    root_a, root_b = (tp_size - 1) // 2, tp_size // 2

    barrier = pltpu.get_barrier_semaphore()
    pl.semaphore_signal(barrier, inc=1, device_id={"cp": across}, device_id_type=MESH)
    pl.semaphore_signal(barrier, inc=1, device_id={"cp": mate}, device_id_type=MESH)

    @pl.when(z > 0)
    def _():
        pl.semaphore_signal(barrier, inc=1, device_id={"tp": z - 1}, device_id_type=MESH)

    @pl.when(z < last)
    def _():
        pl.semaphore_signal(barrier, inc=1, device_id={"tp": z + 1}, device_id_type=MESH)

    inside = jnp.logical_and(z > 0, z < last)

    @pl.when(inside)
    def _():
        pl.semaphore_wait(barrier, 4)

    @pl.when(jnp.logical_not(inside))
    def _():
        pl.semaphore_wait(barrier, 3)

    def at(ref, k):
        return ref.at[pl.ds(pl.multiple_of(k * tokens, tokens), tokens), :]

    def load(k):
        return pltpu.make_async_copy(at(part, k), at(acc, k), in_sem.at[k])

    def remote(src, dst, k, which, arrive, device):
        return pltpu.make_async_remote_copy(
            src_ref=at(src, k), dst_ref=at(dst, k), send_sem=send_sem.at[which], recv_sem=arrive.at[k],
            device_id=device, device_id_type=MESH,
        )

    def send_right(src, k):
        remote(src, from_left, k, 0, left_sem, {"tp": z + 1}).start()

    def send_left(src, k):
        remote(src, from_right, k, 1, right_sem, {"tp": z - 1}).start()

    def arrived(ref, sem, k):
        remote(ref, ref, k, 0, sem, {"cp": j}).wait_recv()

    def drained(ref, which):
        pltpu.make_async_copy(ref, ref, send_sem.at[which]).wait()

    def emit(stream, src, k, row):
        slot = lax.rem(k, STAGES)

        def copy():
            return pltpu.make_async_copy(stage.at[stream, slot], at(out_ref.at[row], k), stage_sem.at[stream, slot])

        @pl.when(k >= STAGES)
        def _():
            copy().wait()

        rows = pl.ds(pl.multiple_of(k * tokens, tokens), tokens)
        stage[stream, slot] = src[rows, :].astype(BF16)
        copy().start()

    def finish(src, k):
        remote(src, from_y, k, 2, y_sem, {"cp": across}).start()
        remote(src, from_core, k, 3, core_sem, {"cp": mate}).start()
        emit(0, src, k, j)

    def gathered(i):
        def lagged(lag, act):
            @pl.when(jnp.logical_and(i >= lag, i < pairs + lag))
            def _():
                for n in range(2):
                    act((i - lag) * 2 + n)

        def core(k):
            arrived(from_core, core_sem, k)
            emit(1, from_core, k, mate)

        def side(k):
            arrived(from_y, y_sem, k)
            remote(from_y, from_last, k, 4, last_sem, {"cp": mate}).start()
            emit(2, from_y, k, across)

        def final(k):
            arrived(from_last, last_sem, k)
            emit(3, from_last, k, corner)

        lagged(LAG_CORE, core)
        lagged(LAG_Y, side)
        lagged(LAG_LAST, final)

    def add(k, *others):
        rows = pl.ds(pl.multiple_of(k * tokens, tokens), tokens)
        total = acc[rows, :]
        for other in others:
            total = total + other[rows, :]
        acc[rows, :] = total

    @pl.loop(0, CHUNKS)
    def _(k):
        load(k).start()

    steps = pairs + LAG_LAST + 1

    def run(near, far):
        @pl.loop(0, steps)
        def _(i):
            @pl.when(i < pairs)
            def _():
                near(i)

            @pl.when(jnp.logical_and(i >= LAG_BACK, i < pairs + LAG_BACK))
            def _():
                far(i - LAG_BACK)

            gathered(i)

    def end(first, send):
        inbox, sem = (from_right, right_sem) if first else (from_left, left_sem)

        @pl.loop(0, CHUNKS)
        def _(k):
            load(k).wait()
            send(acc, k)

        def got(k):
            arrived(inbox, sem, k)
            finish(inbox, k)

        near_bit = 0 if first else 1
        run(lambda i: got(2 * i + near_bit), lambda i: got(2 * i + 1 - near_bit))

    def inner(left_side):
        mine = 0 if left_side else 1
        if left_side:
            (outer, outer_sem, to_outer), (inward, inward_sem, to_inner) = (
                (from_left, left_sem, send_left), (from_right, right_sem, send_right))
        else:
            (outer, outer_sem, to_outer), (inward, inward_sem, to_inner) = (
                (from_right, right_sem, send_right), (from_left, left_sem, send_left))

        def near(i):
            passed, rooted = 2 * i + 1 - mine, 2 * i + mine
            load(passed).wait()
            arrived(outer, outer_sem, passed)
            add(passed, outer)
            to_inner(acc, passed)
            load(rooted).wait()
            arrived(outer, outer_sem, rooted)
            arrived(inward, inward_sem, rooted)
            add(rooted, from_left, from_right)
            to_outer(acc, rooted)
            to_inner(acc, rooted)
            finish(acc, rooted)

        def far(i):
            k = 2 * i + 1 - mine
            arrived(inward, inward_sem, k)
            to_outer(inward, k)
            finish(inward, k)

        run(near, far)

    @pl.when(z == 0)
    def _():
        end(True, send_right)

    @pl.when(z == root_a)
    def _():
        inner(True)

    @pl.when(z == root_b)
    def _():
        inner(False)

    @pl.when(z == last)
    def _():
        end(False, send_left)

    @pl.when(z < last)
    def _():
        drained(acc, 0)

    @pl.when(z > 0)
    def _():
        drained(acc, 1)

    for which in (2, 3, 4):
        drained(acc, which)
    for stream in range(4):
        for slot in range(STAGES):
            pltpu.make_async_copy(stage.at[stream, slot], at(out_ref.at[0], 0), stage_sem.at[stream, slot]).wait()


def share(part, num_rows, tp_size):
    chunk_len, d_model = part.shape
    tokens = chunk_len // CHUNKS
    buffer = pltpu.VMEM((chunk_len, d_model), F32)
    arrivals = pltpu.SemaphoreType.DMA((CHUNKS,))
    return pl.pallas_call(
        functools.partial(share_kernel, tp_size),
        in_specs=[pl.BlockSpec(memory_space=pl.ANY)],
        out_specs=pl.BlockSpec(memory_space=pl.ANY),
        out_shape=jax.ShapeDtypeStruct((num_rows, chunk_len, d_model), BF16),
        scratch_shapes=[buffer] * 6
        + [pltpu.VMEM((4, STAGES, tokens, d_model), BF16)]
        + [arrivals] * 6
        + [pltpu.SemaphoreType.DMA((5,)), pltpu.SemaphoreType.DMA((4, STAGES))],
        compiler_params=pltpu.CompilerParams(collective_id=0, has_side_effects=True, vmem_limit_bytes=VMEM_LIMIT),
        cost_estimate=pl.CostEstimate(flops=100_000_000_000, bytes_accessed=chunk_len * d_model * 16, transcendentals=0),
        name="share",
    )(part)


def solution(mesh):
    in_specs = (P("dp", None, None), P("dp"), P("dp", "tp", "cp", None), P("dp", "tp", "cp", None), P(), P(), P(), P(), P(None, "tp"), P("tp"), P("tp", None), P(), P(None, "tp"), P("tp"), P("tp", None), P())
    out_specs = (P("dp", None, None), P("dp", "tp", None, None), P("dp", "tp", None, None))
    tp_size = mesh.shape["tp"]
    cp_size = mesh.shape["cp"]
    swap_core = [(i, i ^ 1) for i in range(cp_size)]
    swap_y = [(i, i ^ 2) for i in range(cp_size)]

    def local_layer(hidden_in, lengths, k_block, v_block, ln1_gain, ln1_bias, ln2_gain, ln2_bias, w_qkv, b_qkv, w_out, b_out, w_up, b_up, w_down, b_down):
        num_rows, chunk_len, d_model = hidden_in.shape
        heads, block_len, head_dim = k_block.shape[1:]
        j = lax.axis_index("cp")
        start = j * block_len
        table = rope_table(lengths, chunk_len, head_dim)
        q_rot, k_new, v_new = project_qkv(hidden_in, ln1_gain, ln1_bias, w_qkv, b_qkv, table, heads, head_dim)

        far_rows = jnp.stack([j ^ 3, j ^ 2]).astype(jnp.int32)
        near_rows = jnp.stack([j ^ 1, j]).astype(jnp.int32)
        o_s, s_s, o_k, s_k = attend(far_rows, lengths, start, q_rot, k_block, v_block)
        o_r, s_r = lax.ppermute(o_s, "cp", swap_core), lax.ppermute(s_s, "cp", swap_core)
        o_far, peak, total = merge(heads, [(o_k, s_k), (o_r, s_r)])
        s_far = jnp.concatenate([peak, total], axis=0)
        o_y, s_y = lax.ppermute(o_far, "cp", swap_y), lax.ppermute(s_far, "cp", swap_y)

        o_s, s_s, o_own, s_own = attend(near_rows, lengths, start, q_rot, k_block, v_block, k_new, v_new)
        o_c, s_c = lax.ppermute(o_s, "cp", swap_core), lax.ppermute(s_s, "cp", swap_core)

        own_in = lax.dynamic_index_in_dim(hidden_in, j, 0, keepdims=False)
        normed_mlp = layer_norm(own_in, ln2_gain, ln2_bias)
        hidden = jax.nn.gelu(jnp.dot(normed_mlp, w_up, preferred_element_type=F32) + b_up.astype(F32), approximate=False).astype(BF16)
        hidden = lax.optimization_barrier(hidden)
        extra = own_in.astype(F32) + b_out.astype(F32) + b_down.astype(F32)
        mlp_part = jnp.dot(hidden, w_down, preferred_element_type=F32) + jnp.where(lax.axis_index("tp") == 0, extra, 0.0)
        mlp_part = lax.optimization_barrier(mlp_part)

        out, _, total = merge(heads, [(o_own, s_own), (o_c, s_c), (o_y, s_y)])
        context = (out / total[..., None]).astype(BF16)
        attn_part = jnp.einsum("hcd,hde->ce", context, w_out.reshape(heads, head_dim, d_model), preferred_element_type=F32)
        part = attn_part + mlp_part
        return share(part, num_rows, tp_size), k_new, v_new

    return jax.shard_map(local_layer, mesh=mesh, in_specs=in_specs, out_specs=out_specs, check_vma=False)
```

```python
import functools
import math

import jax
import jax.numpy as jnp
from jax import lax
from jax.experimental import pallas as pl
from jax.experimental.pallas import tpu as pltpu
from jax.sharding import PartitionSpec as P

EPSILON = 1e-5
NEG_BIG = -1e30
ROTARY_SHARE = 4
ROPE_BASE = 10000.0
LOG2E = math.log2(math.e)
MESH = pl.DeviceIdType.MESH
F32 = jnp.float32
BF16 = jnp.bfloat16
VMEM_LIMIT = 60 * 1024 * 1024
CHUNKS = 64
STAGES = 4
LAG_AHEAD = 1
LAG_BACK = 1
LAG_CORE = 2
LAG_Y = 5
LAG_LAST = 6


def layer_norm(values_in, gain_vec, bias_vec):
    x_f32 = values_in.astype(F32)
    row_mean = jnp.mean(x_f32, axis=-1, keepdims=True)
    centered = x_f32 - row_mean
    variance = jnp.mean(centered * centered, axis=-1, keepdims=True)
    return (centered * lax.rsqrt(variance + EPSILON) * gain_vec + bias_vec).astype(BF16)


def rope_table(lengths, chunk_len, head_dim):
    rot_dim = head_dim // ROTARY_SHARE
    half_rot = rot_dim // 2
    positions = lengths[:, None] + jnp.arange(chunk_len, dtype=jnp.int32)[None, :]
    inv_freq = ROPE_BASE ** (-2.0 * jnp.arange(half_rot, dtype=F32) / rot_dim)
    angles = positions.astype(F32)[:, None, :] * inv_freq[:, None]
    cos_tab = jnp.cos(angles)
    sin_tab = jnp.sin(angles)
    return jnp.concatenate([cos_tab, cos_tab, -sin_tab, sin_tab], axis=1)


def qkv_kernel(heads, head_dim, rows, x_ref, gain_ref, bias_ref, w_ref, wb_ref, tab_ref, *rest):
    q_ref, k_ref, v_ref = rest[-3:]
    rot_dim = head_dim // ROTARY_SHARE
    half_rot = rot_dim // 2
    normed = layer_norm(x_ref[0], gain_ref[...], bias_ref[...])
    tab = tab_ref[0]
    tab = jnp.concatenate([tab] * (head_dim // tab.shape[0]), axis=0).T
    lane = lax.broadcasted_iota(jnp.int32, tab.shape, 1)
    cos_tab = jnp.where(lane < rot_dim, tab, 1.0)
    sin_tab = jnp.where(lane < rot_dim, pltpu.roll(tab, head_dim - rot_dim, 1), 0.0)

    def rotate(values):
        wide = values.astype(F32)
        other = jnp.where(lane < half_rot, pltpu.roll(wide, head_dim - half_rot, 1), pltpu.roll(wide, half_rot, 1))
        return (wide * cos_tab + other * sin_tab).astype(BF16)

    pair = 2 * 3 * head_dim
    for first in range(0, heads, 2):
        cols = slice(first // 2 * pair, first // 2 * pair + pair)
        both = (jnp.dot(normed, w_ref[:, cols], preferred_element_type=F32) + wb_ref[:, cols]).astype(BF16)
        for h in (first, first + 1):
            base = (h - first) * 3 * head_dim
            q_ref[0, h] = rotate(both[:, base:base + head_dim])
            k_ref[0, h] = rotate(both[:, base + head_dim:base + 2 * head_dim])
            v_ref[0, h] = both[:, base + 2 * head_dim:base + 3 * head_dim]


def project_qkv(rows, hidden_in, gain, bias, w_qkv, b_qkv, table, heads, head_dim, filled=()):
    num_rows, chunk_len, d_model = hidden_in.shape
    here = rows.shape[0]
    tile = chunk_len // 4
    width = w_qkv.shape[1]
    out = jax.ShapeDtypeStruct((num_rows, heads, chunk_len, head_dim), BF16)
    once = dict(pipeline_mode=pl.Buffered(1))
    fixed = lambda b, t, rows: (0, 0)
    return pl.pallas_call(
        functools.partial(qkv_kernel, heads, head_dim),
        grid_spec=pltpu.PrefetchScalarGridSpec(
            num_scalar_prefetch=1,
            grid=(here, chunk_len // tile),
            in_specs=[
                pl.BlockSpec((1, tile, d_model), lambda b, t, rows: (rows[b], t, 0)),
                pl.BlockSpec((1, d_model), fixed, **once),
                pl.BlockSpec((1, d_model), fixed, **once),
                pl.BlockSpec((d_model, width), fixed, **once),
                pl.BlockSpec((1, width), fixed, **once),
                pl.BlockSpec((1, table.shape[1], tile), lambda b, t, rows: (rows[b], 0, t)),
            ] + [pl.BlockSpec(memory_space=pl.ANY)] * len(filled),
            out_specs=[pl.BlockSpec((1, heads, tile, head_dim), lambda b, t, rows: (b, 0, t, 0))]
            + [pl.BlockSpec((1, heads, tile, head_dim), lambda b, t, rows: (rows[b], 0, t, 0))] * 2,
        ),
        out_shape=[jax.ShapeDtypeStruct((here, heads, chunk_len, head_dim), BF16), out, out],
        input_output_aliases={7: 1, 8: 2} if filled else {},
        compiler_params=pltpu.CompilerParams(vmem_limit_bytes=VMEM_LIMIT),
        cost_estimate=pl.CostEstimate(
            flops=2 * here * chunk_len * d_model * width,
            bytes_accessed=2 * (here * chunk_len * (d_model + width) + d_model * width),
            transcendentals=0,
        ),
        name="qkv_rope_near" if filled else "qkv_rope_far",
    )(rows, hidden_in, gain[None], bias[None], w_qkv, b_qkv.astype(F32)[None], table, *filled)


def block_step(heads, scale, q_of, k_of, v_of, m_scr, l_scr, o_scr, mask):
    for h in range(heads):
        scores = lax.dot_general(q_of(h), k_of(h), (((1,), (1,)), ((), ())), preferred_element_type=F32) * scale
        if mask is not None:
            scores = jnp.where(mask, scores, NEG_BIG)
        m_old = m_scr[h]
        m_new = jnp.maximum(m_old, jnp.max(scores, axis=1, keepdims=True))
        probs = jnp.exp2(scores - m_new[:, :1])
        shrink = jnp.exp2(m_old - m_new)
        l_scr[h] = l_scr[h] * shrink + jnp.sum(probs, axis=1, keepdims=True)
        m_scr[h] = m_new
        o_scr[h] = o_scr[h] * shrink + jnp.dot(probs.astype(BF16), v_of(h), preferred_element_type=F32)


def attn_kernel(heads, head_dim, q_tile, key_block, with_self, meta, q_ref, k_ref, v_ref, *rest):
    if with_self:
        kn_ref, vn_ref, *rest = rest
    os_ref, ss_ref, ok_ref, sk_ref, m_scr, l_scr, o_scr = rest
    slot = pl.program_id(0)
    tile = pl.program_id(1)
    valid = jnp.clip(meta[3 + meta[slot]] - meta[2], 0, k_ref.shape[2])
    scale = head_dim ** -0.5 * LOG2E
    m_scr[...] = jnp.full(m_scr.shape, NEG_BIG, F32)
    l_scr[...] = jnp.zeros(l_scr.shape, F32)
    o_scr[...] = jnp.zeros(o_scr.shape, F32)

    def query(h):
        return q_ref[0, h]

    def cache_block(block, mask):
        start = pl.multiple_of(block * key_block, key_block)
        block_step(
            heads, scale, query,
            lambda h: k_ref[0, h, pl.ds(start, key_block), :],
            lambda h: v_ref[0, h, pl.ds(start, key_block), :],
            m_scr, l_scr, o_scr, mask,
        )

    whole = lax.div(valid, key_block)

    @pl.loop(0, whole)
    def _(block):
        cache_block(block, None)

    @pl.when(lax.rem(valid, key_block) > 0)
    def _():
        keys = whole * key_block + lax.broadcasted_iota(jnp.int32, (q_tile, key_block), 1)
        cache_block(whole, keys < valid)

    if with_self:
        def own_block(block, mask):
            start = pl.multiple_of(block * q_tile, q_tile)
            block_step(
                heads, scale, query,
                lambda h: kn_ref[0, h, pl.ds(start, q_tile), :],
                lambda h: vn_ref[0, h, pl.ds(start, q_tile), :],
                m_scr, l_scr, o_scr, mask,
            )

        @pl.when(slot == 1)
        def _():
            @pl.loop(0, tile)
            def _(block):
                own_block(block, None)

            shape = (q_tile, q_tile)
            own_block(tile, lax.broadcasted_iota(jnp.int32, shape, 0) >= lax.broadcasted_iota(jnp.int32, shape, 1))

    lane = lax.broadcasted_iota(jnp.int32, (q_tile, head_dim), 1)
    stats = jnp.zeros((q_tile, head_dim), F32)
    for h in range(heads):
        stats = jnp.where(lane == h, m_scr[h], stats)
        stats = jnp.where(lane == heads + h, l_scr[h], stats)
    stats = stats.T[:8]

    @pl.when(slot == 0)
    def _():
        os_ref[...] = o_scr[...]
        ss_ref[...] = stats

    @pl.when(slot == 1)
    def _():
        ok_ref[...] = o_scr[...]
        sk_ref[...] = stats


def attend(rows, lengths, block_start, q_rows, k_block, v_block, k_new=None, v_new=None):
    heads, chunk_len, head_dim = q_rows.shape[1:]
    block_len = k_block.shape[2]
    q_tile = chunk_len // 4
    key_block = block_len // 2
    tiles = chunk_len // q_tile
    meta = jnp.concatenate([rows, block_start[None], lengths])
    with_self = k_new is not None
    keys = pl.BlockSpec((1, heads, block_len, head_dim), lambda s, t, meta: (meta[s], 0, 0, 0))
    own = pl.BlockSpec((1, heads, chunk_len, head_dim), lambda s, t, meta: (meta[1], 0, 0, 0))
    sent = lambda s, t: jnp.where(s == 0, t, tiles - 1)
    kept = lambda s, t: jnp.where(s == 0, 0, t)
    o_shape = jax.ShapeDtypeStruct((heads, chunk_len, head_dim), F32)
    s_shape = jax.ShapeDtypeStruct((8, chunk_len), F32)
    return pl.pallas_call(
        functools.partial(attn_kernel, heads, head_dim, q_tile, key_block, with_self),
        grid_spec=pltpu.PrefetchScalarGridSpec(
            num_scalar_prefetch=1,
            grid=(2, tiles),
            in_specs=[pl.BlockSpec((1, heads, q_tile, head_dim), lambda s, t, meta: (s, 0, t, 0)), keys, keys]
            + ([own, own] if with_self else []),
            out_specs=[
                pl.BlockSpec((heads, q_tile, head_dim), lambda s, t, meta: (0, sent(s, t), 0)),
                pl.BlockSpec((8, q_tile), lambda s, t, meta: (0, sent(s, t))),
                pl.BlockSpec((heads, q_tile, head_dim), lambda s, t, meta: (0, kept(s, t), 0)),
                pl.BlockSpec((8, q_tile), lambda s, t, meta: (0, kept(s, t))),
            ],
            scratch_shapes=[pltpu.VMEM((heads, q_tile, head_dim), F32)] * 3,
        ),
        out_shape=[o_shape, s_shape, o_shape, s_shape],
        compiler_params=pltpu.CompilerParams(vmem_limit_bytes=VMEM_LIMIT),
        cost_estimate=pl.CostEstimate(
            flops=16 * heads * chunk_len * (block_len + (chunk_len // 4 if with_self else 0)) * head_dim,
            bytes_accessed=2 * heads * (block_len + 2 * chunk_len) * head_dim * 4,
            transcendentals=2 * heads * chunk_len * block_len,
        ),
        name="attend_own" if with_self else "attend",
    )(meta, q_rows, k_block, v_block, *((k_new, v_new) if with_self else ()))


def merge(heads, pieces):
    peak = functools.reduce(jnp.maximum, [s[:heads] for _, s in pieces])
    weights = [jnp.exp2(s[:heads] - peak) for _, s in pieces]
    total = functools.reduce(jnp.add, [s[heads:2 * heads] * w for (_, s), w in zip(pieces, weights)])
    out = functools.reduce(jnp.add, [o * w[..., None] for (o, _), w in zip(pieces, weights)])
    return out, peak, total


def share_kernel(tp_size, part, out_ref, acc, from_left, from_right, from_y, from_core, from_last, stage,
                 in_sem, left_sem, right_sem, y_sem, core_sem, last_sem, send_sem, stage_sem):
    z = lax.axis_index("tp")
    j = lax.axis_index("cp")
    y, c = lax.div(j, 2), lax.rem(j, 2)
    across, mate, corner = (1 - y) * 2 + c, y * 2 + (1 - c), (1 - y) * 2 + (1 - c)
    tokens = part.shape[0] // CHUNKS
    pairs = CHUNKS // 2
    last = tp_size - 1
    root_a, root_b = (tp_size - 1) // 2, tp_size // 2

    barrier = pltpu.get_barrier_semaphore()
    pl.semaphore_signal(barrier, inc=1, device_id={"cp": across}, device_id_type=MESH)
    pl.semaphore_signal(barrier, inc=1, device_id={"cp": mate}, device_id_type=MESH)

    @pl.when(z > 0)
    def _():
        pl.semaphore_signal(barrier, inc=1, device_id={"tp": z - 1}, device_id_type=MESH)

    @pl.when(z < last)
    def _():
        pl.semaphore_signal(barrier, inc=1, device_id={"tp": z + 1}, device_id_type=MESH)

    inside = jnp.logical_and(z > 0, z < last)

    @pl.when(inside)
    def _():
        pl.semaphore_wait(barrier, 4)

    @pl.when(jnp.logical_not(inside))
    def _():
        pl.semaphore_wait(barrier, 3)

    def at(ref, k):
        return ref.at[pl.ds(pl.multiple_of(k * tokens, tokens), tokens), :]

    def load(k):
        return pltpu.make_async_copy(at(part, k), at(acc, k), in_sem.at[k])

    def remote(src, dst, k, which, arrive, device):
        return pltpu.make_async_remote_copy(
            src_ref=at(src, k), dst_ref=at(dst, k), send_sem=send_sem.at[which], recv_sem=arrive.at[k],
            device_id=device, device_id_type=MESH,
        )

    def send_right(src, k):
        remote(src, from_left, k, 0, left_sem, {"tp": z + 1}).start()

    def send_left(src, k):
        remote(src, from_right, k, 1, right_sem, {"tp": z - 1}).start()

    def arrived(ref, sem, k):
        remote(ref, ref, k, 0, sem, {"cp": j}).wait_recv()

    def drained(ref, which):
        pltpu.make_async_copy(ref, ref, send_sem.at[which]).wait()

    def emit(stream, src, k, row):
        slot = lax.rem(k, STAGES)

        def copy():
            return pltpu.make_async_copy(stage.at[stream, slot], at(out_ref.at[row], k), stage_sem.at[stream, slot])

        @pl.when(k >= STAGES)
        def _():
            copy().wait()

        rows = pl.ds(pl.multiple_of(k * tokens, tokens), tokens)
        stage[stream, slot] = src[rows, :].astype(BF16)
        copy().start()

    def finish(src, k):
        remote(src, from_y, k, 2, y_sem, {"cp": across}).start()
        remote(src, from_core, k, 3, core_sem, {"cp": mate}).start()
        emit(0, src, k, j)

    def gathered(i):
        def lagged(lag, act):
            @pl.when(jnp.logical_and(i >= lag, i < pairs + lag))
            def _():
                for n in range(2):
                    act((i - lag) * 2 + n)

        def core(k):
            arrived(from_core, core_sem, k)
            emit(1, from_core, k, mate)

        def side(k):
            arrived(from_y, y_sem, k)
            remote(from_y, from_last, k, 4, last_sem, {"cp": mate}).start()
            emit(2, from_y, k, across)

        def final(k):
            arrived(from_last, last_sem, k)
            emit(3, from_last, k, corner)

        lagged(LAG_CORE, core)
        lagged(LAG_Y, side)
        lagged(LAG_LAST, final)

    def add(k, *others):
        rows = pl.ds(pl.multiple_of(k * tokens, tokens), tokens)
        total = acc[rows, :]
        for other in others:
            total = total + other[rows, :]
        acc[rows, :] = total

    @pl.loop(0, CHUNKS)
    def _(k):
        load(k).start()

    steps = pairs + LAG_LAST + 1

    def run(near, far, early=None):
        if early is not None:
            for i in range(LAG_AHEAD):
                early(i)

        @pl.loop(0, steps)
        def _(i):
            if early is not None:
                @pl.when(i + LAG_AHEAD < pairs)
                def _():
                    early(i + LAG_AHEAD)

            @pl.when(i < pairs)
            def _():
                near(i)

            @pl.when(jnp.logical_and(i >= LAG_BACK, i < pairs + LAG_BACK))
            def _():
                far(i - LAG_BACK)

            gathered(i)

    def end(first, send):
        inbox, sem = (from_right, right_sem) if first else (from_left, left_sem)

        @pl.loop(0, CHUNKS)
        def _(k):
            load(k).wait()
            send(acc, k)

        def got(k):
            arrived(inbox, sem, k)
            finish(inbox, k)

        near_bit = 0 if first else 1
        run(lambda i: got(2 * i + near_bit), lambda i: got(2 * i + 1 - near_bit))

    def inner(left_side):
        mine = 0 if left_side else 1
        if left_side:
            (outer, outer_sem, to_outer), (inward, inward_sem, to_inner) = (
                (from_left, left_sem, send_left), (from_right, right_sem, send_right))
        else:
            (outer, outer_sem, to_outer), (inward, inward_sem, to_inner) = (
                (from_right, right_sem, send_right), (from_left, left_sem, send_left))

        def early(i):
            passed = 2 * i + 1 - mine
            load(passed).wait()
            arrived(outer, outer_sem, passed)
            add(passed, outer)
            to_inner(acc, passed)

        def near(i):
            rooted = 2 * i + mine
            load(rooted).wait()
            arrived(outer, outer_sem, rooted)
            arrived(inward, inward_sem, rooted)
            add(rooted, from_left, from_right)
            to_outer(acc, rooted)
            to_inner(acc, rooted)
            finish(acc, rooted)

        def far(i):
            k = 2 * i + 1 - mine
            arrived(inward, inward_sem, k)
            to_outer(inward, k)
            finish(inward, k)

        run(near, far, early)

    @pl.when(z == 0)
    def _():
        end(True, send_right)

    @pl.when(z == root_a)
    def _():
        inner(True)

    @pl.when(z == root_b)
    def _():
        inner(False)

    @pl.when(z == last)
    def _():
        end(False, send_left)

    @pl.when(z < last)
    def _():
        drained(acc, 0)

    @pl.when(z > 0)
    def _():
        drained(acc, 1)

    for which in (2, 3, 4):
        drained(acc, which)
    for stream in range(4):
        for slot in range(STAGES):
            pltpu.make_async_copy(stage.at[stream, slot], at(out_ref.at[0], 0), stage_sem.at[stream, slot]).wait()


def share(part, num_rows, tp_size):
    chunk_len, d_model = part.shape
    tokens = chunk_len // CHUNKS
    buffer = pltpu.VMEM((chunk_len, d_model), F32)
    arrivals = pltpu.SemaphoreType.DMA((CHUNKS,))
    return pl.pallas_call(
        functools.partial(share_kernel, tp_size),
        in_specs=[pl.BlockSpec(memory_space=pl.ANY)],
        out_specs=pl.BlockSpec(memory_space=pl.ANY),
        out_shape=jax.ShapeDtypeStruct((num_rows, chunk_len, d_model), BF16),
        scratch_shapes=[buffer] * 6
        + [pltpu.VMEM((4, STAGES, tokens, d_model), BF16)]
        + [arrivals] * 6
        + [pltpu.SemaphoreType.DMA((5,)), pltpu.SemaphoreType.DMA((4, STAGES))],
        compiler_params=pltpu.CompilerParams(collective_id=0, has_side_effects=True, vmem_limit_bytes=VMEM_LIMIT),
        cost_estimate=pl.CostEstimate(flops=100_000_000_000, bytes_accessed=chunk_len * d_model * 16, transcendentals=0),
        name="share",
    )(part)


def solution(mesh):
    in_specs = (P("dp", None, None), P("dp"), P("dp", "tp", "cp", None), P("dp", "tp", "cp", None), P(), P(), P(), P(), P(None, "tp"), P("tp"), P("tp", None), P(), P(None, "tp"), P("tp"), P("tp", None), P())
    out_specs = (P("dp", None, None), P("dp", "tp", None, None), P("dp", "tp", None, None))
    tp_size = mesh.shape["tp"]
    cp_size = mesh.shape["cp"]
    swap_core = [(i, i ^ 1) for i in range(cp_size)]
    swap_y = [(i, i ^ 2) for i in range(cp_size)]

    def local_layer(hidden_in, lengths, k_block, v_block, ln1_gain, ln1_bias, ln2_gain, ln2_bias, w_qkv, b_qkv, w_out, b_out, w_up, b_up, w_down, b_down):
        num_rows, chunk_len, d_model = hidden_in.shape
        heads, block_len, head_dim = k_block.shape[1:]
        j = lax.axis_index("cp")
        start = j * block_len
        table = rope_table(lengths, chunk_len, head_dim)
        far_rows = jnp.stack([j ^ 3, j ^ 2])
        near_rows = jnp.stack([j ^ 1, j])
        weights = (ln1_gain, ln1_bias, w_qkv, b_qkv, table, heads, head_dim)

        q_far, *filled = project_qkv(far_rows, hidden_in, *weights)
        o_s, s_s, o_k, s_k = attend(far_rows, lengths, start, q_far, k_block, v_block)
        o_r, s_r = lax.ppermute(o_s, "cp", swap_core), lax.ppermute(s_s, "cp", swap_core)
        q_near, k_new, v_new = project_qkv(near_rows, hidden_in, *weights, filled=filled)
        o_far, peak, total = merge(heads, [(o_k, s_k), (o_r, s_r)])
        s_far = jnp.concatenate([peak, total], axis=0)
        q_near, o_far, s_far = lax.optimization_barrier((q_near, o_far, s_far))
        o_y, s_y = lax.ppermute(o_far, "cp", swap_y), lax.ppermute(s_far, "cp", swap_y)

        o_s, s_s, o_own, s_own = attend(near_rows, lengths, start, q_near, k_block, v_block, k_new, v_new)
        o_c, s_c = lax.ppermute(o_s, "cp", swap_core), lax.ppermute(s_s, "cp", swap_core)

        own_in = lax.dynamic_index_in_dim(hidden_in, j, 0, keepdims=False)
        normed_mlp = layer_norm(own_in, ln2_gain, ln2_bias)
        hidden = jax.nn.gelu(jnp.dot(normed_mlp, w_up, preferred_element_type=F32) + b_up.astype(F32), approximate=False).astype(BF16)
        hidden = lax.optimization_barrier(hidden)
        extra = own_in.astype(F32) + b_out.astype(F32) + b_down.astype(F32)
        mlp_part = jnp.dot(hidden, w_down, preferred_element_type=F32) + jnp.where(lax.axis_index("tp") == 0, extra, 0.0)
        mlp_part = lax.optimization_barrier(mlp_part)

        out, _, total = merge(heads, [(o_own, s_own), (o_c, s_c), (o_y, s_y)])
        context = (out / total[..., None]).astype(BF16)
        attn_part = jnp.einsum("hcd,hde->ce", context, w_out.reshape(heads, head_dim, d_model), preferred_element_type=F32)
        part = attn_part + mlp_part
        return share(part, num_rows, tp_size), k_new, v_new

    return jax.shard_map(local_layer, mesh=mesh, in_specs=in_specs, out_specs=out_specs, check_vma=False)
```

```python
import functools
import math

import jax
import jax.numpy as jnp
from jax import lax
from jax.experimental import pallas as pl
from jax.experimental.pallas import tpu as pltpu
from jax.sharding import PartitionSpec as P

EPSILON = 1e-5
NEG_BIG = -1e30
ROTARY_SHARE = 4
ROPE_BASE = 10000.0
LOG2E = math.log2(math.e)
MESH = pl.DeviceIdType.MESH
F32 = jnp.float32
BF16 = jnp.bfloat16
VMEM_LIMIT = 60 * 1024 * 1024
SHARE_LIMIT = 67_043_328
CHUNKS = 64
STAGES = 4
BLOCKS = 8
SLICES = 4
LAG_START = 2
LAG_AHEAD = 1
LAG_BACK = 1
LAG_CORE = 2
LAG_Y = 5
LAG_LAST = 6


def layer_norm(values_in, gain_vec, bias_vec):
    x_f32 = values_in.astype(F32)
    row_mean = jnp.mean(x_f32, axis=-1, keepdims=True)
    centered = x_f32 - row_mean
    variance = jnp.mean(centered * centered, axis=-1, keepdims=True)
    return (centered * lax.rsqrt(variance + EPSILON) * gain_vec + bias_vec).astype(BF16)


def rope_table(lengths, chunk_len, head_dim):
    rot_dim = head_dim // ROTARY_SHARE
    half_rot = rot_dim // 2
    positions = lengths[:, None] + jnp.arange(chunk_len, dtype=jnp.int32)[None, :]
    inv_freq = ROPE_BASE ** (-2.0 * jnp.arange(half_rot, dtype=F32) / rot_dim)
    angles = positions.astype(F32)[:, None, :] * inv_freq[:, None]
    cos_tab = jnp.cos(angles)
    sin_tab = jnp.sin(angles)
    return jnp.concatenate([cos_tab, cos_tab, -sin_tab, sin_tab], axis=1)


def qkv_kernel(heads, head_dim, rows, x_ref, gain_ref, bias_ref, w_ref, wb_ref, tab_ref, *rest):
    q_ref, k_ref, v_ref = rest[-3:]
    rot_dim = head_dim // ROTARY_SHARE
    half_rot = rot_dim // 2
    normed = layer_norm(x_ref[0], gain_ref[...], bias_ref[...])
    tab = tab_ref[0]
    tab = jnp.concatenate([tab] * (head_dim // tab.shape[0]), axis=0).T
    lane = lax.broadcasted_iota(jnp.int32, tab.shape, 1)
    cos_tab = jnp.where(lane < rot_dim, tab, 1.0)
    sin_tab = jnp.where(lane < rot_dim, pltpu.roll(tab, head_dim - rot_dim, 1), 0.0)

    def rotate(values):
        wide = values.astype(F32)
        other = jnp.where(lane < half_rot, pltpu.roll(wide, head_dim - half_rot, 1), pltpu.roll(wide, half_rot, 1))
        return (wide * cos_tab + other * sin_tab).astype(BF16)

    pair = 2 * 3 * head_dim
    for first in range(0, heads, 2):
        cols = slice(first // 2 * pair, first // 2 * pair + pair)
        both = (jnp.dot(normed, w_ref[:, cols], preferred_element_type=F32) + wb_ref[:, cols]).astype(BF16)
        for h in (first, first + 1):
            base = (h - first) * 3 * head_dim
            q_ref[0, h] = rotate(both[:, base:base + head_dim])
            k_ref[0, h] = rotate(both[:, base + head_dim:base + 2 * head_dim])
            v_ref[0, h] = both[:, base + 2 * head_dim:base + 3 * head_dim]


def project_qkv(rows, hidden_in, gain, bias, w_qkv, b_qkv, table, heads, head_dim, filled=()):
    num_rows, chunk_len, d_model = hidden_in.shape
    here = rows.shape[0]
    tile = chunk_len // 4
    width = w_qkv.shape[1]
    out = jax.ShapeDtypeStruct((num_rows, heads, chunk_len, head_dim), BF16)
    once = dict(pipeline_mode=pl.Buffered(1))
    fixed = lambda b, t, rows: (0, 0)
    return pl.pallas_call(
        functools.partial(qkv_kernel, heads, head_dim),
        grid_spec=pltpu.PrefetchScalarGridSpec(
            num_scalar_prefetch=1,
            grid=(here, chunk_len // tile),
            in_specs=[
                pl.BlockSpec((1, tile, d_model), lambda b, t, rows: (rows[b], t, 0)),
                pl.BlockSpec((1, d_model), fixed, **once),
                pl.BlockSpec((1, d_model), fixed, **once),
                pl.BlockSpec((d_model, width), fixed, **once),
                pl.BlockSpec((1, width), fixed, **once),
                pl.BlockSpec((1, table.shape[1], tile), lambda b, t, rows: (rows[b], 0, t)),
            ] + [pl.BlockSpec(memory_space=pl.ANY)] * len(filled),
            out_specs=[pl.BlockSpec((1, heads, tile, head_dim), lambda b, t, rows: (b, 0, t, 0))]
            + [pl.BlockSpec((1, heads, tile, head_dim), lambda b, t, rows: (rows[b], 0, t, 0))] * 2,
        ),
        out_shape=[jax.ShapeDtypeStruct((here, heads, chunk_len, head_dim), BF16), out, out],
        input_output_aliases={7: 1, 8: 2} if filled else {},
        compiler_params=pltpu.CompilerParams(vmem_limit_bytes=VMEM_LIMIT),
        cost_estimate=pl.CostEstimate(
            flops=2 * here * chunk_len * d_model * width,
            bytes_accessed=2 * (here * chunk_len * (d_model + width) + d_model * width),
            transcendentals=0,
        ),
        name="qkv_rope_near" if filled else "qkv_rope_far",
    )(rows, hidden_in, gain[None], bias[None], w_qkv, b_qkv.astype(F32)[None], table, *filled)


def wide(column, lanes):
    return jnp.concatenate([column] * (lanes // column.shape[1]), axis=1)


def scores_of(query, keys, scale, mask):
    scores = lax.dot_general(query, keys, (((1,), (1,)), ((), ())), preferred_element_type=F32) * scale
    return scores if mask is None else jnp.where(mask, scores, NEG_BIG)


def lane_sum(values, lanes):
    return functools.reduce(jnp.add, [values[:, n:n + lanes] for n in range(0, values.shape[1], lanes)])


def lane_max(values, lanes):
    return functools.reduce(jnp.maximum, [values[:, n:n + lanes] for n in range(0, values.shape[1], lanes)])


def first_step(heads, scale, q_of, k_of, v_of, m_scr, l_scr, o_scr, mask):
    for h in range(heads):
        lanes = o_scr.shape[2]
        scores = scores_of(q_of(h), k_of(h), scale, mask)
        peak = jnp.broadcast_to(jnp.max(lane_max(scores, lanes), axis=1, keepdims=True), m_scr.shape[1:])
        probs = jnp.exp2(scores - wide(peak, scores.shape[1]))
        m_scr[h] = peak
        l_scr[h] = lane_sum(probs, lanes)
        o_scr[h] = jnp.dot(probs.astype(BF16), v_of(h), preferred_element_type=F32)


def block_step(heads, scale, q_of, k_of, v_of, m_scr, l_scr, o_scr, mask):
    for h in range(heads):
        lanes = o_scr.shape[2]
        scores = scores_of(q_of(h), k_of(h), scale, mask)
        m_old = m_scr[h]
        m_new = jnp.maximum(m_old, jnp.max(lane_max(scores, lanes), axis=1, keepdims=True))
        probs = jnp.exp2(scores - wide(m_new, scores.shape[1]))
        shrink = jnp.exp2(m_old - m_new)
        l_scr[h] = l_scr[h] * shrink + lane_sum(probs, lanes)
        m_scr[h] = m_new
        o_scr[h] = o_scr[h] * shrink + jnp.dot(probs.astype(BF16), v_of(h), preferred_element_type=F32)


def attn_kernel(heads, head_dim, q_tile, with_self, meta, q_ref, k_ref, v_ref, *rest):
    if with_self:
        kn_ref, vn_ref, *rest = rest
    os_ref, ss_ref, ok_ref, sk_ref, m_scr, l_scr, o_scr = rest
    slot = pl.program_id(0)
    tile = pl.program_id(1)
    block_len = k_ref.shape[2]
    half = block_len // 2
    valid = jnp.clip(meta[3 + meta[slot]] - meta[2], 0, block_len)
    scale = head_dim ** -0.5 * LOG2E

    def query(h):
        return q_ref[0, h]

    def cache_block(size):
        mask = lax.broadcasted_iota(jnp.int32, (q_tile, size), 1) < valid
        first_step(
            heads, scale, query, lambda h: k_ref[0, h, :size, :], lambda h: v_ref[0, h, :size, :], m_scr, l_scr, o_scr, mask
        )

    @pl.when(valid == 0)
    def _():
        m_scr[...] = jnp.full(m_scr.shape, NEG_BIG, F32)
        l_scr[...] = jnp.zeros(l_scr.shape, F32)
        o_scr[...] = jnp.zeros(o_scr.shape, F32)

    @pl.when(jnp.logical_and(valid > 0, valid <= half))
    def _():
        cache_block(half)

    @pl.when(valid > half)
    def _():
        cache_block(block_len)

    if with_self:
        def own_block(block, mask):
            start = pl.multiple_of(block * q_tile, q_tile)
            block_step(
                heads, scale, query,
                lambda h: kn_ref[0, h, pl.ds(start, q_tile), :],
                lambda h: vn_ref[0, h, pl.ds(start, q_tile), :],
                m_scr, l_scr, o_scr, mask,
            )

        @pl.when(slot == 1)
        def _():
            @pl.loop(0, tile)
            def _(block):
                own_block(block, None)

            shape = (q_tile, q_tile)
            own_block(tile, lax.broadcasted_iota(jnp.int32, shape, 0) >= lax.broadcasted_iota(jnp.int32, shape, 1))

    lane = lax.broadcasted_iota(jnp.int32, (q_tile, head_dim), 1)
    stats = jnp.zeros((q_tile, head_dim), F32)
    for h in range(heads):
        stats = jnp.where(lane == h, m_scr[h], stats)
        stats = jnp.where(lane == heads + h, jnp.sum(l_scr[h], axis=1, keepdims=True), stats)
    stats = stats.T[:8]

    @pl.when(slot == 0)
    def _():
        os_ref[...] = o_scr[...]
        ss_ref[...] = stats

    @pl.when(slot == 1)
    def _():
        ok_ref[...] = o_scr[...]
        sk_ref[...] = stats


def attend(rows, lengths, block_start, q_rows, k_block, v_block, k_new=None, v_new=None):
    heads, chunk_len, head_dim = q_rows.shape[1:]
    block_len = k_block.shape[2]
    q_tile = chunk_len // 4
    tiles = chunk_len // q_tile
    meta = jnp.concatenate([rows, block_start[None], lengths])
    with_self = k_new is not None
    keys = pl.BlockSpec((1, heads, block_len, head_dim), lambda s, t, meta: (meta[s], 0, 0, 0))
    own = pl.BlockSpec((1, heads, chunk_len, head_dim), lambda s, t, meta: (meta[1], 0, 0, 0))
    sent = lambda s, t: jnp.where(s == 0, t, tiles - 1)
    kept = lambda s, t: jnp.where(s == 0, 0, t)
    o_shape = jax.ShapeDtypeStruct((heads, chunk_len, head_dim), F32)
    s_shape = jax.ShapeDtypeStruct((8, chunk_len), F32)
    return pl.pallas_call(
        functools.partial(attn_kernel, heads, head_dim, q_tile, with_self),
        grid_spec=pltpu.PrefetchScalarGridSpec(
            num_scalar_prefetch=1,
            grid=(2, tiles),
            in_specs=[pl.BlockSpec((1, heads, q_tile, head_dim), lambda s, t, meta: (s, 0, t, 0)), keys, keys]
            + ([own, own] if with_self else []),
            out_specs=[
                pl.BlockSpec((heads, q_tile, head_dim), lambda s, t, meta: (0, sent(s, t), 0)),
                pl.BlockSpec((8, q_tile), lambda s, t, meta: (0, sent(s, t))),
                pl.BlockSpec((heads, q_tile, head_dim), lambda s, t, meta: (0, kept(s, t), 0)),
                pl.BlockSpec((8, q_tile), lambda s, t, meta: (0, kept(s, t))),
            ],
            scratch_shapes=[pltpu.VMEM((heads, q_tile, head_dim), F32)] * 3,
        ),
        out_shape=[o_shape, s_shape, o_shape, s_shape],
        compiler_params=pltpu.CompilerParams(vmem_limit_bytes=VMEM_LIMIT),
        cost_estimate=pl.CostEstimate(
            flops=16 * heads * chunk_len * (block_len + (chunk_len // 4 if with_self else 0)) * head_dim,
            bytes_accessed=2 * heads * (block_len + 2 * chunk_len) * head_dim * 4,
            transcendentals=2 * heads * chunk_len * block_len,
        ),
        name="attend_own" if with_self else "attend",
    )(meta, q_rows, k_block, v_block, *((k_new, v_new) if with_self else ()))


def merge(heads, pieces):
    peak = functools.reduce(jnp.maximum, [s[:heads] for _, s in pieces])
    weights = [jnp.exp2(s[:heads] - peak) for _, s in pieces]
    total = functools.reduce(jnp.add, [s[heads:2 * heads] * w for (_, s), w in zip(pieces, weights)])
    out = functools.reduce(jnp.add, [o * w[..., None] for (o, _), w in zip(pieces, weights)])
    return out, peak, total


def share_kernel(tp_size, heads, hidden, o_own, o_core, o_far, s_own, s_core, s_far, gain_ref, bias_ref, w_up, b_up_ref,
                 w_down, w_out, extra_ref, out_ref, core_box, last_box,
                 acc, from_left, from_right, from_y, up, down, proj, x_buf, o_buf, s_buf, m_buf, c_buf, stage, land,
                 up_sem, down_sem, proj_sem, x_sem, o_sem, s_sem,
                 left_sem, right_sem, y_sem, core_sem, last_sem, send_sem, stage_sem, land_sem):
    z = lax.axis_index("tp")
    j = lax.axis_index("cp")
    y, c = lax.div(j, 2), lax.rem(j, 2)
    across, mate, corner = (1 - y) * 2 + c, y * 2 + (1 - c), (1 - y) * 2 + (1 - c)
    chunk_len, d_model = acc.shape
    head_dim = o_own.shape[2]
    tokens = chunk_len // CHUNKS
    block = chunk_len // BLOCKS
    pairs = CHUNKS // 2
    per_block = pairs // BLOCKS
    width = up.shape[2]
    last = tp_size - 1
    root_a, root_b = (tp_size - 1) // 2, tp_size // 2


    def weight_copies(f):
        cols = pl.ds(f * width, width)
        return (pltpu.make_async_copy(w_up.at[:, cols], up.at[f], up_sem.at[f]),
                pltpu.make_async_copy(w_down.at[cols, :], down.at[f], down_sem.at[f]))

    def block_copies(b):
        rows = pl.ds(pl.multiple_of(b * block, block), block)
        slot = lax.rem(b, 2)
        copies = [pltpu.make_async_copy(hidden.at[j, rows, :], x_buf.at[slot], x_sem.at[slot])]
        for n, (o_ref, s_ref) in enumerate(((o_own, s_own), (o_core, s_core), (o_far, s_far))):
            copies.append(pltpu.make_async_copy(o_ref.at[:, rows, :], o_buf.at[slot, n], o_sem.at[slot, n]))
            copies.append(pltpu.make_async_copy(s_ref.at[:, rows], s_buf.at[slot, n], s_sem.at[slot, n]))
        return copies

    for copy in block_copies(0):
        copy.start()
    proj_copy = pltpu.make_async_copy(w_out, proj, proj_sem)
    proj_copy.start()
    for f in range(SLICES):
        for copy in weight_copies(f):
            copy.start()

    barrier = pltpu.get_barrier_semaphore()
    pl.semaphore_signal(barrier, inc=1, device_id={"cp": across}, device_id_type=MESH)
    pl.semaphore_signal(barrier, inc=1, device_id={"cp": mate}, device_id_type=MESH)

    @pl.when(z > 0)
    def _():
        pl.semaphore_signal(barrier, inc=1, device_id={"tp": z - 1}, device_id_type=MESH)

    @pl.when(z < last)
    def _():
        pl.semaphore_signal(barrier, inc=1, device_id={"tp": z + 1}, device_id_type=MESH)

    inside = jnp.logical_and(z > 0, z < last)

    @pl.when(inside)
    def _():
        pl.semaphore_wait(barrier, 4)

    @pl.when(jnp.logical_not(inside))
    def _():
        pl.semaphore_wait(barrier, 3)


    def begin(b):
        slot = lax.rem(b, 2)
        rows = pl.ds(pl.multiple_of(b * block, block), block)

        @pl.when(b + 1 < BLOCKS)
        def _():
            for copy in block_copies(b + 1):
                copy.start()

        for copy in block_copies(b):
            copy.wait()

        @pl.when(b == 0)
        def _():
            proj_copy.wait()

        maxima = [s_buf[slot, n, :heads, :] for n in range(3)]
        peak = jnp.maximum(jnp.maximum(maxima[0], maxima[1]), maxima[2])
        weights = [jnp.exp2(m - peak) for m in maxima]
        total = functools.reduce(jnp.add, [s_buf[slot, n, heads:2 * heads, :] * w for n, w in enumerate(weights)])
        shares = [w / total for w in weights]
        spare = jnp.zeros((head_dim - 3 * heads, block), F32)
        columns = jnp.concatenate(shares + [spare], axis=0).T
        for h in range(heads):
            context = functools.reduce(
                jnp.add, [o_buf[slot, n, h] * columns[:, n * heads + h:n * heads + h + 1] for n in range(3)])
            c_buf[:, h * head_dim:(h + 1) * head_dim] = context.astype(BF16)
        x = x_buf[slot]
        m_buf[...] = layer_norm(x, gain_ref[...], bias_ref[...])
        acc[rows, :] = jnp.dot(c_buf[...], proj[...], preferred_element_type=F32)

        @pl.when(z == 0)
        def _():
            acc[rows, :] += x.astype(F32) + extra_ref[...]

    def slice_of(b, f):
        rows = pl.ds(pl.multiple_of(b * block, block), block)

        @pl.when(b == 0)
        def _():
            for copy in weight_copies(f):
                copy.wait()

        wide_h = jnp.dot(m_buf[...], up[f], preferred_element_type=F32) + b_up_ref[f]
        act = (0.5 * wide_h * (1.0 + lax.erf(wide_h * math.sqrt(0.5)))).astype(BF16)
        acc[rows, :] += jnp.dot(act, down[f], preferred_element_type=F32)


    def at(ref, k):
        return ref.at[pl.ds(pl.multiple_of(k * tokens, tokens), tokens), :]

    def remote(src, dst, k, which, arrive, device):
        return pltpu.make_async_remote_copy(
            src_ref=at(src, k), dst_ref=at(dst, k), send_sem=send_sem.at[which], recv_sem=arrive.at[k],
            device_id=device, device_id_type=MESH,
        )

    def send_right(src, k):
        remote(src, from_left, k, 0, left_sem, {"tp": z + 1}).start()

    def send_left(src, k):
        remote(src, from_right, k, 1, right_sem, {"tp": z - 1}).start()

    def arrived(ref, sem, k):
        remote(ref, ref, k, 0, sem, {"cp": j}).wait_recv()

    def drained(ref, which):
        pltpu.make_async_copy(ref, ref, send_sem.at[which]).wait()

    def emit(stream, values, k, row):
        slot = lax.rem(k, STAGES)

        def copy():
            return pltpu.make_async_copy(stage.at[stream, slot], at(out_ref.at[row], k), stage_sem.at[stream, slot])

        @pl.when(k >= STAGES)
        def _():
            copy().wait()

        stage[stream, slot] = values.astype(BF16)
        copy().start()

    def chunk(ref, k):
        return ref[pl.ds(pl.multiple_of(k * tokens, tokens), tokens), :]

    def finish(src, k):
        remote(src, from_y, k, 2, y_sem, {"cp": across}).start()
        remote(src, core_box, k, 3, core_sem, {"cp": mate}).start()
        emit(0, chunk(src, k), k, j)

    def landing(n, box, k):
        slot = lax.rem(k, STAGES)
        return pltpu.make_async_copy(at(box, k), land.at[n, slot], land_sem.at[n, slot])

    def gathered(i):
        def lagged(lag, act):
            @pl.when(jnp.logical_and(i >= lag, i < pairs + lag))
            def _():
                for n in range(2):
                    act((i - lag) * 2 + n)

        def core(k):
            arrived(core_box, core_sem, k)
            landing(0, core_box, k).start()

        def core_out(k):
            landing(0, core_box, k).wait()
            emit(1, land[0, lax.rem(k, STAGES)], k, mate)

        def side(k):
            arrived(from_y, y_sem, k)
            remote(from_y, last_box, k, 4, last_sem, {"cp": mate}).start()
            emit(2, chunk(from_y, k), k, across)

        def final(k):
            arrived(last_box, last_sem, k)
            landing(1, last_box, k).start()

        def final_out(k):
            landing(1, last_box, k).wait()
            emit(3, land[1, lax.rem(k, STAGES)], k, corner)

        lagged(LAG_CORE + 1, core_out)
        lagged(LAG_LAST + 1, final_out)
        lagged(LAG_CORE, core)
        lagged(LAG_Y, side)
        lagged(LAG_LAST, final)

    def add(k, *others):
        rows = pl.ds(pl.multiple_of(k * tokens, tokens), tokens)
        total = acc[rows, :]
        for other in others:
            total = total + other[rows, :]
        acc[rows, :] = total

    def when(cond, act, *args):
        @pl.when(cond)
        def _():
            act(*args)

    def end(i, first):
        inbox, sem = (from_right, right_sem) if first else (from_left, left_sem)
        near_bit = 0 if first else 1

        def got(k):
            arrived(inbox, sem, k)
            finish(inbox, k)

        when(jnp.logical_and(i >= 0, i < pairs), lambda: got(2 * i + near_bit))
        when(jnp.logical_and(i >= LAG_BACK, i < pairs + LAG_BACK), lambda: got(2 * (i - LAG_BACK) + 1 - near_bit))

    def inner(i, left_side):
        mine = 0 if left_side else 1
        if left_side:
            (outer, outer_sem, to_outer), (inward, inward_sem, to_inner) = (
                (from_left, left_sem, send_left), (from_right, right_sem, send_right))
        else:
            (outer, outer_sem, to_outer), (inward, inward_sem, to_inner) = (
                (from_right, right_sem, send_right), (from_left, left_sem, send_left))

        def early(p):
            passed = 2 * p + 1 - mine
            arrived(outer, outer_sem, passed)
            add(passed, outer)
            to_inner(acc, passed)

        def near(p):
            rooted = 2 * p + mine
            arrived(outer, outer_sem, rooted)
            arrived(inward, inward_sem, rooted)
            add(rooted, from_left, from_right)
            to_outer(acc, rooted)
            to_inner(acc, rooted)
            finish(acc, rooted)

        def far(p):
            k = 2 * p + 1 - mine
            arrived(inward, inward_sem, k)
            to_outer(inward, k)
            finish(inward, k)

        when(jnp.logical_and(i + LAG_AHEAD >= 0, i + LAG_AHEAD < pairs), early, i + LAG_AHEAD)
        when(jnp.logical_and(i >= 0, i < pairs), near, i)
        when(jnp.logical_and(i >= LAG_BACK, i < pairs + LAG_BACK), far, i - LAG_BACK)

    lead = SLICES + LAG_START

    @pl.loop(0, lead + pairs + LAG_LAST + 2)
    def _(s):
        @pl.when(s < BLOCKS * SLICES)
        def _():
            b, f = lax.div(s, SLICES), lax.rem(s, SLICES)
            when(f == 0, begin, b)
            slice_of(b, f)

            def push(send):
                @pl.loop(0, 2 * per_block)
                def _(n):
                    send(acc, b * 2 * per_block + n)

            when(jnp.logical_and(f == SLICES - 1, z == 0), push, send_right)
            when(jnp.logical_and(f == SLICES - 1, z == last), push, send_left)

        i = s - lead
        when(z == 0, end, i, True)
        when(z == root_a, inner, i, True)
        when(z == root_b, inner, i, False)
        when(z == last, end, i, False)
        gathered(i)

    @pl.when(z < last)
    def _():
        drained(acc, 0)

    @pl.when(z > 0)
    def _():
        drained(acc, 1)

    for which in (2, 3, 4):
        drained(acc, which)
    for stream in range(4):
        for slot in range(STAGES):
            pltpu.make_async_copy(stage.at[stream, slot], at(out_ref.at[0], 0), stage_sem.at[stream, slot]).wait()


def share(pieces, hidden_in, gain, bias, w_up, b_up, w_down, w_out, extra, tp_size):
    (o_own, s_own), (o_core, s_core), (o_far, s_far) = pieces
    num_rows, chunk_len, d_model = hidden_in.shape
    heads, _, head_dim = o_own.shape
    ff = w_up.shape[1]
    width = ff // SLICES
    tokens = chunk_len // CHUNKS
    block = chunk_len // BLOCKS
    buffer = pltpu.VMEM((chunk_len, d_model), F32)
    box = jax.ShapeDtypeStruct((chunk_len, d_model), F32)
    arrivals = pltpu.SemaphoreType.DMA((CHUNKS,))
    hbm = pl.BlockSpec(memory_space=pl.ANY)
    vmem = pl.BlockSpec(memory_space=pltpu.VMEM)
    out, _, _ = pl.pallas_call(
        functools.partial(share_kernel, tp_size, heads),
        in_specs=[hbm] * 7 + [vmem, vmem, hbm, vmem, hbm, hbm, vmem],
        out_specs=[hbm] * 3,
        out_shape=[jax.ShapeDtypeStruct((num_rows, chunk_len, d_model), BF16), box, box],
        scratch_shapes=[buffer] * 4
        + [
            pltpu.VMEM((SLICES, d_model, width), BF16),
            pltpu.VMEM((SLICES, width, d_model), BF16),
            pltpu.VMEM((heads * head_dim, d_model), BF16),
            pltpu.VMEM((2, block, d_model), BF16),
            pltpu.VMEM((2, 3, heads, block, head_dim), F32),
            pltpu.VMEM((2, 3, 8, block), F32),
            pltpu.VMEM((block, d_model), BF16),
            pltpu.VMEM((block, heads * head_dim), BF16),
            pltpu.VMEM((4, STAGES, tokens, d_model), BF16),
            pltpu.VMEM((2, STAGES, tokens, d_model), F32),
            pltpu.SemaphoreType.DMA((SLICES,)),
            pltpu.SemaphoreType.DMA((SLICES,)),
            pltpu.SemaphoreType.DMA,
            pltpu.SemaphoreType.DMA((2,)),
            pltpu.SemaphoreType.DMA((2, 3)),
            pltpu.SemaphoreType.DMA((2, 3)),
        ]
        + [arrivals] * 5
        + [pltpu.SemaphoreType.DMA((5,)), pltpu.SemaphoreType.DMA((4, STAGES)), pltpu.SemaphoreType.DMA((2, STAGES))],
        compiler_params=pltpu.CompilerParams(collective_id=0, has_side_effects=True, vmem_limit_bytes=SHARE_LIMIT),
        cost_estimate=pl.CostEstimate(flops=100_000_000_000, bytes_accessed=chunk_len * d_model * 16, transcendentals=0),
        name="share",
    )(hidden_in, o_own, o_core, o_far, s_own, s_core, s_far, gain[None], bias[None], w_up,
      b_up.astype(F32).reshape(SLICES, 1, width), w_down, w_out, extra[None])
    return out


def solution(mesh):
    in_specs = (P("dp", None, None), P("dp"), P("dp", "tp", "cp", None), P("dp", "tp", "cp", None), P(), P(), P(), P(), P(None, "tp"), P("tp"), P("tp", None), P(), P(None, "tp"), P("tp"), P("tp", None), P())
    out_specs = (P("dp", None, None), P("dp", "tp", None, None), P("dp", "tp", None, None))
    tp_size = mesh.shape["tp"]
    cp_size = mesh.shape["cp"]
    swap_core = [(i, i ^ 1) for i in range(cp_size)]
    swap_y = [(i, i ^ 2) for i in range(cp_size)]

    def local_layer(hidden_in, lengths, k_block, v_block, ln1_gain, ln1_bias, ln2_gain, ln2_bias, w_qkv, b_qkv, w_out, b_out, w_up, b_up, w_down, b_down):
        num_rows, chunk_len, d_model = hidden_in.shape
        heads, block_len, head_dim = k_block.shape[1:]
        j = lax.axis_index("cp")
        start = j * block_len
        table = rope_table(lengths, chunk_len, head_dim)
        far_rows = jnp.stack([j ^ 3, j ^ 2])
        near_rows = jnp.stack([j ^ 1, j])
        weights = (ln1_gain, ln1_bias, w_qkv, b_qkv, table, heads, head_dim)

        q_far, *filled = project_qkv(far_rows, hidden_in, *weights)
        o_s, s_s, o_k, s_k = attend(far_rows, lengths, start, q_far, k_block, v_block)
        o_r, s_r = lax.ppermute(o_s, "cp", swap_core), lax.ppermute(s_s, "cp", swap_core)
        o_far, peak, total = merge(heads, [(o_k, s_k), (o_r, s_r)])
        s_far = jnp.concatenate([peak, total, s_k[2 * heads:]], axis=0)
        near_rows, o_far, s_far = lax.optimization_barrier((near_rows, o_far, s_far))
        o_y, s_y = lax.ppermute(o_far, "cp", swap_y), lax.ppermute(s_far, "cp", swap_y)
        q_near, k_new, v_new = project_qkv(near_rows, hidden_in, *weights, filled=filled)

        o_s, s_s, o_own, s_own = attend(near_rows, lengths, start, q_near, k_block, v_block, k_new, v_new)
        o_c, s_c = lax.ppermute(o_s, "cp", swap_core), lax.ppermute(s_s, "cp", swap_core)

        pieces = [(o_own, s_own), (o_c, s_c), (o_y, s_y)]
        extra = b_out.astype(F32) + b_down.astype(F32)
        out = share(pieces, hidden_in, ln2_gain, ln2_bias, w_up, b_up, w_down, w_out, extra, tp_size)
        return out, k_new, v_new

    return jax.shard_map(local_layer, mesh=mesh, in_specs=in_specs, out_specs=out_specs, check_vma=False)
```

```python
import functools
import math

import jax
import jax.numpy as jnp
from jax import lax
from jax.experimental import pallas as pl
from jax.experimental.pallas import tpu as pltpu
from jax.sharding import PartitionSpec as P


EPSILON = 1e-5
NEG_BIG = -1e30
ROTARY_SHARE = 4
ROPE_BASE = 10000.0
LOG2E = math.log2(math.e)
MESH = pl.DeviceIdType.MESH
F32 = jnp.float32
BF16 = jnp.bfloat16
VMEM_LIMIT = 60 * 1024 * 1024
SHARE_LIMIT = 67_043_328
CHUNKS = 64
STAGES = 4
BLOCKS = 8
SLICES = 4
LAG_START = 2
LAG_AHEAD = 1
LAG_BACK = 1
LAG_CORE = 2
LAG_Y = 5
LAG_LAST = 6


def layer_norm(values_in, gain_vec, bias_vec):
    x_f32 = values_in.astype(F32)
    row_mean = jnp.mean(x_f32, axis=-1, keepdims=True)
    centered = x_f32 - row_mean
    variance = jnp.mean(centered * centered, axis=-1, keepdims=True)
    return (centered * lax.rsqrt(variance + EPSILON) * gain_vec + bias_vec).astype(BF16)


def rope_table(lengths, chunk_len, head_dim):
    rot_dim = head_dim // ROTARY_SHARE
    half_rot = rot_dim // 2
    positions = lengths[:, None] + jnp.arange(chunk_len, dtype=jnp.int32)[None, :]
    inv_freq = ROPE_BASE ** (-2.0 * jnp.arange(half_rot, dtype=F32) / rot_dim)
    angles = positions.astype(F32)[:, None, :] * inv_freq[:, None]
    cos_tab = jnp.cos(angles)
    sin_tab = jnp.sin(angles)
    return jnp.concatenate([cos_tab, cos_tab, -sin_tab, sin_tab], axis=1)


def qkv_kernel(heads, head_dim, row, x_ref, gain_ref, bias_ref, w_ref, wb_ref, tab_ref, *rest):
    near_ref, far_ref, k_ref, v_ref = rest[-4:]
    rot_dim = head_dim // ROTARY_SHARE
    half_rot = rot_dim // 2
    normed = layer_norm(x_ref[0], gain_ref[...], bias_ref[...])
    tab = tab_ref[0]
    tab = jnp.concatenate([tab] * (head_dim // tab.shape[0]), axis=0).T
    lane = lax.broadcasted_iota(jnp.int32, tab.shape, 1)
    cos_tab = jnp.where(lane < rot_dim, tab, 1.0)
    sin_tab = jnp.where(lane < rot_dim, pltpu.roll(tab, head_dim - rot_dim, 1), 0.0)

    def rotate(values):
        long = values.astype(F32)
        other = jnp.where(lane < half_rot, pltpu.roll(long, head_dim - half_rot, 1), pltpu.roll(long, half_rot, 1))
        return (long * cos_tab + other * sin_tab).astype(BF16)

    pair = 2 * 3 * head_dim
    for first in range(0, heads, 2):
        cols = slice(first // 2 * pair, first // 2 * pair + pair)
        both = (jnp.dot(normed, w_ref[:, cols], preferred_element_type=F32) + wb_ref[:, cols]).astype(BF16)
        for h in (first, first + 1):
            for part in range(3):
                base = ((h - first) * 3 + part) * head_dim
                values = both[:, base:base + head_dim]
                if part < 2:
                    values = rotate(values)
                near_ref[part, h] = values
                far_ref[part, h] = values.astype(F32)
                if part > 0:
                    (k_ref, v_ref)[part - 1][0, h] = values


def project_qkv(row, hidden_in, gain, bias, w_qkv, b_qkv, table, heads, head_dim, filled=()):
    num_rows, chunk_len, d_model = hidden_in.shape
    tile = chunk_len // 4
    width = w_qkv.shape[1]
    out = jax.ShapeDtypeStruct((num_rows, heads, chunk_len, head_dim), BF16)
    once = dict(pipeline_mode=pl.Buffered(1))
    fixed = lambda t, row: (0, 0)
    packed = pl.BlockSpec((3, heads, tile, head_dim), lambda t, row: (0, 0, t, 0))
    placed = pl.BlockSpec((1, heads, tile, head_dim), lambda t, row: (row[0], 0, t, 0))
    return pl.pallas_call(
        functools.partial(qkv_kernel, heads, head_dim),
        grid_spec=pltpu.PrefetchScalarGridSpec(
            num_scalar_prefetch=1,
            grid=(chunk_len // tile,),
            in_specs=[
                pl.BlockSpec((1, tile, d_model), lambda t, row: (row[0], t, 0)),
                pl.BlockSpec((1, d_model), fixed, **once),
                pl.BlockSpec((1, d_model), fixed, **once),
                pl.BlockSpec((d_model, width), fixed, **once),
                pl.BlockSpec((1, width), fixed, **once),
                pl.BlockSpec((1, table.shape[1], tile), lambda t, row: (row[0], 0, t)),
            ] + [pl.BlockSpec(memory_space=pl.ANY)] * len(filled),
            out_specs=[packed, packed, placed, placed],
        ),
        out_shape=[jax.ShapeDtypeStruct((3, heads, chunk_len, head_dim), BF16),
                   jax.ShapeDtypeStruct((3, heads, chunk_len, head_dim), F32), out, out],
        input_output_aliases={7: 2, 8: 3} if filled else {},
        compiler_params=pltpu.CompilerParams(vmem_limit_bytes=VMEM_LIMIT),
        cost_estimate=pl.CostEstimate(
            flops=2 * chunk_len * d_model * width,
            bytes_accessed=2 * (chunk_len * (d_model + 5 * width) + d_model * width),
            transcendentals=0,
        ),
        name="qkv_rope_near" if filled else "qkv_rope_far",
    )(row, hidden_in, gain[None], bias[None], w_qkv, b_qkv.astype(F32)[None], table, *filled)


def place_kernel(row, k_in, v_in, _k, _v, k_out, v_out):
    k_out[...] = k_in[...].astype(BF16)
    v_out[...] = v_in[...].astype(BF16)


def place(row, received, k_all, v_all):
    _, heads, chunk_len, head_dim = received.shape
    tile = chunk_len // 4
    taken = lambda part: pl.BlockSpec((1, heads, tile, head_dim), lambda t, row: (part, 0, t, 0))
    placed = pl.BlockSpec((1, heads, tile, head_dim), lambda t, row: (row[0], 0, t, 0))
    return pl.pallas_call(
        place_kernel,
        grid_spec=pltpu.PrefetchScalarGridSpec(
            num_scalar_prefetch=1,
            grid=(chunk_len // tile,),
            in_specs=[taken(1), taken(2)] + [pl.BlockSpec(memory_space=pl.ANY)] * 2,
            out_specs=[placed, placed],
        ),
        out_shape=[jax.ShapeDtypeStruct(k_all.shape, BF16)] * 2,
        input_output_aliases={3: 0, 4: 1},
        cost_estimate=pl.CostEstimate(
            flops=10_000_000_000 // 4, bytes_accessed=12 * heads * chunk_len * head_dim, transcendentals=0),
        name="place",
    )(row, received, received, k_all, v_all)


def wide(column, lanes):
    return jnp.concatenate([column] * (lanes // column.shape[1]), axis=1)


def scores_of(query, keys, scale, mask):
    scores = lax.dot_general(query, keys, (((1,), (1,)), ((), ())), preferred_element_type=F32) * scale
    return scores if mask is None else jnp.where(mask, scores, NEG_BIG)


def lane_sum(values, lanes):
    return functools.reduce(jnp.add, [values[:, n:n + lanes] for n in range(0, values.shape[1], lanes)])


def lane_max(values, lanes):
    return functools.reduce(jnp.maximum, [values[:, n:n + lanes] for n in range(0, values.shape[1], lanes)])


def first_step(heads, scale, q_of, k_of, v_of, m_scr, l_scr, o_scr, mask):
    for h in range(heads):
        lanes = o_scr.shape[2]
        scores = scores_of(q_of(h), k_of(h), scale, mask)
        peak = jnp.broadcast_to(jnp.max(lane_max(scores, lanes), axis=1, keepdims=True), m_scr.shape[1:])
        probs = jnp.exp2(scores - wide(peak, scores.shape[1]))
        m_scr[h] = peak
        l_scr[h] = lane_sum(probs, lanes)
        o_scr[h] = jnp.dot(probs.astype(BF16), v_of(h), preferred_element_type=F32)


def block_step(heads, scale, q_of, k_of, v_of, m_scr, l_scr, o_scr, mask):
    for h in range(heads):
        lanes = o_scr.shape[2]
        scores = scores_of(q_of(h), k_of(h), scale, mask)
        m_old = m_scr[h]
        m_new = jnp.maximum(m_old, jnp.max(lane_max(scores, lanes), axis=1, keepdims=True))
        probs = jnp.exp2(scores - wide(m_new, scores.shape[1]))
        shrink = jnp.exp2(m_old - m_new)
        l_scr[h] = l_scr[h] * shrink + lane_sum(probs, lanes)
        m_scr[h] = m_new
        o_scr[h] = o_scr[h] * shrink + jnp.dot(probs.astype(BF16), v_of(h), preferred_element_type=F32)


def attn_kernel(heads, head_dim, q_tile, with_self, meta, q_ref, k_ref, v_ref, *rest):
    if with_self:
        kn_ref, vn_ref, *rest = rest
    o_ref, s_ref, m_scr, l_scr, o_scr = rest
    tile = pl.program_id(0)
    block_len = k_ref.shape[2]
    half = block_len // 2
    valid = jnp.clip(meta[2 + meta[0]] - meta[1], 0, block_len)
    scale = head_dim ** -0.5 * LOG2E

    def query(h):
        return q_ref[0, h].astype(BF16)

    def cache_block(size):
        mask = lax.broadcasted_iota(jnp.int32, (q_tile, size), 1) < valid
        first_step(
            heads, scale, query, lambda h: k_ref[0, h, :size, :], lambda h: v_ref[0, h, :size, :], m_scr, l_scr, o_scr, mask
        )

    @pl.when(valid == 0)
    def _():
        m_scr[...] = jnp.full(m_scr.shape, NEG_BIG, F32)
        l_scr[...] = jnp.zeros(l_scr.shape, F32)
        o_scr[...] = jnp.zeros(o_scr.shape, F32)

    @pl.when(jnp.logical_and(valid > 0, valid <= half))
    def _():
        cache_block(half)

    @pl.when(valid > half)
    def _():
        cache_block(block_len)

    if with_self:
        def own_block(block, mask):
            start = pl.multiple_of(block * q_tile, q_tile)
            block_step(
                heads, scale, query,
                lambda h: kn_ref[0, h, pl.ds(start, q_tile), :],
                lambda h: vn_ref[0, h, pl.ds(start, q_tile), :],
                m_scr, l_scr, o_scr, mask,
            )

        @pl.loop(0, tile)
        def _(block):
            own_block(block, None)

        shape = (q_tile, q_tile)
        own_block(tile, lax.broadcasted_iota(jnp.int32, shape, 0) >= lax.broadcasted_iota(jnp.int32, shape, 1))

    lane = lax.broadcasted_iota(jnp.int32, (q_tile, head_dim), 1)
    stats = jnp.zeros((q_tile, head_dim), F32)
    for h in range(heads):
        stats = jnp.where(lane == h, m_scr[h], stats)
        stats = jnp.where(lane == heads + h, jnp.sum(l_scr[h], axis=1, keepdims=True), stats)
    s_ref[...] = stats.T[:8]
    o_ref[...] = o_scr[...]


def attend(meta, packed, k_block, v_block, with_self=False):
    _, heads, chunk_len, head_dim = packed.shape
    block_len = k_block.shape[2]
    q_tile = chunk_len // 4
    keys = pl.BlockSpec((1, heads, block_len, head_dim), lambda t, meta: (meta[0], 0, 0, 0))
    own = lambda part: pl.BlockSpec((1, heads, chunk_len, head_dim), lambda t, meta: (part, 0, 0, 0))
    return pl.pallas_call(
        functools.partial(attn_kernel, heads, head_dim, q_tile, with_self),
        grid_spec=pltpu.PrefetchScalarGridSpec(
            num_scalar_prefetch=1,
            grid=(chunk_len // q_tile,),
            in_specs=[pl.BlockSpec((1, heads, q_tile, head_dim), lambda t, meta: (0, 0, t, 0)), keys, keys]
            + ([own(1), own(2)] if with_self else []),
            out_specs=[
                pl.BlockSpec((heads, q_tile, head_dim), lambda t, meta: (0, t, 0)),
                pl.BlockSpec((8, q_tile), lambda t, meta: (0, t)),
            ],
            scratch_shapes=[pltpu.VMEM((heads, q_tile, head_dim), F32)] * 3,
        ),
        out_shape=[jax.ShapeDtypeStruct((heads, chunk_len, head_dim), F32), jax.ShapeDtypeStruct((8, chunk_len), F32)],
        compiler_params=pltpu.CompilerParams(vmem_limit_bytes=VMEM_LIMIT),
        cost_estimate=pl.CostEstimate(
            flops=8 * heads * chunk_len * (block_len + (chunk_len if with_self else 0)) * head_dim,
            bytes_accessed=heads * (block_len + 2 * chunk_len) * head_dim * 4,
            transcendentals=heads * chunk_len * block_len,
        ),
        name="attend_own" if with_self else "attend",
    )(meta, packed, k_block, v_block, *((packed, packed) if with_self else ()))


def piece_weights(heads, stats):
    peak = functools.reduce(jnp.maximum, [s[:heads] for s in stats])
    weights = [jnp.exp2(s[:heads] - peak) for s in stats]
    total = functools.reduce(jnp.add, [s[heads:2 * heads] * w for s, w in zip(stats, weights)])
    return peak, weights, total


def as_columns(parts, head_dim):
    count = sum(p.shape[0] for p in parts)
    return jnp.concatenate(parts + [jnp.zeros((head_dim - count, parts[0].shape[1]), F32)], axis=0).T


def merge_kernel(heads, oa_ref, sa_ref, ob_ref, sb_ref, o_ref, s_ref):
    head_dim = o_ref.shape[2]
    stats = [sa_ref[...], sb_ref[...]]
    peak, weights, total = piece_weights(heads, stats)
    columns = as_columns(weights, head_dim)
    for h in range(heads):
        o_ref[h] = oa_ref[h] * columns[:, h:h + 1] + ob_ref[h] * columns[:, heads + h:heads + h + 1]
    spare = [jnp.zeros((8 - 2 * heads, peak.shape[1]), F32)] if heads < 4 else []
    s_ref[...] = jnp.concatenate([peak, total] + spare, axis=0)


def merge(o_a, s_a, o_b, s_b):
    heads, chunk_len, head_dim = o_a.shape
    tile = chunk_len // 4
    o_spec = pl.BlockSpec((heads, tile, head_dim), lambda t: (0, t, 0))
    s_spec = pl.BlockSpec((8, tile), lambda t: (0, t))
    return pl.pallas_call(
        functools.partial(merge_kernel, heads),
        grid=(chunk_len // tile,),
        in_specs=[o_spec, s_spec] * 2,
        out_specs=[o_spec, s_spec],
        out_shape=[jax.ShapeDtypeStruct(o_a.shape, F32), jax.ShapeDtypeStruct(s_a.shape, F32)],
        cost_estimate=pl.CostEstimate(flops=10_000_000_000 // 4, bytes_accessed=12 * o_a.size, transcendentals=0),
        name="merge",
    )(o_a, s_a, o_b, s_b)


def share_kernel(tp_size, heads, hidden, o_own, o_core, o_far, s_own, s_core, s_far, gain_ref, bias_ref, w_up, b_up_ref,
                 w_down, w_out, extra_ref, out_ref, core_box, last_box,
                 acc, from_left, from_right, from_y, up, down, proj, x_buf, o_buf, s_buf, m_buf, c_buf, stage, land,
                 up_sem, down_sem, proj_sem, x_sem, o_sem, s_sem,
                 left_sem, right_sem, y_sem, core_sem, last_sem, send_sem, stage_sem, land_sem):
    z = lax.axis_index("tp")
    j = lax.axis_index("cp")
    y, c = lax.div(j, 2), lax.rem(j, 2)
    across, mate, corner = (1 - y) * 2 + c, y * 2 + (1 - c), (1 - y) * 2 + (1 - c)
    chunk_len, _ = acc.shape
    head_dim = o_own.shape[2]
    tokens = chunk_len // CHUNKS
    block = chunk_len // BLOCKS
    pairs = CHUNKS // 2
    per_block = pairs // BLOCKS
    width = up.shape[2]
    last = tp_size - 1
    root_a, root_b = (tp_size - 1) // 2, tp_size // 2


    def weight_copies(f):
        cols = pl.ds(f * width, width)
        return (pltpu.make_async_copy(w_up.at[:, cols], up.at[f], up_sem.at[f]),
                pltpu.make_async_copy(w_down.at[cols, :], down.at[f], down_sem.at[f]))

    def block_copies(b):
        rows = pl.ds(pl.multiple_of(b * block, block), block)
        slot = lax.rem(b, 2)
        copies = [pltpu.make_async_copy(hidden.at[j, rows, :], x_buf.at[slot], x_sem.at[slot])]
        for n, (o_ref, s_ref) in enumerate(((o_own, s_own), (o_core, s_core), (o_far, s_far))):
            copies.append(pltpu.make_async_copy(o_ref.at[:, rows, :], o_buf.at[slot, n], o_sem.at[slot, n]))
            copies.append(pltpu.make_async_copy(s_ref.at[:, rows], s_buf.at[slot, n], s_sem.at[slot, n]))
        return copies

    for copy in block_copies(0):
        copy.start()
    proj_copy = pltpu.make_async_copy(w_out, proj, proj_sem)
    proj_copy.start()
    for f in range(SLICES):
        for copy in weight_copies(f):
            copy.start()

    barrier = pltpu.get_barrier_semaphore()
    pl.semaphore_signal(barrier, inc=1, device_id={"cp": across}, device_id_type=MESH)
    pl.semaphore_signal(barrier, inc=1, device_id={"cp": mate}, device_id_type=MESH)

    @pl.when(z > 0)
    def _():
        pl.semaphore_signal(barrier, inc=1, device_id={"tp": z - 1}, device_id_type=MESH)

    @pl.when(z < last)
    def _():
        pl.semaphore_signal(barrier, inc=1, device_id={"tp": z + 1}, device_id_type=MESH)

    inside = jnp.logical_and(z > 0, z < last)

    @pl.when(inside)
    def _():
        pl.semaphore_wait(barrier, 4)

    @pl.when(jnp.logical_not(inside))
    def _():
        pl.semaphore_wait(barrier, 3)


    def begin(b):
        slot = lax.rem(b, 2)
        rows = pl.ds(pl.multiple_of(b * block, block), block)

        @pl.when(b + 1 < BLOCKS)
        def _():
            for copy in block_copies(b + 1):
                copy.start()

        for copy in block_copies(b):
            copy.wait()

        @pl.when(b == 0)
        def _():
            proj_copy.wait()

        _, weights, total = piece_weights(heads, [s_buf[slot, n] for n in range(3)])
        columns = as_columns([w / total for w in weights], head_dim)
        for h in range(heads):
            context = functools.reduce(
                jnp.add, [o_buf[slot, n, h] * columns[:, n * heads + h:n * heads + h + 1] for n in range(3)])
            c_buf[:, h * head_dim:(h + 1) * head_dim] = context.astype(BF16)
        x = x_buf[slot]
        m_buf[...] = layer_norm(x, gain_ref[...], bias_ref[...])
        acc[rows, :] = jnp.dot(c_buf[...], proj[...], preferred_element_type=F32)

        @pl.when(z == 0)
        def _():
            acc[rows, :] += x.astype(F32) + extra_ref[...]

    def slice_of(b, f):
        rows = pl.ds(pl.multiple_of(b * block, block), block)

        @pl.when(b == 0)
        def _():
            for copy in weight_copies(f):
                copy.wait()

        wide_h = jnp.dot(m_buf[...], up[f], preferred_element_type=F32) + b_up_ref[f]
        act = (0.5 * wide_h * (1.0 + lax.erf(wide_h * math.sqrt(0.5)))).astype(BF16)
        acc[rows, :] += jnp.dot(act, down[f], preferred_element_type=F32)


    def at(ref, k):
        return ref.at[pl.ds(pl.multiple_of(k * tokens, tokens), tokens), :]

    def remote(src, dst, k, which, arrive, device):
        return pltpu.make_async_remote_copy(
            src_ref=at(src, k), dst_ref=at(dst, k), send_sem=send_sem.at[which], recv_sem=arrive.at[k],
            device_id=device, device_id_type=MESH,
        )

    def send_right(src, k):
        remote(src, from_left, k, 0, left_sem, {"tp": z + 1}).start()

    def send_left(src, k):
        remote(src, from_right, k, 1, right_sem, {"tp": z - 1}).start()

    def arrived(ref, sem, k):
        remote(ref, ref, k, 0, sem, {"cp": j}).wait_recv()

    def drained(ref, which):
        pltpu.make_async_copy(ref, ref, send_sem.at[which]).wait()

    def emit(stream, values, k, row):
        slot = lax.rem(k, STAGES)

        def copy():
            return pltpu.make_async_copy(stage.at[stream, slot], at(out_ref.at[row], k), stage_sem.at[stream, slot])

        @pl.when(k >= STAGES)
        def _():
            copy().wait()

        stage[stream, slot] = values.astype(BF16)
        copy().start()

    def chunk(ref, k):
        return ref[pl.ds(pl.multiple_of(k * tokens, tokens), tokens), :]

    def finish(src, k):
        remote(src, from_y, k, 2, y_sem, {"cp": across}).start()
        remote(src, core_box, k, 3, core_sem, {"cp": mate}).start()
        emit(0, chunk(src, k), k, j)

    def landing(n, box, k):
        slot = lax.rem(k, STAGES)
        return pltpu.make_async_copy(at(box, k), land.at[n, slot], land_sem.at[n, slot])

    def gathered(i):
        def lagged(lag, act):
            @pl.when(jnp.logical_and(i >= lag, i < pairs + lag))
            def _():
                for n in range(2):
                    act((i - lag) * 2 + n)

        def core(k):
            arrived(core_box, core_sem, k)
            landing(0, core_box, k).start()

        def core_out(k):
            landing(0, core_box, k).wait()
            emit(1, land[0, lax.rem(k, STAGES)], k, mate)

        def side(k):
            arrived(from_y, y_sem, k)
            remote(from_y, last_box, k, 4, last_sem, {"cp": mate}).start()
            emit(2, chunk(from_y, k), k, across)

        def final(k):
            arrived(last_box, last_sem, k)
            landing(1, last_box, k).start()

        def final_out(k):
            landing(1, last_box, k).wait()
            emit(3, land[1, lax.rem(k, STAGES)], k, corner)

        lagged(LAG_CORE + 1, core_out)
        lagged(LAG_LAST + 1, final_out)
        lagged(LAG_CORE, core)
        lagged(LAG_Y, side)
        lagged(LAG_LAST, final)

    def add(k, *others):
        rows = pl.ds(pl.multiple_of(k * tokens, tokens), tokens)
        total = acc[rows, :]
        for other in others:
            total = total + other[rows, :]
        acc[rows, :] = total

    def when(cond, act, *args):
        @pl.when(cond)
        def _():
            act(*args)

    def end(i, first):
        inbox, sem = (from_right, right_sem) if first else (from_left, left_sem)
        near_bit = 0 if first else 1

        def got(k):
            arrived(inbox, sem, k)
            finish(inbox, k)

        when(jnp.logical_and(i >= 0, i < pairs), lambda: got(2 * i + near_bit))
        when(jnp.logical_and(i >= LAG_BACK, i < pairs + LAG_BACK), lambda: got(2 * (i - LAG_BACK) + 1 - near_bit))

    def inner(i, left_side):
        mine = 0 if left_side else 1
        if left_side:
            (outer, outer_sem, to_outer), (inward, inward_sem, to_inner) = (
                (from_left, left_sem, send_left), (from_right, right_sem, send_right))
        else:
            (outer, outer_sem, to_outer), (inward, inward_sem, to_inner) = (
                (from_right, right_sem, send_right), (from_left, left_sem, send_left))

        def early(p):
            passed = 2 * p + 1 - mine
            arrived(outer, outer_sem, passed)
            add(passed, outer)
            to_inner(acc, passed)

        def near(p):
            rooted = 2 * p + mine
            arrived(outer, outer_sem, rooted)
            arrived(inward, inward_sem, rooted)
            add(rooted, from_left, from_right)
            to_outer(acc, rooted)
            to_inner(acc, rooted)
            finish(acc, rooted)

        def far(p):
            k = 2 * p + 1 - mine
            arrived(inward, inward_sem, k)
            to_outer(inward, k)
            finish(inward, k)

        when(jnp.logical_and(i + LAG_AHEAD >= 0, i + LAG_AHEAD < pairs), early, i + LAG_AHEAD)
        when(jnp.logical_and(i >= 0, i < pairs), near, i)
        when(jnp.logical_and(i >= LAG_BACK, i < pairs + LAG_BACK), far, i - LAG_BACK)

    lead = SLICES + LAG_START

    @pl.loop(0, lead + pairs + LAG_LAST + 2)
    def _(s):
        @pl.when(s < BLOCKS * SLICES)
        def _():
            b, f = lax.div(s, SLICES), lax.rem(s, SLICES)
            when(f == 0, begin, b)
            slice_of(b, f)

            def push(send):
                @pl.loop(0, 2 * per_block)
                def _(n):
                    send(acc, b * 2 * per_block + n)

            when(jnp.logical_and(f == SLICES - 1, z == 0), push, send_right)
            when(jnp.logical_and(f == SLICES - 1, z == last), push, send_left)

        i = s - lead
        when(z == 0, end, i, True)
        when(z == root_a, inner, i, True)
        when(z == root_b, inner, i, False)
        when(z == last, end, i, False)
        gathered(i)

    @pl.when(z < last)
    def _():
        drained(acc, 0)

    @pl.when(z > 0)
    def _():
        drained(acc, 1)

    for which in (2, 3, 4):
        drained(acc, which)
    for stream in range(4):
        for slot in range(STAGES):
            pltpu.make_async_copy(stage.at[stream, slot], at(out_ref.at[0], 0), stage_sem.at[stream, slot]).wait()


def share(pieces, hidden_in, gain, bias, w_up, b_up, w_down, w_out, extra, tp_size):
    (o_own, s_own), (o_core, s_core), (o_far, s_far) = pieces
    num_rows, chunk_len, d_model = hidden_in.shape
    heads, _, head_dim = o_own.shape
    ff = w_up.shape[1]
    width = ff // SLICES
    tokens = chunk_len // CHUNKS
    block = chunk_len // BLOCKS
    buffer = pltpu.VMEM((chunk_len, d_model), F32)
    box = jax.ShapeDtypeStruct((chunk_len, d_model), F32)
    arrivals = pltpu.SemaphoreType.DMA((CHUNKS,))
    hbm = pl.BlockSpec(memory_space=pl.ANY)
    vmem = pl.BlockSpec(memory_space=pltpu.VMEM)
    out, _, _ = pl.pallas_call(
        functools.partial(share_kernel, tp_size, heads),
        in_specs=[hbm] * 7 + [vmem, vmem, hbm, vmem, hbm, hbm, vmem],
        out_specs=[hbm] * 3,
        out_shape=[jax.ShapeDtypeStruct((num_rows, chunk_len, d_model), BF16), box, box],
        scratch_shapes=[buffer] * 4
        + [
            pltpu.VMEM((SLICES, d_model, width), BF16),
            pltpu.VMEM((SLICES, width, d_model), BF16),
            pltpu.VMEM((heads * head_dim, d_model), BF16),
            pltpu.VMEM((2, block, d_model), BF16),
            pltpu.VMEM((2, 3, heads, block, head_dim), F32),
            pltpu.VMEM((2, 3, 8, block), F32),
            pltpu.VMEM((block, d_model), BF16),
            pltpu.VMEM((block, heads * head_dim), BF16),
            pltpu.VMEM((4, STAGES, tokens, d_model), BF16),
            pltpu.VMEM((2, STAGES, tokens, d_model), F32),
            pltpu.SemaphoreType.DMA((SLICES,)),
            pltpu.SemaphoreType.DMA((SLICES,)),
            pltpu.SemaphoreType.DMA,
            pltpu.SemaphoreType.DMA((2,)),
            pltpu.SemaphoreType.DMA((2, 3)),
            pltpu.SemaphoreType.DMA((2, 3)),
        ]
        + [arrivals] * 5
        + [pltpu.SemaphoreType.DMA((5,)), pltpu.SemaphoreType.DMA((4, STAGES)), pltpu.SemaphoreType.DMA((2, STAGES))],
        compiler_params=pltpu.CompilerParams(collective_id=0, has_side_effects=True, vmem_limit_bytes=SHARE_LIMIT),
        cost_estimate=pl.CostEstimate(flops=100_000_000_000, bytes_accessed=chunk_len * d_model * 16, transcendentals=0),
        name="share",
    )(hidden_in, o_own, o_core, o_far, s_own, s_core, s_far, gain[None], bias[None], w_up,
      b_up.astype(F32).reshape(SLICES, 1, width), w_down, w_out, extra[None])
    return out


def copy_kernel(in_ref, out_ref):
    out_ref[...] = in_ref[...]


def copy_out(array):
    rows, chunk_len, d_model = array.shape
    tile = chunk_len // 2
    spec = pl.BlockSpec((1, tile, d_model), lambda b, t: (b, t, 0))
    return pl.pallas_call(
        copy_kernel,
        grid=(rows, chunk_len // tile),
        in_specs=[spec],
        out_specs=spec,
        out_shape=jax.ShapeDtypeStruct(array.shape, array.dtype),
        compiler_params=pltpu.CompilerParams(vmem_limit_bytes=VMEM_LIMIT),
        cost_estimate=pl.CostEstimate(flops=10_000_000_000, bytes_accessed=4 * array.size, transcendentals=0),
        name="copy_out",
    )(array)


def solution(mesh):
    in_specs = (P("dp", None, None), P("dp"), P("dp", "tp", "cp", None), P("dp", "tp", "cp", None), P(), P(), P(), P(), P(None, "tp"), P("tp"), P("tp", None), P(), P(None, "tp"), P("tp"), P("tp", None), P())
    out_specs = (P("dp", None, None), P("dp", "tp", None, None), P("dp", "tp", None, None))
    tp_size = mesh.shape["tp"]
    cp_size = mesh.shape["cp"]
    swap_core = [(i, i ^ 1) for i in range(cp_size)]
    swap_y = [(i, i ^ 2) for i in range(cp_size)]

    def local_layer(hidden_in, lengths, k_block, v_block, ln1_gain, ln1_bias, ln2_gain, ln2_bias, w_qkv, b_qkv, w_out, b_out, w_up, b_up, w_down, b_down):
        _, chunk_len, _ = hidden_in.shape
        heads, block_len, head_dim = k_block.shape[1:]
        j = lax.axis_index("cp")
        start = j * block_len
        table = rope_table(lengths, chunk_len, head_dim)
        weights = (ln1_gain, ln1_bias, w_qkv, b_qkv, table, heads, head_dim)
        row = lambda n: (j ^ n)[None]
        meta = lambda n: jnp.concatenate([row(n), start[None], lengths])

        def core(*arrays):
            return [lax.ppermute(x, "cp", swap_core) for x in arrays]

        q_far, sent, *filled = project_qkv(row(2), hidden_in, *weights)
        (got,) = core(sent)
        kept = attend(meta(2), q_far, k_block, v_block)
        o_s, s_s = attend(meta(3), got, k_block, v_block)
        joined = core(o_s, s_s)
        filled = place(row(3), got, *filled)
        o_far, s_far = merge(*kept, *joined)
        o_y = lax.ppermute(o_far, "cp", swap_y)
        s_y = lax.ppermute(s_far, "cp", swap_y)

        near, o_far = lax.optimization_barrier((row(0), o_far))
        own, sent, *filled = project_qkv(near, hidden_in, *weights, filled=filled)
        (got,) = core(sent)
        o_own, s_own = attend(meta(0), own, k_block, v_block, with_self=True)
        o_c, s_c = core(*attend(meta(1), got, k_block, v_block))
        k_new, v_new = place(row(1), got, *filled)

        pieces = [(o_own, s_own), (o_c, s_c), (o_y, s_y)]
        extra = b_out.astype(F32) + b_down.astype(F32)
        out = share(pieces, hidden_in, ln2_gain, ln2_bias, w_up, b_up, w_down, w_out, extra, tp_size)
        return copy_out(out), k_new, v_new

    return jax.shard_map(local_layer, mesh=mesh, in_specs=in_specs, out_specs=out_specs, check_vma=False)
```

```python
import functools
import math

import jax
import jax.numpy as jnp
from jax import lax
from jax.experimental import pallas as pl
from jax.experimental.pallas import tpu as pltpu
from jax.sharding import PartitionSpec as P


EPSILON = 1e-5
NEG_BIG = -1e30
ROTARY_SHARE = 4
ROPE_BASE = 10000.0
LOG2E = math.log2(math.e)
MESH = pl.DeviceIdType.MESH
F32 = jnp.float32
BF16 = jnp.bfloat16
VMEM_LIMIT = 60 * 1024 * 1024
SHARE_LIMIT = 67_043_328
CHUNKS = 64
STAGES = 4
BLOCKS = 8
SLICES = 4
LAG_START = 2
LAG_AHEAD = 1
LAG_BACK = 1
LAG_CORE = 2
LAG_Y = 5
LAG_LAST = 6


def layer_norm(values_in, gain_vec, bias_vec):
    x_f32 = values_in.astype(F32)
    row_mean = jnp.mean(x_f32, axis=-1, keepdims=True)
    centered = x_f32 - row_mean
    variance = jnp.mean(centered * centered, axis=-1, keepdims=True)
    return (centered * lax.rsqrt(variance + EPSILON) * gain_vec + bias_vec).astype(BF16)


def rope_table(lengths, chunk_len, head_dim):
    rot_dim = head_dim // ROTARY_SHARE
    half_rot = rot_dim // 2
    positions = lengths[:, None] + jnp.arange(chunk_len, dtype=jnp.int32)[None, :]
    inv_freq = ROPE_BASE ** (-2.0 * jnp.arange(half_rot, dtype=F32) / rot_dim)
    angles = positions.astype(F32)[:, None, :] * inv_freq[:, None]
    cos_tab = jnp.cos(angles)
    sin_tab = jnp.sin(angles)
    return jnp.concatenate([cos_tab, cos_tab, -sin_tab, sin_tab], axis=1)


def qkv_kernel(heads, head_dim, meta, x_ref, gain_ref, bias_ref, w_hbm, wb_ref, tab_ref, *rest):
    near_ref, far_ref, k_ref, v_ref, w_ref, w_sem = rest[-6:]
    pair = 2 * 3 * head_dim

    def weights(n):
        cols = pl.ds(n * pair, pair)
        return pltpu.make_async_copy(w_hbm.at[:, cols], w_ref.at[:, cols], w_sem.at[n])

    def once(act):
        @pl.when(pl.program_id(0) == 0)
        def _():
            act()

    for n in range(heads // 2):
        once(weights(n).start)
    rot_dim = head_dim // ROTARY_SHARE
    half_rot = rot_dim // 2
    normed = layer_norm(x_ref[0], gain_ref[...], bias_ref[...])
    tab = tab_ref[0]
    tab = jnp.concatenate([tab] * (head_dim // tab.shape[0]), axis=0).T
    lane = lax.broadcasted_iota(jnp.int32, tab.shape, 1)
    cos_tab = jnp.where(lane < rot_dim, tab, 1.0)
    sin_tab = jnp.where(lane < rot_dim, pltpu.roll(tab, head_dim - rot_dim, 1), 0.0)

    def rotate(values):
        long = values.astype(F32)
        other = jnp.where(lane < half_rot, pltpu.roll(long, head_dim - half_rot, 1), pltpu.roll(long, half_rot, 1))
        return (long * cos_tab + other * sin_tab).astype(BF16)

    for first in range(0, heads, 2):
        once(weights(first // 2).wait)
        cols = slice(first // 2 * pair, first // 2 * pair + pair)
        both = (jnp.dot(normed, w_ref[:, cols], preferred_element_type=F32) + wb_ref[:, cols]).astype(BF16)
        for h in (first, first + 1):
            for part in range(3):
                base = ((h - first) * 3 + part) * head_dim
                values = both[:, base:base + head_dim]
                if part < 2:
                    values = rotate(values)
                near_ref[part, h] = values
                far_ref[part, h] = values.astype(F32)
                if part > 0:
                    (k_ref, v_ref)[part - 1][0, h] = values


def project_qkv(meta, other, hidden_in, gain, bias, w_qkv, b_qkv, table, heads, head_dim, filled=()):
    num_rows, chunk_len, d_model = hidden_in.shape
    tile = chunk_len // 4
    width = w_qkv.shape[1]
    out = jax.ShapeDtypeStruct((num_rows, heads, chunk_len, head_dim), BF16)
    once = dict(pipeline_mode=pl.Buffered(1))
    fixed = lambda t, meta: (0, 0)
    packed = pl.BlockSpec((3, heads, tile, head_dim), lambda t, meta: (0, 0, t, 0))
    placed = pl.BlockSpec((1, heads, tile, head_dim), lambda t, meta: (meta[0] ^ other, 0, t, 0))
    return pl.pallas_call(
        functools.partial(qkv_kernel, heads, head_dim),
        grid_spec=pltpu.PrefetchScalarGridSpec(
            num_scalar_prefetch=1,
            grid=(chunk_len // tile,),
            in_specs=[
                pl.BlockSpec((1, tile, d_model), lambda t, meta: (meta[0] ^ other, t, 0)),
                pl.BlockSpec((1, d_model), fixed, **once),
                pl.BlockSpec((1, d_model), fixed, **once),
                pl.BlockSpec(memory_space=pl.ANY),
                pl.BlockSpec((1, width), fixed, **once),
                pl.BlockSpec((1, table.shape[1], tile), lambda t, meta: (meta[0] ^ other, 0, t)),
            ] + [pl.BlockSpec(memory_space=pl.ANY)] * len(filled),
            out_specs=[packed, packed, placed, placed],
            scratch_shapes=[pltpu.VMEM((d_model, width), BF16), pltpu.SemaphoreType.DMA((heads // 2,))],
        ),
        out_shape=[jax.ShapeDtypeStruct((3, heads, chunk_len, head_dim), BF16),
                   jax.ShapeDtypeStruct((3, heads, chunk_len, head_dim), F32), out, out],
        input_output_aliases={7: 2, 8: 3} if filled else {},
        compiler_params=pltpu.CompilerParams(vmem_limit_bytes=VMEM_LIMIT),
        cost_estimate=pl.CostEstimate(
            flops=2 * chunk_len * d_model * width,
            bytes_accessed=2 * (chunk_len * (d_model + 5 * width) + d_model * width),
            transcendentals=0,
        ),
        name="qkv_rope_near" if filled else "qkv_rope_far",
    )(meta, hidden_in, gain[None], bias[None], w_qkv, b_qkv.astype(F32)[None], table, *filled)


def place_kernel(row, k_in, v_in, _k, _v, k_out, v_out):
    k_out[...] = k_in[...].astype(BF16)
    v_out[...] = v_in[...].astype(BF16)


def place(meta, other, received, k_all, v_all):
    _, heads, chunk_len, head_dim = received.shape
    tile = chunk_len // 4
    taken = lambda part: pl.BlockSpec((1, heads, tile, head_dim), lambda t, meta: (part, 0, t, 0))
    placed = pl.BlockSpec((1, heads, tile, head_dim), lambda t, meta: (meta[0] ^ other, 0, t, 0))
    return pl.pallas_call(
        place_kernel,
        grid_spec=pltpu.PrefetchScalarGridSpec(
            num_scalar_prefetch=1,
            grid=(chunk_len // tile,),
            in_specs=[taken(1), taken(2)] + [pl.BlockSpec(memory_space=pl.ANY)] * 2,
            out_specs=[placed, placed],
        ),
        out_shape=[jax.ShapeDtypeStruct(k_all.shape, BF16)] * 2,
        input_output_aliases={3: 0, 4: 1},
        cost_estimate=pl.CostEstimate(
            flops=10_000_000_000 // 4, bytes_accessed=12 * heads * chunk_len * head_dim, transcendentals=0),
        name="place",
    )(meta, received, received, k_all, v_all)


def wide(column, lanes):
    return jnp.concatenate([column] * (lanes // column.shape[1]), axis=1)


def scores_of(query, keys, scale, mask):
    scores = lax.dot_general(query, keys, (((1,), (1,)), ((), ())), preferred_element_type=F32) * scale
    return scores if mask is None else jnp.where(mask, scores, NEG_BIG)


def lane_sum(values, lanes):
    return functools.reduce(jnp.add, [values[:, n:n + lanes] for n in range(0, values.shape[1], lanes)])


def lane_max(values, lanes):
    return functools.reduce(jnp.maximum, [values[:, n:n + lanes] for n in range(0, values.shape[1], lanes)])


def first_step(heads, scale, q_of, k_of, v_of, m_scr, l_scr, o_scr, mask):
    for h in heads:
        lanes = o_scr.shape[2]
        scores = scores_of(q_of(h), k_of(h), scale, mask)
        peak = jnp.broadcast_to(jnp.max(lane_max(scores, lanes), axis=1, keepdims=True), m_scr.shape[1:])
        probs = jnp.exp2(scores - wide(peak, scores.shape[1]))
        m_scr[h] = peak
        l_scr[h] = lane_sum(probs, lanes)
        o_scr[h] = jnp.dot(probs.astype(BF16), v_of(h), preferred_element_type=F32)


def block_step(heads, scale, q_of, k_of, v_of, m_scr, l_scr, o_scr, mask):
    for h in range(heads):
        lanes = o_scr.shape[2]
        scores = scores_of(q_of(h), k_of(h), scale, mask)
        m_old = m_scr[h]
        m_new = jnp.maximum(m_old, jnp.max(lane_max(scores, lanes), axis=1, keepdims=True))
        probs = jnp.exp2(scores - wide(m_new, scores.shape[1]))
        shrink = jnp.exp2(m_old - m_new)
        l_scr[h] = l_scr[h] * shrink + lane_sum(probs, lanes)
        m_scr[h] = m_new
        o_scr[h] = o_scr[h] * shrink + jnp.dot(probs.astype(BF16), v_of(h), preferred_element_type=F32)


def attn_kernel(heads, head_dim, q_tile, with_self, other, meta, q_ref, k_ref, v_ref, *rest):
    if with_self:
        kn_ref, vn_ref, *rest = rest
    o_ref, s_ref, m_scr, l_scr, o_scr = rest
    tile = pl.program_id(0)
    block_len = k_ref.shape[2]
    half = block_len // 2
    valid = jnp.clip(meta[2 + (meta[0] ^ other)] - meta[1], 0, block_len)
    scale = head_dim ** -0.5 * LOG2E

    def query(h):
        return q_ref[0, h].astype(BF16)

    def cache_block(size, some):
        mask = lax.broadcasted_iota(jnp.int32, (q_tile, size), 1) < valid
        first_step(
            some, scale, query, lambda h: k_ref[0, h, :size, :], lambda h: v_ref[0, h, :size, :], m_scr, l_scr, o_scr, mask
        )

    @pl.when(valid == 0)
    def _():
        m_scr[...] = jnp.full(m_scr.shape, NEG_BIG, F32)
        l_scr[...] = jnp.zeros(l_scr.shape, F32)
        o_scr[...] = jnp.zeros(o_scr.shape, F32)

    @pl.when(jnp.logical_and(valid > 0, valid <= half))
    def _():
        @pl.loop(0, heads, step=2)
        def _(h):
            cache_block(half, (h, h + 1))

    @pl.when(valid > half)
    def _():
        cache_block(block_len, range(heads))

    if with_self:
        def own_block(block, mask):
            start = pl.multiple_of(block * q_tile, q_tile)
            block_step(
                heads, scale, query,
                lambda h: kn_ref[0, h, pl.ds(start, q_tile), :],
                lambda h: vn_ref[0, h, pl.ds(start, q_tile), :],
                m_scr, l_scr, o_scr, mask,
            )

        @pl.loop(0, tile)
        def _(block):
            own_block(block, None)

        shape = (q_tile, q_tile)
        own_block(tile, lax.broadcasted_iota(jnp.int32, shape, 0) >= lax.broadcasted_iota(jnp.int32, shape, 1))

    lane = lax.broadcasted_iota(jnp.int32, (q_tile, head_dim), 1)
    stats = jnp.zeros((q_tile, head_dim), F32)
    for h in range(heads):
        stats = jnp.where(lane == h, m_scr[h], stats)
        stats = jnp.where(lane == heads + h, jnp.sum(l_scr[h], axis=1, keepdims=True), stats)
    s_ref[...] = stats.T[:8]
    o_ref[...] = o_scr[...]


def attend(meta, other, packed, k_block, v_block, with_self=False):
    _, heads, chunk_len, head_dim = packed.shape
    block_len = k_block.shape[2]
    q_tile = chunk_len // 2
    keys = pl.BlockSpec((1, heads, block_len, head_dim), lambda t, meta: (meta[0] ^ other, 0, 0, 0))
    own = lambda part: pl.BlockSpec((1, heads, chunk_len, head_dim), lambda t, meta: (part, 0, 0, 0))
    return pl.pallas_call(
        functools.partial(attn_kernel, heads, head_dim, q_tile, with_self, other),
        grid_spec=pltpu.PrefetchScalarGridSpec(
            num_scalar_prefetch=1,
            grid=(chunk_len // q_tile,),
            in_specs=[pl.BlockSpec((1, heads, q_tile, head_dim), lambda t, meta: (0, 0, t, 0)), keys, keys]
            + ([own(1), own(2)] if with_self else []),
            out_specs=[
                pl.BlockSpec((heads, q_tile, head_dim), lambda t, meta: (0, t, 0)),
                pl.BlockSpec((8, q_tile), lambda t, meta: (0, t)),
            ],
            scratch_shapes=[pltpu.VMEM((heads, q_tile, head_dim), F32)] * 3,
        ),
        out_shape=[jax.ShapeDtypeStruct((heads, chunk_len, head_dim), F32), jax.ShapeDtypeStruct((8, chunk_len), F32)],
        compiler_params=pltpu.CompilerParams(vmem_limit_bytes=VMEM_LIMIT),
        cost_estimate=pl.CostEstimate(
            flops=8 * heads * chunk_len * (block_len + (chunk_len if with_self else 0)) * head_dim,
            bytes_accessed=heads * (block_len + 2 * chunk_len) * head_dim * 4,
            transcendentals=heads * chunk_len * block_len,
        ),
        name="attend_own" if with_self else "attend",
    )(meta, packed, k_block, v_block, *((packed, packed) if with_self else ()))


def piece_weights(heads, stats):
    peak = functools.reduce(jnp.maximum, [s[:heads] for s in stats])
    weights = [jnp.exp2(s[:heads] - peak) for s in stats]
    total = functools.reduce(jnp.add, [s[heads:2 * heads] * w for s, w in zip(stats, weights)])
    return peak, weights, total


def as_columns(parts, head_dim):
    count = sum(p.shape[0] for p in parts)
    return jnp.concatenate(parts + [jnp.zeros((head_dim - count, parts[0].shape[1]), F32)], axis=0).T


def merge_kernel(heads, oa_ref, sa_ref, ob_ref, sb_ref, o_ref, s_ref):
    head_dim = o_ref.shape[2]
    stats = [sa_ref[...], sb_ref[...]]
    peak, weights, total = piece_weights(heads, stats)
    columns = as_columns(weights, head_dim)
    for h in range(heads):
        o_ref[h] = oa_ref[h] * columns[:, h:h + 1] + ob_ref[h] * columns[:, heads + h:heads + h + 1]
    spare = [jnp.zeros((8 - 2 * heads, peak.shape[1]), F32)] if heads < 4 else []
    s_ref[...] = jnp.concatenate([peak, total] + spare, axis=0)


def merge(o_a, s_a, o_b, s_b):
    heads, chunk_len, head_dim = o_a.shape
    tile = chunk_len // 4
    o_spec = pl.BlockSpec((heads, tile, head_dim), lambda t: (0, t, 0))
    s_spec = pl.BlockSpec((8, tile), lambda t: (0, t))
    return pl.pallas_call(
        functools.partial(merge_kernel, heads),
        grid=(chunk_len // tile,),
        in_specs=[o_spec, s_spec] * 2,
        out_specs=[o_spec, s_spec],
        out_shape=[jax.ShapeDtypeStruct(o_a.shape, F32), jax.ShapeDtypeStruct(s_a.shape, F32)],
        cost_estimate=pl.CostEstimate(flops=10_000_000_000 // 4, bytes_accessed=12 * o_a.size, transcendentals=0),
        name="merge",
    )(o_a, s_a, o_b, s_b)


def share_kernel(tp_size, heads, hidden, o_own, o_core, o_far, s_own, s_core, s_far, gain_ref, bias_ref, w_up, b_up_ref,
                 w_down, w_out, extra_ref, out_ref, core_box, last_box,
                 acc, from_left, from_right, from_y, up, down, proj, x_buf, o_buf, s_buf, m_buf, c_buf, stage, land,
                 up_sem, down_sem, proj_sem, x_sem, o_sem, s_sem,
                 left_sem, right_sem, y_sem, core_sem, last_sem, send_sem, stage_sem, land_sem):
    z = lax.axis_index("tp")
    j = lax.axis_index("cp")
    y, c = lax.div(j, 2), lax.rem(j, 2)
    across, mate, corner = (1 - y) * 2 + c, y * 2 + (1 - c), (1 - y) * 2 + (1 - c)
    chunk_len, _ = acc.shape
    head_dim = o_own.shape[2]
    tokens = chunk_len // CHUNKS
    block = chunk_len // BLOCKS
    pairs = CHUNKS // 2
    per_block = pairs // BLOCKS
    width = up.shape[2]
    last = tp_size - 1
    root_a, root_b = (tp_size - 1) // 2, tp_size // 2


    def weight_copies(f):
        cols = pl.ds(f * width, width)
        return (pltpu.make_async_copy(w_up.at[:, cols], up.at[f], up_sem.at[f]),
                pltpu.make_async_copy(w_down.at[cols, :], down.at[f], down_sem.at[f]))

    def block_copies(b):
        rows = pl.ds(pl.multiple_of(b * block, block), block)
        slot = lax.rem(b, 2)
        copies = [pltpu.make_async_copy(hidden.at[j, rows, :], x_buf.at[slot], x_sem.at[slot])]
        for n, (o_ref, s_ref) in enumerate(((o_own, s_own), (o_core, s_core), (o_far, s_far))):
            copies.append(pltpu.make_async_copy(o_ref.at[:, rows, :], o_buf.at[slot, n], o_sem.at[slot, n]))
            copies.append(pltpu.make_async_copy(s_ref.at[:, rows], s_buf.at[slot, n], s_sem.at[slot, n]))
        return copies

    for copy in block_copies(0):
        copy.start()
    proj_copy = pltpu.make_async_copy(w_out, proj, proj_sem)
    proj_copy.start()
    for f in range(SLICES):
        for copy in weight_copies(f):
            copy.start()

    barrier = pltpu.get_barrier_semaphore()
    pl.semaphore_signal(barrier, inc=1, device_id={"cp": across}, device_id_type=MESH)
    pl.semaphore_signal(barrier, inc=1, device_id={"cp": mate}, device_id_type=MESH)

    @pl.when(z > 0)
    def _():
        pl.semaphore_signal(barrier, inc=1, device_id={"tp": z - 1}, device_id_type=MESH)

    @pl.when(z < last)
    def _():
        pl.semaphore_signal(barrier, inc=1, device_id={"tp": z + 1}, device_id_type=MESH)

    inside = jnp.logical_and(z > 0, z < last)

    @pl.when(inside)
    def _():
        pl.semaphore_wait(barrier, 4)

    @pl.when(jnp.logical_not(inside))
    def _():
        pl.semaphore_wait(barrier, 3)


    def begin(b):
        slot = lax.rem(b, 2)
        rows = pl.ds(pl.multiple_of(b * block, block), block)

        @pl.when(b + 1 < BLOCKS)
        def _():
            for copy in block_copies(b + 1):
                copy.start()

        for copy in block_copies(b):
            copy.wait()

        @pl.when(b == 0)
        def _():
            proj_copy.wait()

        _, weights, total = piece_weights(heads, [s_buf[slot, n] for n in range(3)])
        columns = as_columns([w / total for w in weights], head_dim)
        for h in range(heads):
            context = functools.reduce(
                jnp.add, [o_buf[slot, n, h] * columns[:, n * heads + h:n * heads + h + 1] for n in range(3)])
            c_buf[:, h * head_dim:(h + 1) * head_dim] = context.astype(BF16)
        x = x_buf[slot]
        m_buf[...] = layer_norm(x, gain_ref[...], bias_ref[...])
        acc[rows, :] = jnp.dot(c_buf[...], proj[...], preferred_element_type=F32)

        @pl.when(z == 0)
        def _():
            acc[rows, :] += x.astype(F32) + extra_ref[...]

    def slice_of(b, f):
        rows = pl.ds(pl.multiple_of(b * block, block), block)

        @pl.when(b == 0)
        def _():
            for copy in weight_copies(f):
                copy.wait()

        wide_h = jnp.dot(m_buf[...], up[f], preferred_element_type=F32) + b_up_ref[f]
        act = (0.5 * wide_h * (1.0 + lax.erf(wide_h * math.sqrt(0.5)))).astype(BF16)
        acc[rows, :] += jnp.dot(act, down[f], preferred_element_type=F32)


    def at(ref, k):
        return ref.at[pl.ds(pl.multiple_of(k * tokens, tokens), tokens), :]

    def remote(src, dst, k, which, arrive, device):
        return pltpu.make_async_remote_copy(
            src_ref=at(src, k), dst_ref=at(dst, k), send_sem=send_sem.at[which], recv_sem=arrive.at[k],
            device_id=device, device_id_type=MESH,
        )

    def send_right(src, k):
        remote(src, from_left, k, 0, left_sem, {"tp": z + 1}).start()

    def send_left(src, k):
        remote(src, from_right, k, 1, right_sem, {"tp": z - 1}).start()

    def arrived(ref, sem, k):
        remote(ref, ref, k, 0, sem, {"cp": j}).wait_recv()

    def drained(ref, which):
        pltpu.make_async_copy(ref, ref, send_sem.at[which]).wait()

    def emit(stream, values, k, row):
        slot = lax.rem(k, STAGES)

        def copy():
            return pltpu.make_async_copy(stage.at[stream, slot], at(out_ref.at[row], k), stage_sem.at[stream, slot])

        @pl.when(k >= STAGES)
        def _():
            copy().wait()

        stage[stream, slot] = values.astype(BF16)
        copy().start()

    def chunk(ref, k):
        return ref[pl.ds(pl.multiple_of(k * tokens, tokens), tokens), :]

    def finish(src, k):
        remote(src, from_y, k, 2, y_sem, {"cp": across}).start()
        remote(src, core_box, k, 3, core_sem, {"cp": mate}).start()
        emit(0, chunk(src, k), k, j)

    def landing(n, box, k):
        slot = lax.rem(k, STAGES)
        return pltpu.make_async_copy(at(box, k), land.at[n, slot], land_sem.at[n, slot])

    def gathered(i):
        def lagged(lag, act):
            @pl.when(jnp.logical_and(i >= lag, i < pairs + lag))
            def _():
                for n in range(2):
                    act((i - lag) * 2 + n)

        def core(k):
            arrived(core_box, core_sem, k)
            landing(0, core_box, k).start()

        def core_out(k):
            landing(0, core_box, k).wait()
            emit(1, land[0, lax.rem(k, STAGES)], k, mate)

        def side(k):
            arrived(from_y, y_sem, k)
            remote(from_y, last_box, k, 4, last_sem, {"cp": mate}).start()
            emit(2, chunk(from_y, k), k, across)

        def final(k):
            arrived(last_box, last_sem, k)
            landing(1, last_box, k).start()

        def final_out(k):
            landing(1, last_box, k).wait()
            emit(3, land[1, lax.rem(k, STAGES)], k, corner)

        lagged(LAG_CORE + 1, core_out)
        lagged(LAG_LAST + 1, final_out)
        lagged(LAG_CORE, core)
        lagged(LAG_Y, side)
        lagged(LAG_LAST, final)

    def add(k, *others):
        rows = pl.ds(pl.multiple_of(k * tokens, tokens), tokens)
        total = acc[rows, :]
        for other in others:
            total = total + other[rows, :]
        acc[rows, :] = total

    def when(cond, act, *args):
        @pl.when(cond)
        def _():
            act(*args)

    def end(i, first):
        inbox, sem = (from_right, right_sem) if first else (from_left, left_sem)
        near_bit = 0 if first else 1

        def got(k):
            arrived(inbox, sem, k)
            finish(inbox, k)

        when(jnp.logical_and(i >= 0, i < pairs), lambda: got(2 * i + near_bit))
        when(jnp.logical_and(i >= LAG_BACK, i < pairs + LAG_BACK), lambda: got(2 * (i - LAG_BACK) + 1 - near_bit))

    def inner(i, left_side):
        mine = 0 if left_side else 1
        if left_side:
            (outer, outer_sem, to_outer), (inward, inward_sem, to_inner) = (
                (from_left, left_sem, send_left), (from_right, right_sem, send_right))
        else:
            (outer, outer_sem, to_outer), (inward, inward_sem, to_inner) = (
                (from_right, right_sem, send_right), (from_left, left_sem, send_left))

        def early(p):
            passed = 2 * p + 1 - mine
            arrived(outer, outer_sem, passed)
            add(passed, outer)
            to_inner(acc, passed)

        def near(p):
            rooted = 2 * p + mine
            arrived(outer, outer_sem, rooted)
            arrived(inward, inward_sem, rooted)
            add(rooted, from_left, from_right)
            to_outer(acc, rooted)
            to_inner(acc, rooted)
            finish(acc, rooted)

        def far(p):
            k = 2 * p + 1 - mine
            arrived(inward, inward_sem, k)
            to_outer(inward, k)
            finish(inward, k)

        when(jnp.logical_and(i + LAG_AHEAD >= 0, i + LAG_AHEAD < pairs), early, i + LAG_AHEAD)
        when(jnp.logical_and(i >= 0, i < pairs), near, i)
        when(jnp.logical_and(i >= LAG_BACK, i < pairs + LAG_BACK), far, i - LAG_BACK)

    lead = SLICES + LAG_START

    @pl.loop(0, lead + pairs + LAG_LAST + 2)
    def _(s):
        @pl.when(s < BLOCKS * SLICES)
        def _():
            b, f = lax.div(s, SLICES), lax.rem(s, SLICES)
            when(f == 0, begin, b)
            slice_of(b, f)

            def push(send):
                @pl.loop(0, 2 * per_block)
                def _(n):
                    send(acc, b * 2 * per_block + n)

            when(jnp.logical_and(f == SLICES - 1, z == 0), push, send_right)
            when(jnp.logical_and(f == SLICES - 1, z == last), push, send_left)

        i = s - lead
        when(z == 0, end, i, True)
        when(z == root_a, inner, i, True)
        when(z == root_b, inner, i, False)
        when(z == last, end, i, False)
        gathered(i)

    @pl.when(z < last)
    def _():
        drained(acc, 0)

    @pl.when(z > 0)
    def _():
        drained(acc, 1)

    for which in (2, 3, 4):
        drained(acc, which)
    for stream in range(4):
        for slot in range(STAGES):
            pltpu.make_async_copy(stage.at[stream, slot], at(out_ref.at[0], 0), stage_sem.at[stream, slot]).wait()


def share(pieces, hidden_in, gain, bias, w_up, b_up, w_down, w_out, extra, tp_size):
    (o_own, s_own), (o_core, s_core), (o_far, s_far) = pieces
    num_rows, chunk_len, d_model = hidden_in.shape
    heads, _, head_dim = o_own.shape
    ff = w_up.shape[1]
    width = ff // SLICES
    tokens = chunk_len // CHUNKS
    block = chunk_len // BLOCKS
    buffer = pltpu.VMEM((chunk_len, d_model), F32)
    box = jax.ShapeDtypeStruct((chunk_len, d_model), F32)
    arrivals = pltpu.SemaphoreType.DMA((CHUNKS,))
    hbm = pl.BlockSpec(memory_space=pl.ANY)
    vmem = pl.BlockSpec(memory_space=pltpu.VMEM)
    out, _, _ = pl.pallas_call(
        functools.partial(share_kernel, tp_size, heads),
        in_specs=[hbm] * 7 + [vmem, vmem, hbm, vmem, hbm, hbm, vmem],
        out_specs=[hbm] * 3,
        out_shape=[jax.ShapeDtypeStruct((num_rows, chunk_len, d_model), BF16), box, box],
        scratch_shapes=[buffer] * 4
        + [
            pltpu.VMEM((SLICES, d_model, width), BF16),
            pltpu.VMEM((SLICES, width, d_model), BF16),
            pltpu.VMEM((heads * head_dim, d_model), BF16),
            pltpu.VMEM((2, block, d_model), BF16),
            pltpu.VMEM((2, 3, heads, block, head_dim), F32),
            pltpu.VMEM((2, 3, 8, block), F32),
            pltpu.VMEM((block, d_model), BF16),
            pltpu.VMEM((block, heads * head_dim), BF16),
            pltpu.VMEM((4, STAGES, tokens, d_model), BF16),
            pltpu.VMEM((2, STAGES, tokens, d_model), F32),
            pltpu.SemaphoreType.DMA((SLICES,)),
            pltpu.SemaphoreType.DMA((SLICES,)),
            pltpu.SemaphoreType.DMA,
            pltpu.SemaphoreType.DMA((2,)),
            pltpu.SemaphoreType.DMA((2, 3)),
            pltpu.SemaphoreType.DMA((2, 3)),
        ]
        + [arrivals] * 5
        + [pltpu.SemaphoreType.DMA((5,)), pltpu.SemaphoreType.DMA((4, STAGES)), pltpu.SemaphoreType.DMA((2, STAGES))],
        compiler_params=pltpu.CompilerParams(collective_id=0, has_side_effects=True, vmem_limit_bytes=SHARE_LIMIT),
        cost_estimate=pl.CostEstimate(flops=100_000_000_000, bytes_accessed=chunk_len * d_model * 16, transcendentals=0),
        name="share",
    )(hidden_in, o_own, o_core, o_far, s_own, s_core, s_far, gain[None], bias[None], w_up,
      b_up.astype(F32).reshape(SLICES, 1, width), w_down, w_out, extra[None])
    return out


def copy_kernel(in_ref, out_ref, buf, in_sem, out_sem):
    pieces = in_sem.shape[1]
    tile = buf.shape[1] // pieces
    places = [(b, pl.ds(t * tile, tile), t) for b in range(buf.shape[0]) for t in range(pieces)]
    inward = [pltpu.make_async_copy(in_ref.at[b, rows], buf.at[b, rows], in_sem.at[b, t]) for b, rows, t in places]
    outward = [pltpu.make_async_copy(buf.at[b, rows], out_ref.at[b, rows], out_sem.at[b, t]) for b, rows, t in places]
    for copy in inward:
        copy.start()
    for one, other in zip(inward, outward):
        one.wait()
        other.start()
    for copy in outward:
        copy.wait()


def copy_out(array):
    rows = array.shape[0]
    hbm = pl.BlockSpec(memory_space=pl.ANY)
    return pl.pallas_call(
        copy_kernel,
        in_specs=[hbm],
        out_specs=hbm,
        out_shape=jax.ShapeDtypeStruct(array.shape, array.dtype),
        scratch_shapes=[pltpu.VMEM(array.shape, array.dtype)] + [pltpu.SemaphoreType.DMA((rows, 4))] * 2,
        compiler_params=pltpu.CompilerParams(vmem_limit_bytes=VMEM_LIMIT),
        cost_estimate=pl.CostEstimate(flops=10_000_000_000, bytes_accessed=4 * array.size, transcendentals=0),
        name="copy_out",
    )(array)


def solution(mesh):
    in_specs = (P("dp", None, None), P("dp"), P("dp", "tp", "cp", None), P("dp", "tp", "cp", None), P(), P(), P(), P(), P(None, "tp"), P("tp"), P("tp", None), P(), P(None, "tp"), P("tp"), P("tp", None), P())
    out_specs = (P("dp", None, None), P("dp", "tp", None, None), P("dp", "tp", None, None))
    tp_size = mesh.shape["tp"]
    cp_size = mesh.shape["cp"]
    swap_core = [(i, i ^ 1) for i in range(cp_size)]
    swap_y = [(i, i ^ 2) for i in range(cp_size)]

    def local_layer(hidden_in, lengths, k_block, v_block, ln1_gain, ln1_bias, ln2_gain, ln2_bias, w_qkv, b_qkv, w_out, b_out, w_up, b_up, w_down, b_down):
        _, chunk_len, _ = hidden_in.shape
        heads, block_len, head_dim = k_block.shape[1:]
        j = lax.axis_index("cp")
        start = j * block_len
        table = rope_table(lengths, chunk_len, head_dim)
        weights = (ln1_gain, ln1_bias, w_qkv, b_qkv, table, heads, head_dim)
        meta = jnp.concatenate([j[None], start[None], lengths])

        def core(*arrays):
            return [lax.ppermute(x, "cp", swap_core) for x in arrays]

        q_far, sent, *filled = project_qkv(meta, 2, hidden_in, *weights)
        (got,) = core(sent)
        kept = attend(meta, 2, q_far, k_block, v_block)
        o_s, s_s = attend(meta, 3, got, k_block, v_block)
        joined = core(o_s, s_s)
        filled = place(meta, 3, got, *filled)
        o_far, s_far = merge(*kept, *joined)
        o_y, s_y = [lax.ppermute(x, "cp", swap_y) for x in (o_far, s_far)]

        near, s_far, o_far = lax.optimization_barrier((meta, s_far, o_far))
        own, sent, *filled = project_qkv(near, 0, hidden_in, *weights, filled=filled)
        (got,) = core(sent)
        o_own, s_own = attend(meta, 0, own, k_block, v_block, with_self=True)
        o_c, s_c = core(*attend(meta, 1, got, k_block, v_block))
        k_new, v_new = place(meta, 1, got, *filled)

        pieces = [(o_own, s_own), (o_c, s_c), (o_y, s_y)]
        extra = b_out.astype(F32) + b_down.astype(F32)
        out = share(pieces, hidden_in, ln2_gain, ln2_bias, w_up, b_up, w_down, w_out, extra, tp_size)
        return copy_out(out), k_new, v_new

    return jax.shard_map(local_layer, mesh=mesh, in_specs=in_specs, out_specs=out_specs, check_vma=False)
```

```python
import functools
import math

import jax
import jax.numpy as jnp
from jax import lax
from jax.experimental import pallas as pl
from jax.experimental.pallas import tpu as pltpu
from jax.sharding import PartitionSpec as P


EPSILON = 1e-5
NEG_BIG = -1e30
ROTARY_SHARE = 4
ROPE_BASE = 10000.0
LOG2E = math.log2(math.e)
MESH = pl.DeviceIdType.MESH
F32 = jnp.float32
BF16 = jnp.bfloat16
VMEM_LIMIT = 60 * 1024 * 1024
SHARE_LIMIT = 67_043_328
CHUNKS = 128
STAGES = 4
BLOCKS = 8
SLICES = 8
LAG_START = 4
LAG_AHEAD = 1
LAG_BACK = 2
LAG_CORE = 3
LAG_Y = 6
LAG_LAST = 7


def layer_norm(values_in, gain_vec, bias_vec):
    x_f32 = values_in.astype(F32)
    row_mean = jnp.mean(x_f32, axis=-1, keepdims=True)
    centered = x_f32 - row_mean
    variance = jnp.mean(centered * centered, axis=-1, keepdims=True)
    return (centered * lax.rsqrt(variance + EPSILON) * gain_vec + bias_vec).astype(BF16)


def rope_table(lengths, chunk_len, head_dim):
    rot_dim = head_dim // ROTARY_SHARE
    half_rot = rot_dim // 2
    positions = lengths[:, None] + jnp.arange(chunk_len, dtype=jnp.int32)[None, :]
    inv_freq = ROPE_BASE ** (-2.0 * jnp.arange(half_rot, dtype=F32) / rot_dim)
    angles = positions.astype(F32)[:, None, :] * inv_freq[:, None]
    cos_tab = jnp.cos(angles)
    sin_tab = jnp.sin(angles)
    return jnp.concatenate([cos_tab, cos_tab, -sin_tab, sin_tab], axis=1)


def qkv_kernel(heads, head_dim, meta, x_ref, gain_ref, bias_ref, w_ref, wb_ref, tab_ref, *rest):
    near_ref, far_ref, k_ref, v_ref = rest[-4:]
    pair = 2 * 3 * head_dim
    rot_dim = head_dim // ROTARY_SHARE
    half_rot = rot_dim // 2
    normed = layer_norm(x_ref[0], gain_ref[...], bias_ref[...])
    tab = tab_ref[0]
    tab = jnp.concatenate([tab] * (head_dim // tab.shape[0]), axis=0).T
    lane = lax.broadcasted_iota(jnp.int32, tab.shape, 1)
    cos_tab = jnp.where(lane < rot_dim, tab, 1.0)
    sin_tab = jnp.where(lane < rot_dim, pltpu.roll(tab, head_dim - rot_dim, 1), 0.0)

    def rotate(values):
        long = values.astype(F32)
        other = jnp.where(lane < half_rot, pltpu.roll(long, head_dim - half_rot, 1), pltpu.roll(long, half_rot, 1))
        return (long * cos_tab + other * sin_tab).astype(BF16)

    for first in range(0, heads, 2):
        cols = slice(first // 2 * pair, first // 2 * pair + pair)
        both = (jnp.dot(normed, w_ref[:, cols], preferred_element_type=F32) + wb_ref[:, cols]).astype(BF16)
        for h in (first, first + 1):
            for part in range(3):
                base = ((h - first) * 3 + part) * head_dim
                values = both[:, base:base + head_dim]
                if part < 2:
                    values = rotate(values)
                near_ref[part, h] = values
                far_ref[part, h] = values.astype(F32)
                if part > 0:
                    (k_ref, v_ref)[part - 1][0, h] = values


def project_qkv(meta, other, hidden_in, gain, bias, w_qkv, b_qkv, table, heads, head_dim, filled=()):
    num_rows, chunk_len, d_model = hidden_in.shape
    tile = chunk_len // 4
    width = w_qkv.shape[1]
    out = jax.ShapeDtypeStruct((num_rows, heads, chunk_len, head_dim), BF16)
    once = dict(pipeline_mode=pl.Buffered(1))
    fixed = lambda t, meta: (0, 0)
    packed = pl.BlockSpec((3, heads, tile, head_dim), lambda t, meta: (0, 0, t, 0))
    placed = pl.BlockSpec((1, heads, tile, head_dim), lambda t, meta: (meta[0] ^ other, 0, t, 0))
    return pl.pallas_call(
        functools.partial(qkv_kernel, heads, head_dim),
        grid_spec=pltpu.PrefetchScalarGridSpec(
            num_scalar_prefetch=1,
            grid=(chunk_len // tile,),
            in_specs=[
                pl.BlockSpec((1, tile, d_model), lambda t, meta: (meta[0] ^ other, t, 0)),
                pl.BlockSpec((1, d_model), fixed, **once),
                pl.BlockSpec((1, d_model), fixed, **once),
                pl.BlockSpec((d_model, width), fixed, **once),
                pl.BlockSpec((1, width), fixed, **once),
                pl.BlockSpec((1, table.shape[1], tile), lambda t, meta: (meta[0] ^ other, 0, t)),
            ] + [pl.BlockSpec(memory_space=pl.ANY)] * len(filled),
            out_specs=[packed, packed, placed, placed],
        ),
        out_shape=[jax.ShapeDtypeStruct((3, heads, chunk_len, head_dim), BF16),
                   jax.ShapeDtypeStruct((3, heads, chunk_len, head_dim), F32), out, out],
        input_output_aliases={7: 2, 8: 3} if filled else {},
        compiler_params=pltpu.CompilerParams(vmem_limit_bytes=VMEM_LIMIT),
        cost_estimate=pl.CostEstimate(
            flops=2 * chunk_len * d_model * width,
            bytes_accessed=2 * (chunk_len * (d_model + 5 * width) + d_model * width),
            transcendentals=0,
        ),
        name="qkv_rope_near" if filled else "qkv_rope_far",
    )(meta, hidden_in, gain[None], bias[None], w_qkv, b_qkv.astype(F32)[None], table, *filled)


def place_kernel(row, k_in, v_in, _k, _v, k_out, v_out):
    k_out[...] = k_in[...].astype(BF16)
    v_out[...] = v_in[...].astype(BF16)


def place(meta, other, received, k_all, v_all):
    _, heads, chunk_len, head_dim = received.shape
    tile = chunk_len // 4
    taken = lambda part: pl.BlockSpec((1, heads, tile, head_dim), lambda t, meta: (part, 0, t, 0))
    placed = pl.BlockSpec((1, heads, tile, head_dim), lambda t, meta: (meta[0] ^ other, 0, t, 0))
    return pl.pallas_call(
        place_kernel,
        grid_spec=pltpu.PrefetchScalarGridSpec(
            num_scalar_prefetch=1,
            grid=(chunk_len // tile,),
            in_specs=[taken(1), taken(2)] + [pl.BlockSpec(memory_space=pl.ANY)] * 2,
            out_specs=[placed, placed],
        ),
        out_shape=[jax.ShapeDtypeStruct(k_all.shape, BF16)] * 2,
        input_output_aliases={3: 0, 4: 1},
        cost_estimate=pl.CostEstimate(
            flops=10_000_000_000 // 4, bytes_accessed=12 * heads * chunk_len * head_dim, transcendentals=0),
        name="place",
    )(meta, received, received, k_all, v_all)


def wide(column, lanes):
    return jnp.concatenate([column] * (lanes // column.shape[1]), axis=1)


def scores_of(query, keys, scale, mask):
    scores = lax.dot_general(query, keys, (((1,), (1,)), ((), ())), preferred_element_type=F32) * scale
    return scores if mask is None else jnp.where(mask, scores, NEG_BIG)


def lane_sum(values, lanes):
    return functools.reduce(jnp.add, [values[:, n:n + lanes] for n in range(0, values.shape[1], lanes)])


def lane_max(values, lanes):
    return functools.reduce(jnp.maximum, [values[:, n:n + lanes] for n in range(0, values.shape[1], lanes)])


def first_step(heads, scale, q_of, k_of, v_of, m_scr, l_scr, o_scr, mask):
    for h in heads:
        lanes = o_scr.shape[2]
        scores = scores_of(q_of(h), k_of(h), scale, mask)
        peak = jnp.broadcast_to(jnp.max(lane_max(scores, lanes), axis=1, keepdims=True), m_scr.shape[1:])
        probs = jnp.exp2(scores - wide(peak, scores.shape[1]))
        m_scr[h] = peak
        l_scr[h] = lane_sum(probs, lanes)
        o_scr[h] = jnp.dot(probs.astype(BF16), v_of(h), preferred_element_type=F32)


def block_step(heads, scale, q_of, k_of, v_of, m_scr, l_scr, o_scr, mask):
    for h in range(heads):
        lanes = o_scr.shape[2]
        scores = scores_of(q_of(h), k_of(h), scale, mask)
        m_old = m_scr[h]
        m_new = jnp.maximum(m_old, jnp.max(lane_max(scores, lanes), axis=1, keepdims=True))
        probs = jnp.exp2(scores - wide(m_new, scores.shape[1]))
        shrink = jnp.exp2(m_old - m_new)
        l_scr[h] = l_scr[h] * shrink + lane_sum(probs, lanes)
        m_scr[h] = m_new
        o_scr[h] = o_scr[h] * shrink + jnp.dot(probs.astype(BF16), v_of(h), preferred_element_type=F32)


def attn_kernel(heads, head_dim, q_tile, with_self, other, meta, q_ref, k_ref, v_ref, *rest):
    if with_self:
        kn_ref, vn_ref, *rest = rest
    o_ref, s_ref, m_scr, l_scr, o_scr = rest
    tile = pl.program_id(0)
    block_len = k_ref.shape[2]
    half = block_len // 2
    valid = jnp.clip(meta[2 + (meta[0] ^ other)] - meta[1], 0, block_len)
    scale = head_dim ** -0.5 * LOG2E

    def query(h):
        return q_ref[0, h].astype(BF16)

    def cache_block(size, some):
        mask = lax.broadcasted_iota(jnp.int32, (q_tile, size), 1) < valid
        first_step(
            some, scale, query, lambda h: k_ref[0, h, :size, :], lambda h: v_ref[0, h, :size, :], m_scr, l_scr, o_scr, mask
        )

    @pl.when(valid == 0)
    def _():
        m_scr[...] = jnp.full(m_scr.shape, NEG_BIG, F32)
        l_scr[...] = jnp.zeros(l_scr.shape, F32)
        o_scr[...] = jnp.zeros(o_scr.shape, F32)

    @pl.when(jnp.logical_and(valid > 0, valid <= half))
    def _():
        @pl.loop(0, heads, step=2)
        def _(h):
            cache_block(half, (h, h + 1))

    @pl.when(valid > half)
    def _():
        cache_block(block_len, range(heads))

    if with_self:
        def own_block(block, mask):
            start = pl.multiple_of(block * q_tile, q_tile)
            block_step(
                heads, scale, query,
                lambda h: kn_ref[0, h, pl.ds(start, q_tile), :],
                lambda h: vn_ref[0, h, pl.ds(start, q_tile), :],
                m_scr, l_scr, o_scr, mask,
            )

        @pl.loop(0, tile)
        def _(block):
            own_block(block, None)

        shape = (q_tile, q_tile)
        own_block(tile, lax.broadcasted_iota(jnp.int32, shape, 0) >= lax.broadcasted_iota(jnp.int32, shape, 1))

    lane = lax.broadcasted_iota(jnp.int32, (q_tile, head_dim), 1)
    stats = jnp.zeros((q_tile, head_dim), F32)
    for h in range(heads):
        stats = jnp.where(lane == h, m_scr[h], stats)
        stats = jnp.where(lane == heads + h, jnp.sum(l_scr[h], axis=1, keepdims=True), stats)
    s_ref[...] = stats.T[:8]
    o_ref[...] = o_scr[...]


def attend(meta, other, packed, k_block, v_block, with_self=False):
    _, heads, chunk_len, head_dim = packed.shape
    block_len = k_block.shape[2]
    q_tile = chunk_len // 2
    keys = pl.BlockSpec((1, heads, block_len, head_dim), lambda t, meta: (meta[0] ^ other, 0, 0, 0))
    own = lambda part: pl.BlockSpec((1, heads, chunk_len, head_dim), lambda t, meta: (part, 0, 0, 0))
    return pl.pallas_call(
        functools.partial(attn_kernel, heads, head_dim, q_tile, with_self, other),
        grid_spec=pltpu.PrefetchScalarGridSpec(
            num_scalar_prefetch=1,
            grid=(chunk_len // q_tile,),
            in_specs=[pl.BlockSpec((1, heads, q_tile, head_dim), lambda t, meta: (0, 0, t, 0)), keys, keys]
            + ([own(1), own(2)] if with_self else []),
            out_specs=[
                pl.BlockSpec((heads, q_tile, head_dim), lambda t, meta: (0, t, 0)),
                pl.BlockSpec((8, q_tile), lambda t, meta: (0, t)),
            ],
            scratch_shapes=[pltpu.VMEM((heads, q_tile, head_dim), F32)] * 3,
        ),
        out_shape=[jax.ShapeDtypeStruct((heads, chunk_len, head_dim), F32), jax.ShapeDtypeStruct((8, chunk_len), F32)],
        compiler_params=pltpu.CompilerParams(vmem_limit_bytes=VMEM_LIMIT),
        cost_estimate=pl.CostEstimate(
            flops=8 * heads * chunk_len * (block_len + (chunk_len if with_self else 0)) * head_dim,
            bytes_accessed=heads * (block_len + 2 * chunk_len) * head_dim * 4,
            transcendentals=heads * chunk_len * block_len,
        ),
        name="attend_own" if with_self else "attend",
    )(meta, packed, k_block, v_block, *((packed, packed) if with_self else ()))


def piece_weights(heads, stats):
    peak = functools.reduce(jnp.maximum, [s[:heads] for s in stats])
    weights = [jnp.exp2(s[:heads] - peak) for s in stats]
    total = functools.reduce(jnp.add, [s[heads:2 * heads] * w for s, w in zip(stats, weights)])
    return peak, weights, total


def as_columns(parts, head_dim):
    count = sum(p.shape[0] for p in parts)
    return jnp.concatenate(parts + [jnp.zeros((head_dim - count, parts[0].shape[1]), F32)], axis=0).T


def merge_kernel(heads, oa_ref, sa_ref, ob_ref, sb_ref, o_ref, s_ref):
    head_dim = o_ref.shape[2]
    stats = [sa_ref[...], sb_ref[...]]
    peak, weights, total = piece_weights(heads, stats)
    columns = as_columns(weights, head_dim)
    for h in range(heads):
        o_ref[h] = oa_ref[h] * columns[:, h:h + 1] + ob_ref[h] * columns[:, heads + h:heads + h + 1]
    spare = [jnp.zeros((8 - 2 * heads, peak.shape[1]), F32)] if heads < 4 else []
    s_ref[...] = jnp.concatenate([peak, total] + spare, axis=0)


def merge(o_a, s_a, o_b, s_b):
    heads, chunk_len, head_dim = o_a.shape
    tile = chunk_len // 4
    o_spec = pl.BlockSpec((heads, tile, head_dim), lambda t: (0, t, 0))
    s_spec = pl.BlockSpec((8, tile), lambda t: (0, t))
    return pl.pallas_call(
        functools.partial(merge_kernel, heads),
        grid=(chunk_len // tile,),
        in_specs=[o_spec, s_spec] * 2,
        out_specs=[o_spec, s_spec],
        out_shape=[jax.ShapeDtypeStruct(o_a.shape, F32), jax.ShapeDtypeStruct(s_a.shape, F32)],
        cost_estimate=pl.CostEstimate(flops=10_000_000_000 // 4, bytes_accessed=12 * o_a.size, transcendentals=0),
        name="merge",
    )(o_a, s_a, o_b, s_b)


def share_kernel(tp_size, heads, hidden, o_own, o_core, o_far, s_own, s_core, s_far, gain_ref, bias_ref, w_up, b_up_ref,
                 w_down, w_out, extra_ref, out_ref, core_box, last_box,
                 acc, from_left, from_right, from_y, up, down, proj, x_buf, o_buf, s_buf, m_buf, c_buf, stage, land,
                 up_sem, down_sem, proj_sem, x_sem, o_sem, s_sem,
                 left_sem, right_sem, y_sem, core_sem, last_sem, send_sem, stage_sem, land_sem):
    z = lax.axis_index("tp")
    j = lax.axis_index("cp")
    y, c = lax.div(j, 2), lax.rem(j, 2)
    across, mate, corner = (1 - y) * 2 + c, y * 2 + (1 - c), (1 - y) * 2 + (1 - c)
    chunk_len, _ = acc.shape
    head_dim = o_own.shape[2]
    tokens = chunk_len // CHUNKS
    block = chunk_len // BLOCKS
    pairs = CHUNKS // 2
    per_block = pairs // BLOCKS
    width = up.shape[2]
    last = tp_size - 1
    root_a, root_b = (tp_size - 1) // 2, tp_size // 2


    def weight_copies(f):
        cols = pl.ds(f * width, width)
        return (pltpu.make_async_copy(w_up.at[:, cols], up.at[f], up_sem.at[f]),
                pltpu.make_async_copy(w_down.at[cols, :], down.at[f], down_sem.at[f]))

    def block_copies(b):
        rows = pl.ds(pl.multiple_of(b * block, block), block)
        slot = lax.rem(b, 2)
        copies = [pltpu.make_async_copy(hidden.at[j, rows, :], x_buf.at[slot], x_sem.at[slot])]
        for n, (o_ref, s_ref) in enumerate(((o_own, s_own), (o_core, s_core), (o_far, s_far))):
            copies.append(pltpu.make_async_copy(o_ref.at[:, rows, :], o_buf.at[slot, n], o_sem.at[slot, n]))
            copies.append(pltpu.make_async_copy(s_ref.at[:, rows], s_buf.at[slot, n], s_sem.at[slot, n]))
        return copies

    for copy in block_copies(0):
        copy.start()
    proj_copy = pltpu.make_async_copy(w_out, proj, proj_sem)
    proj_copy.start()
    for f in range(SLICES):
        for copy in weight_copies(f):
            copy.start()

    barrier = pltpu.get_barrier_semaphore()
    pl.semaphore_signal(barrier, inc=1, device_id={"cp": across}, device_id_type=MESH)
    pl.semaphore_signal(barrier, inc=1, device_id={"cp": mate}, device_id_type=MESH)

    @pl.when(z > 0)
    def _():
        pl.semaphore_signal(barrier, inc=1, device_id={"tp": z - 1}, device_id_type=MESH)

    @pl.when(z < last)
    def _():
        pl.semaphore_signal(barrier, inc=1, device_id={"tp": z + 1}, device_id_type=MESH)

    inside = jnp.logical_and(z > 0, z < last)

    @pl.when(inside)
    def _():
        pl.semaphore_wait(barrier, 4)

    @pl.when(jnp.logical_not(inside))
    def _():
        pl.semaphore_wait(barrier, 3)


    def begin(b):
        slot = lax.rem(b, 2)
        rows = pl.ds(pl.multiple_of(b * block, block), block)

        @pl.when(b + 1 < BLOCKS)
        def _():
            for copy in block_copies(b + 1):
                copy.start()

        for copy in block_copies(b):
            copy.wait()

        @pl.when(b == 0)
        def _():
            proj_copy.wait()

        _, weights, total = piece_weights(heads, [s_buf[slot, n] for n in range(3)])
        columns = as_columns([w / total for w in weights], head_dim)
        for h in range(heads):
            context = functools.reduce(
                jnp.add, [o_buf[slot, n, h] * columns[:, n * heads + h:n * heads + h + 1] for n in range(3)])
            c_buf[:, h * head_dim:(h + 1) * head_dim] = context.astype(BF16)
        x = x_buf[slot]
        m_buf[...] = layer_norm(x, gain_ref[...], bias_ref[...])
        acc[rows, :] = jnp.dot(c_buf[...], proj[...], preferred_element_type=F32)

        @pl.when(z == 0)
        def _():
            acc[rows, :] += x.astype(F32) + extra_ref[...]

    def slice_of(b, f):
        rows = pl.ds(pl.multiple_of(b * block, block), block)

        @pl.when(b == 0)
        def _():
            for copy in weight_copies(f):
                copy.wait()

        wide_h = jnp.dot(m_buf[...], up[f], preferred_element_type=F32) + b_up_ref[f]
        act = (0.5 * wide_h * (1.0 + lax.erf(wide_h * math.sqrt(0.5)))).astype(BF16)
        acc[rows, :] += jnp.dot(act, down[f], preferred_element_type=F32)


    def at(ref, k):
        return ref.at[pl.ds(pl.multiple_of(k * tokens, tokens), tokens), :]

    def remote(src, dst, k, which, arrive, device):
        return pltpu.make_async_remote_copy(
            src_ref=at(src, k), dst_ref=at(dst, k), send_sem=send_sem.at[which], recv_sem=arrive.at[k],
            device_id=device, device_id_type=MESH,
        )

    def send_right(src, k):
        remote(src, from_left, k, 0, left_sem, {"tp": z + 1}).start()

    def send_left(src, k):
        remote(src, from_right, k, 1, right_sem, {"tp": z - 1}).start()

    def arrived(ref, sem, k):
        remote(ref, ref, k, 0, sem, {"cp": j}).wait_recv()

    def drained(ref, which):
        pltpu.make_async_copy(ref, ref, send_sem.at[which]).wait()

    def emit(stream, values, k, row):
        slot = lax.rem(k, STAGES)

        def copy():
            return pltpu.make_async_copy(stage.at[stream, slot], at(out_ref.at[row], k), stage_sem.at[stream, slot])

        @pl.when(k >= STAGES)
        def _():
            copy().wait()

        stage[stream, slot] = values.astype(BF16)
        copy().start()

    def chunk(ref, k):
        return ref[pl.ds(pl.multiple_of(k * tokens, tokens), tokens), :]

    def finish(src, k):
        remote(src, from_y, k, 2, y_sem, {"cp": across}).start()
        remote(src, core_box, k, 3, core_sem, {"cp": mate}).start()
        emit(0, chunk(src, k), k, j)

    def landing(n, box, k):
        slot = lax.rem(k, STAGES)
        return pltpu.make_async_copy(at(box, k), land.at[n, slot], land_sem.at[n, slot])

    def gathered(i):
        def lagged(lag, act):
            @pl.when(jnp.logical_and(i >= lag, i < pairs + lag))
            def _():
                for n in range(2):
                    act((i - lag) * 2 + n)

        def core(k):
            arrived(core_box, core_sem, k)
            landing(0, core_box, k).start()

        def core_out(k):
            landing(0, core_box, k).wait()
            emit(1, land[0, lax.rem(k, STAGES)], k, mate)

        def side(k):
            arrived(from_y, y_sem, k)
            remote(from_y, last_box, k, 4, last_sem, {"cp": mate}).start()
            emit(2, chunk(from_y, k), k, across)

        def final(k):
            arrived(last_box, last_sem, k)
            landing(1, last_box, k).start()

        def final_out(k):
            landing(1, last_box, k).wait()
            emit(3, land[1, lax.rem(k, STAGES)], k, corner)

        lagged(LAG_CORE + 1, core_out)
        lagged(LAG_LAST + 1, final_out)
        lagged(LAG_CORE, core)
        lagged(LAG_Y, side)
        lagged(LAG_LAST, final)

    def add(k, *others):
        rows = pl.ds(pl.multiple_of(k * tokens, tokens), tokens)
        total = acc[rows, :]
        for other in others:
            total = total + other[rows, :]
        acc[rows, :] = total

    def when(cond, act, *args):
        @pl.when(cond)
        def _():
            act(*args)

    def end(i, first):
        inbox, sem = (from_right, right_sem) if first else (from_left, left_sem)
        near_bit = 0 if first else 1

        def got(k):
            arrived(inbox, sem, k)
            finish(inbox, k)

        when(jnp.logical_and(i >= 0, i < pairs), lambda: got(2 * i + near_bit))
        when(jnp.logical_and(i >= LAG_BACK, i < pairs + LAG_BACK), lambda: got(2 * (i - LAG_BACK) + 1 - near_bit))

    def inner(i, left_side):
        mine = 0 if left_side else 1
        if left_side:
            (outer, outer_sem, to_outer), (inward, inward_sem, to_inner) = (
                (from_left, left_sem, send_left), (from_right, right_sem, send_right))
        else:
            (outer, outer_sem, to_outer), (inward, inward_sem, to_inner) = (
                (from_right, right_sem, send_right), (from_left, left_sem, send_left))

        def early(p):
            passed = 2 * p + 1 - mine
            arrived(outer, outer_sem, passed)
            add(passed, outer)
            to_inner(acc, passed)

        def near(p):
            rooted = 2 * p + mine
            arrived(outer, outer_sem, rooted)
            arrived(inward, inward_sem, rooted)
            add(rooted, from_left, from_right)
            to_outer(acc, rooted)
            to_inner(acc, rooted)
            finish(acc, rooted)

        def far(p):
            k = 2 * p + 1 - mine
            arrived(inward, inward_sem, k)
            to_outer(inward, k)
            finish(inward, k)

        when(jnp.logical_and(i + LAG_AHEAD >= 0, i + LAG_AHEAD < pairs), early, i + LAG_AHEAD)
        when(jnp.logical_and(i >= 0, i < pairs), near, i)
        when(jnp.logical_and(i >= LAG_BACK, i < pairs + LAG_BACK), far, i - LAG_BACK)

    lead = SLICES + LAG_START

    @pl.loop(0, lead + pairs + LAG_LAST + 2)
    def _(s):
        @pl.when(s < BLOCKS * SLICES)
        def _():
            b, f = lax.div(s, SLICES), lax.rem(s, SLICES)
            when(f == 0, begin, b)
            slice_of(b, f)

            def push(send):
                @pl.loop(0, 2 * per_block)
                def _(n):
                    send(acc, b * 2 * per_block + n)

            when(jnp.logical_and(f == SLICES - 1, z == 0), push, send_right)
            when(jnp.logical_and(f == SLICES - 1, z == last), push, send_left)

        i = s - lead
        when(z == 0, end, i, True)
        when(z == root_a, inner, i, True)
        when(z == root_b, inner, i, False)
        when(z == last, end, i, False)
        gathered(i)

    @pl.when(z < last)
    def _():
        drained(acc, 0)

    @pl.when(z > 0)
    def _():
        drained(acc, 1)

    for which in (2, 3, 4):
        drained(acc, which)
    for stream in range(4):
        for slot in range(STAGES):
            pltpu.make_async_copy(stage.at[stream, slot], at(out_ref.at[0], 0), stage_sem.at[stream, slot]).wait()


def share(pieces, hidden_in, gain, bias, w_up, b_up, w_down, w_out, extra, tp_size):
    (o_own, s_own), (o_core, s_core), (o_far, s_far) = pieces
    num_rows, chunk_len, d_model = hidden_in.shape
    heads, _, head_dim = o_own.shape
    ff = w_up.shape[1]
    width = ff // SLICES
    tokens = chunk_len // CHUNKS
    block = chunk_len // BLOCKS
    buffer = pltpu.VMEM((chunk_len, d_model), F32)
    box = jax.ShapeDtypeStruct((chunk_len, d_model), F32)
    arrivals = pltpu.SemaphoreType.DMA((CHUNKS,))
    hbm = pl.BlockSpec(memory_space=pl.ANY)
    vmem = pl.BlockSpec(memory_space=pltpu.VMEM)
    out, _, _ = pl.pallas_call(
        functools.partial(share_kernel, tp_size, heads),
        in_specs=[hbm] * 7 + [vmem, vmem, hbm, vmem, hbm, hbm, vmem],
        out_specs=[hbm] * 3,
        out_shape=[jax.ShapeDtypeStruct((num_rows, chunk_len, d_model), BF16), box, box],
        scratch_shapes=[buffer] * 4
        + [
            pltpu.VMEM((SLICES, d_model, width), BF16),
            pltpu.VMEM((SLICES, width, d_model), BF16),
            pltpu.VMEM((heads * head_dim, d_model), BF16),
            pltpu.VMEM((2, block, d_model), BF16),
            pltpu.VMEM((2, 3, heads, block, head_dim), F32),
            pltpu.VMEM((2, 3, 8, block), F32),
            pltpu.VMEM((block, d_model), BF16),
            pltpu.VMEM((block, heads * head_dim), BF16),
            pltpu.VMEM((4, STAGES, tokens, d_model), BF16),
            pltpu.VMEM((2, STAGES, tokens, d_model), F32),
            pltpu.SemaphoreType.DMA((SLICES,)),
            pltpu.SemaphoreType.DMA((SLICES,)),
            pltpu.SemaphoreType.DMA,
            pltpu.SemaphoreType.DMA((2,)),
            pltpu.SemaphoreType.DMA((2, 3)),
            pltpu.SemaphoreType.DMA((2, 3)),
        ]
        + [arrivals] * 5
        + [pltpu.SemaphoreType.DMA((5,)), pltpu.SemaphoreType.DMA((4, STAGES)), pltpu.SemaphoreType.DMA((2, STAGES))],
        compiler_params=pltpu.CompilerParams(collective_id=0, has_side_effects=True, vmem_limit_bytes=SHARE_LIMIT),
        cost_estimate=pl.CostEstimate(flops=100_000_000_000, bytes_accessed=chunk_len * d_model * 16, transcendentals=0),
        name="share",
    )(hidden_in, o_own, o_core, o_far, s_own, s_core, s_far, gain[None], bias[None], w_up,
      b_up.astype(F32).reshape(SLICES, 1, width), w_down, w_out, extra[None])
    return out


def copy_kernel(in_ref, out_ref, buf, in_sem, out_sem):
    pieces = in_sem.shape[1]
    tile = buf.shape[1] // pieces
    places = [(b, pl.ds(t * tile, tile), t) for b in range(buf.shape[0]) for t in range(pieces)]
    inward = [pltpu.make_async_copy(in_ref.at[b, rows], buf.at[b, rows], in_sem.at[b, t]) for b, rows, t in places]
    outward = [pltpu.make_async_copy(buf.at[b, rows], out_ref.at[b, rows], out_sem.at[b, t]) for b, rows, t in places]
    for copy in inward:
        copy.start()
    for one, other in zip(inward, outward):
        one.wait()
        other.start()
    for copy in outward:
        copy.wait()


def copy_out(array):
    rows = array.shape[0]
    hbm = pl.BlockSpec(memory_space=pl.ANY)
    return pl.pallas_call(
        copy_kernel,
        in_specs=[hbm],
        out_specs=hbm,
        out_shape=jax.ShapeDtypeStruct(array.shape, array.dtype),
        scratch_shapes=[pltpu.VMEM(array.shape, array.dtype)] + [pltpu.SemaphoreType.DMA((rows, 4))] * 2,
        compiler_params=pltpu.CompilerParams(vmem_limit_bytes=VMEM_LIMIT),
        cost_estimate=pl.CostEstimate(flops=10_000_000_000, bytes_accessed=4 * array.size, transcendentals=0),
        name="copy_out",
    )(array)


def solution(mesh):
    in_specs = (P("dp", None, None), P("dp"), P("dp", "tp", "cp", None), P("dp", "tp", "cp", None), P(), P(), P(), P(), P(None, "tp"), P("tp"), P("tp", None), P(), P(None, "tp"), P("tp"), P("tp", None), P())
    out_specs = (P("dp", None, None), P("dp", "tp", None, None), P("dp", "tp", None, None))
    tp_size = mesh.shape["tp"]
    cp_size = mesh.shape["cp"]
    swap_core = [(i, i ^ 1) for i in range(cp_size)]
    swap_y = [(i, i ^ 2) for i in range(cp_size)]

    def local_layer(hidden_in, lengths, k_block, v_block, ln1_gain, ln1_bias, ln2_gain, ln2_bias, w_qkv, b_qkv, w_out, b_out, w_up, b_up, w_down, b_down):
        _, chunk_len, _ = hidden_in.shape
        heads, block_len, head_dim = k_block.shape[1:]
        j = lax.axis_index("cp")
        start = j * block_len
        table = rope_table(lengths, chunk_len, head_dim)
        weights = (ln1_gain, ln1_bias, w_qkv, b_qkv, table, heads, head_dim)
        meta = jnp.concatenate([j[None], start[None], lengths])

        def core(*arrays):
            return [lax.ppermute(x, "cp", swap_core) for x in arrays]

        q_far, sent, *filled = project_qkv(meta, 2, hidden_in, *weights)
        (got,) = core(sent)
        kept = attend(meta, 2, q_far, k_block, v_block)
        o_s, s_s = attend(meta, 3, got, k_block, v_block)
        joined = core(o_s, s_s)
        filled = place(meta, 3, got, *filled)
        o_far, s_far = merge(*kept, *joined)
        o_y, s_y = [lax.ppermute(x, "cp", swap_y) for x in (o_far, s_far)]

        near, s_far, o_far = lax.optimization_barrier((meta, s_far, o_far))
        own, sent, *filled = project_qkv(near, 0, hidden_in, *weights, filled=filled)
        (got,) = core(sent)
        o_own, s_own = attend(meta, 0, own, k_block, v_block, with_self=True)
        o_c, s_c = core(*attend(meta, 1, got, k_block, v_block))
        k_new, v_new = place(meta, 1, got, *filled)

        pieces = [(o_own, s_own), (o_c, s_c), (o_y, s_y)]
        extra = b_out.astype(F32) + b_down.astype(F32)
        out = share(pieces, hidden_in, ln2_gain, ln2_bias, w_up, b_up, w_down, w_out, extra, tp_size)
        return copy_out(out), k_new, v_new

    return jax.shard_map(local_layer, mesh=mesh, in_specs=in_specs, out_specs=out_specs, check_vma=False)
```

```python
import functools
import math

import jax
import jax.numpy as jnp
from jax import lax
from jax.experimental import pallas as pl
from jax.experimental.pallas import tpu as pltpu
from jax.sharding import PartitionSpec as P

EPSILON = 1e-5
NEG_BIG = -1e30
ROTARY_SHARE = 4
ROPE_BASE = 10000.0
LOG2E = math.log2(math.e)
MESH = pl.DeviceIdType.MESH
F32 = jnp.float32
BF16 = jnp.bfloat16
VMEM_LIMIT = 60 * 1024 * 1024
LAYER_LIMIT = 67_043_328
EMPTY = -1e29
CHUNKS = 64
STAGES = 4
BLOCKS = 8
SLICES = 4
TILES = 4
HALVES = 2
LAG_START = 2
LAG_AHEAD = 1
LAG_BACK = 1
LAG_CORE = 2
LAG_Y = 5
LAG_LAST = 6


def layer_norm(values_in, gain_vec, bias_vec):
    x_f32 = values_in.astype(F32)
    row_mean = jnp.mean(x_f32, axis=-1, keepdims=True)
    centered = x_f32 - row_mean
    variance = jnp.mean(centered * centered, axis=-1, keepdims=True)
    return (centered * lax.rsqrt(variance + EPSILON) * gain_vec + bias_vec).astype(BF16)


def rope_table(lengths, chunk_len, head_dim):
    rot_dim = head_dim // ROTARY_SHARE
    half_rot = rot_dim // 2
    positions = lengths[:, None] + jnp.arange(chunk_len, dtype=jnp.int32)[None, :]
    inv_freq = ROPE_BASE ** (-2.0 * jnp.arange(half_rot, dtype=F32) / rot_dim)
    angles = positions.astype(F32)[:, None, :] * inv_freq[:, None]
    cos_tab = jnp.cos(angles)
    sin_tab = jnp.sin(angles)
    return jnp.concatenate([cos_tab, cos_tab, -sin_tab, sin_tab], axis=1)


def wide(column, lanes):
    return jnp.concatenate([column] * (lanes // column.shape[1]), axis=1)


def scores_of(query, keys, scale, mask):
    scores = lax.dot_general(query, keys, (((1,), (1,)), ((), ())), preferred_element_type=F32) * scale
    return scores if mask is None else jnp.where(mask, scores, NEG_BIG)


def lane_sum(values, lanes):
    return functools.reduce(jnp.add, [values[:, n:n + lanes] for n in range(0, values.shape[1], lanes)])


def lane_max(values, lanes):
    return functools.reduce(jnp.maximum, [values[:, n:n + lanes] for n in range(0, values.shape[1], lanes)])


def first_step(heads, scale, q_of, k_of, v_of, m_scr, l_scr, o_scr, mask):
    for h in range(heads):
        lanes = o_scr.shape[2]
        scores = scores_of(q_of(h), k_of(h), scale, mask)
        peak = jnp.maximum(jnp.max(lane_max(scores, lanes), axis=1, keepdims=True), EMPTY)
        peak = jnp.broadcast_to(peak, m_scr.shape[1:])
        probs = jnp.exp2(scores - wide(peak, scores.shape[1]))
        m_scr[h] = peak
        l_scr[h] = lane_sum(probs, lanes)
        o_scr[h] = jnp.dot(probs.astype(BF16), v_of(h), preferred_element_type=F32)


def block_step(heads, scale, q_of, k_of, v_of, m_scr, l_scr, o_scr, mask):
    for h in range(heads):
        lanes = o_scr.shape[2]
        scores = scores_of(q_of(h), k_of(h), scale, mask)
        m_old = m_scr[h]
        m_new = jnp.maximum(m_old, jnp.max(lane_max(scores, lanes), axis=1, keepdims=True))
        probs = jnp.exp2(scores - wide(m_new, scores.shape[1]))
        shrink = jnp.exp2(m_old - m_new)
        l_scr[h] = l_scr[h] * shrink + lane_sum(probs, lanes)
        m_scr[h] = m_new
        o_scr[h] = o_scr[h] * shrink + jnp.dot(probs.astype(BF16), v_of(h), preferred_element_type=F32)


def piece_weights(heads, stats, head_dim):
    peak = functools.reduce(jnp.maximum, [s[:heads] for s in stats])
    weights = [jnp.exp2(s[:heads] - peak) for s in stats]
    total = functools.reduce(jnp.add, [s[heads:2 * heads] * w for s, w in zip(stats, weights)])
    return peak, weights, total


def as_columns(parts, head_dim):
    count = sum(p.shape[0] for p in parts)
    return jnp.concatenate(parts + [jnp.zeros((head_dim - count, parts[0].shape[1]), F32)], axis=0).T


def layer_kernel(tp_size, heads, lengths, hidden, table, k_cache, v_cache, w_qkv, w_up, w_down, w_out,
                 gain1, bias1, gain2, bias2, b_qkv, b_up_ref, extra_ref,
                 out_ref, y_box, core_box, last_box, pk, qb, ob,
                 acc, from_left, from_right, up, down, proj, x_big, tab_buf, kv, ob_far, m_scr, l_scr, o_scr, st, sbox,
                 stage, land,
                 up_sem, down_sem, proj_sem, xb_sem, tab_sem, pk_sem, kv_sem, q_sem, x_sem, o_sem,
                 qs_sem, qr_sem, fs_sem, fr_sem, ns_sem, nr_sem, ys_sem, yr_sem, ss_sem, sr_sem,
                 left_sem, right_sem, y_sem, core_sem, last_sem, send_sem, stage_sem, land_sem):
    z = lax.axis_index("tp")
    j = lax.axis_index("cp")
    y, c = lax.div(j, 2), lax.rem(j, 2)
    across, mate, corner = (1 - y) * 2 + c, y * 2 + (1 - c), (1 - y) * 2 + (1 - c)
    chunk_len, d_model = acc.shape
    head_dim = o_scr.shape[2]
    span = heads * head_dim
    slots = k_cache.shape[2]
    tokens = chunk_len // CHUNKS
    block = chunk_len // BLOCKS
    half = chunk_len // HALVES
    tile = chunk_len // TILES
    pairs = CHUNKS // 2
    per_block = pairs // BLOCKS
    width = up.shape[2]
    last = tp_size - 1
    root_a, root_b = (tp_size - 1) // 2, tp_size // 2
    rot_dim = head_dim // ROTARY_SHARE
    half_rot = rot_dim // 2
    scale = head_dim ** -0.5 * LOG2E
    own_at, sent_at, kept_at, q_at = 0, span, 2 * span, 3 * span

    def rows_of(n, size):
        return pl.ds(pl.multiple_of(n * size, size), size)

    def weight_copies(f):
        cols = pl.ds(f * width, width)
        return (pltpu.make_async_copy(w_up.at[:, cols], up.at[f], up_sem.at[f]),
                pltpu.make_async_copy(w_down.at[cols, :], down.at[f], down_sem.at[f]))

    def row_of(n):
        return across * (1 - n) + j * n

    def big_x(i):
        return pltpu.make_async_copy(
            hidden.at[row_of(lax.div(i, TILES)), rows_of(lax.rem(i, TILES), tile), :], x_big.at[lax.rem(i, 2)], xb_sem.at[lax.rem(i, 2)])

    def cache_copies(row, slot):
        return (pltpu.make_async_copy(k_cache.at[row], kv.at[slot, 0], kv_sem.at[slot, 0]),
                pltpu.make_async_copy(v_cache.at[row], kv.at[slot, 1], kv_sem.at[slot, 1]))

    def start(copies):
        for copy in copies:
            copy.start()

    def wait(copies):
        for copy in copies:
            copy.wait()

    qkv_copies = [pltpu.make_async_copy(w_qkv.at[:, pl.ds(s * width, width)], up.at[s], up_sem.at[s]) for s in range(3)]
    tab_copies = [pltpu.make_async_copy(table.at[row], tab_buf.at[n], tab_sem.at[n]) for n, row in enumerate((across, j))]
    proj_copy = pltpu.make_async_copy(w_out, proj, proj_sem)
    big_x(0).start()
    start(qkv_copies)
    start(tab_copies)
    start(cache_copies(corner, 0))
    start(cache_copies(across, 1))
    proj_copy.start()

    barrier = pltpu.get_barrier_semaphore()
    pl.semaphore_signal(barrier, inc=1, device_id={"cp": across}, device_id_type=MESH)
    pl.semaphore_signal(barrier, inc=1, device_id={"cp": mate}, device_id_type=MESH)

    @pl.when(z > 0)
    def _():
        pl.semaphore_signal(barrier, inc=1, device_id={"tp": z - 1}, device_id_type=MESH)

    @pl.when(z < last)
    def _():
        pl.semaphore_signal(barrier, inc=1, device_id={"tp": z + 1}, device_id_type=MESH)

    inside = jnp.logical_and(z > 0, z < last)

    @pl.when(inside)
    def _():
        pl.semaphore_wait(barrier, 4)

    @pl.when(jnp.logical_not(inside))
    def _():
        pl.semaphore_wait(barrier, 3)

    def to_core(src, dst, send, arrive):
        return pltpu.make_async_remote_copy(
            src_ref=src, dst_ref=dst, send_sem=send, recv_sem=arrive, device_id={"cp": mate}, device_id_type=MESH)

    def to_y(src, dst, send, arrive):
        return pltpu.make_async_remote_copy(
            src_ref=src, dst_ref=dst, send_sem=send, recv_sem=arrive, device_id={"cp": across}, device_id_type=MESH)


    def sent_tile(n, t):
        slot = lax.rem(t, 2)
        return to_core(acc.at[rows_of(slot, tile), pl.ds(0, 3 * span)], qb.at[n, rows_of(t, tile), :], qs_sem.at[slot], qr_sem.at[n, t])

    wait(qkv_copies)
    wait(tab_copies)

    @pl.loop(0, 2 * TILES)
    def _(i):
        n, t, slot = lax.div(i, TILES), lax.rem(i, TILES), lax.rem(i, 2)

        @pl.when(i + 1 < 2 * TILES)
        def _():
            big_x(i + 1).start()

        big_x(i).wait()

        @pl.when(i >= 2)
        def _():
            sent_tile(n, t).wait_send()

        normed = layer_norm(x_big[slot], gain1[...], bias1[...])
        tab = tab_buf[n, :, rows_of(t, tile)]
        tab = jnp.concatenate([tab] * (head_dim // tab.shape[0]), axis=0).T
        lane = lax.broadcasted_iota(jnp.int32, tab.shape, 1)
        cos_tab = jnp.where(lane < rot_dim, tab, 1.0)
        sin_tab = jnp.where(lane < rot_dim, pltpu.roll(tab, head_dim - rot_dim, 1), 0.0)

        def rotate(values):
            long = values.astype(F32)
            other = jnp.where(lane < half_rot, pltpu.roll(long, head_dim - half_rot, 1), pltpu.roll(long, half_rot, 1))
            return (long * cos_tab + other * sin_tab).astype(BF16)

        place = down.at[n * HALVES + lax.div(t, TILES // HALVES), rows_of(lax.rem(t, TILES // HALVES), tile), :]
        hold = acc.at[rows_of(slot, tile), :]
        for s in range(3):
            part = slice(s * width, (s + 1) * width)
            some = (jnp.dot(normed, up[s], preferred_element_type=F32) + b_qkv[:, part]).astype(BF16)
            for g in range(width // head_dim):
                group = s * (width // head_dim) + g
                values = some[:, g * head_dim:(g + 1) * head_dim]
                if group % 3 < 2:
                    values = rotate(values)
                cols = slice(group * head_dim, (group + 1) * head_dim)
                place[:, cols] = values
                hold[:, cols] = values.astype(F32)
        sent_tile(n, t).start()

    for f in range(SLICES):
        weight_copies(f)[0].start()
    pack_copies = [
        pltpu.make_async_copy(down.at[n * HALVES + e, pl.ds(0, half), pl.ds(0, 3 * span)], pk.at[n, pl.ds(e * half, half), :],
                              pk_sem.at[n, e])
        for n in range(2) for e in range(HALVES)]
    start(pack_copies)
    for t in range(2):
        sent_tile(1, TILES - 2 + t).wait_send()


    def got_queries(n):
        for t in range(TILES):
            sent_tile(n, t).wait_recv()
        copies = [pltpu.make_async_copy(qb.at[n, :, pl.ds(3 * h * head_dim, head_dim)],
                                        acc.at[:, pl.ds(q_at + h * head_dim, head_dim)], q_sem.at[h]) for h in range(heads)]
        start(copies)
        return copies

    def attend(row, slot, query, at, kind, after=None, own=False):
        valid = jnp.clip(lengths[row] - j * slots, 0, slots)

        @pl.loop(0, HALVES)
        def _(e):
            def keys(h):
                return kv[slot, 0, h]

            def values(h):
                return kv[slot, 1, h]

            mask = lax.broadcasted_iota(jnp.int32, (half, slots), 1) < valid
            first_step(heads, scale, lambda h: query(e, h), keys, values, m_scr, l_scr, o_scr, mask)

            def own_block(b, mask):
                def part(p):
                    return lambda h: down[HALVES + b, :half, (3 * h + p) * head_dim:(3 * h + p + 1) * head_dim]

                block_step(heads, scale, lambda h: query(e, h), part(1), part(2), m_scr, l_scr, o_scr, mask)

            if own:
                @pl.loop(0, e)
                def _(b):
                    own_block(b, None)

                shape = (half, half)
                own_block(e, lax.broadcasted_iota(jnp.int32, shape, 0) >= lax.broadcasted_iota(jnp.int32, shape, 1))

            lane = lax.broadcasted_iota(jnp.int32, (half, head_dim), 1)
            stats = jnp.zeros((half, head_dim), F32)
            for h in range(heads):
                stats = jnp.where(lane == h, m_scr[h], stats)
                stats = jnp.where(lane == heads + h, jnp.sum(l_scr[h], axis=1, keepdims=True), stats)
                acc[rows_of(e, half), at + h * head_dim:at + (h + 1) * head_dim] = o_scr[h]
            st[kind, :, rows_of(e, half)] = stats.T[:8]
            if after is not None:
                after(e)

    def held(n):
        return lambda e, h: down[n * HALVES + e, :half, 3 * h * head_dim:(3 * h + 1) * head_dim]

    def taken(e, h):
        return acc[rows_of(e, half), q_at + h * head_dim:q_at + (h + 1) * head_dim].astype(BF16)

    def far_piece(e):
        return to_core(acc.at[rows_of(e, half), pl.ds(sent_at, span)], ob_far.at[rows_of(e, half), :], fs_sem.at[e], fr_sem.at[e])

    def near_piece(e):
        return to_core(acc.at[rows_of(e, half), pl.ds(sent_at, span)], ob.at[0, rows_of(e, half), :], ns_sem.at[e], nr_sem.at[e])

    def y_piece(b):
        return to_y(acc.at[rows_of(b, block), pl.ds(kept_at, span)], ob.at[1, rows_of(b, block), :], ys_sem.at[b], yr_sem.at[b])

    far_stats = to_core(st.at[0], sbox.at[0], ss_sem.at[0], sr_sem.at[0])
    y_stats = to_y(st.at[1], sbox.at[2], ss_sem.at[1], sr_sem.at[2])
    near_stats = to_core(st.at[2], sbox.at[1], ss_sem.at[2], sr_sem.at[1])

    wait(got_queries(0))
    wait(cache_copies(corner, 0))
    attend(corner, 0, taken, sent_at, 0, after=lambda e: far_piece(e).start())
    far_stats.start()
    start(cache_copies(mate, 0))
    near_queries = got_queries(1)
    wait(cache_copies(across, 1))
    attend(across, 1, held(0), kept_at, 1)
    start(cache_copies(j, 1))

    far_stats.wait()
    _, weights, total = piece_weights(heads, [st[1], sbox[0]], head_dim)
    peak = jnp.maximum(st[1, :heads, :], sbox[0, :heads, :])

    @pl.loop(0, HALVES)
    def _(e):
        far_piece(e).wait_recv()

    for b in range(BLOCKS):
        part = slice(b * block, (b + 1) * block)
        columns = as_columns([w[:, part] for w in weights], head_dim)
        for h in range(heads):
            mine = slice(kept_at + h * head_dim, kept_at + (h + 1) * head_dim)
            acc[part, mine] = (acc[part, mine] * columns[:, h:h + 1]
                               + ob_far[part, h * head_dim:(h + 1) * head_dim] * columns[:, heads + h:heads + h + 1])
        y_piece(b).start()
    st[1, :heads, :] = peak
    st[1, heads:2 * heads, :] = total
    y_stats.start()

    for e in range(HALVES):
        far_piece(e).wait_send()
    wait(near_queries)
    wait(cache_copies(mate, 0))
    attend(mate, 0, taken, sent_at, 2, after=lambda e: near_piece(e).start())
    near_stats.start()
    wait(cache_copies(j, 1))
    wait(pack_copies)
    for f in range(HALVES):
        weight_copies(f)[1].start()
    attend(j, 1, held(1), own_at, 3, own=True)
    for f in range(HALVES, SLICES):
        weight_copies(f)[1].start()

    def block_copies(b):
        rows = rows_of(b, block)
        slot = lax.rem(b, 2)
        return [pltpu.make_async_copy(hidden.at[j, rows, :], x_big.at[slot, pl.ds(0, block), :], x_sem.at[slot])] + [
            pltpu.make_async_copy(ob.at[n, rows, :], ob_far.at[rows_of(2 * slot + n, block), :], o_sem.at[slot, n]) for n in range(2)]

    def fetch(b):
        y_piece(b).wait_recv()
        start(block_copies(b))

    near_stats.wait()
    y_stats.wait()
    for e in range(HALVES):
        near_piece(e).wait_recv()
        near_piece(e).wait_send()
    proj_copy.wait()
    fetch(0)


    def begin(b):
        slot = lax.rem(b, 2)
        rows = rows_of(b, block)

        @pl.when(b + 1 < BLOCKS)
        def _():
            fetch(b + 1)

        wait(block_copies(b))
        y_piece(b).wait_send()
        _, weights, total = piece_weights(heads, [st[3, :, rows], sbox[1, :, rows], sbox[2, :, rows]], head_dim)
        columns = as_columns([w / total for w in weights], head_dim)
        for h in range(heads):
            cols = slice(h * head_dim, (h + 1) * head_dim)
            pieces = [acc[rows, own_at + h * head_dim:own_at + (h + 1) * head_dim]]
            pieces += [ob_far[rows_of(2 * slot + n, block), cols] for n in range(2)]
            context = functools.reduce(
                jnp.add, [o * columns[:, n * heads + h:n * heads + h + 1] for n, o in enumerate(pieces)])
            x_big[1, block:2 * block, cols] = context.astype(BF16)
        x = x_big[slot, :block, :]
        x_big[0, block:2 * block, :] = layer_norm(x, gain2[...], bias2[...])
        acc[rows, :] = jnp.dot(x_big[1, block:2 * block, :span], proj[...], preferred_element_type=F32)

        @pl.when(z == 0)
        def _():
            acc[rows, :] += x.astype(F32) + extra_ref[...]

    def slice_of(b, f):
        rows = rows_of(b, block)

        @pl.when(b == 0)
        def _():
            wait(weight_copies(f))

        wide_h = jnp.dot(x_big[0, block:2 * block, :], up[f], preferred_element_type=F32) + b_up_ref[f]
        act = (0.5 * wide_h * (1.0 + lax.erf(wide_h * math.sqrt(0.5)))).astype(BF16)
        acc[rows, :] += jnp.dot(act, down[f], preferred_element_type=F32)


    def at(ref, k):
        return ref.at[pl.ds(pl.multiple_of(k * tokens, tokens), tokens), :]

    def remote(src, dst, k, which, arrive, device):
        return pltpu.make_async_remote_copy(
            src_ref=at(src, k), dst_ref=at(dst, k), send_sem=send_sem.at[which], recv_sem=arrive.at[k],
            device_id=device, device_id_type=MESH,
        )

    def send_right(src, k):
        remote(src, from_left, k, 0, left_sem, {"tp": z + 1}).start()

    def send_left(src, k):
        remote(src, from_right, k, 1, right_sem, {"tp": z - 1}).start()

    def arrived(ref, sem, k):
        remote(ref, ref, k, 0, sem, {"cp": j}).wait_recv()

    def drained(ref, which):
        pltpu.make_async_copy(ref, ref, send_sem.at[which]).wait()

    def emit(stream, values, k, row):
        slot = lax.rem(k, STAGES)

        def copy():
            return pltpu.make_async_copy(stage.at[stream, slot], at(out_ref.at[row], k), stage_sem.at[stream, slot])

        @pl.when(k >= STAGES)
        def _():
            copy().wait()

        stage[stream, slot] = values.astype(BF16)
        copy().start()

    def chunk(ref, k):
        return ref[pl.ds(pl.multiple_of(k * tokens, tokens), tokens), :]

    def finish(src, k):
        remote(src, y_box, k, 2, y_sem, {"cp": across}).start()
        remote(src, core_box, k, 3, core_sem, {"cp": mate}).start()
        emit(0, chunk(src, k), k, j)

    def landing(n, box, k):
        slot = lax.rem(k, STAGES)
        return pltpu.make_async_copy(at(box, k), land.at[n, slot], land_sem.at[n, slot])

    def gathered(i):
        def lagged(lag, act):
            @pl.when(jnp.logical_and(i >= lag, i < pairs + lag))
            def _():
                for n in range(2):
                    act((i - lag) * 2 + n)

        def core(k):
            arrived(core_box, core_sem, k)
            landing(0, core_box, k).start()

        def core_out(k):
            landing(0, core_box, k).wait()
            emit(1, land[0, lax.rem(k, STAGES)], k, mate)

        def side(k):
            arrived(y_box, y_sem, k)
            remote(y_box, last_box, k, 4, last_sem, {"cp": mate}).start()
            landing(2, y_box, k).start()

        def side_out(k):
            landing(2, y_box, k).wait()
            emit(2, land[2, lax.rem(k, STAGES)], k, across)

        def final(k):
            arrived(last_box, last_sem, k)
            landing(1, last_box, k).start()

        def final_out(k):
            landing(1, last_box, k).wait()
            emit(3, land[1, lax.rem(k, STAGES)], k, corner)

        lagged(LAG_CORE + 1, core_out)
        lagged(LAG_Y + 1, side_out)
        lagged(LAG_LAST + 1, final_out)
        lagged(LAG_CORE, core)
        lagged(LAG_Y, side)
        lagged(LAG_LAST, final)

    def add(k, *others):
        rows = pl.ds(pl.multiple_of(k * tokens, tokens), tokens)
        total = acc[rows, :]
        for other in others:
            total = total + other[rows, :]
        acc[rows, :] = total

    def when(cond, act, *args):
        @pl.when(cond)
        def _():
            act(*args)

    def end(i, first):
        inbox, sem = (from_right, right_sem) if first else (from_left, left_sem)
        near_bit = 0 if first else 1

        def got(k):
            arrived(inbox, sem, k)
            finish(inbox, k)

        when(jnp.logical_and(i >= 0, i < pairs), lambda: got(2 * i + near_bit))
        when(jnp.logical_and(i >= LAG_BACK, i < pairs + LAG_BACK), lambda: got(2 * (i - LAG_BACK) + 1 - near_bit))

    def inner(i, left_side):
        mine = 0 if left_side else 1
        if left_side:
            (outer, outer_sem, to_outer), (inward, inward_sem, to_inner) = (
                (from_left, left_sem, send_left), (from_right, right_sem, send_right))
        else:
            (outer, outer_sem, to_outer), (inward, inward_sem, to_inner) = (
                (from_right, right_sem, send_right), (from_left, left_sem, send_left))

        def early(p):
            passed = 2 * p + 1 - mine
            arrived(outer, outer_sem, passed)
            add(passed, outer)
            to_inner(acc, passed)

        def near(p):
            rooted = 2 * p + mine
            arrived(outer, outer_sem, rooted)
            arrived(inward, inward_sem, rooted)
            add(rooted, from_left, from_right)
            to_outer(acc, rooted)
            to_inner(acc, rooted)
            finish(acc, rooted)

        def far(p):
            k = 2 * p + 1 - mine
            arrived(inward, inward_sem, k)
            to_outer(inward, k)
            finish(inward, k)

        when(jnp.logical_and(i + LAG_AHEAD >= 0, i + LAG_AHEAD < pairs), early, i + LAG_AHEAD)
        when(jnp.logical_and(i >= 0, i < pairs), near, i)
        when(jnp.logical_and(i >= LAG_BACK, i < pairs + LAG_BACK), far, i - LAG_BACK)

    lead = SLICES + LAG_START

    @pl.loop(0, lead + pairs + LAG_LAST + 2)
    def _(s):
        @pl.when(s < BLOCKS * SLICES)
        def _():
            b, f = lax.div(s, SLICES), lax.rem(s, SLICES)
            when(f == 0, begin, b)
            slice_of(b, f)

            def push(send):
                @pl.loop(0, 2 * per_block)
                def _(n):
                    send(acc, b * 2 * per_block + n)

            when(jnp.logical_and(f == SLICES - 1, z == 0), push, send_right)
            when(jnp.logical_and(f == SLICES - 1, z == last), push, send_left)

        i = s - lead
        when(z == 0, end, i, True)
        when(z == root_a, inner, i, True)
        when(z == root_b, inner, i, False)
        when(z == last, end, i, False)
        gathered(i)

    @pl.when(z < last)
    def _():
        drained(acc, 0)

    @pl.when(z > 0)
    def _():
        drained(acc, 1)

    for which in (2, 3, 4):
        drained(acc, which)
    for stream in range(4):
        for slot in range(STAGES):
            pltpu.make_async_copy(stage.at[stream, slot], at(out_ref.at[0], 0), stage_sem.at[stream, slot]).wait()


def run_layer(lengths, hidden_in, table, k_block, v_block, w_qkv, w_up, w_down, w_out, norms, b_qkv, b_up, extra, tp_size):
    num_rows, chunk_len, d_model = hidden_in.shape
    heads, slots, head_dim = k_block.shape[1:]
    span = heads * head_dim
    width = w_up.shape[1] // SLICES
    tokens = chunk_len // CHUNKS
    block = chunk_len // BLOCKS
    half = chunk_len // HALVES
    tile = chunk_len // TILES
    dma = pltpu.SemaphoreType.DMA
    buffer = pltpu.VMEM((chunk_len, d_model), F32)
    box = jax.ShapeDtypeStruct((chunk_len, d_model), F32)
    hbm = pl.BlockSpec(memory_space=pl.ANY)
    vmem = pl.BlockSpec(memory_space=pltpu.VMEM)
    out, _, _, _, pk, qb, _ = pl.pallas_call(
        functools.partial(layer_kernel, tp_size, heads),
        in_specs=[pl.BlockSpec(memory_space=pltpu.SMEM)] + [hbm] * 8 + [vmem] * 7,
        out_specs=[hbm] * 7,
        out_shape=[
            jax.ShapeDtypeStruct((num_rows, chunk_len, d_model), BF16), box, box, box,
            jax.ShapeDtypeStruct((2, chunk_len, 3 * span), BF16),
            jax.ShapeDtypeStruct((2, chunk_len, 3 * span), F32),
            jax.ShapeDtypeStruct((2, chunk_len, span), F32),
        ],
        scratch_shapes=[buffer] * 3
        + [
            pltpu.VMEM((SLICES, d_model, width), BF16),
            pltpu.VMEM((SLICES, width, d_model), BF16),
            pltpu.VMEM((span, d_model), BF16),
            pltpu.VMEM((2, tile, d_model), BF16),
            pltpu.VMEM((2,) + table.shape[1:], F32),
            pltpu.VMEM((2, 2, heads, slots, head_dim), BF16),
            pltpu.VMEM((chunk_len, span), F32),
            pltpu.VMEM((heads, half, head_dim), F32),
            pltpu.VMEM((heads, half, head_dim), F32),
            pltpu.VMEM((heads, half, head_dim), F32),
            pltpu.VMEM((4, 8, chunk_len), F32),
            pltpu.VMEM((3, 8, chunk_len), F32),
            pltpu.VMEM((4, STAGES, tokens, d_model), BF16),
            pltpu.VMEM((3, STAGES, tokens, d_model), F32),
        ]
        + [dma((SLICES,)), dma((SLICES,)), dma, dma((2,)), dma((2,)), dma((2, HALVES)), dma((2, 2)), dma((heads,)), dma((2,)), dma((2, 2))]
        + [dma((2,)), dma((2, TILES)), dma((HALVES,)), dma((HALVES,)), dma((HALVES,)), dma((HALVES,)), dma((BLOCKS,)), dma((BLOCKS,)),
           dma((3,)), dma((3,))]
        + [dma((CHUNKS,))] * 5
        + [dma((5,)), dma((4, STAGES)), dma((3, STAGES))],
        compiler_params=pltpu.CompilerParams(collective_id=0, has_side_effects=True, vmem_limit_bytes=LAYER_LIMIT),
        cost_estimate=pl.CostEstimate(flops=100_000_000_000, bytes_accessed=chunk_len * d_model * 16, transcendentals=0),
        name="layer",
    )(lengths, hidden_in, table, k_block, v_block, w_qkv, w_up, w_down, w_out, *norms, b_qkv.astype(F32)[None],
      b_up.astype(F32).reshape(SLICES, 1, width), extra[None])
    return out, pk, qb


def finish_kernel(heads, meta, in_ref, pk, qb, out_ref, k_ref, v_ref, buf, low, high, in_sem, out_sem, low_sem, high_sem, kv_sem):
    pieces = in_sem.shape[1]
    tile = buf.shape[1] // pieces
    head_dim = k_ref.shape[3]
    places = [(b, pl.ds(t * tile, tile), t) for b in range(buf.shape[0]) for t in range(pieces)]
    inward = [pltpu.make_async_copy(in_ref.at[b, rows], buf.at[b, rows], in_sem.at[b, t]) for b, rows, t in places]
    outward = [pltpu.make_async_copy(buf.at[b, rows], out_ref.at[b, rows], out_sem.at[b, t]) for b, rows, t in places]
    lows = [pltpu.make_async_copy(pk.at[n], low.at[n], low_sem.at[n]) for n in range(2)]
    highs = [pltpu.make_async_copy(qb.at[n], high.at[n], high_sem.at[n]) for n in range(2)]
    stored = []

    def store(src, n, row):
        for h in range(heads):
            for p, ref in ((1, k_ref), (2, v_ref)):
                cols = pl.ds((3 * h + p) * head_dim, head_dim)
                copy = pltpu.make_async_copy(src.at[:, cols], ref.at[row, h], kv_sem.at[n, h, p - 1])
                copy.start()
                stored.append(copy)

    for copy in highs + lows + inward:
        copy.start()
    j = meta[0]
    for n in range(2):
        lows[n].wait()
        store(low.at[n], n, j ^ (2 - 2 * n))
    for n in range(2):
        highs[n].wait()
        for h in range(heads):
            for p in (1, 2):
                cols = slice((3 * h + p) * head_dim, (3 * h + p + 1) * head_dim)
                low[2 + n, :, cols] = high[n, :, cols].astype(BF16)
        store(low.at[2 + n], 2 + n, j ^ (3 - 2 * n))
    for one, other in zip(inward, outward):
        one.wait()
        other.start()
    for copy in outward + stored:
        copy.wait()


def finish(meta, out, pk, qb, heads, head_dim):
    rows, chunk_len, _ = out.shape
    span = pk.shape[2]
    hbm = pl.BlockSpec(memory_space=pl.ANY)
    cache = jax.ShapeDtypeStruct((rows, heads, chunk_len, head_dim), BF16)
    dma = pltpu.SemaphoreType.DMA
    return pl.pallas_call(
        functools.partial(finish_kernel, heads),
        in_specs=[pl.BlockSpec(memory_space=pltpu.SMEM)] + [hbm] * 3,
        out_specs=[hbm] * 3,
        out_shape=[jax.ShapeDtypeStruct(out.shape, out.dtype), cache, cache],
        scratch_shapes=[
            pltpu.VMEM(out.shape, out.dtype), pltpu.VMEM((4, chunk_len, span), BF16), pltpu.VMEM((2, chunk_len, span), F32),
            dma((rows, 4)), dma((rows, 4)), dma((2,)), dma((2,)), dma((4, heads, 2)),
        ],
        compiler_params=pltpu.CompilerParams(vmem_limit_bytes=VMEM_LIMIT),
        name="finish",
    )(meta, out, pk, qb)


def solution(mesh):
    in_specs = (P("dp", None, None), P("dp"), P("dp", "tp", "cp", None), P("dp", "tp", "cp", None), P(), P(), P(), P(), P(None, "tp"), P("tp"), P("tp", None), P(), P(None, "tp"), P("tp"), P("tp", None), P())
    out_specs = (P("dp", None, None), P("dp", "tp", None, None), P("dp", "tp", None, None))
    tp_size = mesh.shape["tp"]

    def local_layer(hidden_in, lengths, k_block, v_block, ln1_gain, ln1_bias, ln2_gain, ln2_bias, w_qkv, b_qkv, w_out, b_out, w_up, b_up, w_down, b_down):
        num_rows, chunk_len, d_model = hidden_in.shape
        heads, block_len, head_dim = k_block.shape[1:]
        table = rope_table(lengths, chunk_len, head_dim)
        norms = [p[None] for p in (ln1_gain, ln1_bias, ln2_gain, ln2_bias)]
        extra = b_out.astype(F32) + b_down.astype(F32)
        out, pk, qb = run_layer(
            lengths, hidden_in, table, k_block, v_block, w_qkv, w_up, w_down, w_out, norms, b_qkv, b_up, extra, tp_size)
        return tuple(finish(lax.axis_index("cp")[None], out, pk, qb, heads, head_dim))

    return jax.shard_map(local_layer, mesh=mesh, in_specs=in_specs, out_specs=out_specs, check_vma=False)
```

```python
import functools
import math

import jax
import jax.numpy as jnp
from jax import lax
from jax.experimental import pallas as pl
from jax.experimental.pallas import tpu as pltpu
from jax.sharding import PartitionSpec as P

EPSILON = 1e-5
NEG_BIG = -1e30
ROTARY_SHARE = 4
ROPE_BASE = 10000.0
LOG2E = math.log2(math.e)
MESH = pl.DeviceIdType.MESH
F32 = jnp.float32
BF16 = jnp.bfloat16
VMEM_LIMIT = 60 * 1024 * 1024
LAYER_LIMIT = 67_043_328
EMPTY = -1e29
CHUNKS = 64
STAGES = 4
BLOCKS = 8
SLICES = 4
TILES = 4
HALVES = 2
LAG_START = 2
LAG_AHEAD = 1
LAG_BACK = 1
LAG_CORE = 2
LAG_Y = 5
LAG_LAST = 6


def layer_norm(values_in, gain_vec, bias_vec):
    x_f32 = values_in.astype(F32)
    row_mean = jnp.mean(x_f32, axis=-1, keepdims=True)
    centered = x_f32 - row_mean
    variance = jnp.mean(centered * centered, axis=-1, keepdims=True)
    return (centered * lax.rsqrt(variance + EPSILON) * gain_vec + bias_vec).astype(BF16)


def rope_table(lengths, chunk_len, head_dim):
    rot_dim = head_dim // ROTARY_SHARE
    half_rot = rot_dim // 2
    positions = lengths[:, None] + jnp.arange(chunk_len, dtype=jnp.int32)[None, :]
    inv_freq = ROPE_BASE ** (-2.0 * jnp.arange(half_rot, dtype=F32) / rot_dim)
    angles = positions.astype(F32)[:, None, :] * inv_freq[:, None]
    cos_tab = jnp.cos(angles)
    sin_tab = jnp.sin(angles)
    return jnp.concatenate([cos_tab, cos_tab, -sin_tab, sin_tab], axis=1)


def wide(column, lanes):
    return jnp.concatenate([column] * (lanes // column.shape[1]), axis=1)


def scores_of(query, keys, scale, mask):
    scores = lax.dot_general(query, keys, (((1,), (1,)), ((), ())), preferred_element_type=F32) * scale
    return scores if mask is None else jnp.where(mask, scores, NEG_BIG)


def lane_sum(values, lanes):
    return functools.reduce(jnp.add, [values[:, n:n + lanes] for n in range(0, values.shape[1], lanes)])


def lane_max(values, lanes):
    return functools.reduce(jnp.maximum, [values[:, n:n + lanes] for n in range(0, values.shape[1], lanes)])


def first_step(heads, scale, q_of, k_of, v_of, m_scr, l_scr, o_scr, mask):
    for h in range(heads):
        lanes = o_scr.shape[2]
        scores = scores_of(q_of(h), k_of(h), scale, mask)
        peak = jnp.maximum(jnp.max(lane_max(scores, lanes), axis=1, keepdims=True), EMPTY)
        peak = jnp.broadcast_to(peak, m_scr.shape[1:])
        probs = jnp.exp2(scores - wide(peak, scores.shape[1]))
        m_scr[h] = peak
        l_scr[h] = lane_sum(probs, lanes)
        o_scr[h] = jnp.dot(probs.astype(BF16), v_of(h), preferred_element_type=F32)


def block_step(heads, scale, q_of, k_of, v_of, m_scr, l_scr, o_scr, mask):
    for h in range(heads):
        lanes = o_scr.shape[2]
        scores = scores_of(q_of(h), k_of(h), scale, mask)
        m_old = m_scr[h]
        m_new = jnp.maximum(m_old, jnp.max(lane_max(scores, lanes), axis=1, keepdims=True))
        probs = jnp.exp2(scores - wide(m_new, scores.shape[1]))
        shrink = jnp.exp2(m_old - m_new)
        l_scr[h] = l_scr[h] * shrink + lane_sum(probs, lanes)
        m_scr[h] = m_new
        o_scr[h] = o_scr[h] * shrink + jnp.dot(probs.astype(BF16), v_of(h), preferred_element_type=F32)


def piece_weights(heads, stats, head_dim):
    peak = functools.reduce(jnp.maximum, [s[:heads] for s in stats])
    weights = [jnp.exp2(s[:heads] - peak) for s in stats]
    total = functools.reduce(jnp.add, [s[heads:2 * heads] * w for s, w in zip(stats, weights)])
    return peak, weights, total


def as_columns(parts, head_dim):
    count = sum(p.shape[0] for p in parts)
    return jnp.concatenate(parts + [jnp.zeros((head_dim - count, parts[0].shape[1]), F32)], axis=0).T


def layer_kernel(tp_size, heads, lengths, hidden, table, k_cache, v_cache, w_qkv, w_up, w_down, w_out,
                 gain1, bias1, gain2, bias2, small,
                 out_ref, y_box, core_box, last_box, pk, qb, ob,
                 acc, from_left, from_right, up, down, proj, x_big, tab_buf, kv, ob_far, m_scr, l_scr, o_scr, st, sbox,
                 stage, land,
                 up_sem, down_sem, proj_sem, xb_sem, tab_sem, pk_sem, kv_sem, q_sem, x_sem, o_sem,
                 qs_sem, qr_sem, fs_sem, fr_sem, ns_sem, nr_sem, ys_sem, yr_sem, ss_sem, sr_sem,
                 left_sem, right_sem, y_sem, core_sem, last_sem, send_sem, stage_sem, land_sem):
    z = lax.axis_index("tp")
    j = lax.axis_index("cp")
    y, c = lax.div(j, 2), lax.rem(j, 2)
    across, mate, corner = (1 - y) * 2 + c, y * 2 + (1 - c), (1 - y) * 2 + (1 - c)
    chunk_len, d_model = acc.shape
    head_dim = o_scr.shape[2]
    span = heads * head_dim
    slots = k_cache.shape[2]
    tokens = chunk_len // CHUNKS
    block = chunk_len // BLOCKS
    half = chunk_len // HALVES
    tile = chunk_len // TILES
    pairs = CHUNKS // 2
    per_block = pairs // BLOCKS
    width = up.shape[2]
    last = tp_size - 1
    root_a, root_b = (tp_size - 1) // 2, tp_size // 2
    rot_dim = head_dim // ROTARY_SHARE
    half_rot = rot_dim // 2
    scale = head_dim ** -0.5 * LOG2E
    own_at, sent_at, kept_at, q_at = 0, span, 2 * span, 3 * span
    extra_at = 3 * span + SLICES * width

    def rows_of(n, size):
        return pl.ds(pl.multiple_of(n * size, size), size)

    def weight_copies(f):
        cols = pl.ds(f * width, width)
        return (pltpu.make_async_copy(w_up.at[:, cols], up.at[f], up_sem.at[f]),
                pltpu.make_async_copy(w_down.at[cols, :], down.at[f], down_sem.at[f]))

    def row_of(n):
        return across * (1 - n) + j * n

    def big_x(i):
        return pltpu.make_async_copy(
            hidden.at[row_of(lax.div(i, TILES)), rows_of(lax.rem(i, TILES), tile), :], x_big.at[lax.rem(i, 2)], xb_sem.at[lax.rem(i, 2)])

    def cache_copies(row, slot):
        return (pltpu.make_async_copy(k_cache.at[row], kv.at[slot, 0], kv_sem.at[slot, 0]),
                pltpu.make_async_copy(v_cache.at[row], kv.at[slot, 1], kv_sem.at[slot, 1]))

    def start(copies):
        for copy in copies:
            copy.start()

    def wait(copies):
        for copy in copies:
            copy.wait()

    qkv_copies = [pltpu.make_async_copy(w_qkv.at[:, pl.ds(s * width, width)], up.at[s], up_sem.at[s]) for s in range(3)]
    tab_copies = [pltpu.make_async_copy(table.at[row], tab_buf.at[n], tab_sem.at[n]) for n, row in enumerate((across, j))]
    proj_copy = pltpu.make_async_copy(w_out, proj, proj_sem)
    big_x(0).start()
    start(qkv_copies)
    start(tab_copies)
    start(cache_copies(corner, 0))
    start(cache_copies(across, 1))
    proj_copy.start()

    barrier = pltpu.get_barrier_semaphore()
    pl.semaphore_signal(barrier, inc=1, device_id={"cp": across}, device_id_type=MESH)
    pl.semaphore_signal(barrier, inc=1, device_id={"cp": mate}, device_id_type=MESH)

    @pl.when(z > 0)
    def _():
        pl.semaphore_signal(barrier, inc=1, device_id={"tp": z - 1}, device_id_type=MESH)

    @pl.when(z < last)
    def _():
        pl.semaphore_signal(barrier, inc=1, device_id={"tp": z + 1}, device_id_type=MESH)

    inside = jnp.logical_and(z > 0, z < last)

    @pl.when(inside)
    def _():
        pl.semaphore_wait(barrier, 4)

    @pl.when(jnp.logical_not(inside))
    def _():
        pl.semaphore_wait(barrier, 3)

    def to_core(src, dst, send, arrive):
        return pltpu.make_async_remote_copy(
            src_ref=src, dst_ref=dst, send_sem=send, recv_sem=arrive, device_id={"cp": mate}, device_id_type=MESH)

    def to_y(src, dst, send, arrive):
        return pltpu.make_async_remote_copy(
            src_ref=src, dst_ref=dst, send_sem=send, recv_sem=arrive, device_id={"cp": across}, device_id_type=MESH)


    def sent_tile(n, t):
        slot = lax.rem(t, 2)
        return to_core(acc.at[rows_of(slot, tile), pl.ds(0, 3 * span)], qb.at[n, rows_of(t, tile), :], qs_sem.at[slot], qr_sem.at[n, t])

    wait(qkv_copies)
    wait(tab_copies)

    @pl.loop(0, 2 * TILES)
    def _(i):
        n, t, slot = lax.div(i, TILES), lax.rem(i, TILES), lax.rem(i, 2)

        @pl.when(i + 1 < 2 * TILES)
        def _():
            big_x(i + 1).start()

        big_x(i).wait()

        @pl.when(i >= 2)
        def _():
            sent_tile(n, t).wait_send()

        normed = layer_norm(x_big[slot], gain1[...], bias1[...])
        tab = tab_buf[n, :, rows_of(t, tile)]
        tab = jnp.concatenate([tab] * (head_dim // tab.shape[0]), axis=0).T
        lane = lax.broadcasted_iota(jnp.int32, tab.shape, 1)
        cos_tab = jnp.where(lane < rot_dim, tab, 1.0)
        sin_tab = jnp.where(lane < rot_dim, pltpu.roll(tab, head_dim - rot_dim, 1), 0.0)

        def rotate(values):
            long = values.astype(F32)
            other = jnp.where(lane < half_rot, pltpu.roll(long, head_dim - half_rot, 1), pltpu.roll(long, half_rot, 1))
            return (long * cos_tab + other * sin_tab).astype(BF16)

        place = down.at[n * HALVES + lax.div(t, TILES // HALVES), rows_of(lax.rem(t, TILES // HALVES), tile), :]
        hold = acc.at[rows_of(slot, tile), :]
        for s in range(3):
            part = slice(s * width, (s + 1) * width)
            some = (jnp.dot(normed, up[s], preferred_element_type=F32) + small[:, part]).astype(BF16)
            for g in range(width // head_dim):
                group = s * (width // head_dim) + g
                values = some[:, g * head_dim:(g + 1) * head_dim]
                if group % 3 < 2:
                    values = rotate(values)
                cols = slice(group * head_dim, (group + 1) * head_dim)
                place[:, cols] = values
                hold[:, cols] = values.astype(F32)
        sent_tile(n, t).start()

    for f in range(SLICES):
        weight_copies(f)[0].start()
    pack_copies = [
        pltpu.make_async_copy(down.at[n * HALVES + e, pl.ds(0, half), pl.ds(0, 3 * span)], pk.at[n, pl.ds(e * half, half), :],
                              pk_sem.at[n, e])
        for n in range(2) for e in range(HALVES)]
    start(pack_copies)
    for t in range(2):
        sent_tile(1, TILES - 2 + t).wait_send()


    def got_queries(n):
        for t in range(TILES):
            sent_tile(n, t).wait_recv()
        copies = [pltpu.make_async_copy(qb.at[n, :, pl.ds(3 * h * head_dim, head_dim)],
                                        acc.at[:, pl.ds(q_at + h * head_dim, head_dim)], q_sem.at[h]) for h in range(heads)]
        start(copies)
        return copies

    def attend(row, slot, query, at, kind, after=None, own=False):
        valid = jnp.clip(lengths[row] - j * slots, 0, slots)

        @pl.loop(0, HALVES)
        def _(e):
            def keys(h):
                return kv[slot, 0, h]

            def values(h):
                return kv[slot, 1, h]

            mask = lax.broadcasted_iota(jnp.int32, (half, slots), 1) < valid
            first_step(heads, scale, lambda h: query(e, h), keys, values, m_scr, l_scr, o_scr, mask)

            def own_block(b, mask):
                def part(p):
                    return lambda h: down[HALVES + b, :half, (3 * h + p) * head_dim:(3 * h + p + 1) * head_dim]

                block_step(heads, scale, lambda h: query(e, h), part(1), part(2), m_scr, l_scr, o_scr, mask)

            if own:
                @pl.loop(0, e)
                def _(b):
                    own_block(b, None)

                shape = (half, half)
                own_block(e, lax.broadcasted_iota(jnp.int32, shape, 0) >= lax.broadcasted_iota(jnp.int32, shape, 1))

            lane = lax.broadcasted_iota(jnp.int32, (half, head_dim), 1)
            stats = jnp.zeros((half, head_dim), F32)
            for h in range(heads):
                stats = jnp.where(lane == h, m_scr[h], stats)
                stats = jnp.where(lane == heads + h, jnp.sum(l_scr[h], axis=1, keepdims=True), stats)
                acc[rows_of(e, half), at + h * head_dim:at + (h + 1) * head_dim] = o_scr[h]
            st[kind, :, rows_of(e, half)] = stats.T[:8]
            if after is not None:
                after(e)

    def held(n):
        return lambda e, h: down[n * HALVES + e, :half, 3 * h * head_dim:(3 * h + 1) * head_dim]

    def taken(e, h):
        return acc[rows_of(e, half), q_at + h * head_dim:q_at + (h + 1) * head_dim].astype(BF16)

    def far_piece(e):
        return to_core(acc.at[rows_of(e, half), pl.ds(sent_at, span)], ob_far.at[rows_of(e, half), :], fs_sem.at[e], fr_sem.at[e])

    def near_piece(e):
        return to_core(acc.at[rows_of(e, half), pl.ds(sent_at, span)], ob.at[0, rows_of(e, half), :], ns_sem.at[e], nr_sem.at[e])

    def y_piece(b):
        return to_y(acc.at[rows_of(b, block), pl.ds(kept_at, span)], ob.at[1, rows_of(b, block), :], ys_sem.at[b], yr_sem.at[b])

    far_stats = to_core(st.at[0], sbox.at[0], ss_sem.at[0], sr_sem.at[0])
    y_stats = to_y(st.at[1], sbox.at[2], ss_sem.at[1], sr_sem.at[2])
    near_stats = to_core(st.at[2], sbox.at[1], ss_sem.at[2], sr_sem.at[1])

    wait(got_queries(0))
    wait(cache_copies(corner, 0))
    attend(corner, 0, taken, sent_at, 0, after=lambda e: far_piece(e).start())
    far_stats.start()
    start(cache_copies(mate, 0))
    near_queries = got_queries(1)
    wait(cache_copies(across, 1))
    attend(across, 1, held(0), kept_at, 1)
    start(cache_copies(j, 1))

    far_stats.wait()
    _, weights, total = piece_weights(heads, [st[1], sbox[0]], head_dim)
    peak = jnp.maximum(st[1, :heads, :], sbox[0, :heads, :])

    st[1, :heads, :] = peak
    st[1, heads:2 * heads, :] = total
    y_stats.start()

    @pl.loop(0, HALVES)
    def _(e):
        far_piece(e).wait_recv()

    for b in range(BLOCKS):
        part = slice(b * block, (b + 1) * block)
        columns = as_columns([w[:, part] for w in weights], head_dim)
        for h in range(heads):
            mine = slice(kept_at + h * head_dim, kept_at + (h + 1) * head_dim)
            acc[part, mine] = (acc[part, mine] * columns[:, h:h + 1]
                               + ob_far[part, h * head_dim:(h + 1) * head_dim] * columns[:, heads + h:heads + h + 1])
        y_piece(b).start()

    for e in range(HALVES):
        far_piece(e).wait_send()
    wait(near_queries)
    wait(cache_copies(mate, 0))
    attend(mate, 0, taken, sent_at, 2, after=lambda e: near_piece(e).start())
    near_stats.start()
    wait(cache_copies(j, 1))
    wait(pack_copies)
    for f in range(HALVES):
        weight_copies(f)[1].start()
    attend(j, 1, held(1), own_at, 3, own=True)
    for f in range(HALVES, SLICES):
        weight_copies(f)[1].start()

    def block_copies(b):
        rows = rows_of(b, block)
        slot = lax.rem(b, 2)
        return [pltpu.make_async_copy(hidden.at[j, rows, :], x_big.at[slot, pl.ds(0, block), :], x_sem.at[slot])] + [
            pltpu.make_async_copy(ob.at[n, rows, :], ob_far.at[rows_of(2 * slot + n, block), :], o_sem.at[slot, n]) for n in range(2)]

    def fetch(b):
        y_piece(b).wait_recv()
        start(block_copies(b))

    near_stats.wait()
    y_stats.wait()
    for e in range(HALVES):
        near_piece(e).wait_recv()
        near_piece(e).wait_send()
    proj_copy.wait()
    fetch(0)


    def begin(b):
        slot = lax.rem(b, 2)
        rows = rows_of(b, block)

        @pl.when(b + 1 < BLOCKS)
        def _():
            fetch(b + 1)

        wait(block_copies(b))
        y_piece(b).wait_send()
        _, weights, total = piece_weights(heads, [st[3, :, rows], sbox[1, :, rows], sbox[2, :, rows]], head_dim)
        columns = as_columns([w / total for w in weights], head_dim)
        for h in range(heads):
            cols = slice(h * head_dim, (h + 1) * head_dim)
            pieces = [acc[rows, own_at + h * head_dim:own_at + (h + 1) * head_dim]]
            pieces += [ob_far[rows_of(2 * slot + n, block), cols] for n in range(2)]
            context = functools.reduce(
                jnp.add, [o * columns[:, n * heads + h:n * heads + h + 1] for n, o in enumerate(pieces)])
            x_big[1, block:2 * block, cols] = context.astype(BF16)
        x = x_big[slot, :block, :]
        x_big[0, block:2 * block, :] = layer_norm(x, gain2[...], bias2[...])
        acc[rows, :] = jnp.dot(x_big[1, block:2 * block, :span], proj[...], preferred_element_type=F32)

        @pl.when(z == 0)
        def _():
            acc[rows, :] += x.astype(F32) + small[:, extra_at:]

    def slice_of(b, f):
        rows = rows_of(b, block)

        @pl.when(b == 0)
        def _():
            wait(weight_copies(f))

        b_up = small[:, pl.ds(pl.multiple_of(3 * span + f * width, width), width)]
        wide_h = jnp.dot(x_big[0, block:2 * block, :], up[f], preferred_element_type=F32) + b_up
        act = (0.5 * wide_h * (1.0 + lax.erf(wide_h * math.sqrt(0.5)))).astype(BF16)
        acc[rows, :] += jnp.dot(act, down[f], preferred_element_type=F32)


    def at(ref, k):
        return ref.at[pl.ds(pl.multiple_of(k * tokens, tokens), tokens), :]

    def remote(src, dst, k, which, arrive, device):
        return pltpu.make_async_remote_copy(
            src_ref=at(src, k), dst_ref=at(dst, k), send_sem=send_sem.at[which], recv_sem=arrive.at[k],
            device_id=device, device_id_type=MESH,
        )

    def send_right(src, k):
        remote(src, from_left, k, 0, left_sem, {"tp": z + 1}).start()

    def send_left(src, k):
        remote(src, from_right, k, 1, right_sem, {"tp": z - 1}).start()

    def arrived(ref, sem, k):
        remote(ref, ref, k, 0, sem, {"cp": j}).wait_recv()

    def drained(ref, which):
        pltpu.make_async_copy(ref, ref, send_sem.at[which]).wait()

    def emit(stream, values, k, row):
        slot = lax.rem(k, STAGES)

        def copy():
            return pltpu.make_async_copy(stage.at[stream, slot], at(out_ref.at[row], k), stage_sem.at[stream, slot])

        @pl.when(k >= STAGES)
        def _():
            copy().wait()

        stage[stream, slot] = values.astype(BF16)
        copy().start()

    def chunk(ref, k):
        return ref[pl.ds(pl.multiple_of(k * tokens, tokens), tokens), :]

    def finish(src, k):
        remote(src, y_box, k, 2, y_sem, {"cp": across}).start()
        remote(src, core_box, k, 3, core_sem, {"cp": mate}).start()
        emit(0, chunk(src, k), k, j)

    def landing(n, box, k):
        slot = lax.rem(k, STAGES)
        return pltpu.make_async_copy(at(box, k), land.at[n, slot], land_sem.at[n, slot])

    def gathered(i):
        def lagged(lag, act):
            @pl.when(jnp.logical_and(i >= lag, i < pairs + lag))
            def _():
                for n in range(2):
                    act((i - lag) * 2 + n)

        def core(k):
            arrived(core_box, core_sem, k)
            landing(0, core_box, k).start()

        def core_out(k):
            landing(0, core_box, k).wait()
            emit(1, land[0, lax.rem(k, STAGES)], k, mate)

        def side(k):
            arrived(y_box, y_sem, k)
            remote(y_box, last_box, k, 4, last_sem, {"cp": mate}).start()
            landing(2, y_box, k).start()

        def side_out(k):
            landing(2, y_box, k).wait()
            emit(2, land[2, lax.rem(k, STAGES)], k, across)

        def final(k):
            arrived(last_box, last_sem, k)
            landing(1, last_box, k).start()

        def final_out(k):
            landing(1, last_box, k).wait()
            emit(3, land[1, lax.rem(k, STAGES)], k, corner)

        lagged(LAG_CORE + 1, core_out)
        lagged(LAG_Y + 1, side_out)
        lagged(LAG_LAST + 1, final_out)
        lagged(LAG_CORE, core)
        lagged(LAG_Y, side)
        lagged(LAG_LAST, final)

    def add(k, *others):
        rows = pl.ds(pl.multiple_of(k * tokens, tokens), tokens)
        total = acc[rows, :]
        for other in others:
            total = total + other[rows, :]
        acc[rows, :] = total

    def when(cond, act, *args):
        @pl.when(cond)
        def _():
            act(*args)

    def end(i, first):
        inbox, sem = (from_right, right_sem) if first else (from_left, left_sem)
        near_bit = 0 if first else 1

        def got(k):
            arrived(inbox, sem, k)
            finish(inbox, k)

        when(jnp.logical_and(i >= 0, i < pairs), lambda: got(2 * i + near_bit))
        when(jnp.logical_and(i >= LAG_BACK, i < pairs + LAG_BACK), lambda: got(2 * (i - LAG_BACK) + 1 - near_bit))

    def inner(i, left_side):
        mine = 0 if left_side else 1
        if left_side:
            (outer, outer_sem, to_outer), (inward, inward_sem, to_inner) = (
                (from_left, left_sem, send_left), (from_right, right_sem, send_right))
        else:
            (outer, outer_sem, to_outer), (inward, inward_sem, to_inner) = (
                (from_right, right_sem, send_right), (from_left, left_sem, send_left))

        def early(p):
            passed = 2 * p + 1 - mine
            arrived(outer, outer_sem, passed)
            add(passed, outer)
            to_inner(acc, passed)

        def near(p):
            rooted = 2 * p + mine
            arrived(outer, outer_sem, rooted)
            arrived(inward, inward_sem, rooted)
            add(rooted, from_left, from_right)
            to_outer(acc, rooted)
            to_inner(acc, rooted)
            finish(acc, rooted)

        def far(p):
            k = 2 * p + 1 - mine
            arrived(inward, inward_sem, k)
            to_outer(inward, k)
            finish(inward, k)

        when(jnp.logical_and(i + LAG_AHEAD >= 0, i + LAG_AHEAD < pairs), early, i + LAG_AHEAD)
        when(jnp.logical_and(i >= 0, i < pairs), near, i)
        when(jnp.logical_and(i >= LAG_BACK, i < pairs + LAG_BACK), far, i - LAG_BACK)

    lead = SLICES + LAG_START

    @pl.loop(0, lead + pairs + LAG_LAST + 2)
    def _(s):
        @pl.when(s < BLOCKS * SLICES)
        def _():
            b, f = lax.div(s, SLICES), lax.rem(s, SLICES)
            when(f == 0, begin, b)
            slice_of(b, f)

            def push(send):
                @pl.loop(0, 2 * per_block)
                def _(n):
                    send(acc, b * 2 * per_block + n)

            when(jnp.logical_and(f == SLICES - 1, z == 0), push, send_right)
            when(jnp.logical_and(f == SLICES - 1, z == last), push, send_left)

        i = s - lead
        when(z == 0, end, i, True)
        when(z == root_a, inner, i, True)
        when(z == root_b, inner, i, False)
        when(z == last, end, i, False)
        gathered(i)

    @pl.when(z < last)
    def _():
        drained(acc, 0)

    @pl.when(z > 0)
    def _():
        drained(acc, 1)

    for which in (2, 3, 4):
        drained(acc, which)
    for stream in range(4):
        for slot in range(STAGES):
            pltpu.make_async_copy(stage.at[stream, slot], at(out_ref.at[0], 0), stage_sem.at[stream, slot]).wait()


def run_layer(lengths, hidden_in, table, k_block, v_block, w_qkv, w_up, w_down, w_out, norms, small, tp_size):
    num_rows, chunk_len, d_model = hidden_in.shape
    heads, slots, head_dim = k_block.shape[1:]
    span = heads * head_dim
    width = w_up.shape[1] // SLICES
    tokens = chunk_len // CHUNKS
    block = chunk_len // BLOCKS
    half = chunk_len // HALVES
    tile = chunk_len // TILES
    dma = pltpu.SemaphoreType.DMA
    buffer = pltpu.VMEM((chunk_len, d_model), F32)
    box = jax.ShapeDtypeStruct((chunk_len, d_model), F32)
    hbm = pl.BlockSpec(memory_space=pl.ANY)
    vmem = pl.BlockSpec(memory_space=pltpu.VMEM)
    out, _, _, _, pk, qb, _ = pl.pallas_call(
        functools.partial(layer_kernel, tp_size, heads),
        in_specs=[pl.BlockSpec(memory_space=pltpu.SMEM)] + [hbm] * 8 + [vmem] * 5,
        out_specs=[hbm] * 7,
        out_shape=[
            jax.ShapeDtypeStruct((num_rows, chunk_len, d_model), BF16), box, box, box,
            jax.ShapeDtypeStruct((2, chunk_len, 3 * span), BF16),
            jax.ShapeDtypeStruct((2, chunk_len, 3 * span), F32),
            jax.ShapeDtypeStruct((2, chunk_len, span), F32),
        ],
        scratch_shapes=[buffer] * 3
        + [
            pltpu.VMEM((SLICES, d_model, width), BF16),
            pltpu.VMEM((SLICES, width, d_model), BF16),
            pltpu.VMEM((span, d_model), BF16),
            pltpu.VMEM((2, tile, d_model), BF16),
            pltpu.VMEM((2,) + table.shape[1:], F32),
            pltpu.VMEM((2, 2, heads, slots, head_dim), BF16),
            pltpu.VMEM((chunk_len, span), F32),
            pltpu.VMEM((heads, half, head_dim), F32),
            pltpu.VMEM((heads, half, head_dim), F32),
            pltpu.VMEM((heads, half, head_dim), F32),
            pltpu.VMEM((4, 8, chunk_len), F32),
            pltpu.VMEM((3, 8, chunk_len), F32),
            pltpu.VMEM((4, STAGES, tokens, d_model), BF16),
            pltpu.VMEM((3, STAGES, tokens, d_model), F32),
        ]
        + [dma((SLICES,)), dma((SLICES,)), dma, dma((2,)), dma((2,)), dma((2, HALVES)), dma((2, 2)), dma((heads,)), dma((2,)), dma((2, 2))]
        + [dma((2,)), dma((2, TILES)), dma((HALVES,)), dma((HALVES,)), dma((HALVES,)), dma((HALVES,)), dma((BLOCKS,)), dma((BLOCKS,)),
           dma((3,)), dma((3,))]
        + [dma((CHUNKS,))] * 5
        + [dma((5,)), dma((4, STAGES)), dma((3, STAGES))],
        compiler_params=pltpu.CompilerParams(collective_id=0, has_side_effects=True, vmem_limit_bytes=LAYER_LIMIT),
        cost_estimate=pl.CostEstimate(flops=100_000_000_000, bytes_accessed=chunk_len * d_model * 16, transcendentals=0),
        name="layer",
    )(lengths, hidden_in, table, k_block, v_block, w_qkv, w_up, w_down, w_out, *norms, small[None])
    return out, pk, qb


def finish_kernel(heads, meta, in_ref, pk, qb, out_ref, k_ref, v_ref, buf, low, high, in_sem, out_sem, low_sem, high_sem, kv_sem):
    pieces = in_sem.shape[1]
    tile = buf.shape[1] // pieces
    head_dim = k_ref.shape[3]
    places = [(b, pl.ds(t * tile, tile), t) for b in range(buf.shape[0]) for t in range(pieces)]
    inward = [pltpu.make_async_copy(in_ref.at[b, rows], buf.at[b, rows], in_sem.at[b, t]) for b, rows, t in places]
    outward = [pltpu.make_async_copy(buf.at[b, rows], out_ref.at[b, rows], out_sem.at[b, t]) for b, rows, t in places]
    both = 2 * head_dim

    def taken(src, dst, sem):
        return [[pltpu.make_async_copy(src.at[n, :, pl.ds((3 * h + 1) * head_dim, both)], dst.at[n, :, pl.ds(h * both, both)], sem.at[n, h])
                 for h in range(heads)] for n in range(2)]

    lows, highs = taken(pk, low, low_sem), taken(qb, high, high_sem)
    stored = []

    def store(n, h, row):
        for p, ref in enumerate((k_ref, v_ref)):
            cols = pl.ds(h * both + p * head_dim, head_dim)
            copy = pltpu.make_async_copy(low.at[n, :, cols], ref.at[row, h], kv_sem.at[n, h, p])
            copy.start()
            stored.append(copy)

    for copy in highs[0] + highs[1] + lows[0] + lows[1] + inward:
        copy.start()
    j = meta[0]
    for n in range(2):
        for h in range(heads):
            lows[n][h].wait()
            store(n, h, j ^ (2 - 2 * n))
    for n in range(2):
        for h in range(heads):
            highs[n][h].wait()
            cols = slice(h * both, (h + 1) * both)
            low[2 + n, :, cols] = high[n, :, cols].astype(BF16)
            store(2 + n, h, j ^ (3 - 2 * n))
    for one, other in zip(inward, outward):
        one.wait()
        other.start()
    for copy in outward + stored:
        copy.wait()


def finish(meta, out, pk, qb, heads, head_dim):
    rows, chunk_len, _ = out.shape
    span = 2 * heads * head_dim
    hbm = pl.BlockSpec(memory_space=pl.ANY)
    cache = jax.ShapeDtypeStruct((rows, heads, chunk_len, head_dim), BF16)
    dma = pltpu.SemaphoreType.DMA
    return pl.pallas_call(
        functools.partial(finish_kernel, heads),
        in_specs=[pl.BlockSpec(memory_space=pltpu.SMEM)] + [hbm] * 3,
        out_specs=[hbm] * 3,
        out_shape=[jax.ShapeDtypeStruct(out.shape, out.dtype), cache, cache],
        scratch_shapes=[
            pltpu.VMEM(out.shape, out.dtype), pltpu.VMEM((4, chunk_len, span), BF16), pltpu.VMEM((2, chunk_len, span), F32),
            dma((rows, 4)), dma((rows, 4)), dma((2, heads)), dma((2, heads)), dma((4, heads, 2)),
        ],
        compiler_params=pltpu.CompilerParams(vmem_limit_bytes=VMEM_LIMIT),
        name="finish",
    )(meta, out, pk, qb)


def solution(mesh):
    in_specs = (P("dp", None, None), P("dp"), P("dp", "tp", "cp", None), P("dp", "tp", "cp", None), P(), P(), P(), P(), P(None, "tp"), P("tp"), P("tp", None), P(), P(None, "tp"), P("tp"), P("tp", None), P())
    out_specs = (P("dp", None, None), P("dp", "tp", None, None), P("dp", "tp", None, None))
    tp_size = mesh.shape["tp"]

    def local_layer(hidden_in, lengths, k_block, v_block, ln1_gain, ln1_bias, ln2_gain, ln2_bias, w_qkv, b_qkv, w_out, b_out, w_up, b_up, w_down, b_down):
        num_rows, chunk_len, d_model = hidden_in.shape
        heads, block_len, head_dim = k_block.shape[1:]
        table = rope_table(lengths, chunk_len, head_dim)
        norms = [p[None] for p in (ln1_gain, ln1_bias, ln2_gain, ln2_bias)]
        small = jnp.concatenate([b_qkv.astype(F32), b_up.astype(F32), b_out.astype(F32) + b_down.astype(F32)])
        out, pk, qb = run_layer(lengths, hidden_in, table, k_block, v_block, w_qkv, w_up, w_down, w_out, norms, small, tp_size)
        return tuple(finish(lax.axis_index("cp")[None], out, pk, qb, heads, head_dim))

    return jax.shard_map(local_layer, mesh=mesh, in_specs=in_specs, out_specs=out_specs, check_vma=False)
```

```python
import functools
import math

import jax
import jax.numpy as jnp
from jax import lax
from jax.experimental import pallas as pl
from jax.experimental.pallas import tpu as pltpu
from jax.sharding import PartitionSpec as P

EPSILON = 1e-5
NEG_BIG = -1e30
ROTARY_SHARE = 4
ROPE_BASE = 10000.0
LOG2E = math.log2(math.e)
MESH = pl.DeviceIdType.MESH
F32 = jnp.float32
BF16 = jnp.bfloat16
VMEM_LIMIT = 60 * 1024 * 1024
LAYER_LIMIT = 67_043_328
EMPTY = -1e29
CHUNKS = 64
STAGES = 4
BLOCKS = 8
SLICES = 4
TILES = 4
HALVES = 4
LAG_START = 2
LAG_AHEAD = 1
LAG_BACK = 1
LAG_CORE = 2
LAG_Y = 5
LAG_LAST = 6


def layer_norm(values_in, gain_vec, bias_vec):
    x_f32 = values_in.astype(F32)
    row_mean = jnp.mean(x_f32, axis=-1, keepdims=True)
    centered = x_f32 - row_mean
    variance = jnp.mean(centered * centered, axis=-1, keepdims=True)
    return (centered * lax.rsqrt(variance + EPSILON) * gain_vec + bias_vec).astype(BF16)


def rope_table(lengths, chunk_len, head_dim):
    rot_dim = head_dim // ROTARY_SHARE
    half_rot = rot_dim // 2
    positions = lengths[:, None] + jnp.arange(chunk_len, dtype=jnp.int32)[None, :]
    inv_freq = ROPE_BASE ** (-2.0 * jnp.arange(half_rot, dtype=F32) / rot_dim)
    angles = positions.astype(F32)[:, None, :] * inv_freq[:, None]
    cos_tab = jnp.cos(angles)
    sin_tab = jnp.sin(angles)
    return jnp.concatenate([cos_tab, cos_tab, -sin_tab, sin_tab], axis=1)


def wide(column, lanes):
    return jnp.concatenate([column] * (lanes // column.shape[1]), axis=1)


def scores_of(query, keys, scale, mask):
    scores = lax.dot_general(query, keys, (((1,), (1,)), ((), ())), preferred_element_type=F32) * scale
    return scores if mask is None else jnp.where(mask, scores, NEG_BIG)


def lane_sum(values, lanes):
    return functools.reduce(jnp.add, [values[:, n:n + lanes] for n in range(0, values.shape[1], lanes)])


def lane_max(values, lanes):
    return functools.reduce(jnp.maximum, [values[:, n:n + lanes] for n in range(0, values.shape[1], lanes)])


def first_step(heads, scale, q_of, k_of, v_of, m_scr, l_scr, o_scr, mask):
    for h in range(heads):
        lanes = o_scr.shape[2]
        scores = scores_of(q_of(h), k_of(h), scale, mask)
        peak = jnp.maximum(jnp.max(lane_max(scores, lanes), axis=1, keepdims=True), EMPTY)
        peak = jnp.broadcast_to(peak, m_scr.shape[1:])
        probs = jnp.exp2(scores - wide(peak, scores.shape[1]))
        m_scr[h] = peak
        l_scr[h] = lane_sum(probs, lanes)
        o_scr[h] = jnp.dot(probs.astype(BF16), v_of(h), preferred_element_type=F32)


def block_step(heads, scale, q_of, k_of, v_of, m_scr, l_scr, o_scr, mask):
    for h in range(heads):
        lanes = o_scr.shape[2]
        scores = scores_of(q_of(h), k_of(h), scale, mask)
        m_old = m_scr[h]
        m_new = jnp.maximum(m_old, jnp.max(lane_max(scores, lanes), axis=1, keepdims=True))
        probs = jnp.exp2(scores - wide(m_new, scores.shape[1]))
        shrink = jnp.exp2(m_old - m_new)
        l_scr[h] = l_scr[h] * shrink + lane_sum(probs, lanes)
        m_scr[h] = m_new
        o_scr[h] = o_scr[h] * shrink + jnp.dot(probs.astype(BF16), v_of(h), preferred_element_type=F32)


def piece_weights(heads, stats, head_dim):
    peak = functools.reduce(jnp.maximum, [s[:heads] for s in stats])
    weights = [jnp.exp2(s[:heads] - peak) for s in stats]
    total = functools.reduce(jnp.add, [s[heads:2 * heads] * w for s, w in zip(stats, weights)])
    return peak, weights, total


def as_columns(parts, head_dim):
    count = sum(p.shape[0] for p in parts)
    return jnp.concatenate(parts + [jnp.zeros((head_dim - count, parts[0].shape[1]), F32)], axis=0).T


def layer_kernel(tp_size, heads, lengths, hidden, table, k_cache, v_cache, w_qkv, w_up, w_down, w_out,
                 gain1, bias1, gain2, bias2, small,
                 out_ref, y_box, core_box, last_box, pk, qb, ob,
                 acc, from_left, from_right, up, down, proj, mine, x_big, tab_buf, kv, ob_far, m_scr, l_scr, o_scr, st, sbox,
                 stage, land,
                 up_sem, down_sem, proj_sem, xb_sem, tab_sem, pk_sem, mine_sem, kv_sem, q_sem, x_sem, o_sem,
                 qs_sem, qr_sem, fs_sem, fr_sem, ns_sem, nr_sem, ys_sem, yr_sem,
                 fss_sem, fsr_sem, nss_sem, nsr_sem, yss_sem, ysr_sem,
                 left_sem, right_sem, y_sem, core_sem, last_sem, send_sem, stage_sem, land_sem):
    z = lax.axis_index("tp")
    j = lax.axis_index("cp")
    y, c = lax.div(j, 2), lax.rem(j, 2)
    across, mate, corner = (1 - y) * 2 + c, y * 2 + (1 - c), (1 - y) * 2 + (1 - c)
    chunk_len, d_model = acc.shape
    head_dim = o_scr.shape[2]
    span = heads * head_dim
    slots = k_cache.shape[2]
    tokens = chunk_len // CHUNKS
    block = chunk_len // BLOCKS
    half = chunk_len // HALVES
    tile = chunk_len // TILES
    pairs = CHUNKS // 2
    per_block = pairs // BLOCKS
    width = up.shape[2]
    last = tp_size - 1
    root_a, root_b = (tp_size - 1) // 2, tp_size // 2
    rot_dim = head_dim // ROTARY_SHARE
    half_rot = rot_dim // 2
    scale = head_dim ** -0.5 * LOG2E
    own_at, sent_at, kept_at, q_at = 0, span, 2 * span, 3 * span
    extra_at = 3 * span + SLICES * width
    per_half = BLOCKS // HALVES
    waited = per_half * SLICES

    def rows_of(n, size):
        return pl.ds(pl.multiple_of(n * size, size), size)

    def weight_copies(f):
        cols = pl.ds(f * width, width)
        return (pltpu.make_async_copy(w_up.at[:, cols], up.at[f], up_sem.at[f]),
                pltpu.make_async_copy(w_down.at[cols, :], down.at[f], down_sem.at[f]))

    def row_of(n):
        return across * (1 - n) + j * n

    def big_x(i):
        return pltpu.make_async_copy(
            hidden.at[row_of(lax.div(i, TILES)), rows_of(lax.rem(i, TILES), tile), :], x_big.at[lax.rem(i, 2)], xb_sem.at[lax.rem(i, 2)])

    def cache_copies(row, slot):
        return (pltpu.make_async_copy(k_cache.at[row], kv.at[slot, 0], kv_sem.at[slot, 0]),
                pltpu.make_async_copy(v_cache.at[row], kv.at[slot, 1], kv_sem.at[slot, 1]))

    def start(copies):
        for copy in copies:
            copy.start()

    def wait(copies):
        for copy in copies:
            copy.wait()

    qkv_copies = [pltpu.make_async_copy(w_qkv.at[:, pl.ds(s * width, width)], up.at[s], up_sem.at[s]) for s in range(3)]
    tab_copies = [pltpu.make_async_copy(table.at[row], tab_buf.at[n], tab_sem.at[n]) for n, row in enumerate((across, j))]
    proj_copy = pltpu.make_async_copy(w_out, proj, proj_sem)
    big_x(0).start()
    start(qkv_copies)
    start(tab_copies)
    start(cache_copies(corner, 0))
    start(cache_copies(across, 1))
    proj_copy.start()

    barrier = pltpu.get_barrier_semaphore()
    pl.semaphore_signal(barrier, inc=1, device_id={"cp": across}, device_id_type=MESH)
    pl.semaphore_signal(barrier, inc=1, device_id={"cp": mate}, device_id_type=MESH)

    @pl.when(z > 0)
    def _():
        pl.semaphore_signal(barrier, inc=1, device_id={"tp": z - 1}, device_id_type=MESH)

    @pl.when(z < last)
    def _():
        pl.semaphore_signal(barrier, inc=1, device_id={"tp": z + 1}, device_id_type=MESH)

    inside = jnp.logical_and(z > 0, z < last)

    @pl.when(inside)
    def _():
        pl.semaphore_wait(barrier, 4)

    @pl.when(jnp.logical_not(inside))
    def _():
        pl.semaphore_wait(barrier, 3)

    def to_core(src, dst, send, arrive):
        return pltpu.make_async_remote_copy(
            src_ref=src, dst_ref=dst, send_sem=send, recv_sem=arrive, device_id={"cp": mate}, device_id_type=MESH)

    def to_y(src, dst, send, arrive):
        return pltpu.make_async_remote_copy(
            src_ref=src, dst_ref=dst, send_sem=send, recv_sem=arrive, device_id={"cp": across}, device_id_type=MESH)


    def staged(t, part):
        return acc.at[rows_of(t, tile), pl.ds(part * span, span)]

    def sent_tile(n, t):
        return [to_core(staged(t, p), qb.at[n, rows_of(t, tile), pl.ds(p * span, span)], qs_sem.at[n, t, p], qr_sem.at[n, t, p])
                for p in range(3)]

    def sent_off(n, t):
        for copy in sent_tile(n, t):
            copy.wait_send()

    def project(n, t, place):
        i = n * TILES + t

        @pl.when(i + 1 < 2 * TILES)
        def _():
            big_x(i + 1).start()

        big_x(i).wait()
        if n == 1:
            sent_off(0, t)
        normed = layer_norm(x_big[lax.rem(i, 2)], gain1[...], bias1[...])
        tab = tab_buf[n, :, rows_of(t, tile)]
        tab = jnp.concatenate([tab] * (head_dim // tab.shape[0]), axis=0).T
        lane = lax.broadcasted_iota(jnp.int32, tab.shape, 1)
        cos_tab = jnp.where(lane < rot_dim, tab, 1.0)
        sin_tab = jnp.where(lane < rot_dim, pltpu.roll(tab, head_dim - rot_dim, 1), 0.0)

        def rotate(values):
            long = values.astype(F32)
            other = jnp.where(lane < half_rot, pltpu.roll(long, head_dim - half_rot, 1), pltpu.roll(long, half_rot, 1))
            return (long * cos_tab + other * sin_tab).astype(BF16)

        for p in range(3):
            part = slice(p * span, (p + 1) * span)
            some = (jnp.dot(normed, up[p], preferred_element_type=F32) + small[:, part]).astype(BF16)
            for g in range(heads):
                group = p * heads + g
                values = some[:, g * head_dim:(g + 1) * head_dim]
                if group % 3 < 2:
                    values = rotate(values)
                place[:, group * head_dim:(group + 1) * head_dim] = values
                staged(t, p)[:, g * head_dim:(g + 1) * head_dim] = values.astype(F32)
        start(sent_tile(n, t))

    per_slice = width // tile

    def far_place(t):
        return down.at[lax.div(t, per_slice), rows_of(lax.rem(t, per_slice), tile), pl.ds(0, 3 * span)]

    def mine_out(t):
        return pltpu.make_async_copy(mine.at[t], pk.at[1, rows_of(t, tile), :], mine_sem.at[t])

    wait(qkv_copies)
    wait(tab_copies)

    @pl.loop(0, TILES)
    def _(t):
        project(0, t, far_place(t))

    pack_copies = [pltpu.make_async_copy(far_place(t), pk.at[0, rows_of(t, tile), :], pk_sem.at[t]) for t in range(TILES)]
    start(pack_copies)

    @pl.loop(0, TILES)
    def _(t):
        project(1, t, mine.at[t])
        mine_out(t).start()

    for f in range(SLICES):
        weight_copies(f)[0].start()


    def got_queries(n):
        for t in range(TILES):
            for copy in sent_tile(n, t):
                copy.wait_recv()
        copies = [pltpu.make_async_copy(qb.at[n, :, pl.ds(3 * h * head_dim, head_dim)],
                                        acc.at[:, pl.ds(q_at + h * head_dim, head_dim)], q_sem.at[h]) for h in range(heads)]
        start(copies)
        return copies

    def attend(row, slot, query, e):
        valid = jnp.clip(lengths[row] - j * slots, 0, slots)
        mask = lax.broadcasted_iota(jnp.int32, (half, slots), 1) < valid
        first_step(heads, scale, lambda h: query(e, h), lambda h: kv[slot, 0, h], lambda h: kv[slot, 1, h],
                   m_scr, l_scr, o_scr, mask)

    def attend_own(e):
        def own_block(b, mask):
            def part(p):
                return lambda h: mine[b, :, (3 * h + p) * head_dim:(3 * h + p + 1) * head_dim]

            block_step(heads, scale, lambda h: held_mine(e, h), part(1), part(2), m_scr, l_scr, o_scr, mask)

        @pl.loop(0, e)
        def _(b):
            own_block(b, None)

        shape = (half, half)
        own_block(e, lax.broadcasted_iota(jnp.int32, shape, 0) >= lax.broadcasted_iota(jnp.int32, shape, 1))

    def keep(e, at, kind):
        lane = lax.broadcasted_iota(jnp.int32, (half, head_dim), 1)
        stats = jnp.zeros((half, head_dim), F32)
        for h in range(heads):
            stats = jnp.where(lane == h, m_scr[h], stats)
            stats = jnp.where(lane == heads + h, jnp.sum(l_scr[h], axis=1, keepdims=True), stats)
            acc[rows_of(e, half), at + h * head_dim:at + (h + 1) * head_dim] = o_scr[h]
        st[kind, :, rows_of(e, half)] = stats.T[:8]

    def held_far(e, h):
        return far_place(e)[:, 3 * h * head_dim:(3 * h + 1) * head_dim]

    def held_mine(e, h):
        return mine[e, :, 3 * h * head_dim:(3 * h + 1) * head_dim]

    def taken(e, h):
        return acc[rows_of(e, half), q_at + h * head_dim:q_at + (h + 1) * head_dim].astype(BF16)

    def far_piece(e):
        return to_core(acc.at[rows_of(e, half), pl.ds(sent_at, span)], ob_far.at[rows_of(e, half), :], fs_sem.at[e], fr_sem.at[e])

    def near_piece(e):
        return to_core(acc.at[rows_of(e, half), pl.ds(sent_at, span)], ob.at[0, rows_of(e, half), :], ns_sem.at[e], nr_sem.at[e])

    def y_piece(e):
        return to_y(acc.at[rows_of(e, half), pl.ds(kept_at, span)], ob.at[1, rows_of(e, half), :], ys_sem.at[e], yr_sem.at[e])

    def far_stats(e):
        return to_core(st.at[0, :, rows_of(e, half)], sbox.at[0, :, rows_of(e, half)], fss_sem.at[e], fsr_sem.at[e])

    def near_stats(e):
        return to_core(st.at[2, :, rows_of(e, half)], sbox.at[1, :, rows_of(e, half)], nss_sem.at[e], nsr_sem.at[e])

    def y_stats(e):
        return to_y(st.at[1, :, rows_of(e, half)], sbox.at[2, :, rows_of(e, half)], yss_sem.at[e], ysr_sem.at[e])

    wait(got_queries(0))
    wait(cache_copies(corner, 0))

    @pl.loop(0, HALVES)
    def _(e):
        sent_off(1, e)
        attend(corner, 0, taken, e)
        keep(e, sent_at, 0)
        far_stats(e).start()
        far_piece(e).start()

    start(cache_copies(mate, 0))
    near_queries = got_queries(1)
    wait(cache_copies(across, 1))

    @pl.loop(0, HALVES)
    def _(e):
        attend(across, 1, held_far, e)
        keep(e, kept_at, 1)

        far_stats(e).wait_recv()
        far_piece(e).wait_recv()
        rows = rows_of(e, half)
        peak, weights, total = piece_weights(heads, [st[1, :, rows], sbox[0, :, rows]], head_dim)
        columns = as_columns(weights, head_dim)
        for h in range(heads):
            at = kept_at + h * head_dim
            acc[rows, at:at + head_dim] = (acc[rows, at:at + head_dim] * columns[:, h:h + 1]
                                           + ob_far[rows, h * head_dim:(h + 1) * head_dim] * columns[:, heads + h:heads + h + 1])
        st[1, :heads, rows] = peak
        st[1, heads:2 * heads, rows] = total
        y_stats(e).start()
        y_piece(e).start()

    start(cache_copies(j, 1))
    wait(pack_copies)
    for f in range(SLICES):
        weight_copies(f)[1].start()
    for e in range(HALVES):
        far_stats(e).wait_send()
        far_piece(e).wait_send()
    wait(near_queries)
    wait(cache_copies(mate, 0))
    wait(cache_copies(j, 1))
    proj_copy.wait()


    def near(e, phase):
        @pl.when(phase == 2)
        def _():
            attend(mate, 0, taken, e)
            keep(e, sent_at, 2)
            near_stats(e).start()
            near_piece(e).start()

        @pl.when(phase == 4)
        def _():
            attend(j, 1, held_mine, e)

        @pl.when(phase == 5)
        def _():
            attend_own(e)
            keep(e, own_at, 3)

    def block_copies(b):
        rows = rows_of(b, block)
        slot = lax.rem(b, 2)
        return [pltpu.make_async_copy(hidden.at[j, rows, :], x_big.at[slot, pl.ds(0, block), :], x_sem.at[slot])] + [
            pltpu.make_async_copy(ob.at[n, rows, :], ob_far.at[rows_of(2 * slot + n, block), :], o_sem.at[slot, n]) for n in range(2)]

    def fetch(b):
        @pl.when(lax.rem(b, per_half) == 0)
        def _():
            e = lax.div(b, per_half)
            near_stats(e).wait_recv()
            near_piece(e).wait_recv()
            y_stats(e).wait_recv()
            y_piece(e).wait_recv()

        start(block_copies(b))

    def begin(b):
        slot = lax.rem(b, 2)
        rows = rows_of(b, block)

        @pl.when(b + 1 < BLOCKS)
        def _():
            fetch(b + 1)

        wait(block_copies(b))

        @pl.when(lax.rem(b, per_half) == 0)
        def _():
            e = lax.div(b, per_half)
            for copy in (near_stats(e), near_piece(e), y_stats(e), y_piece(e)):
                copy.wait_send()

        _, weights, total = piece_weights(heads, [st[3, :, rows], sbox[1, :, rows], sbox[2, :, rows]], head_dim)
        columns = as_columns([w / total for w in weights], head_dim)
        for h in range(heads):
            cols = slice(h * head_dim, (h + 1) * head_dim)
            pieces = [acc[rows, own_at + h * head_dim:own_at + (h + 1) * head_dim]]
            pieces += [ob_far[rows_of(2 * slot + n, block), cols] for n in range(2)]
            context = functools.reduce(
                jnp.add, [o * columns[:, n * heads + h:n * heads + h + 1] for n, o in enumerate(pieces)])
            x_big[1, block:2 * block, cols] = context.astype(BF16)
        x = x_big[slot, :block, :]
        x_big[0, block:2 * block, :] = layer_norm(x, gain2[...], bias2[...])
        acc[rows, :] = jnp.dot(x_big[1, block:2 * block, :span], proj[...], preferred_element_type=F32)

        @pl.when(z == 0)
        def _():
            acc[rows, :] += x.astype(F32) + small[:, extra_at:]

    def slice_of(b, f):
        rows = rows_of(b, block)

        @pl.when(b == 0)
        def _():
            wait(weight_copies(f))

        b_up = small[:, pl.ds(pl.multiple_of(3 * span + f * width, width), width)]
        wide_h = jnp.dot(x_big[0, block:2 * block, :], up[f], preferred_element_type=F32) + b_up
        act = (0.5 * wide_h * (1.0 + lax.erf(wide_h * math.sqrt(0.5)))).astype(BF16)
        acc[rows, :] += jnp.dot(act, down[f], preferred_element_type=F32)


    def at(ref, k):
        return ref.at[pl.ds(pl.multiple_of(k * tokens, tokens), tokens), :]

    def remote(src, dst, k, which, arrive, device):
        return pltpu.make_async_remote_copy(
            src_ref=at(src, k), dst_ref=at(dst, k), send_sem=send_sem.at[which], recv_sem=arrive.at[k],
            device_id=device, device_id_type=MESH,
        )

    def send_right(src, k):
        remote(src, from_left, k, 0, left_sem, {"tp": z + 1}).start()

    def send_left(src, k):
        remote(src, from_right, k, 1, right_sem, {"tp": z - 1}).start()

    def arrived(ref, sem, k):
        remote(ref, ref, k, 0, sem, {"cp": j}).wait_recv()

    def drained(ref, which):
        pltpu.make_async_copy(ref, ref, send_sem.at[which]).wait()

    def emit(stream, values, k, row):
        slot = lax.rem(k, STAGES)

        def copy():
            return pltpu.make_async_copy(stage.at[stream, slot], at(out_ref.at[row], k), stage_sem.at[stream, slot])

        @pl.when(k >= STAGES)
        def _():
            copy().wait()

        stage[stream, slot] = values.astype(BF16)
        copy().start()

    def chunk(ref, k):
        return ref[pl.ds(pl.multiple_of(k * tokens, tokens), tokens), :]

    def finish(src, k):
        remote(src, y_box, k, 2, y_sem, {"cp": across}).start()
        remote(src, core_box, k, 3, core_sem, {"cp": mate}).start()
        emit(0, chunk(src, k), k, j)

    def landing(n, box, k):
        slot = lax.rem(k, STAGES)
        return pltpu.make_async_copy(at(box, k), land.at[n, slot], land_sem.at[n, slot])

    def gathered(i):
        def lagged(lag, act):
            @pl.when(jnp.logical_and(i >= lag, i < pairs + lag))
            def _():
                for n in range(2):
                    act((i - lag) * 2 + n)

        def core(k):
            arrived(core_box, core_sem, k)
            landing(0, core_box, k).start()

        def core_out(k):
            landing(0, core_box, k).wait()
            emit(1, land[0, lax.rem(k, STAGES)], k, mate)

        def side(k):
            arrived(y_box, y_sem, k)
            remote(y_box, last_box, k, 4, last_sem, {"cp": mate}).start()
            landing(2, y_box, k).start()

        def side_out(k):
            landing(2, y_box, k).wait()
            emit(2, land[2, lax.rem(k, STAGES)], k, across)

        def final(k):
            arrived(last_box, last_sem, k)
            landing(1, last_box, k).start()

        def final_out(k):
            landing(1, last_box, k).wait()
            emit(3, land[1, lax.rem(k, STAGES)], k, corner)

        lagged(LAG_CORE + 1, core_out)
        lagged(LAG_Y + 1, side_out)
        lagged(LAG_LAST + 1, final_out)
        lagged(LAG_CORE, core)
        lagged(LAG_Y, side)
        lagged(LAG_LAST, final)

    def add(k, *others):
        rows = pl.ds(pl.multiple_of(k * tokens, tokens), tokens)
        total = acc[rows, :]
        for other in others:
            total = total + other[rows, :]
        acc[rows, :] = total

    def when(cond, act, *args):
        @pl.when(cond)
        def _():
            act(*args)

    def end(i, first):
        inbox, sem = (from_right, right_sem) if first else (from_left, left_sem)
        near_bit = 0 if first else 1

        def got(k):
            arrived(inbox, sem, k)
            finish(inbox, k)

        when(jnp.logical_and(i >= 0, i < pairs), lambda: got(2 * i + near_bit))
        when(jnp.logical_and(i >= LAG_BACK, i < pairs + LAG_BACK), lambda: got(2 * (i - LAG_BACK) + 1 - near_bit))

    def inner(i, left_side):
        mine = 0 if left_side else 1
        if left_side:
            (outer, outer_sem, to_outer), (inward, inward_sem, to_inner) = (
                (from_left, left_sem, send_left), (from_right, right_sem, send_right))
        else:
            (outer, outer_sem, to_outer), (inward, inward_sem, to_inner) = (
                (from_right, right_sem, send_right), (from_left, left_sem, send_left))

        def early(p):
            passed = 2 * p + 1 - mine
            arrived(outer, outer_sem, passed)
            add(passed, outer)
            to_inner(acc, passed)

        def near(p):
            rooted = 2 * p + mine
            arrived(outer, outer_sem, rooted)
            arrived(inward, inward_sem, rooted)
            add(rooted, from_left, from_right)
            to_outer(acc, rooted)
            to_inner(acc, rooted)
            finish(acc, rooted)

        def far(p):
            k = 2 * p + 1 - mine
            arrived(inward, inward_sem, k)
            to_outer(inward, k)
            finish(inward, k)

        when(jnp.logical_and(i + LAG_AHEAD >= 0, i + LAG_AHEAD < pairs), early, i + LAG_AHEAD)
        when(jnp.logical_and(i >= 0, i < pairs), near, i)
        when(jnp.logical_and(i >= LAG_BACK, i < pairs + LAG_BACK), far, i - LAG_BACK)

    lead = SLICES + LAG_START

    @pl.loop(0, waited + lead + pairs + LAG_LAST + 2)
    def _(step):
        s = step - waited

        @pl.when(step < HALVES * waited)
        def _():
            near(lax.div(step, waited), lax.rem(step, waited))

        @pl.when(step == waited - 1)
        def _():
            fetch(0)

        @pl.when(jnp.logical_and(s >= 0, s < BLOCKS * SLICES))
        def _():
            b, f = lax.div(s, SLICES), lax.rem(s, SLICES)
            when(f == 0, begin, b)
            slice_of(b, f)

            def push(send):
                @pl.loop(0, 2 * per_block)
                def _(n):
                    send(acc, b * 2 * per_block + n)

            when(jnp.logical_and(f == SLICES - 1, z == 0), push, send_right)
            when(jnp.logical_and(f == SLICES - 1, z == last), push, send_left)

        i = s - lead
        when(z == 0, end, i, True)
        when(z == root_a, inner, i, True)
        when(z == root_b, inner, i, False)
        when(z == last, end, i, False)
        gathered(i)

    @pl.when(z < last)
    def _():
        drained(acc, 0)

    @pl.when(z > 0)
    def _():
        drained(acc, 1)

    for which in (2, 3, 4):
        drained(acc, which)
    for t in range(TILES):
        mine_out(t).wait()
    for stream in range(4):
        for slot in range(STAGES):
            pltpu.make_async_copy(stage.at[stream, slot], at(out_ref.at[0], 0), stage_sem.at[stream, slot]).wait()


def run_layer(lengths, hidden_in, table, k_block, v_block, w_qkv, w_up, w_down, w_out, norms, small, tp_size):
    num_rows, chunk_len, d_model = hidden_in.shape
    heads, slots, head_dim = k_block.shape[1:]
    span = heads * head_dim
    width = w_up.shape[1] // SLICES
    tokens = chunk_len // CHUNKS
    block = chunk_len // BLOCKS
    half = chunk_len // HALVES
    tile = chunk_len // TILES
    dma = pltpu.SemaphoreType.DMA
    buffer = pltpu.VMEM((chunk_len, d_model), F32)
    box = jax.ShapeDtypeStruct((chunk_len, d_model), F32)
    hbm = pl.BlockSpec(memory_space=pl.ANY)
    vmem = pl.BlockSpec(memory_space=pltpu.VMEM)
    out, _, _, _, pk, qb, _ = pl.pallas_call(
        functools.partial(layer_kernel, tp_size, heads),
        in_specs=[pl.BlockSpec(memory_space=pltpu.SMEM)] + [hbm] * 8 + [vmem] * 5,
        out_specs=[hbm] * 7,
        out_shape=[
            jax.ShapeDtypeStruct((num_rows, chunk_len, d_model), BF16), box, box, box,
            jax.ShapeDtypeStruct((2, chunk_len, 3 * span), BF16),
            jax.ShapeDtypeStruct((2, chunk_len, 3 * span), F32),
            jax.ShapeDtypeStruct((2, chunk_len, span), F32),
        ],
        scratch_shapes=[buffer] * 3
        + [
            pltpu.VMEM((SLICES, d_model, width), BF16),
            pltpu.VMEM((SLICES, width, d_model), BF16),
            pltpu.VMEM((span, d_model), BF16),
            pltpu.VMEM((TILES, tile, 3 * span), BF16),
            pltpu.VMEM((2, tile, d_model), BF16),
            pltpu.VMEM((2,) + table.shape[1:], F32),
            pltpu.VMEM((2, 2, heads, slots, head_dim), BF16),
            pltpu.VMEM((chunk_len, span), F32),
            pltpu.VMEM((heads, half, head_dim), F32),
            pltpu.VMEM((heads, half, head_dim), F32),
            pltpu.VMEM((heads, half, head_dim), F32),
            pltpu.VMEM((4, 8, chunk_len), F32),
            pltpu.VMEM((3, 8, chunk_len), F32),
            pltpu.VMEM((4, STAGES, tokens, d_model), BF16),
            pltpu.VMEM((3, STAGES, tokens, d_model), F32),
        ]
        + [dma((SLICES,)), dma((SLICES,)), dma, dma((2,)), dma((2,)), dma((TILES,)), dma((TILES,)), dma((2, 2)), dma((heads,)),
           dma((2,)), dma((2, 2))]
        + [dma((2, TILES, 3))] * 2
        + [dma((HALVES,))] * 12
        + [dma((CHUNKS,))] * 5
        + [dma((5,)), dma((4, STAGES)), dma((3, STAGES))],
        compiler_params=pltpu.CompilerParams(collective_id=0, has_side_effects=True, vmem_limit_bytes=LAYER_LIMIT),
        cost_estimate=pl.CostEstimate(flops=100_000_000_000, bytes_accessed=chunk_len * d_model * 16, transcendentals=0),
        name="layer",
    )(lengths, hidden_in, table, k_block, v_block, w_qkv, w_up, w_down, w_out, *norms, small[None])
    return out, pk, qb


def finish_kernel(heads, meta, in_ref, pk, qb, out_ref, k_ref, v_ref, buf, low, high, in_sem, out_sem, low_sem, high_sem, kv_sem):
    pieces = in_sem.shape[1]
    tile = buf.shape[1] // pieces
    head_dim = k_ref.shape[3]
    places = [(b, pl.ds(t * tile, tile), t) for b in range(buf.shape[0]) for t in range(pieces)]
    inward = [pltpu.make_async_copy(in_ref.at[b, rows], buf.at[b, rows], in_sem.at[b, t]) for b, rows, t in places]
    outward = [pltpu.make_async_copy(buf.at[b, rows], out_ref.at[b, rows], out_sem.at[b, t]) for b, rows, t in places]
    both = 2 * head_dim

    def taken(src, dst, sem):
        return [[pltpu.make_async_copy(src.at[n, :, pl.ds((3 * h + 1) * head_dim, both)], dst.at[n, :, pl.ds(h * both, both)], sem.at[n, h])
                 for h in range(heads)] for n in range(2)]

    lows, highs = taken(pk, low, low_sem), taken(qb, high, high_sem)
    stored = []

    def store(n, h, row):
        for p, ref in enumerate((k_ref, v_ref)):
            cols = pl.ds(h * both + p * head_dim, head_dim)
            copy = pltpu.make_async_copy(low.at[n, :, cols], ref.at[row, h], kv_sem.at[n, h, p])
            copy.start()
            stored.append(copy)

    for copy in highs[0] + highs[1] + lows[0] + lows[1] + inward:
        copy.start()
    j = meta[0]
    for n in range(2):
        for h in range(heads):
            lows[n][h].wait()
            store(n, h, j ^ (2 - 2 * n))
    for n in range(2):
        for h in range(heads):
            highs[n][h].wait()
            cols = slice(h * both, (h + 1) * both)
            low[2 + n, :, cols] = high[n, :, cols].astype(BF16)
            store(2 + n, h, j ^ (3 - 2 * n))
    for one, other in zip(inward, outward):
        one.wait()
        other.start()
    for copy in outward + stored:
        copy.wait()


def finish(meta, out, pk, qb, heads, head_dim):
    rows, chunk_len, _ = out.shape
    span = 2 * heads * head_dim
    hbm = pl.BlockSpec(memory_space=pl.ANY)
    cache = jax.ShapeDtypeStruct((rows, heads, chunk_len, head_dim), BF16)
    dma = pltpu.SemaphoreType.DMA
    return pl.pallas_call(
        functools.partial(finish_kernel, heads),
        in_specs=[pl.BlockSpec(memory_space=pltpu.SMEM)] + [hbm] * 3,
        out_specs=[hbm] * 3,
        out_shape=[jax.ShapeDtypeStruct(out.shape, out.dtype), cache, cache],
        scratch_shapes=[
            pltpu.VMEM(out.shape, out.dtype), pltpu.VMEM((4, chunk_len, span), BF16), pltpu.VMEM((2, chunk_len, span), F32),
            dma((rows, 4)), dma((rows, 4)), dma((2, heads)), dma((2, heads)), dma((4, heads, 2)),
        ],
        compiler_params=pltpu.CompilerParams(vmem_limit_bytes=VMEM_LIMIT),
        name="finish",
    )(meta, out, pk, qb)


def solution(mesh):
    in_specs = (P("dp", None, None), P("dp"), P("dp", "tp", "cp", None), P("dp", "tp", "cp", None), P(), P(), P(), P(), P(None, "tp"), P("tp"), P("tp", None), P(), P(None, "tp"), P("tp"), P("tp", None), P())
    out_specs = (P("dp", None, None), P("dp", "tp", None, None), P("dp", "tp", None, None))
    tp_size = mesh.shape["tp"]

    def local_layer(hidden_in, lengths, k_block, v_block, ln1_gain, ln1_bias, ln2_gain, ln2_bias, w_qkv, b_qkv, w_out, b_out, w_up, b_up, w_down, b_down):
        num_rows, chunk_len, d_model = hidden_in.shape
        heads, block_len, head_dim = k_block.shape[1:]
        table = rope_table(lengths, chunk_len, head_dim)
        norms = [p[None] for p in (ln1_gain, ln1_bias, ln2_gain, ln2_bias)]
        small = jnp.concatenate([b_qkv.astype(F32), b_up.astype(F32), b_out.astype(F32) + b_down.astype(F32)])
        out, pk, qb = run_layer(lengths, hidden_in, table, k_block, v_block, w_qkv, w_up, w_down, w_out, norms, small, tp_size)
        return tuple(finish(lax.axis_index("cp")[None], out, pk, qb, heads, head_dim))

    return jax.shard_map(local_layer, mesh=mesh, in_specs=in_specs, out_specs=out_specs, check_vma=False)
```

```python
import functools
import math

import jax
import jax.numpy as jnp
from jax import lax
from jax.experimental import pallas as pl
from jax.experimental.pallas import tpu as pltpu
from jax.sharding import PartitionSpec as P

EPSILON = 1e-5
NEG_BIG = -1e30
ROTARY_SHARE = 4
ROPE_BASE = 10000.0
LOG2E = math.log2(math.e)
MESH = pl.DeviceIdType.MESH
F32 = jnp.float32
BF16 = jnp.bfloat16
VMEM_LIMIT = 60 * 1024 * 1024
LAYER_LIMIT = 67_043_328
EMPTY = -1e29
CHUNKS = 64
STAGES = 4
BLOCKS = 8
SLICES = 4
TILES = 4
HALVES = 4
LAG_START = 2
LAG_AHEAD = 1
LAG_BACK = 1
LAG_CORE = 2
LAG_Y = 5
LAG_LAST = 6


def layer_norm(values_in, gain_vec, bias_vec):
    x_f32 = values_in.astype(F32)
    row_mean = jnp.mean(x_f32, axis=-1, keepdims=True)
    centered = x_f32 - row_mean
    variance = jnp.mean(centered * centered, axis=-1, keepdims=True)
    return (centered * lax.rsqrt(variance + EPSILON) * gain_vec + bias_vec).astype(BF16)


def rope_table(lengths, chunk_len, head_dim):
    rot_dim = head_dim // ROTARY_SHARE
    half_rot = rot_dim // 2
    positions = lengths[:, None] + jnp.arange(chunk_len, dtype=jnp.int32)[None, :]
    inv_freq = ROPE_BASE ** (-2.0 * jnp.arange(half_rot, dtype=F32) / rot_dim)
    angles = positions.astype(F32)[:, None, :] * inv_freq[:, None]
    cos_tab = jnp.cos(angles)
    sin_tab = jnp.sin(angles)
    return jnp.concatenate([cos_tab, cos_tab, -sin_tab, sin_tab], axis=1)


def wide(column, lanes):
    return jnp.concatenate([column] * (lanes // column.shape[1]), axis=1)


def scores_of(query, keys, scale, mask):
    scores = lax.dot_general(query, keys, (((1,), (1,)), ((), ())), preferred_element_type=F32) * scale
    return scores if mask is None else jnp.where(mask, scores, NEG_BIG)


def lane_sum(values, lanes):
    return functools.reduce(jnp.add, [values[:, n:n + lanes] for n in range(0, values.shape[1], lanes)])


def lane_max(values, lanes):
    return functools.reduce(jnp.maximum, [values[:, n:n + lanes] for n in range(0, values.shape[1], lanes)])


def ahead(heads, scores):
    coming = scores(0)
    for h in range(heads):
        now = coming
        if h + 1 < heads:
            coming = scores(h + 1)
        yield h, now


def first_step(heads, scale, q_of, k_of, v_of, m_scr, l_scr, o_scr, mask):
    lanes = o_scr.shape[2]
    for h, scores in ahead(heads, lambda h: scores_of(q_of(h), k_of(h), scale, mask)):
        peak = jnp.maximum(jnp.max(lane_max(scores, lanes), axis=1, keepdims=True), EMPTY)
        peak = jnp.broadcast_to(peak, m_scr.shape[1:])
        probs = jnp.exp2(scores - wide(peak, scores.shape[1]))
        m_scr[h] = peak
        l_scr[h] = lane_sum(probs, lanes)
        o_scr[h] = jnp.dot(probs.astype(BF16), v_of(h), preferred_element_type=F32)


def block_step(heads, scale, q_of, k_of, v_of, m_scr, l_scr, o_scr, mask):
    lanes = o_scr.shape[2]
    for h, scores in ahead(heads, lambda h: scores_of(q_of(h), k_of(h), scale, mask)):
        m_old = m_scr[h]
        m_new = jnp.maximum(m_old, jnp.max(lane_max(scores, lanes), axis=1, keepdims=True))
        probs = jnp.exp2(scores - wide(m_new, scores.shape[1]))
        shrink = jnp.exp2(m_old - m_new)
        l_scr[h] = l_scr[h] * shrink + lane_sum(probs, lanes)
        m_scr[h] = m_new
        o_scr[h] = o_scr[h] * shrink + jnp.dot(probs.astype(BF16), v_of(h), preferred_element_type=F32)


def piece_weights(heads, stats, head_dim):
    peak = functools.reduce(jnp.maximum, [s[:heads] for s in stats])
    weights = [jnp.exp2(s[:heads] - peak) for s in stats]
    total = functools.reduce(jnp.add, [s[heads:2 * heads] * w for s, w in zip(stats, weights)])
    return peak, weights, total


def as_columns(parts, head_dim):
    count = sum(p.shape[0] for p in parts)
    return jnp.concatenate(parts + [jnp.zeros((head_dim - count, parts[0].shape[1]), F32)], axis=0).T


def layer_kernel(tp_size, heads, lengths, hidden, table, k_cache, v_cache, w_qkv, w_up, w_down, w_out,
                 gain1, bias1, gain2, bias2, small,
                 out_ref, y_box, core_box, last_box, pk, qb, ob,
                 acc, from_left, from_right, up, down, proj, mine, far_q, x_big, tab_buf, kv, ob_far, m_scr, l_scr, o_scr, st, sbox,
                 stage, land,
                 up_sem, down_sem, proj_sem, xb_sem, tab_sem, pk_sem, mine_sem, kv_sem, q_sem, x_sem, o_sem,
                 qs_sem, qr_sem, fs_sem, fr_sem, ns_sem, nr_sem, ys_sem, yr_sem,
                 fss_sem, fsr_sem, nss_sem, nsr_sem, yss_sem, ysr_sem,
                 left_sem, right_sem, y_sem, core_sem, last_sem, send_sem, stage_sem, land_sem):
    z = lax.axis_index("tp")
    j = lax.axis_index("cp")
    y, c = lax.div(j, 2), lax.rem(j, 2)
    across, mate, corner = (1 - y) * 2 + c, y * 2 + (1 - c), (1 - y) * 2 + (1 - c)
    chunk_len, d_model = acc.shape
    head_dim = o_scr.shape[2]
    span = heads * head_dim
    slots = k_cache.shape[2]
    tokens = chunk_len // CHUNKS
    block = chunk_len // BLOCKS
    half = chunk_len // HALVES
    tile = chunk_len // TILES
    pairs = CHUNKS // 2
    per_block = pairs // BLOCKS
    width = up.shape[2]
    last = tp_size - 1
    root_a, root_b = (tp_size - 1) // 2, tp_size // 2
    rot_dim = head_dim // ROTARY_SHARE
    half_rot = rot_dim // 2
    scale = head_dim ** -0.5 * LOG2E
    own_at, sent_at, kept_at, q_at = 0, span, 2 * span, 3 * span
    extra_at = 3 * span + SLICES * width
    per_half = BLOCKS // HALVES
    waited = per_half * SLICES

    def rows_of(n, size):
        return pl.ds(pl.multiple_of(n * size, size), size)

    def weight_copies(f):
        cols = pl.ds(f * width, width)
        return (pltpu.make_async_copy(w_up.at[:, cols], up.at[f], up_sem.at[f]),
                pltpu.make_async_copy(w_down.at[cols, :], down.at[f], down_sem.at[f]))

    def row_of(n):
        return across * (1 - n) + j * n

    def big_x(i):
        return pltpu.make_async_copy(
            hidden.at[row_of(lax.div(i, TILES)), rows_of(lax.rem(i, TILES), tile), :], x_big.at[lax.rem(i, 2)], xb_sem.at[lax.rem(i, 2)])

    def cache_copies(row, slot):
        return (pltpu.make_async_copy(k_cache.at[row], kv.at[slot, 0], kv_sem.at[slot, 0]),
                pltpu.make_async_copy(v_cache.at[row], kv.at[slot, 1], kv_sem.at[slot, 1]))

    def start(copies):
        for copy in copies:
            copy.start()

    def wait(copies):
        for copy in copies:
            copy.wait()

    qkv_copies = [pltpu.make_async_copy(w_qkv.at[:, pl.ds(s * width, width)], up.at[s], up_sem.at[s]) for s in range(3)]
    tab_copies = [pltpu.make_async_copy(table.at[row], tab_buf.at[n], tab_sem.at[n]) for n, row in enumerate((across, j))]
    proj_copy = pltpu.make_async_copy(w_out, proj, proj_sem)
    big_x(0).start()
    start(qkv_copies)
    start(tab_copies)
    start(cache_copies(corner, 0))
    start(cache_copies(across, 1))
    proj_copy.start()

    barrier = pltpu.get_barrier_semaphore()
    pl.semaphore_signal(barrier, inc=1, device_id={"cp": across}, device_id_type=MESH)
    pl.semaphore_signal(barrier, inc=1, device_id={"cp": mate}, device_id_type=MESH)

    @pl.when(z > 0)
    def _():
        pl.semaphore_signal(barrier, inc=1, device_id={"tp": z - 1}, device_id_type=MESH)

    @pl.when(z < last)
    def _():
        pl.semaphore_signal(barrier, inc=1, device_id={"tp": z + 1}, device_id_type=MESH)

    inside = jnp.logical_and(z > 0, z < last)

    @pl.when(inside)
    def _():
        pl.semaphore_wait(barrier, 4)

    @pl.when(jnp.logical_not(inside))
    def _():
        pl.semaphore_wait(barrier, 3)

    def to_core(src, dst, send, arrive):
        return pltpu.make_async_remote_copy(
            src_ref=src, dst_ref=dst, send_sem=send, recv_sem=arrive, device_id={"cp": mate}, device_id_type=MESH)

    def to_y(src, dst, send, arrive):
        return pltpu.make_async_remote_copy(
            src_ref=src, dst_ref=dst, send_sem=send, recv_sem=arrive, device_id={"cp": across}, device_id_type=MESH)


    def staged(t, part):
        return acc.at[rows_of(t, tile), pl.ds(part * span, span)]

    def sent_tile(n, t):
        return [to_core(staged(t, p), qb.at[n, rows_of(t, tile), pl.ds(p * span, span)], qs_sem.at[n, t, p], qr_sem.at[n, t, p])
                for p in range(3)]

    def sent_off(n, t):
        for copy in sent_tile(n, t):
            copy.wait_send()

    def project(n, t, place):
        i = n * TILES + t

        @pl.when(i + 1 < 2 * TILES)
        def _():
            big_x(i + 1).start()

        big_x(i).wait()
        if n == 1:
            sent_off(0, t)
        normed = layer_norm(x_big[lax.rem(i, 2)], gain1[...], bias1[...])
        tab = tab_buf[n, :, rows_of(t, tile)]
        tab = jnp.concatenate([tab] * (head_dim // tab.shape[0]), axis=0).T
        lane = lax.broadcasted_iota(jnp.int32, tab.shape, 1)
        cos_tab = jnp.where(lane < rot_dim, tab, 1.0)
        sin_tab = jnp.where(lane < rot_dim, pltpu.roll(tab, head_dim - rot_dim, 1), 0.0)

        def rotate(values):
            long = values.astype(F32)
            other = jnp.where(lane < half_rot, pltpu.roll(long, head_dim - half_rot, 1), pltpu.roll(long, half_rot, 1))
            return (long * cos_tab + other * sin_tab).astype(BF16)

        for p, product in ahead(3, lambda p: jnp.dot(normed, up[p], preferred_element_type=F32)):
            some = (product + small[:, p * span:(p + 1) * span]).astype(BF16)
            for g in range(heads):
                group = p * heads + g
                values = some[:, g * head_dim:(g + 1) * head_dim]
                if group % 3 < 2:
                    values = rotate(values)
                place[:, group * head_dim:(group + 1) * head_dim] = values
                staged(t, p)[:, g * head_dim:(g + 1) * head_dim] = values.astype(F32)
        start(sent_tile(n, t))

    per_slice = width // tile

    def far_place(t):
        return down.at[lax.div(t, per_slice), rows_of(lax.rem(t, per_slice), tile), pl.ds(0, 3 * span)]

    def mine_out(t):
        return pltpu.make_async_copy(mine.at[t], pk.at[1, rows_of(t, tile), :], mine_sem.at[t])

    wait(qkv_copies)
    wait(tab_copies)

    @pl.loop(0, TILES)
    def _(t):
        project(0, t, far_place(t))

    for t in range(TILES):
        for h in range(heads):
            far_q[t, :, h * head_dim:(h + 1) * head_dim] = far_place(t)[:, 3 * h * head_dim:(3 * h + 1) * head_dim]
    pack_copies = [pltpu.make_async_copy(far_place(t), pk.at[0, rows_of(t, tile), :], pk_sem.at[t]) for t in range(TILES)]
    start(pack_copies)

    @pl.loop(0, TILES)
    def _(t):
        project(1, t, mine.at[t])
        mine_out(t).start()

    for f in range(SLICES):
        weight_copies(f)[0].start()


    def arrived_tiles(n):
        for t in range(TILES):
            for copy in sent_tile(n, t):
                copy.wait_recv()

    def query_copies(n, part):
        rows = pl.ds(part * (chunk_len // 2), chunk_len // 2)
        return [pltpu.make_async_copy(qb.at[n, rows, pl.ds(3 * h * head_dim, head_dim)],
                                      acc.at[rows, pl.ds(q_at + h * head_dim, head_dim)], q_sem.at[part, h]) for h in range(heads)]

    def attend(row, slot, query, e):
        valid = jnp.clip(lengths[row] - j * slots, 0, slots)
        mask = lax.broadcasted_iota(jnp.int32, (half, slots), 1) < valid
        first_step(heads, scale, lambda h: query(e, h), lambda h: kv[slot, 0, h], lambda h: kv[slot, 1, h],
                   m_scr, l_scr, o_scr, mask)

    def attend_own(e):
        def own_block(b, mask):
            def part(p):
                return lambda h: mine[b, :, (3 * h + p) * head_dim:(3 * h + p + 1) * head_dim]

            block_step(heads, scale, lambda h: held_mine(e, h), part(1), part(2), m_scr, l_scr, o_scr, mask)

        @pl.loop(0, e)
        def _(b):
            own_block(b, None)

        shape = (half, half)
        own_block(e, lax.broadcasted_iota(jnp.int32, shape, 0) >= lax.broadcasted_iota(jnp.int32, shape, 1))

    def keep(e, at, kind):
        lane = lax.broadcasted_iota(jnp.int32, (half, head_dim), 1)
        stats = jnp.zeros((half, head_dim), F32)
        for h in range(heads):
            stats = jnp.where(lane == h, m_scr[h], stats)
            stats = jnp.where(lane == heads + h, jnp.sum(l_scr[h], axis=1, keepdims=True), stats)
            acc[rows_of(e, half), at + h * head_dim:at + (h + 1) * head_dim] = o_scr[h]
        st[kind, :, rows_of(e, half)] = stats.T[:8]

    def held_far(e, h):
        return far_q[e, :, h * head_dim:(h + 1) * head_dim]

    def held_mine(e, h):
        return mine[e, :, 3 * h * head_dim:(3 * h + 1) * head_dim]

    def taken(e, h):
        return acc[rows_of(e, half), q_at + h * head_dim:q_at + (h + 1) * head_dim].astype(BF16)

    def far_piece(e):
        return to_core(acc.at[rows_of(e, half), pl.ds(sent_at, span)], ob_far.at[rows_of(e, half), :], fs_sem.at[e], fr_sem.at[e])

    def near_piece(e):
        return to_core(acc.at[rows_of(e, half), pl.ds(sent_at, span)], ob.at[0, rows_of(e, half), :], ns_sem.at[e], nr_sem.at[e])

    def y_piece(e):
        return to_y(acc.at[rows_of(e, half), pl.ds(kept_at, span)], ob.at[1, rows_of(e, half), :], ys_sem.at[e], yr_sem.at[e])

    def far_stats(e):
        return to_core(st.at[0, :, rows_of(e, half)], sbox.at[0, :, rows_of(e, half)], fss_sem.at[e], fsr_sem.at[e])

    def near_stats(e):
        return to_core(st.at[2, :, rows_of(e, half)], sbox.at[1, :, rows_of(e, half)], nss_sem.at[e], nsr_sem.at[e])

    def y_stats(e):
        return to_y(st.at[1, :, rows_of(e, half)], sbox.at[2, :, rows_of(e, half)], yss_sem.at[e], ysr_sem.at[e])

    def far_sent(e):
        attend(corner, 0, taken, e)
        keep(e, sent_at, 0)
        far_stats(e).start()
        far_piece(e).start()

    def far_kept(e):
        attend(across, 1, held_far, e)
        keep(e, kept_at, 1)
        far_stats(e).wait_recv()
        far_piece(e).wait_recv()
        rows = rows_of(e, half)
        peak, weights, total = piece_weights(heads, [st[1, :, rows], sbox[0, :, rows]], head_dim)
        columns = as_columns(weights, head_dim)
        for h in range(heads):
            at = kept_at + h * head_dim
            acc[rows, at:at + head_dim] = (acc[rows, at:at + head_dim] * columns[:, h:h + 1]
                                           + ob_far[rows, h * head_dim:(h + 1) * head_dim] * columns[:, heads + h:heads + h + 1])
        st[1, :heads, rows] = peak
        st[1, heads:2 * heads, rows] = total
        y_stats(e).start()
        y_piece(e).start()

    first = HALVES // 2
    arrived_tiles(0)
    for part in range(2):
        start(query_copies(0, part))
    for part in range(2):
        wait(query_copies(0, part))
    wait(cache_copies(corner, 0))

    @pl.loop(0, first)
    def _(e):
        sent_off(1, e)
        far_sent(e)

    for e in range(first, HALVES):
        sent_off(1, e)
    start(cache_copies(mate, 0))
    arrived_tiles(1)
    start(query_copies(1, 0))
    wait(cache_copies(across, 1))

    @pl.loop(0, first)
    def _(e):
        far_kept(e)

    start(cache_copies(j, 1))
    wait(pack_copies)
    for f in range(SLICES):
        weight_copies(f)[1].start()
    wait(query_copies(1, 0))
    proj_copy.wait()


    def near_mate(e):
        far_stats(e).wait_send()
        far_piece(e).wait_send()
        attend(mate, 0, taken, e)
        keep(e, sent_at, 2)
        near_stats(e).start()
        near_piece(e).start()

    def near_own(e):
        attend_own(e)
        keep(e, own_at, 3)

    def tasks(step):
        e, phase = lax.div(step, waited), lax.rem(step, waited)

        def at(n):
            return phase == n

        @pl.when(step == 0)
        def _():
            wait(cache_copies(mate, 0))
            wait(cache_copies(j, 1))

        @pl.when(at(1))
        def _():
            @pl.when(step == first * waited + 1)
            def _():
                wait(query_copies(1, 1))
                wait(cache_copies(mate, 0))
                wait(cache_copies(j, 1))

            near_mate(e)

        @pl.when(at(2))
        def _():
            attend(j, 1, held_mine, e)

        @pl.when(at(3))
        def _():
            near_own(e)

        @pl.when(step == (first - 1) * waited + 2)
        def _():
            start(cache_copies(corner, 0))

        @pl.when(step == (first - 1) * waited + 3)
        def _():
            start(cache_copies(across, 1))

        for n in range(HALVES - first):
            @pl.when(step == (first - 1) * waited + 4 + 2 * n)
            def _():
                if n == 0:
                    wait(cache_copies(corner, 0))
                far_sent(first + n)

            @pl.when(step == (first - 1) * waited + 5 + 2 * n)
            def _():
                if n == 0:
                    wait(cache_copies(across, 1))
                far_kept(first + n)

        @pl.when(step == first * waited)
        def _():
            start(query_copies(1, 1))
            start(cache_copies(mate, 0))
            start(cache_copies(j, 1))

    def block_copies(b):
        rows = rows_of(b, block)
        slot = lax.rem(b, 2)
        return [pltpu.make_async_copy(hidden.at[j, rows, :], x_big.at[slot, pl.ds(0, block), :], x_sem.at[slot])] + [
            pltpu.make_async_copy(ob.at[n, rows, :], ob_far.at[rows_of(2 * slot + n, block), :], o_sem.at[slot, n]) for n in range(2)]

    def fetch(b):
        @pl.when(lax.rem(b, per_half) == 0)
        def _():
            e = lax.div(b, per_half)
            near_stats(e).wait_recv()
            near_piece(e).wait_recv()
            y_stats(e).wait_recv()
            y_piece(e).wait_recv()

        start(block_copies(b))

    def begin(b):
        slot = lax.rem(b, 2)
        rows = rows_of(b, block)

        @pl.when(b + 1 < BLOCKS)
        def _():
            fetch(b + 1)

        wait(block_copies(b))

        @pl.when(lax.rem(b, per_half) == 0)
        def _():
            e = lax.div(b, per_half)
            for copy in (near_stats(e), near_piece(e), y_stats(e), y_piece(e)):
                copy.wait_send()

        _, weights, total = piece_weights(heads, [st[3, :, rows], sbox[1, :, rows], sbox[2, :, rows]], head_dim)
        columns = as_columns([w / total for w in weights], head_dim)
        for h in range(heads):
            cols = slice(h * head_dim, (h + 1) * head_dim)
            pieces = [acc[rows, own_at + h * head_dim:own_at + (h + 1) * head_dim]]
            pieces += [ob_far[rows_of(2 * slot + n, block), cols] for n in range(2)]
            context = functools.reduce(
                jnp.add, [o * columns[:, n * heads + h:n * heads + h + 1] for n, o in enumerate(pieces)])
            x_big[1, block:2 * block, cols] = context.astype(BF16)
        x = x_big[slot, :block, :]
        x_big[0, block:2 * block, :] = layer_norm(x, gain2[...], bias2[...])
        acc[rows, :] = jnp.dot(x_big[1, block:2 * block, :span], proj[...], preferred_element_type=F32)

        @pl.when(z == 0)
        def _():
            acc[rows, :] += x.astype(F32) + (small[:, extra_at:extra_at + d_model] + small[:, extra_at + d_model:])

    def slice_of(b, f):
        rows = rows_of(b, block)

        @pl.when(b == 0)
        def _():
            wait(weight_copies(f))

        b_up = small[:, pl.ds(pl.multiple_of(3 * span + f * width, width), width)]
        wide_h = jnp.dot(x_big[0, block:2 * block, :], up[f], preferred_element_type=F32) + b_up
        act = (0.5 * wide_h * (1.0 + lax.erf(wide_h * math.sqrt(0.5)))).astype(BF16)
        acc[rows, :] += jnp.dot(act, down[f], preferred_element_type=F32)


    def at(ref, k):
        return ref.at[pl.ds(pl.multiple_of(k * tokens, tokens), tokens), :]

    def remote(src, dst, k, which, arrive, device):
        return pltpu.make_async_remote_copy(
            src_ref=at(src, k), dst_ref=at(dst, k), send_sem=send_sem.at[which], recv_sem=arrive.at[k],
            device_id=device, device_id_type=MESH,
        )

    def send_right(src, k):
        remote(src, from_left, k, 0, left_sem, {"tp": z + 1}).start()

    def send_left(src, k):
        remote(src, from_right, k, 1, right_sem, {"tp": z - 1}).start()

    def arrived(ref, sem, k):
        remote(ref, ref, k, 0, sem, {"cp": j}).wait_recv()

    def drained(ref, which):
        pltpu.make_async_copy(ref, ref, send_sem.at[which]).wait()

    def emit(stream, values, k, row):
        slot = lax.rem(k, STAGES)

        def copy():
            return pltpu.make_async_copy(stage.at[stream, slot], at(out_ref.at[row], k), stage_sem.at[stream, slot])

        @pl.when(k >= STAGES)
        def _():
            copy().wait()

        stage[stream, slot] = values.astype(BF16)
        copy().start()

    def chunk(ref, k):
        return ref[pl.ds(pl.multiple_of(k * tokens, tokens), tokens), :]

    def finish(src, k):
        remote(src, y_box, k, 2, y_sem, {"cp": across}).start()
        remote(src, core_box, k, 3, core_sem, {"cp": mate}).start()
        emit(0, chunk(src, k), k, j)

    def landing(n, box, k):
        slot = lax.rem(k, STAGES)
        return pltpu.make_async_copy(at(box, k), land.at[n, slot], land_sem.at[n, slot])

    def gathered(i):
        def lagged(lag, act):
            @pl.when(jnp.logical_and(i >= lag, i < pairs + lag))
            def _():
                for n in range(2):
                    act((i - lag) * 2 + n)

        def core(k):
            arrived(core_box, core_sem, k)
            landing(0, core_box, k).start()

        def core_out(k):
            landing(0, core_box, k).wait()
            emit(1, land[0, lax.rem(k, STAGES)], k, mate)

        def side(k):
            arrived(y_box, y_sem, k)
            remote(y_box, last_box, k, 4, last_sem, {"cp": mate}).start()
            landing(2, y_box, k).start()

        def side_out(k):
            landing(2, y_box, k).wait()
            emit(2, land[2, lax.rem(k, STAGES)], k, across)

        def final(k):
            arrived(last_box, last_sem, k)
            landing(1, last_box, k).start()

        def final_out(k):
            landing(1, last_box, k).wait()
            emit(3, land[1, lax.rem(k, STAGES)], k, corner)

        lagged(LAG_CORE + 1, core_out)
        lagged(LAG_Y + 1, side_out)
        lagged(LAG_LAST + 1, final_out)
        lagged(LAG_CORE, core)
        lagged(LAG_Y, side)
        lagged(LAG_LAST, final)

    def add(k, *others):
        rows = pl.ds(pl.multiple_of(k * tokens, tokens), tokens)
        total = acc[rows, :]
        for other in others:
            total = total + other[rows, :]
        acc[rows, :] = total

    def when(cond, act, *args):
        @pl.when(cond)
        def _():
            act(*args)

    def end(i, first):
        inbox, sem = (from_right, right_sem) if first else (from_left, left_sem)
        near_bit = 0 if first else 1

        def got(k):
            arrived(inbox, sem, k)
            finish(inbox, k)

        when(jnp.logical_and(i >= 0, i < pairs), lambda: got(2 * i + near_bit))
        when(jnp.logical_and(i >= LAG_BACK, i < pairs + LAG_BACK), lambda: got(2 * (i - LAG_BACK) + 1 - near_bit))

    def inner(i, left_side):
        mine = 0 if left_side else 1
        if left_side:
            (outer, outer_sem, to_outer), (inward, inward_sem, to_inner) = (
                (from_left, left_sem, send_left), (from_right, right_sem, send_right))
        else:
            (outer, outer_sem, to_outer), (inward, inward_sem, to_inner) = (
                (from_right, right_sem, send_right), (from_left, left_sem, send_left))

        def early(p):
            passed = 2 * p + 1 - mine
            arrived(outer, outer_sem, passed)
            add(passed, outer)
            to_inner(acc, passed)

        def near(p):
            rooted = 2 * p + mine
            arrived(outer, outer_sem, rooted)
            arrived(inward, inward_sem, rooted)
            add(rooted, from_left, from_right)
            to_outer(acc, rooted)
            to_inner(acc, rooted)
            finish(acc, rooted)

        def far(p):
            k = 2 * p + 1 - mine
            arrived(inward, inward_sem, k)
            to_outer(inward, k)
            finish(inward, k)

        when(jnp.logical_and(i + LAG_AHEAD >= 0, i + LAG_AHEAD < pairs), early, i + LAG_AHEAD)
        when(jnp.logical_and(i >= 0, i < pairs), near, i)
        when(jnp.logical_and(i >= LAG_BACK, i < pairs + LAG_BACK), far, i - LAG_BACK)

    lead = SLICES + LAG_START

    @pl.loop(0, waited + lead + pairs + LAG_LAST + 2)
    def _(step):
        s = step - waited

        @pl.when(step < HALVES * waited)
        def _():
            tasks(step)

        @pl.when(step == waited - 1)
        def _():
            fetch(0)

        @pl.when(jnp.logical_and(s >= 0, s < BLOCKS * SLICES))
        def _():
            b, f = lax.div(s, SLICES), lax.rem(s, SLICES)
            when(f == 0, begin, b)
            slice_of(b, f)

            def push(send):
                @pl.loop(0, 2 * per_block)
                def _(n):
                    send(acc, b * 2 * per_block + n)

            when(jnp.logical_and(f == SLICES - 1, z == 0), push, send_right)
            when(jnp.logical_and(f == SLICES - 1, z == last), push, send_left)

        i = s - lead
        when(z == 0, end, i, True)
        when(z == root_a, inner, i, True)
        when(z == root_b, inner, i, False)
        when(z == last, end, i, False)
        gathered(i)

    @pl.when(z < last)
    def _():
        drained(acc, 0)

    @pl.when(z > 0)
    def _():
        drained(acc, 1)

    for which in (2, 3, 4):
        drained(acc, which)
    for t in range(TILES):
        mine_out(t).wait()
    for stream in range(4):
        for slot in range(STAGES):
            pltpu.make_async_copy(stage.at[stream, slot], at(out_ref.at[0], 0), stage_sem.at[stream, slot]).wait()


def run_layer(lengths, hidden_in, table, k_block, v_block, w_qkv, w_up, w_down, w_out, norms, small, tp_size):
    num_rows, chunk_len, d_model = hidden_in.shape
    heads, slots, head_dim = k_block.shape[1:]
    span = heads * head_dim
    width = w_up.shape[1] // SLICES
    tokens = chunk_len // CHUNKS
    block = chunk_len // BLOCKS
    half = chunk_len // HALVES
    tile = chunk_len // TILES
    dma = pltpu.SemaphoreType.DMA
    buffer = pltpu.VMEM((chunk_len, d_model), F32)
    box = jax.ShapeDtypeStruct((chunk_len, d_model), F32)
    hbm = pl.BlockSpec(memory_space=pl.ANY)
    vmem = pl.BlockSpec(memory_space=pltpu.VMEM)
    out, _, _, _, pk, qb, _ = pl.pallas_call(
        functools.partial(layer_kernel, tp_size, heads),
        in_specs=[pl.BlockSpec(memory_space=pltpu.SMEM)] + [hbm] * 8 + [vmem] * 5,
        out_specs=[hbm] * 7,
        out_shape=[
            jax.ShapeDtypeStruct((num_rows, chunk_len, d_model), BF16), box, box, box,
            jax.ShapeDtypeStruct((2, chunk_len, 3 * span), BF16),
            jax.ShapeDtypeStruct((2, chunk_len, 3 * span), F32),
            jax.ShapeDtypeStruct((2, chunk_len, span), F32),
        ],
        scratch_shapes=[buffer] * 3
        + [
            pltpu.VMEM((SLICES, d_model, width), BF16),
            pltpu.VMEM((SLICES, width, d_model), BF16),
            pltpu.VMEM((span, d_model), BF16),
            pltpu.VMEM((TILES, tile, 3 * span), BF16),
            pltpu.VMEM((TILES, tile, span), BF16),
            pltpu.VMEM((2, tile, d_model), BF16),
            pltpu.VMEM((2,) + table.shape[1:], F32),
            pltpu.VMEM((2, 2, heads, slots, head_dim), BF16),
            pltpu.VMEM((chunk_len, span), F32),
            pltpu.VMEM((heads, half, head_dim), F32),
            pltpu.VMEM((heads, half, head_dim), F32),
            pltpu.VMEM((heads, half, head_dim), F32),
            pltpu.VMEM((4, 8, chunk_len), F32),
            pltpu.VMEM((3, 8, chunk_len), F32),
            pltpu.VMEM((4, STAGES, tokens, d_model), BF16),
            pltpu.VMEM((3, STAGES, tokens, d_model), F32),
        ]
        + [dma((SLICES,)), dma((SLICES,)), dma, dma((2,)), dma((2,)), dma((TILES,)), dma((TILES,)), dma((2, 2)), dma((2, heads)),
           dma((2,)), dma((2, 2))]
        + [dma((2, TILES, 3))] * 2
        + [dma((HALVES,))] * 12
        + [dma((CHUNKS,))] * 5
        + [dma((5,)), dma((4, STAGES)), dma((3, STAGES))],
        compiler_params=pltpu.CompilerParams(collective_id=0, has_side_effects=True, vmem_limit_bytes=LAYER_LIMIT),
        cost_estimate=pl.CostEstimate(flops=100_000_000_000, bytes_accessed=chunk_len * d_model * 16, transcendentals=0),
        name="layer",
    )(lengths, hidden_in, table, k_block, v_block, w_qkv, w_up, w_down, w_out, *norms, small[None])
    return out, pk, qb


def finish_kernel(heads, meta, in_ref, pk, qb, out_ref, k_ref, v_ref, buf, low, high, in_sem, out_sem, low_sem, high_sem, kv_sem):
    pieces = in_sem.shape[1]
    tile = buf.shape[1] // pieces
    head_dim = k_ref.shape[3]
    places = [(b, pl.ds(t * tile, tile), t) for b in range(buf.shape[0]) for t in range(pieces)]
    inward = [pltpu.make_async_copy(in_ref.at[b, rows], buf.at[b, rows], in_sem.at[b, t]) for b, rows, t in places]
    outward = [pltpu.make_async_copy(buf.at[b, rows], out_ref.at[b, rows], out_sem.at[b, t]) for b, rows, t in places]
    both = 2 * head_dim

    def taken(src, dst, sem):
        return [[pltpu.make_async_copy(src.at[n, :, pl.ds((3 * h + 1) * head_dim, both)], dst.at[n, :, pl.ds(h * both, both)], sem.at[n, h])
                 for h in range(heads)] for n in range(2)]

    lows, highs = taken(pk, low, low_sem), taken(qb, high, high_sem)
    stored = []

    def store(n, h, row):
        for p, ref in enumerate((k_ref, v_ref)):
            cols = pl.ds(h * both + p * head_dim, head_dim)
            copy = pltpu.make_async_copy(low.at[n, :, cols], ref.at[row, h], kv_sem.at[n, h, p])
            copy.start()
            stored.append(copy)

    for copy in highs[0] + highs[1] + lows[0] + lows[1] + inward:
        copy.start()
    j = meta[0]
    for n in range(2):
        for h in range(heads):
            lows[n][h].wait()
            store(n, h, j ^ (2 - 2 * n))
    for n in range(2):
        for h in range(heads):
            highs[n][h].wait()
            cols = slice(h * both, (h + 1) * both)
            low[2 + n, :, cols] = high[n, :, cols].astype(BF16)
            store(2 + n, h, j ^ (3 - 2 * n))
    for one, other in zip(inward, outward):
        one.wait()
        other.start()
    for copy in outward + stored:
        copy.wait()


def finish(meta, out, pk, qb, heads, head_dim):
    rows, chunk_len, _ = out.shape
    span = 2 * heads * head_dim
    hbm = pl.BlockSpec(memory_space=pl.ANY)
    cache = jax.ShapeDtypeStruct((rows, heads, chunk_len, head_dim), BF16)
    dma = pltpu.SemaphoreType.DMA
    return pl.pallas_call(
        functools.partial(finish_kernel, heads),
        in_specs=[pl.BlockSpec(memory_space=pltpu.SMEM)] + [hbm] * 3,
        out_specs=[hbm] * 3,
        out_shape=[jax.ShapeDtypeStruct(out.shape, out.dtype), cache, cache],
        scratch_shapes=[
            pltpu.VMEM(out.shape, out.dtype), pltpu.VMEM((4, chunk_len, span), BF16), pltpu.VMEM((2, chunk_len, span), F32),
            dma((rows, 4)), dma((rows, 4)), dma((2, heads)), dma((2, heads)), dma((4, heads, 2)),
        ],
        compiler_params=pltpu.CompilerParams(vmem_limit_bytes=VMEM_LIMIT),
        name="finish",
    )(meta, out, pk, qb)


def solution(mesh):
    in_specs = (P("dp", None, None), P("dp"), P("dp", "tp", "cp", None), P("dp", "tp", "cp", None), P(), P(), P(), P(), P(None, "tp"), P("tp"), P("tp", None), P(), P(None, "tp"), P("tp"), P("tp", None), P())
    out_specs = (P("dp", None, None), P("dp", "tp", None, None), P("dp", "tp", None, None))
    tp_size = mesh.shape["tp"]

    def local_layer(hidden_in, lengths, k_block, v_block, ln1_gain, ln1_bias, ln2_gain, ln2_bias, w_qkv, b_qkv, w_out, b_out, w_up, b_up, w_down, b_down):
        num_rows, chunk_len, d_model = hidden_in.shape
        heads, block_len, head_dim = k_block.shape[1:]
        table = rope_table(lengths, chunk_len, head_dim)
        norms = [p[None] for p in (ln1_gain, ln1_bias, ln2_gain, ln2_bias)]
        small = jnp.concatenate([b_qkv, b_up, b_out, b_down]).astype(F32)
        out, pk, qb = run_layer(lengths, hidden_in, table, k_block, v_block, w_qkv, w_up, w_down, w_out, norms, small, tp_size)
        return tuple(finish(lax.axis_index("cp")[None], out, pk, qb, heads, head_dim))

    return jax.shard_map(local_layer, mesh=mesh, in_specs=in_specs, out_specs=out_specs, check_vma=False)
```

```python
import functools
import math

import jax
import jax.numpy as jnp
from jax import lax
from jax.experimental import pallas as pl
from jax.experimental.pallas import tpu as pltpu
from jax.sharding import PartitionSpec as P

EPSILON = 1e-5
NEG_BIG = -1e30
ROTARY_SHARE = 4
ROPE_BASE = 10000.0
LOG2E = math.log2(math.e)
MESH = pl.DeviceIdType.MESH
F32 = jnp.float32
BF16 = jnp.bfloat16
VMEM_LIMIT = 60 * 1024 * 1024
LAYER_LIMIT = 67_043_328
EMPTY = -1e29
CHUNKS = 64
STAGES = 4
BLOCKS = 8
SLICES = 4
TILES = 4
HALVES = 4
LAG_START = 2
LAG_AHEAD = 1
LAG_BACK = 1
LAG_CORE = 2
LAG_Y = 5
LAG_LAST = 6


def layer_norm(values_in, gain_vec, bias_vec):
    x_f32 = values_in.astype(F32)
    row_mean = jnp.mean(x_f32, axis=-1, keepdims=True)
    centered = x_f32 - row_mean
    variance = jnp.mean(centered * centered, axis=-1, keepdims=True)
    return (centered * lax.rsqrt(variance + EPSILON) * gain_vec + bias_vec).astype(BF16)


def rope_table(lengths, chunk_len, head_dim):
    rot_dim = head_dim // ROTARY_SHARE
    half_rot = rot_dim // 2
    positions = lengths[:, None] + jnp.arange(chunk_len, dtype=jnp.int32)[None, :]
    inv_freq = ROPE_BASE ** (-2.0 * jnp.arange(half_rot, dtype=F32) / rot_dim)
    angles = positions.astype(F32)[:, None, :] * inv_freq[:, None]
    cos_tab = jnp.cos(angles)
    sin_tab = jnp.sin(angles)
    return jnp.concatenate([cos_tab, cos_tab, -sin_tab, sin_tab], axis=1)


def wide(column, lanes):
    return jnp.concatenate([column] * (lanes // column.shape[1]), axis=1)


def scores_of(query, keys, scale, mask):
    scores = lax.dot_general(query, keys, (((1,), (1,)), ((), ())), preferred_element_type=F32) * scale
    return scores if mask is None else jnp.where(mask, scores, NEG_BIG)


def lane_sum(values, lanes):
    return functools.reduce(jnp.add, [values[:, n:n + lanes] for n in range(0, values.shape[1], lanes)])


def lane_max(values, lanes):
    return functools.reduce(jnp.maximum, [values[:, n:n + lanes] for n in range(0, values.shape[1], lanes)])


def ahead(heads, scores):
    coming = scores(0)
    for h in range(heads):
        now = coming
        if h + 1 < heads:
            coming = scores(h + 1)
        yield h, now


def first_step(heads, scale, q_of, k_of, v_of, m_scr, l_scr, o_scr, mask):
    lanes = o_scr.shape[2]
    for h, scores in ahead(heads, lambda h: scores_of(q_of(h), k_of(h), scale, mask)):
        peak = jnp.maximum(jnp.max(lane_max(scores, lanes), axis=1, keepdims=True), EMPTY)
        peak = jnp.broadcast_to(peak, m_scr.shape[1:])
        probs = jnp.exp2(scores - wide(peak, scores.shape[1]))
        m_scr[h] = peak
        l_scr[h] = lane_sum(probs, lanes)
        o_scr[h] = jnp.dot(probs.astype(BF16), v_of(h), preferred_element_type=F32)


def block_step(heads, scale, q_of, k_of, v_of, m_scr, l_scr, o_scr, mask):
    lanes = o_scr.shape[2]
    for h, scores in ahead(heads, lambda h: scores_of(q_of(h), k_of(h), scale, mask)):
        m_old = m_scr[h]
        m_new = jnp.maximum(m_old, jnp.max(lane_max(scores, lanes), axis=1, keepdims=True))
        probs = jnp.exp2(scores - wide(m_new, scores.shape[1]))
        shrink = jnp.exp2(m_old - m_new)
        l_scr[h] = l_scr[h] * shrink + lane_sum(probs, lanes)
        m_scr[h] = m_new
        o_scr[h] = o_scr[h] * shrink + jnp.dot(probs.astype(BF16), v_of(h), preferred_element_type=F32)


def piece_weights(heads, stats, head_dim):
    peak = functools.reduce(jnp.maximum, [s[:heads] for s in stats])
    weights = [jnp.exp2(s[:heads] - peak) for s in stats]
    total = functools.reduce(jnp.add, [s[heads:2 * heads] * w for s, w in zip(stats, weights)])
    return peak, weights, total


def as_columns(parts, head_dim):
    count = sum(p.shape[0] for p in parts)
    return jnp.concatenate(parts + [jnp.zeros((head_dim - count, parts[0].shape[1]), F32)], axis=0).T


def layer_kernel(tp_size, heads, lengths, hidden, table, k_cache, v_cache, w_qkv, w_up, w_down, w_out,
                 gain1, bias1, gain2, bias2, small,
                 out_ref, y_box, core_box, last_box, pk, qb, ob,
                 acc, from_left, from_right, up, down, proj, mine, x_big, tab_buf, kv, ob_far, m_scr, l_scr, o_scr, st, sbox,
                 stage, land,
                 up_sem, down_sem, proj_sem, xb_sem, tab_sem, pk_sem, mine_sem, kv_sem, q_sem, x_sem, o_sem,
                 qs_sem, qr_sem, fs_sem, fr_sem, ns_sem, nr_sem, ys_sem, yr_sem,
                 fss_sem, fsr_sem, nss_sem, nsr_sem, yss_sem, ysr_sem,
                 left_sem, right_sem, y_sem, core_sem, last_sem, send_sem, stage_sem, land_sem):
    z = lax.axis_index("tp")
    j = lax.axis_index("cp")
    y, c = lax.div(j, 2), lax.rem(j, 2)
    across, mate, corner = (1 - y) * 2 + c, y * 2 + (1 - c), (1 - y) * 2 + (1 - c)
    chunk_len, d_model = acc.shape
    head_dim = o_scr.shape[2]
    span = heads * head_dim
    slots = k_cache.shape[2]
    tokens = chunk_len // CHUNKS
    block = chunk_len // BLOCKS
    half = chunk_len // HALVES
    tile = chunk_len // TILES
    pairs = CHUNKS // 2
    per_block = pairs // BLOCKS
    width = up.shape[2]
    last = tp_size - 1
    root_a, root_b = (tp_size - 1) // 2, tp_size // 2
    rot_dim = head_dim // ROTARY_SHARE
    half_rot = rot_dim // 2
    scale = head_dim ** -0.5 * LOG2E
    own_at, sent_at, kept_at, q_at = 0, span, 2 * span, 3 * span
    extra_at = 3 * span + SLICES * width
    per_half = BLOCKS // HALVES
    waited = per_half * SLICES

    def rows_of(n, size):
        return pl.ds(pl.multiple_of(n * size, size), size)

    def weight_copies(f):
        cols = pl.ds(f * width, width)
        return (pltpu.make_async_copy(w_up.at[:, cols], up.at[f], up_sem.at[f]),
                pltpu.make_async_copy(w_down.at[cols, :], down.at[f], down_sem.at[f]))

    def row_of(n):
        return across * (1 - n) + j * n

    def big_x(i):
        return pltpu.make_async_copy(
            hidden.at[row_of(lax.div(i, TILES)), rows_of(lax.rem(i, TILES), tile), :], x_big.at[lax.rem(i, 2)], xb_sem.at[lax.rem(i, 2)])

    def cache_copies(row, slot):
        return (pltpu.make_async_copy(k_cache.at[row], kv.at[slot, 0], kv_sem.at[slot, 0]),
                pltpu.make_async_copy(v_cache.at[row], kv.at[slot, 1], kv_sem.at[slot, 1]))

    def start(copies):
        for copy in copies:
            copy.start()

    def wait(copies):
        for copy in copies:
            copy.wait()

    qkv_copies = [pltpu.make_async_copy(w_qkv.at[:, pl.ds(s * width, width)], up.at[s], up_sem.at[s]) for s in range(3)]
    tab_copies = [pltpu.make_async_copy(table.at[row], tab_buf.at[n], tab_sem.at[n]) for n, row in enumerate((across, j))]
    proj_copy = pltpu.make_async_copy(w_out, proj, proj_sem)
    big_x(0).start()
    start(qkv_copies)
    start(tab_copies)
    start(cache_copies(corner, 0))
    start(cache_copies(across, 1))
    proj_copy.start()

    barrier = pltpu.get_barrier_semaphore()
    pl.semaphore_signal(barrier, inc=1, device_id={"cp": across}, device_id_type=MESH)
    pl.semaphore_signal(barrier, inc=1, device_id={"cp": mate}, device_id_type=MESH)

    @pl.when(z > 0)
    def _():
        pl.semaphore_signal(barrier, inc=1, device_id={"tp": z - 1}, device_id_type=MESH)

    @pl.when(z < last)
    def _():
        pl.semaphore_signal(barrier, inc=1, device_id={"tp": z + 1}, device_id_type=MESH)

    inside = jnp.logical_and(z > 0, z < last)

    @pl.when(inside)
    def _():
        pl.semaphore_wait(barrier, 4)

    @pl.when(jnp.logical_not(inside))
    def _():
        pl.semaphore_wait(barrier, 3)

    def to_core(src, dst, send, arrive):
        return pltpu.make_async_remote_copy(
            src_ref=src, dst_ref=dst, send_sem=send, recv_sem=arrive, device_id={"cp": mate}, device_id_type=MESH)

    def to_y(src, dst, send, arrive):
        return pltpu.make_async_remote_copy(
            src_ref=src, dst_ref=dst, send_sem=send, recv_sem=arrive, device_id={"cp": across}, device_id_type=MESH)


    def staged(t, part):
        return acc.at[rows_of(t, tile), pl.ds(part * span, span)]

    def sent_tile(n, t):
        return [to_core(staged(t, p), qb.at[n, rows_of(t, tile), pl.ds(p * span, span)], qs_sem.at[n, t, p], qr_sem.at[n, t, p])
                for p in range(3)]

    def sent_off(n, t):
        for copy in sent_tile(n, t):
            copy.wait_send()

    def project(n, t, place):
        i = n * TILES + t

        @pl.when(i + 1 < 2 * TILES)
        def _():
            big_x(i + 1).start()

        big_x(i).wait()
        if n == 1:
            sent_off(0, t)
        normed = layer_norm(x_big[lax.rem(i, 2)], gain1[...], bias1[...])
        tab = tab_buf[n, :, rows_of(t, tile)]
        tab = jnp.concatenate([tab] * (head_dim // tab.shape[0]), axis=0).T
        lane = lax.broadcasted_iota(jnp.int32, tab.shape, 1)
        cos_tab = jnp.where(lane < rot_dim, tab, 1.0)
        sin_tab = jnp.where(lane < rot_dim, pltpu.roll(tab, head_dim - rot_dim, 1), 0.0)

        def rotate(values):
            long = values.astype(F32)
            other = jnp.where(lane < half_rot, pltpu.roll(long, head_dim - half_rot, 1), pltpu.roll(long, half_rot, 1))
            return (long * cos_tab + other * sin_tab).astype(BF16)

        for p, product in ahead(3, lambda p: jnp.dot(normed, up[p], preferred_element_type=F32)):
            some = (product + small[:, p * span:(p + 1) * span]).astype(BF16)
            for g in range(heads):
                group = p * heads + g
                values = some[:, g * head_dim:(g + 1) * head_dim]
                if group % 3 < 2:
                    values = rotate(values)
                place[:, group * head_dim:(group + 1) * head_dim] = values
                staged(t, p)[:, g * head_dim:(g + 1) * head_dim] = values.astype(F32)
        start(sent_tile(n, t))

    def arrived_tiles(n):
        for t in range(TILES):
            for copy in sent_tile(n, t):
                copy.wait_recv()

    def query_copies(n):
        return [pltpu.make_async_copy(qb.at[n, :, pl.ds(3 * h * head_dim, head_dim)],
                                      acc.at[:, pl.ds(q_at + h * head_dim, head_dim)], q_sem.at[h]) for h in range(heads)]

    per_slice = width // tile

    def far_place(t):
        return down.at[lax.div(t, per_slice), rows_of(lax.rem(t, per_slice), tile), pl.ds(0, 3 * span)]

    def mine_out(t):
        return pltpu.make_async_copy(mine.at[t], pk.at[1, rows_of(t, tile), :], mine_sem.at[t])

    wait(qkv_copies)
    wait(tab_copies)

    @pl.loop(0, TILES)
    def _(t):
        project(0, t, far_place(t))

    pack_copies = [pltpu.make_async_copy(far_place(t), pk.at[0, rows_of(t, tile), :], pk_sem.at[t]) for t in range(TILES)]
    start(pack_copies)

    @pl.loop(0, TILES)
    def _(t):
        @pl.when(t == TILES // 2)
        def _():
            arrived_tiles(0)
            start(query_copies(0))

        project(1, t, mine.at[t])
        mine_out(t).start()

    for f in range(SLICES):
        weight_copies(f)[0].start()


    def attend(row, slot, query, e):
        valid = jnp.clip(lengths[row] - j * slots, 0, slots)
        mask = lax.broadcasted_iota(jnp.int32, (half, slots), 1) < valid
        first_step(heads, scale, lambda h: query(e, h), lambda h: kv[slot, 0, h], lambda h: kv[slot, 1, h],
                   m_scr, l_scr, o_scr, mask)

    def attend_own(e):
        def own_block(b, mask):
            def part(p):
                return lambda h: mine[b, :, (3 * h + p) * head_dim:(3 * h + p + 1) * head_dim]

            block_step(heads, scale, lambda h: held_mine(e, h), part(1), part(2), m_scr, l_scr, o_scr, mask)

        @pl.loop(0, e)
        def _(b):
            own_block(b, None)

        shape = (half, half)
        own_block(e, lax.broadcasted_iota(jnp.int32, shape, 0) >= lax.broadcasted_iota(jnp.int32, shape, 1))

    def keep(e, at, kind):
        lane = lax.broadcasted_iota(jnp.int32, (half, head_dim), 1)
        stats = jnp.zeros((half, head_dim), F32)
        for h in range(heads):
            stats = jnp.where(lane == h, m_scr[h], stats)
            stats = jnp.where(lane == heads + h, jnp.sum(l_scr[h], axis=1, keepdims=True), stats)
            acc[rows_of(e, half), at + h * head_dim:at + (h + 1) * head_dim] = o_scr[h]
        st[kind, :, rows_of(e, half)] = stats.T[:8]

    def held_far(e, h):
        return far_place(e)[:, 3 * h * head_dim:(3 * h + 1) * head_dim]

    def held_mine(e, h):
        return mine[e, :, 3 * h * head_dim:(3 * h + 1) * head_dim]

    def taken(e, h):
        return acc[rows_of(e, half), q_at + h * head_dim:q_at + (h + 1) * head_dim].astype(BF16)

    def far_piece(e):
        return to_core(acc.at[rows_of(e, half), pl.ds(sent_at, span)], ob_far.at[rows_of(e, half), :], fs_sem.at[e], fr_sem.at[e])

    def near_piece(e):
        return to_core(acc.at[rows_of(e, half), pl.ds(sent_at, span)], ob.at[0, rows_of(e, half), :], ns_sem.at[e], nr_sem.at[e])

    def y_piece(e):
        return to_y(acc.at[rows_of(e, half), pl.ds(kept_at, span)], ob.at[1, rows_of(e, half), :], ys_sem.at[e], yr_sem.at[e])

    def far_stats(e):
        return to_core(st.at[0, :, rows_of(e, half)], sbox.at[0, :, rows_of(e, half)], fss_sem.at[e], fsr_sem.at[e])

    def near_stats(e):
        return to_core(st.at[2, :, rows_of(e, half)], sbox.at[1, :, rows_of(e, half)], nss_sem.at[e], nsr_sem.at[e])

    def y_stats(e):
        return to_y(st.at[1, :, rows_of(e, half)], sbox.at[2, :, rows_of(e, half)], yss_sem.at[e], ysr_sem.at[e])

    wait(query_copies(0))
    wait(cache_copies(corner, 0))
    wait(cache_copies(across, 1))

    @pl.loop(0, HALVES)
    def _(e):
        sent_off(1, e)
        attend(corner, 0, taken, e)
        keep(e, sent_at, 0)
        far_stats(e).start()
        far_piece(e).start()

        @pl.when(e == HALVES - 1)
        def _():
            start(cache_copies(mate, 0))
            arrived_tiles(1)
            start(query_copies(1))

        attend(across, 1, held_far, e)
        keep(e, kept_at, 1)

        far_stats(e).wait_recv()
        far_piece(e).wait_recv()
        rows = rows_of(e, half)
        peak, weights, total = piece_weights(heads, [st[1, :, rows], sbox[0, :, rows]], head_dim)
        columns = as_columns(weights, head_dim)
        for h in range(heads):
            at = kept_at + h * head_dim
            acc[rows, at:at + head_dim] = (acc[rows, at:at + head_dim] * columns[:, h:h + 1]
                                           + ob_far[rows, h * head_dim:(h + 1) * head_dim] * columns[:, heads + h:heads + h + 1])
        st[1, :heads, rows] = peak
        st[1, heads:2 * heads, rows] = total
        y_stats(e).start()
        y_piece(e).start()

    start(cache_copies(j, 1))
    wait(pack_copies)
    for f in range(SLICES):
        weight_copies(f)[1].start()
    for e in range(HALVES):
        far_stats(e).wait_send()
        far_piece(e).wait_send()
    wait(query_copies(1))
    wait(cache_copies(mate, 0))


    def near(e, phase):
        @pl.when(phase == 4)
        def _():
            attend(mate, 0, taken, e)
            keep(e, sent_at, 2)
            near_stats(e).start()
            near_piece(e).start()

            @pl.when(e == 0)
            def _():
                wait(cache_copies(j, 1))

        @pl.when(phase == 5)
        def _():
            attend(j, 1, held_mine, e)

        @pl.when(phase == 6)
        def _():
            attend_own(e)
            keep(e, own_at, 3)

            @pl.when(e == 0)
            def _():
                proj_copy.wait()

    def block_copies(b):
        rows = rows_of(b, block)
        slot = lax.rem(b, 2)
        return [pltpu.make_async_copy(hidden.at[j, rows, :], x_big.at[slot, pl.ds(0, block), :], x_sem.at[slot])] + [
            pltpu.make_async_copy(ob.at[n, rows, :], ob_far.at[rows_of(2 * slot + n, block), :], o_sem.at[slot, n]) for n in range(2)]

    def fetch(b):
        @pl.when(lax.rem(b, per_half) == 0)
        def _():
            e = lax.div(b, per_half)
            near_stats(e).wait_recv()
            near_piece(e).wait_recv()
            y_stats(e).wait_recv()
            y_piece(e).wait_recv()

        start(block_copies(b))

    def begin(b):
        slot = lax.rem(b, 2)
        rows = rows_of(b, block)

        wait(block_copies(b))

        @pl.when(lax.rem(b, per_half) == 0)
        def _():
            e = lax.div(b, per_half)
            for copy in (near_stats(e), near_piece(e), y_stats(e), y_piece(e)):
                copy.wait_send()

        _, weights, total = piece_weights(heads, [st[3, :, rows], sbox[1, :, rows], sbox[2, :, rows]], head_dim)
        columns = as_columns([w / total for w in weights], head_dim)
        for h in range(heads):
            cols = slice(h * head_dim, (h + 1) * head_dim)
            pieces = [acc[rows, own_at + h * head_dim:own_at + (h + 1) * head_dim]]
            pieces += [ob_far[rows_of(2 * slot + n, block), cols] for n in range(2)]
            context = functools.reduce(
                jnp.add, [o * columns[:, n * heads + h:n * heads + h + 1] for n, o in enumerate(pieces)])
            x_big[1, block:2 * block, cols] = context.astype(BF16)
        x = x_big[slot, :block, :]
        x_big[0, block:2 * block, :] = layer_norm(x, gain2[...], bias2[...])
        acc[rows, :] = jnp.dot(x_big[1, block:2 * block, :span], proj[...], preferred_element_type=F32)

        @pl.when(z == 0)
        def _():
            acc[rows, :] += x.astype(F32) + small[:, extra_at:]

    def slice_of(b, f):
        rows = rows_of(b, block)

        @pl.when(b == 0)
        def _():
            wait(weight_copies(f))

        b_up = small[:, pl.ds(pl.multiple_of(3 * span + f * width, width), width)]
        wide_h = jnp.dot(x_big[0, block:2 * block, :], up[f], preferred_element_type=F32) + b_up
        act = (0.5 * wide_h * (1.0 + lax.erf(wide_h * math.sqrt(0.5)))).astype(BF16)
        acc[rows, :] += jnp.dot(act, down[f], preferred_element_type=F32)


    def at(ref, k):
        return ref.at[pl.ds(pl.multiple_of(k * tokens, tokens), tokens), :]

    def remote(src, dst, k, which, arrive, device):
        return pltpu.make_async_remote_copy(
            src_ref=at(src, k), dst_ref=at(dst, k), send_sem=send_sem.at[which], recv_sem=arrive.at[k],
            device_id=device, device_id_type=MESH,
        )

    def send_right(src, k):
        remote(src, from_left, k, 0, left_sem, {"tp": z + 1}).start()

    def send_left(src, k):
        remote(src, from_right, k, 1, right_sem, {"tp": z - 1}).start()

    def arrived(ref, sem, k):
        remote(ref, ref, k, 0, sem, {"cp": j}).wait_recv()

    def drained(ref, which):
        pltpu.make_async_copy(ref, ref, send_sem.at[which]).wait()

    def emit(stream, values, k, row):
        slot = lax.rem(k, STAGES)

        def copy():
            return pltpu.make_async_copy(stage.at[stream, slot], at(out_ref.at[row], k), stage_sem.at[stream, slot])

        @pl.when(k >= STAGES)
        def _():
            copy().wait()

        stage[stream, slot] = values.astype(BF16)
        copy().start()

    def chunk(ref, k):
        return ref[pl.ds(pl.multiple_of(k * tokens, tokens), tokens), :]

    def finish(src, k):
        remote(src, y_box, k, 2, y_sem, {"cp": across}).start()
        remote(src, core_box, k, 3, core_sem, {"cp": mate}).start()
        emit(0, chunk(src, k), k, j)

    def landing(n, box, k):
        slot = lax.rem(k, STAGES)
        return pltpu.make_async_copy(at(box, k), land.at[n, slot], land_sem.at[n, slot])

    def gathered(i):
        def lagged(lag, act):
            @pl.when(jnp.logical_and(i >= lag, i < pairs + lag))
            def _():
                for n in range(2):
                    act((i - lag) * 2 + n)

        def core(k):
            arrived(core_box, core_sem, k)
            landing(0, core_box, k).start()

        def core_out(k):
            landing(0, core_box, k).wait()
            emit(1, land[0, lax.rem(k, STAGES)], k, mate)

        def side(k):
            arrived(y_box, y_sem, k)
            remote(y_box, last_box, k, 4, last_sem, {"cp": mate}).start()
            landing(2, y_box, k).start()

        def side_out(k):
            landing(2, y_box, k).wait()
            emit(2, land[2, lax.rem(k, STAGES)], k, across)

        def final(k):
            arrived(last_box, last_sem, k)
            landing(1, last_box, k).start()

        def final_out(k):
            landing(1, last_box, k).wait()
            emit(3, land[1, lax.rem(k, STAGES)], k, corner)

        lagged(LAG_CORE + 1, core_out)
        lagged(LAG_Y + 1, side_out)
        lagged(LAG_LAST + 1, final_out)
        lagged(LAG_CORE, core)
        lagged(LAG_Y, side)
        lagged(LAG_LAST, final)

    def add(k, *others):
        rows = pl.ds(pl.multiple_of(k * tokens, tokens), tokens)
        total = acc[rows, :]
        for other in others:
            total = total + other[rows, :]
        acc[rows, :] = total

    def when(cond, act, *args):
        @pl.when(cond)
        def _():
            act(*args)

    def end(i, first):
        inbox, sem = (from_right, right_sem) if first else (from_left, left_sem)
        near_bit = 0 if first else 1

        def got(k):
            arrived(inbox, sem, k)
            finish(inbox, k)

        when(jnp.logical_and(i >= 0, i < pairs), lambda: got(2 * i + near_bit))
        when(jnp.logical_and(i >= LAG_BACK, i < pairs + LAG_BACK), lambda: got(2 * (i - LAG_BACK) + 1 - near_bit))

    def inner(i, left_side):
        mine = 0 if left_side else 1
        if left_side:
            (outer, outer_sem, to_outer), (inward, inward_sem, to_inner) = (
                (from_left, left_sem, send_left), (from_right, right_sem, send_right))
        else:
            (outer, outer_sem, to_outer), (inward, inward_sem, to_inner) = (
                (from_right, right_sem, send_right), (from_left, left_sem, send_left))

        def early(p):
            passed = 2 * p + 1 - mine
            arrived(outer, outer_sem, passed)
            add(passed, outer)
            to_inner(acc, passed)

        def near(p):
            rooted = 2 * p + mine
            arrived(outer, outer_sem, rooted)
            arrived(inward, inward_sem, rooted)
            add(rooted, from_left, from_right)
            to_outer(acc, rooted)
            to_inner(acc, rooted)
            finish(acc, rooted)

        def far(p):
            k = 2 * p + 1 - mine
            arrived(inward, inward_sem, k)
            to_outer(inward, k)
            finish(inward, k)

        when(jnp.logical_and(i + LAG_AHEAD >= 0, i + LAG_AHEAD < pairs), early, i + LAG_AHEAD)
        when(jnp.logical_and(i >= 0, i < pairs), near, i)
        when(jnp.logical_and(i >= LAG_BACK, i < pairs + LAG_BACK), far, i - LAG_BACK)

    lead = SLICES + LAG_START

    @pl.loop(0, waited + lead + pairs + LAG_LAST + 2)
    def _(step):
        s = step - waited

        @pl.when(step < HALVES * waited)
        def _():
            near(lax.div(step, waited), lax.rem(step, waited))

        @pl.when(step == waited - 1)
        def _():
            fetch(0)

        @pl.when(jnp.logical_and(s >= 0, s < BLOCKS * SLICES))
        def _():
            b, f = lax.div(s, SLICES), lax.rem(s, SLICES)
            when(f == 0, begin, b)
            when(jnp.logical_and(f == SLICES // 2, b + 1 < BLOCKS), fetch, b + 1)
            slice_of(b, f)

            def push(send):
                @pl.loop(0, 2 * per_block)
                def _(n):
                    send(acc, b * 2 * per_block + n)

            when(jnp.logical_and(f == SLICES - 1, z == 0), push, send_right)
            when(jnp.logical_and(f == SLICES - 1, z == last), push, send_left)

        i = s - lead
        when(z == 0, end, i, True)
        when(z == root_a, inner, i, True)
        when(z == root_b, inner, i, False)
        when(z == last, end, i, False)
        gathered(i)

    @pl.when(z < last)
    def _():
        drained(acc, 0)

    @pl.when(z > 0)
    def _():
        drained(acc, 1)

    for which in (2, 3, 4):
        drained(acc, which)
    for t in range(TILES):
        mine_out(t).wait()
    for stream in range(4):
        for slot in range(STAGES):
            pltpu.make_async_copy(stage.at[stream, slot], at(out_ref.at[0], 0), stage_sem.at[stream, slot]).wait()


def run_layer(lengths, hidden_in, table, k_block, v_block, w_qkv, w_up, w_down, w_out, norms, small, tp_size):
    num_rows, chunk_len, d_model = hidden_in.shape
    heads, slots, head_dim = k_block.shape[1:]
    span = heads * head_dim
    width = w_up.shape[1] // SLICES
    tokens = chunk_len // CHUNKS
    block = chunk_len // BLOCKS
    half = chunk_len // HALVES
    tile = chunk_len // TILES
    dma = pltpu.SemaphoreType.DMA
    buffer = pltpu.VMEM((chunk_len, d_model), F32)
    box = jax.ShapeDtypeStruct((chunk_len, d_model), F32)
    hbm = pl.BlockSpec(memory_space=pl.ANY)
    vmem = pl.BlockSpec(memory_space=pltpu.VMEM)
    out, _, _, _, pk, qb, _ = pl.pallas_call(
        functools.partial(layer_kernel, tp_size, heads),
        in_specs=[pl.BlockSpec(memory_space=pltpu.SMEM)] + [hbm] * 8 + [vmem] * 5,
        out_specs=[hbm] * 7,
        out_shape=[
            jax.ShapeDtypeStruct((num_rows, chunk_len, d_model), BF16), box, box, box,
            jax.ShapeDtypeStruct((2, chunk_len, 3 * span), BF16),
            jax.ShapeDtypeStruct((2, chunk_len, 3 * span), F32),
            jax.ShapeDtypeStruct((2, chunk_len, span), F32),
        ],
        scratch_shapes=[buffer] * 3
        + [
            pltpu.VMEM((SLICES, d_model, width), BF16),
            pltpu.VMEM((SLICES, width, d_model), BF16),
            pltpu.VMEM((span, d_model), BF16),
            pltpu.VMEM((TILES, tile, 3 * span), BF16),
            pltpu.VMEM((2, tile, d_model), BF16),
            pltpu.VMEM((2,) + table.shape[1:], F32),
            pltpu.VMEM((2, 2, heads, slots, head_dim), BF16),
            pltpu.VMEM((chunk_len, span), F32),
            pltpu.VMEM((heads, half, head_dim), F32),
            pltpu.VMEM((heads, half, head_dim), F32),
            pltpu.VMEM((heads, half, head_dim), F32),
            pltpu.VMEM((4, 8, chunk_len), F32),
            pltpu.VMEM((3, 8, chunk_len), F32),
            pltpu.VMEM((4, STAGES, tokens, d_model), BF16),
            pltpu.VMEM((3, STAGES, tokens, d_model), F32),
        ]
        + [dma((SLICES,)), dma((SLICES,)), dma, dma((2,)), dma((2,)), dma((TILES,)), dma((TILES,)), dma((2, 2)), dma((heads,)),
           dma((2,)), dma((2, 2))]
        + [dma((2, TILES, 3))] * 2
        + [dma((HALVES,))] * 12
        + [dma((CHUNKS,))] * 5
        + [dma((5,)), dma((4, STAGES)), dma((3, STAGES))],
        compiler_params=pltpu.CompilerParams(collective_id=0, has_side_effects=True, vmem_limit_bytes=LAYER_LIMIT),
        cost_estimate=pl.CostEstimate(flops=100_000_000_000, bytes_accessed=chunk_len * d_model * 16, transcendentals=0),
        name="layer",
    )(lengths, hidden_in, table, k_block, v_block, w_qkv, w_up, w_down, w_out, *norms, small[None])
    return out, pk, qb


def finish_kernel(heads, meta, in_ref, pk, qb, out_ref, k_ref, v_ref, buf, low, high, in_sem, out_sem, low_sem, high_sem, kv_sem):
    pieces = in_sem.shape[1]
    tile = buf.shape[1] // pieces
    head_dim = k_ref.shape[3]
    places = [(b, pl.ds(t * tile, tile), t) for b in range(buf.shape[0]) for t in range(pieces)]
    inward = [pltpu.make_async_copy(in_ref.at[b, rows], buf.at[b, rows], in_sem.at[b, t]) for b, rows, t in places]
    outward = [pltpu.make_async_copy(buf.at[b, rows], out_ref.at[b, rows], out_sem.at[b, t]) for b, rows, t in places]
    both = 2 * head_dim

    def taken(src, dst, sem):
        return [[pltpu.make_async_copy(src.at[n, :, pl.ds((3 * h + 1) * head_dim, both)], dst.at[n, :, pl.ds(h * both, both)], sem.at[n, h])
                 for h in range(heads)] for n in range(2)]

    lows, highs = taken(pk, low, low_sem), taken(qb, high, high_sem)
    stored = []

    def store(n, h, row):
        for p, ref in enumerate((k_ref, v_ref)):
            cols = pl.ds(h * both + p * head_dim, head_dim)
            copy = pltpu.make_async_copy(low.at[n, :, cols], ref.at[row, h], kv_sem.at[n, h, p])
            copy.start()
            stored.append(copy)

    for copy in highs[0] + highs[1] + lows[0] + lows[1] + inward:
        copy.start()
    j = meta[0]
    for n in range(2):
        for h in range(heads):
            lows[n][h].wait()
            store(n, h, j ^ (2 - 2 * n))
    for n in range(2):
        for h in range(heads):
            highs[n][h].wait()
            cols = slice(h * both, (h + 1) * both)
            low[2 + n, :, cols] = high[n, :, cols].astype(BF16)
            store(2 + n, h, j ^ (3 - 2 * n))
    for one, other in zip(inward, outward):
        one.wait()
        other.start()
    for copy in outward + stored:
        copy.wait()


def finish(meta, out, pk, qb, heads, head_dim):
    rows, chunk_len, _ = out.shape
    span = 2 * heads * head_dim
    hbm = pl.BlockSpec(memory_space=pl.ANY)
    cache = jax.ShapeDtypeStruct((rows, heads, chunk_len, head_dim), BF16)
    dma = pltpu.SemaphoreType.DMA
    return pl.pallas_call(
        functools.partial(finish_kernel, heads),
        in_specs=[pl.BlockSpec(memory_space=pltpu.SMEM)] + [hbm] * 3,
        out_specs=[hbm] * 3,
        out_shape=[jax.ShapeDtypeStruct(out.shape, out.dtype), cache, cache],
        scratch_shapes=[
            pltpu.VMEM(out.shape, out.dtype), pltpu.VMEM((4, chunk_len, span), BF16), pltpu.VMEM((2, chunk_len, span), F32),
            dma((rows, 4)), dma((rows, 4)), dma((2, heads)), dma((2, heads)), dma((4, heads, 2)),
        ],
        compiler_params=pltpu.CompilerParams(vmem_limit_bytes=VMEM_LIMIT),
        name="finish",
    )(meta, out, pk, qb)


def solution(mesh):
    in_specs = (P("dp", None, None), P("dp"), P("dp", "tp", "cp", None), P("dp", "tp", "cp", None), P(), P(), P(), P(), P(None, "tp"), P("tp"), P("tp", None), P(), P(None, "tp"), P("tp"), P("tp", None), P())
    out_specs = (P("dp", None, None), P("dp", "tp", None, None), P("dp", "tp", None, None))
    tp_size = mesh.shape["tp"]

    def local_layer(hidden_in, lengths, k_block, v_block, ln1_gain, ln1_bias, ln2_gain, ln2_bias, w_qkv, b_qkv, w_out, b_out, w_up, b_up, w_down, b_down):
        num_rows, chunk_len, d_model = hidden_in.shape
        heads, block_len, head_dim = k_block.shape[1:]
        table = rope_table(lengths, chunk_len, head_dim)
        norms = [p[None] for p in (ln1_gain, ln1_bias, ln2_gain, ln2_bias)]
        small = jnp.concatenate([b_qkv.astype(F32), b_up.astype(F32), b_out.astype(F32) + b_down.astype(F32)])
        out, pk, qb = run_layer(lengths, hidden_in, table, k_block, v_block, w_qkv, w_up, w_down, w_out, norms, small, tp_size)
        return tuple(finish(lax.axis_index("cp")[None], out, pk, qb, heads, head_dim))

    return jax.shard_map(local_layer, mesh=mesh, in_specs=in_specs, out_specs=out_specs, check_vma=False)
```

```python
import functools
import math

import jax
import jax.numpy as jnp
from jax import lax
from jax.experimental import pallas as pl
from jax.experimental.pallas import tpu as pltpu
from jax.sharding import PartitionSpec as P

EPSILON = 1e-5
NEG_BIG = -1e30
ROTARY_SHARE = 4
ROPE_BASE = 10000.0
LOG2E = math.log2(math.e)
MESH = pl.DeviceIdType.MESH
F32 = jnp.float32
BF16 = jnp.bfloat16
VMEM_LIMIT = 60 * 1024 * 1024
LAYER_LIMIT = 67_043_328
EMPTY = -1e29
CHUNKS = 64
STAGES = 4
BLOCKS = 8
SLICES = 4
TILES = 4
HALVES = 4
LAG_START = 2
LAG_AHEAD = 1
LAG_BACK = 1
LAG_CORE = 2
LAG_Y = 5
LAG_LAST = 6


def layer_norm(values_in, gain_vec, bias_vec):
    x_f32 = values_in.astype(F32)
    row_mean = jnp.mean(x_f32, axis=-1, keepdims=True)
    centered = x_f32 - row_mean
    variance = jnp.mean(centered * centered, axis=-1, keepdims=True)
    return (centered * lax.rsqrt(variance + EPSILON) * gain_vec + bias_vec).astype(BF16)


def rope_tables(lengths, chunk_len, head_dim):
    rot_dim = head_dim // ROTARY_SHARE
    shape = (lengths.shape[0], rot_dim // 2, chunk_len)
    positions = lengths[:, None, None] + lax.broadcasted_iota(jnp.int32, shape, 2)
    inv_freq = ROPE_BASE ** (-2.0 * jnp.arange(rot_dim // 2, dtype=F32) / rot_dim)
    angles = positions.astype(F32) * inv_freq[:, None]
    return jnp.cos(angles), jnp.sin(angles)


def wide(column, lanes):
    return jnp.concatenate([column] * (lanes // column.shape[1]), axis=1)


def scores_of(query, keys, scale, mask):
    scores = lax.dot_general(query, keys, (((1,), (1,)), ((), ())), preferred_element_type=F32) * scale
    return scores if mask is None else jnp.where(mask, scores, NEG_BIG)


def lane_sum(values, lanes):
    return functools.reduce(jnp.add, [values[:, n:n + lanes] for n in range(0, values.shape[1], lanes)])


def lane_max(values, lanes):
    return functools.reduce(jnp.maximum, [values[:, n:n + lanes] for n in range(0, values.shape[1], lanes)])


def ahead(heads, scores):
    coming = scores(0)
    for h in range(heads):
        now = coming
        if h + 1 < heads:
            coming = scores(h + 1)
        yield h, now


def first_step(heads, scale, q_of, k_of, v_of, m_scr, l_scr, o_scr, mask):
    lanes = o_scr.shape[2]
    for h, scores in ahead(heads, lambda h: scores_of(q_of(h), k_of(h), scale, mask)):
        peak = jnp.maximum(jnp.max(lane_max(scores, lanes), axis=1, keepdims=True), EMPTY)
        peak = jnp.broadcast_to(peak, m_scr.shape[1:])
        probs = jnp.exp2(scores - wide(peak, scores.shape[1]))
        m_scr[h] = peak
        l_scr[h] = lane_sum(probs, lanes)
        o_scr[h] = jnp.dot(probs.astype(BF16), v_of(h), preferred_element_type=F32)


def block_step(heads, scale, q_of, k_of, v_of, m_scr, l_scr, o_scr, mask):
    lanes = o_scr.shape[2]
    for h, scores in ahead(heads, lambda h: scores_of(q_of(h), k_of(h), scale, mask)):
        m_old = m_scr[h]
        m_new = jnp.maximum(m_old, jnp.max(lane_max(scores, lanes), axis=1, keepdims=True))
        probs = jnp.exp2(scores - wide(m_new, scores.shape[1]))
        shrink = jnp.exp2(m_old - m_new)
        l_scr[h] = l_scr[h] * shrink + lane_sum(probs, lanes)
        m_scr[h] = m_new
        o_scr[h] = o_scr[h] * shrink + jnp.dot(probs.astype(BF16), v_of(h), preferred_element_type=F32)


def piece_weights(heads, stats, head_dim):
    peak = functools.reduce(jnp.maximum, [s[:heads] for s in stats])
    weights = [jnp.exp2(s[:heads] - peak) for s in stats]
    total = functools.reduce(jnp.add, [s[heads:2 * heads] * w for s, w in zip(stats, weights)])
    return peak, weights, total


def as_columns(parts, head_dim):
    count = sum(p.shape[0] for p in parts)
    return jnp.concatenate(parts + [jnp.zeros((head_dim - count, parts[0].shape[1]), F32)], axis=0).T


def layer_kernel(tp_size, heads, lengths, hidden, cos_all, sin_all, k_cache, v_cache, w_qkv, w_up, w_down, w_out,
                 gain1, bias1, gain2, bias2, small,
                 out_ref, y_box, core_box, last_box, pk, qb, ob,
                 acc, from_left, from_right, up, down, proj, mine, x_big, tab_buf, kv, ob_far, m_scr, l_scr, o_scr, st, sbox,
                 stage, land,
                 up_sem, down_sem, proj_sem, xb_sem, tab_sem, pk_sem, mine_sem, kv_sem, q_sem, x_sem, o_sem,
                 qs_sem, qr_sem, fs_sem, fr_sem, ns_sem, nr_sem, ys_sem, yr_sem,
                 fss_sem, fsr_sem, nss_sem, nsr_sem, yss_sem, ysr_sem,
                 left_sem, right_sem, y_sem, core_sem, last_sem, send_sem, stage_sem, land_sem):
    z = lax.axis_index("tp")
    j = lax.axis_index("cp")
    y, c = lax.div(j, 2), lax.rem(j, 2)
    across, mate, corner = (1 - y) * 2 + c, y * 2 + (1 - c), (1 - y) * 2 + (1 - c)
    chunk_len, d_model = acc.shape
    head_dim = o_scr.shape[2]
    span = heads * head_dim
    slots = k_cache.shape[2]
    tokens = chunk_len // CHUNKS
    block = chunk_len // BLOCKS
    half = chunk_len // HALVES
    tile = chunk_len // TILES
    pairs = CHUNKS // 2
    per_block = pairs // BLOCKS
    width = up.shape[2]
    last = tp_size - 1
    root_a, root_b = (tp_size - 1) // 2, tp_size // 2
    rot_dim = head_dim // ROTARY_SHARE
    half_rot = rot_dim // 2
    scale = head_dim ** -0.5 * LOG2E
    own_at, sent_at, kept_at, q_at = 0, span, 2 * span, 3 * span
    extra_at = 3 * span + SLICES * width
    per_half = BLOCKS // HALVES
    waited = per_half * SLICES

    def rows_of(n, size):
        return pl.ds(pl.multiple_of(n * size, size), size)

    def weight_copies(f):
        cols = pl.ds(f * width, width)
        return (pltpu.make_async_copy(w_up.at[:, cols], up.at[f], up_sem.at[f]),
                pltpu.make_async_copy(w_down.at[cols, :], down.at[f], down_sem.at[f]))

    def row_of(n):
        return across * (1 - n) + j * n

    def big_x(i):
        return pltpu.make_async_copy(
            hidden.at[row_of(lax.div(i, TILES)), rows_of(lax.rem(i, TILES), tile), :], x_big.at[lax.rem(i, 2)], xb_sem.at[lax.rem(i, 2)])

    def cache_copies(row, slot):
        return (pltpu.make_async_copy(k_cache.at[row], kv.at[slot, 0], kv_sem.at[slot, 0]),
                pltpu.make_async_copy(v_cache.at[row], kv.at[slot, 1], kv_sem.at[slot, 1]))

    def start(copies):
        for copy in copies:
            copy.start()

    def wait(copies):
        for copy in copies:
            copy.wait()

    qkv_copies = [pltpu.make_async_copy(w_qkv.at[:, pl.ds(s * width, width)], up.at[s], up_sem.at[s]) for s in range(3)]
    tab_copies = [pltpu.make_async_copy(ref.at[row], tab_buf.at[n, p], tab_sem.at[n, p])
                  for n, row in enumerate((across, j)) for p, ref in enumerate((cos_all, sin_all))]
    proj_copy = pltpu.make_async_copy(w_out, proj, proj_sem)
    big_x(0).start()
    start(qkv_copies)
    start(tab_copies)
    start(cache_copies(corner, 0))
    start(cache_copies(across, 1))
    proj_copy.start()

    barrier = pltpu.get_barrier_semaphore()
    pl.semaphore_signal(barrier, inc=1, device_id={"cp": across}, device_id_type=MESH)
    pl.semaphore_signal(barrier, inc=1, device_id={"cp": mate}, device_id_type=MESH)

    @pl.when(z > 0)
    def _():
        pl.semaphore_signal(barrier, inc=1, device_id={"tp": z - 1}, device_id_type=MESH)

    @pl.when(z < last)
    def _():
        pl.semaphore_signal(barrier, inc=1, device_id={"tp": z + 1}, device_id_type=MESH)

    inside = jnp.logical_and(z > 0, z < last)

    @pl.when(inside)
    def _():
        pl.semaphore_wait(barrier, 4)

    @pl.when(jnp.logical_not(inside))
    def _():
        pl.semaphore_wait(barrier, 3)

    def to_core(src, dst, send, arrive):
        return pltpu.make_async_remote_copy(
            src_ref=src, dst_ref=dst, send_sem=send, recv_sem=arrive, device_id={"cp": mate}, device_id_type=MESH)

    def to_y(src, dst, send, arrive):
        return pltpu.make_async_remote_copy(
            src_ref=src, dst_ref=dst, send_sem=send, recv_sem=arrive, device_id={"cp": across}, device_id_type=MESH)


    def staged(t, part):
        return acc.at[rows_of(t, tile), pl.ds(part * span, span)]

    def sent_tile(n, t):
        return [to_core(staged(t, p), qb.at[n, rows_of(t, tile), pl.ds(p * span, span)], qs_sem.at[n, t, p], qr_sem.at[n, t, p])
                for p in range(3)]

    def sent_off(n, t):
        for copy in sent_tile(n, t):
            copy.wait_send()

    def project(n, t, place):
        i = n * TILES + t

        @pl.when(i + 1 < 2 * TILES)
        def _():
            big_x(i + 1).start()

        big_x(i).wait()
        if n == 1:
            sent_off(0, t)
        normed = layer_norm(x_big[lax.rem(i, 2)], gain1[...], bias1[...])
        cos_part, sin_part = tab_buf[n, 0, :, rows_of(t, tile)], tab_buf[n, 1, :, rows_of(t, tile)]
        tab = jnp.concatenate([cos_part, cos_part, -sin_part, sin_part] * (head_dim // (4 * half_rot)), axis=0).T
        lane = lax.broadcasted_iota(jnp.int32, tab.shape, 1)
        cos_tab = jnp.where(lane < rot_dim, tab, 1.0)
        sin_tab = jnp.where(lane < rot_dim, pltpu.roll(tab, head_dim - rot_dim, 1), 0.0)

        def rotate(values):
            long = values.astype(F32)
            other = jnp.where(lane < half_rot, pltpu.roll(long, head_dim - half_rot, 1), pltpu.roll(long, half_rot, 1))
            return (long * cos_tab + other * sin_tab).astype(BF16)

        for p, product in ahead(3, lambda p: jnp.dot(normed, up[p], preferred_element_type=F32)):
            some = (product + small[:, p * span:(p + 1) * span]).astype(BF16)
            for g in range(heads):
                group = p * heads + g
                values = some[:, g * head_dim:(g + 1) * head_dim]
                if group % 3 < 2:
                    values = rotate(values)
                place[:, group * head_dim:(group + 1) * head_dim] = values
                staged(t, p)[:, g * head_dim:(g + 1) * head_dim] = values.astype(F32)
        start(sent_tile(n, t))

    def arrived_tiles(n):
        for t in range(TILES):
            for copy in sent_tile(n, t):
                copy.wait_recv()

    def query_copies(n):
        return [pltpu.make_async_copy(qb.at[n, :, pl.ds(3 * h * head_dim, head_dim)],
                                      acc.at[:, pl.ds(q_at + h * head_dim, head_dim)], q_sem.at[h]) for h in range(heads)]

    per_slice = width // tile

    def far_place(t):
        return down.at[lax.div(t, per_slice), rows_of(lax.rem(t, per_slice), tile), pl.ds(0, 3 * span)]

    def mine_out(t):
        return pltpu.make_async_copy(mine.at[t], pk.at[1, rows_of(t, tile), :], mine_sem.at[t])

    wait(qkv_copies)
    wait(tab_copies)

    @pl.loop(0, TILES)
    def _(t):
        project(0, t, far_place(t))

    pack_copies = [pltpu.make_async_copy(far_place(t), pk.at[0, rows_of(t, tile), :], pk_sem.at[t]) for t in range(TILES)]
    start(pack_copies)

    @pl.loop(0, TILES)
    def _(t):
        @pl.when(t == TILES // 2)
        def _():
            arrived_tiles(0)
            start(query_copies(0))

        project(1, t, mine.at[t])
        mine_out(t).start()

    for f in range(SLICES):
        weight_copies(f)[0].start()


    def attend(row, slot, query, e):
        valid = jnp.clip(lengths[row] - j * slots, 0, slots)
        mask = lax.broadcasted_iota(jnp.int32, (half, slots), 1) < valid
        first_step(heads, scale, lambda h: query(e, h), lambda h: kv[slot, 0, h], lambda h: kv[slot, 1, h],
                   m_scr, l_scr, o_scr, mask)

    def attend_own(e):
        def own_block(b, mask):
            def part(p):
                return lambda h: mine[b, :, (3 * h + p) * head_dim:(3 * h + p + 1) * head_dim]

            block_step(heads, scale, lambda h: held_mine(e, h), part(1), part(2), m_scr, l_scr, o_scr, mask)

        @pl.loop(0, e)
        def _(b):
            own_block(b, None)

        shape = (half, half)
        own_block(e, lax.broadcasted_iota(jnp.int32, shape, 0) >= lax.broadcasted_iota(jnp.int32, shape, 1))

    def keep(e, at, kind):
        lane = lax.broadcasted_iota(jnp.int32, (half, head_dim), 1)
        stats = jnp.zeros((half, head_dim), F32)
        for h in range(heads):
            stats = jnp.where(lane == h, m_scr[h], stats)
            stats = jnp.where(lane == heads + h, jnp.sum(l_scr[h], axis=1, keepdims=True), stats)
            acc[rows_of(e, half), at + h * head_dim:at + (h + 1) * head_dim] = o_scr[h]
        st[kind, :, rows_of(e, half)] = stats.T[:8]

    def held_far(e, h):
        return far_place(e)[:, 3 * h * head_dim:(3 * h + 1) * head_dim]

    def held_mine(e, h):
        return mine[e, :, 3 * h * head_dim:(3 * h + 1) * head_dim]

    def taken(e, h):
        return acc[rows_of(e, half), q_at + h * head_dim:q_at + (h + 1) * head_dim].astype(BF16)

    def far_piece(e):
        return to_core(acc.at[rows_of(e, half), pl.ds(sent_at, span)], ob_far.at[rows_of(e, half), :], fs_sem.at[e], fr_sem.at[e])

    def near_piece(e):
        return to_core(acc.at[rows_of(e, half), pl.ds(sent_at, span)], ob.at[0, rows_of(e, half), :], ns_sem.at[e], nr_sem.at[e])

    def y_piece(e):
        return to_y(acc.at[rows_of(e, half), pl.ds(kept_at, span)], ob.at[1, rows_of(e, half), :], ys_sem.at[e], yr_sem.at[e])

    def far_stats(e):
        return to_core(st.at[0, :, rows_of(e, half)], sbox.at[0, :, rows_of(e, half)], fss_sem.at[e], fsr_sem.at[e])

    def near_stats(e):
        return to_core(st.at[2, :, rows_of(e, half)], sbox.at[1, :, rows_of(e, half)], nss_sem.at[e], nsr_sem.at[e])

    def y_stats(e):
        return to_y(st.at[1, :, rows_of(e, half)], sbox.at[2, :, rows_of(e, half)], yss_sem.at[e], ysr_sem.at[e])

    wait(query_copies(0))
    wait(cache_copies(corner, 0))
    wait(cache_copies(across, 1))

    @pl.loop(0, HALVES)
    def _(e):
        sent_off(1, e)
        attend(corner, 0, taken, e)
        keep(e, sent_at, 0)
        far_stats(e).start()
        far_piece(e).start()

        @pl.when(e == HALVES - 1)
        def _():
            start(cache_copies(mate, 0))
            arrived_tiles(1)
            start(query_copies(1))

        attend(across, 1, held_far, e)
        keep(e, kept_at, 1)

        far_stats(e).wait_recv()
        far_piece(e).wait_recv()
        rows = rows_of(e, half)
        peak, weights, total = piece_weights(heads, [st[1, :, rows], sbox[0, :, rows]], head_dim)
        columns = as_columns(weights, head_dim)
        for h in range(heads):
            at = kept_at + h * head_dim
            acc[rows, at:at + head_dim] = (acc[rows, at:at + head_dim] * columns[:, h:h + 1]
                                           + ob_far[rows, h * head_dim:(h + 1) * head_dim] * columns[:, heads + h:heads + h + 1])
        st[1, :heads, rows] = peak
        st[1, heads:2 * heads, rows] = total
        y_stats(e).start()
        y_piece(e).start()

    start(cache_copies(j, 1))
    wait(pack_copies)
    for f in range(SLICES):
        weight_copies(f)[1].start()
    for e in range(HALVES):
        far_stats(e).wait_send()
        far_piece(e).wait_send()
    wait(query_copies(1))
    wait(cache_copies(mate, 0))


    def near(e, phase):
        @pl.when(phase == 5)
        def _():
            attend(mate, 0, taken, e)
            keep(e, sent_at, 2)
            near_stats(e).start()
            near_piece(e).start()

            @pl.when(e == 0)
            def _():
                wait(cache_copies(j, 1))

        @pl.when(phase == 6)
        def _():
            attend(j, 1, held_mine, e)

        @pl.when(phase == 7)
        def _():
            attend_own(e)
            keep(e, own_at, 3)

            @pl.when(e == 0)
            def _():
                proj_copy.wait()

    def block_copies(b):
        rows = rows_of(b, block)
        slot = lax.rem(b, 2)
        return [pltpu.make_async_copy(hidden.at[j, rows, :], x_big.at[slot, pl.ds(0, block), :], x_sem.at[slot])] + [
            pltpu.make_async_copy(ob.at[n, rows, :], ob_far.at[rows_of(2 * slot + n, block), :], o_sem.at[slot, n]) for n in range(2)]

    def fetch(b):
        @pl.when(lax.rem(b, per_half) == 0)
        def _():
            e = lax.div(b, per_half)
            near_stats(e).wait_recv()
            near_piece(e).wait_recv()
            y_stats(e).wait_recv()
            y_piece(e).wait_recv()

        start(block_copies(b))

    def begin(b):
        slot = lax.rem(b, 2)
        rows = rows_of(b, block)

        wait(block_copies(b))

        @pl.when(lax.rem(b, per_half) == 0)
        def _():
            e = lax.div(b, per_half)
            for copy in (near_stats(e), near_piece(e), y_stats(e), y_piece(e)):
                copy.wait_send()

        _, weights, total = piece_weights(heads, [st[3, :, rows], sbox[1, :, rows], sbox[2, :, rows]], head_dim)
        columns = as_columns([w / total for w in weights], head_dim)
        for h in range(heads):
            cols = slice(h * head_dim, (h + 1) * head_dim)
            pieces = [acc[rows, own_at + h * head_dim:own_at + (h + 1) * head_dim]]
            pieces += [ob_far[rows_of(2 * slot + n, block), cols] for n in range(2)]
            context = functools.reduce(
                jnp.add, [o * columns[:, n * heads + h:n * heads + h + 1] for n, o in enumerate(pieces)])
            x_big[1, block:2 * block, cols] = context.astype(BF16)
        x = x_big[slot, :block, :]
        x_big[0, block:2 * block, :] = layer_norm(x, gain2[...], bias2[...])
        acc[rows, :] = jnp.dot(x_big[1, block:2 * block, :span], proj[...], preferred_element_type=F32)

        @pl.when(z == 0)
        def _():
            acc[rows, :] += x.astype(F32) + small[:, extra_at:]

    def slice_of(b, f):
        rows = rows_of(b, block)

        @pl.when(b == 0)
        def _():
            wait(weight_copies(f))

        b_up = small[:, pl.ds(pl.multiple_of(3 * span + f * width, width), width)]
        wide_h = jnp.dot(x_big[0, block:2 * block, :], up[f], preferred_element_type=F32) + b_up
        act = (0.5 * wide_h * (1.0 + lax.erf(wide_h * math.sqrt(0.5)))).astype(BF16)
        acc[rows, :] += jnp.dot(act, down[f], preferred_element_type=F32)


    def at(ref, k):
        return ref.at[pl.ds(pl.multiple_of(k * tokens, tokens), tokens), :]

    def remote(src, dst, k, which, arrive, device):
        return pltpu.make_async_remote_copy(
            src_ref=at(src, k), dst_ref=at(dst, k), send_sem=send_sem.at[which], recv_sem=arrive.at[k],
            device_id=device, device_id_type=MESH,
        )

    def send_right(src, k):
        remote(src, from_left, k, 0, left_sem, {"tp": z + 1}).start()

    def send_left(src, k):
        remote(src, from_right, k, 1, right_sem, {"tp": z - 1}).start()

    def arrived(ref, sem, k):
        remote(ref, ref, k, 0, sem, {"cp": j}).wait_recv()

    def drained(ref, which):
        pltpu.make_async_copy(ref, ref, send_sem.at[which]).wait()

    def emit(stream, values, k, row):
        slot = lax.rem(k, STAGES)

        def copy():
            return pltpu.make_async_copy(stage.at[stream, slot], at(out_ref.at[row], k), stage_sem.at[stream, slot])

        @pl.when(k >= STAGES)
        def _():
            copy().wait()

        stage[stream, slot] = values.astype(BF16)
        copy().start()

    def chunk(ref, k):
        return ref[pl.ds(pl.multiple_of(k * tokens, tokens), tokens), :]

    def finish(src, k):
        remote(src, y_box, k, 2, y_sem, {"cp": across}).start()
        remote(src, core_box, k, 3, core_sem, {"cp": mate}).start()
        emit(0, chunk(src, k), k, j)

    def landing(n, box, k):
        slot = lax.rem(k, STAGES)
        return pltpu.make_async_copy(at(box, k), land.at[n, slot], land_sem.at[n, slot])

    def gathered(i):
        def lagged(lag, act):
            @pl.when(jnp.logical_and(i >= lag, i < pairs + lag))
            def _():
                for n in range(2):
                    act((i - lag) * 2 + n)

        def core(k):
            arrived(core_box, core_sem, k)
            landing(0, core_box, k).start()

        def core_out(k):
            landing(0, core_box, k).wait()
            emit(1, land[0, lax.rem(k, STAGES)], k, mate)

        def side(k):
            arrived(y_box, y_sem, k)
            remote(y_box, last_box, k, 4, last_sem, {"cp": mate}).start()
            landing(2, y_box, k).start()

        def side_out(k):
            landing(2, y_box, k).wait()
            emit(2, land[2, lax.rem(k, STAGES)], k, across)

        def final(k):
            arrived(last_box, last_sem, k)
            landing(1, last_box, k).start()

        def final_out(k):
            landing(1, last_box, k).wait()
            emit(3, land[1, lax.rem(k, STAGES)], k, corner)

        lagged(LAG_CORE + 1, core_out)
        lagged(LAG_Y + 1, side_out)
        lagged(LAG_LAST + 1, final_out)
        lagged(LAG_CORE, core)
        lagged(LAG_Y, side)
        lagged(LAG_LAST, final)

    def add(k, *others):
        rows = pl.ds(pl.multiple_of(k * tokens, tokens), tokens)
        total = acc[rows, :]
        for other in others:
            total = total + other[rows, :]
        acc[rows, :] = total

    def when(cond, act, *args):
        @pl.when(cond)
        def _():
            act(*args)

    def end(i, first):
        inbox, sem = (from_right, right_sem) if first else (from_left, left_sem)
        near_bit = 0 if first else 1

        def got(k):
            arrived(inbox, sem, k)
            finish(inbox, k)

        when(jnp.logical_and(i >= 0, i < pairs), lambda: got(2 * i + near_bit))
        when(jnp.logical_and(i >= LAG_BACK, i < pairs + LAG_BACK), lambda: got(2 * (i - LAG_BACK) + 1 - near_bit))

    def inner(i, left_side):
        mine = 0 if left_side else 1
        if left_side:
            (outer, outer_sem, to_outer), (inward, inward_sem, to_inner) = (
                (from_left, left_sem, send_left), (from_right, right_sem, send_right))
        else:
            (outer, outer_sem, to_outer), (inward, inward_sem, to_inner) = (
                (from_right, right_sem, send_right), (from_left, left_sem, send_left))

        def early(p):
            passed = 2 * p + 1 - mine
            arrived(outer, outer_sem, passed)
            add(passed, outer)
            to_inner(acc, passed)

        def near(p):
            rooted = 2 * p + mine
            arrived(outer, outer_sem, rooted)
            arrived(inward, inward_sem, rooted)
            add(rooted, from_left, from_right)
            to_outer(acc, rooted)
            to_inner(acc, rooted)
            finish(acc, rooted)

        def far(p):
            k = 2 * p + 1 - mine
            arrived(inward, inward_sem, k)
            to_outer(inward, k)
            finish(inward, k)

        when(jnp.logical_and(i + LAG_AHEAD >= 0, i + LAG_AHEAD < pairs), early, i + LAG_AHEAD)
        when(jnp.logical_and(i >= 0, i < pairs), near, i)
        when(jnp.logical_and(i >= LAG_BACK, i < pairs + LAG_BACK), far, i - LAG_BACK)

    lead = SLICES + LAG_START

    @pl.loop(0, waited + lead + pairs + LAG_LAST + 2)
    def _(step):
        s = step - waited

        @pl.when(step < HALVES * waited)
        def _():
            near(lax.div(step, waited), lax.rem(step, waited))

        @pl.when(step == waited - 2)
        def _():
            fetch(0)

        @pl.when(jnp.logical_and(s >= 0, s < BLOCKS * SLICES))
        def _():
            b, f = lax.div(s, SLICES), lax.rem(s, SLICES)
            when(f == 0, begin, b)
            when(jnp.logical_and(f == SLICES - 1, b + 1 < BLOCKS), fetch, b + 1)
            slice_of(b, f)

            def push(send):
                @pl.loop(0, 2 * per_block)
                def _(n):
                    send(acc, b * 2 * per_block + n)

            when(jnp.logical_and(f == SLICES - 1, z == 0), push, send_right)
            when(jnp.logical_and(f == SLICES - 1, z == last), push, send_left)

        i = s - lead
        when(z == 0, end, i, True)
        when(z == root_a, inner, i, True)
        when(z == root_b, inner, i, False)
        when(z == last, end, i, False)
        gathered(i)

    @pl.when(z < last)
    def _():
        drained(acc, 0)

    @pl.when(z > 0)
    def _():
        drained(acc, 1)

    for which in (2, 3, 4):
        drained(acc, which)
    for t in range(TILES):
        mine_out(t).wait()
    for stream in range(4):
        for slot in range(STAGES):
            pltpu.make_async_copy(stage.at[stream, slot], at(out_ref.at[0], 0), stage_sem.at[stream, slot]).wait()


def run_layer(lengths, hidden_in, tables, k_block, v_block, w_qkv, w_up, w_down, w_out, norms, small, tp_size):
    num_rows, chunk_len, d_model = hidden_in.shape
    heads, slots, head_dim = k_block.shape[1:]
    span = heads * head_dim
    width = w_up.shape[1] // SLICES
    tokens = chunk_len // CHUNKS
    block = chunk_len // BLOCKS
    half = chunk_len // HALVES
    tile = chunk_len // TILES
    dma = pltpu.SemaphoreType.DMA
    buffer = pltpu.VMEM((chunk_len, d_model), F32)
    box = jax.ShapeDtypeStruct((chunk_len, d_model), F32)
    hbm = pl.BlockSpec(memory_space=pl.ANY)
    vmem = pl.BlockSpec(memory_space=pltpu.VMEM)
    out, _, _, _, pk, qb, _ = pl.pallas_call(
        functools.partial(layer_kernel, tp_size, heads),
        in_specs=[pl.BlockSpec(memory_space=pltpu.SMEM)] + [hbm] * 9 + [vmem] * 5,
        out_specs=[hbm] * 7,
        out_shape=[
            jax.ShapeDtypeStruct((num_rows, chunk_len, d_model), BF16), box, box, box,
            jax.ShapeDtypeStruct((2, chunk_len, 3 * span), BF16),
            jax.ShapeDtypeStruct((2, chunk_len, 3 * span), F32),
            jax.ShapeDtypeStruct((2, chunk_len, span), F32),
        ],
        scratch_shapes=[buffer] * 3
        + [
            pltpu.VMEM((SLICES, d_model, width), BF16),
            pltpu.VMEM((SLICES, width, d_model), BF16),
            pltpu.VMEM((span, d_model), BF16),
            pltpu.VMEM((TILES, tile, 3 * span), BF16),
            pltpu.VMEM((2, tile, d_model), BF16),
            pltpu.VMEM((2, 2) + tables[0].shape[1:], F32),
            pltpu.VMEM((2, 2, heads, slots, head_dim), BF16),
            pltpu.VMEM((chunk_len, span), F32),
            pltpu.VMEM((heads, half, head_dim), F32),
            pltpu.VMEM((heads, half, head_dim), F32),
            pltpu.VMEM((heads, half, head_dim), F32),
            pltpu.VMEM((4, 8, chunk_len), F32),
            pltpu.VMEM((3, 8, chunk_len), F32),
            pltpu.VMEM((4, STAGES, tokens, d_model), BF16),
            pltpu.VMEM((3, STAGES, tokens, d_model), F32),
        ]
        + [dma((SLICES,)), dma((SLICES,)), dma, dma((2,)), dma((2, 2)), dma((TILES,)), dma((TILES,)), dma((2, 2)), dma((heads,)),
           dma((2,)), dma((2, 2))]
        + [dma((2, TILES, 3))] * 2
        + [dma((HALVES,))] * 12
        + [dma((CHUNKS,))] * 5
        + [dma((5,)), dma((4, STAGES)), dma((3, STAGES))],
        compiler_params=pltpu.CompilerParams(collective_id=0, has_side_effects=True, vmem_limit_bytes=LAYER_LIMIT),
        cost_estimate=pl.CostEstimate(flops=100_000_000_000, bytes_accessed=chunk_len * d_model * 16, transcendentals=0),
        name="layer",
    )(lengths, hidden_in, *tables, k_block, v_block, w_qkv, w_up, w_down, w_out, *norms, small[None])
    return out, pk, qb


def finish_kernel(heads, meta, in_ref, pk, qb, out_ref, k_ref, v_ref, buf, low, high, in_sem, out_sem, low_sem, high_sem, kv_sem):
    pieces = in_sem.shape[1]
    tile = buf.shape[1] // pieces
    head_dim = k_ref.shape[3]
    places = [(b, pl.ds(t * tile, tile), t) for b in range(buf.shape[0]) for t in range(pieces)]
    inward = [pltpu.make_async_copy(in_ref.at[b, rows], buf.at[b, rows], in_sem.at[b, t]) for b, rows, t in places]
    outward = [pltpu.make_async_copy(buf.at[b, rows], out_ref.at[b, rows], out_sem.at[b, t]) for b, rows, t in places]
    both = 2 * head_dim

    def taken(src, dst, sem):
        return [[pltpu.make_async_copy(src.at[n, :, pl.ds((3 * h + 1) * head_dim, both)], dst.at[n, :, pl.ds(h * both, both)], sem.at[n, h])
                 for h in range(heads)] for n in range(2)]

    lows, highs = taken(pk, low, low_sem), taken(qb, high, high_sem)
    stored = []

    def store(n, h, row):
        for p, ref in enumerate((k_ref, v_ref)):
            cols = pl.ds(h * both + p * head_dim, head_dim)
            copy = pltpu.make_async_copy(low.at[n, :, cols], ref.at[row, h], kv_sem.at[n, h, p])
            copy.start()
            stored.append(copy)

    for copy in highs[0] + highs[1] + lows[0] + lows[1] + inward:
        copy.start()
    j = meta[0]
    for n in range(2):
        for h in range(heads):
            lows[n][h].wait()
            store(n, h, j ^ (2 - 2 * n))
    for n in range(2):
        for h in range(heads):
            highs[n][h].wait()
            cols = slice(h * both, (h + 1) * both)
            low[2 + n, :, cols] = high[n, :, cols].astype(BF16)
            store(2 + n, h, j ^ (3 - 2 * n))
    for one, other in zip(inward, outward):
        one.wait()
        other.start()
    for copy in outward + stored:
        copy.wait()


def finish(meta, out, pk, qb, heads, head_dim):
    rows, chunk_len, _ = out.shape
    span = 2 * heads * head_dim
    hbm = pl.BlockSpec(memory_space=pl.ANY)
    cache = jax.ShapeDtypeStruct((rows, heads, chunk_len, head_dim), BF16)
    dma = pltpu.SemaphoreType.DMA
    return pl.pallas_call(
        functools.partial(finish_kernel, heads),
        in_specs=[pl.BlockSpec(memory_space=pltpu.SMEM)] + [hbm] * 3,
        out_specs=[hbm] * 3,
        out_shape=[jax.ShapeDtypeStruct(out.shape, out.dtype), cache, cache],
        scratch_shapes=[
            pltpu.VMEM(out.shape, out.dtype), pltpu.VMEM((4, chunk_len, span), BF16), pltpu.VMEM((2, chunk_len, span), F32),
            dma((rows, 4)), dma((rows, 4)), dma((2, heads)), dma((2, heads)), dma((4, heads, 2)),
        ],
        compiler_params=pltpu.CompilerParams(vmem_limit_bytes=VMEM_LIMIT),
        name="finish",
    )(meta, out, pk, qb)


def solution(mesh):
    in_specs = (P("dp", None, None), P("dp"), P("dp", "tp", "cp", None), P("dp", "tp", "cp", None), P(), P(), P(), P(), P(None, "tp"), P("tp"), P("tp", None), P(), P(None, "tp"), P("tp"), P("tp", None), P())
    out_specs = (P("dp", None, None), P("dp", "tp", None, None), P("dp", "tp", None, None))
    tp_size = mesh.shape["tp"]

    def local_layer(hidden_in, lengths, k_block, v_block, ln1_gain, ln1_bias, ln2_gain, ln2_bias, w_qkv, b_qkv, w_out, b_out, w_up, b_up, w_down, b_down):
        num_rows, chunk_len, d_model = hidden_in.shape
        heads, block_len, head_dim = k_block.shape[1:]
        tables = rope_tables(lengths, chunk_len, head_dim)
        norms = [p[None] for p in (ln1_gain, ln1_bias, ln2_gain, ln2_bias)]
        parts = [(b_qkv, 0), (b_up, b_qkv.shape[0]), (b_out, b_qkv.shape[0] + b_up.shape[0]), (b_down, b_qkv.shape[0] + b_up.shape[0])]
        total = b_qkv.shape[0] + b_up.shape[0] + d_model
        small = functools.reduce(jnp.add, [jnp.pad(p.astype(F32), (at, total - at - p.shape[0])) for p, at in parts])
        out, pk, qb = run_layer(lengths, hidden_in, tables, k_block, v_block, w_qkv, w_up, w_down, w_out, norms, small, tp_size)
        return tuple(finish(lax.axis_index("cp")[None], out, pk, qb, heads, head_dim))

    return jax.shard_map(local_layer, mesh=mesh, in_specs=in_specs, out_specs=out_specs, check_vma=False)
```

```python
import functools
import math

import jax
import jax.numpy as jnp
from jax import lax
from jax.experimental import pallas as pl
from jax.experimental.pallas import tpu as pltpu
from jax.sharding import PartitionSpec as P

EPSILON = 1e-5
NEG_BIG = -1e30
ROTARY_SHARE = 4
ROPE_BASE = 10000.0
LOG2E = math.log2(math.e)
MESH = pl.DeviceIdType.MESH
F32 = jnp.float32
BF16 = jnp.bfloat16
VMEM_LIMIT = 60 * 1024 * 1024
LAYER_LIMIT = 67_043_328
EMPTY = -1e29
CHUNKS = 64
STAGES = 4
BLOCKS = 8
SLICES = 4
TILES = 4
HALVES = 4
LAG_START = 2
LAG_AHEAD = 1
LAG_BACK = 1
LAG_CORE = 2
LAG_Y = 5
LAG_LAST = 6


def layer_norm(values_in, gain_vec, bias_vec):
    x_f32 = values_in.astype(F32)
    row_mean = jnp.mean(x_f32, axis=-1, keepdims=True)
    centered = x_f32 - row_mean
    variance = jnp.mean(centered * centered, axis=-1, keepdims=True)
    return (centered * lax.rsqrt(variance + EPSILON) * gain_vec + bias_vec).astype(BF16)


def rope_tables(lengths, chunk_len, head_dim):
    rot_dim = head_dim // ROTARY_SHARE
    positions = lengths[:, None] + jnp.arange(chunk_len, dtype=jnp.int32)[None, :]
    inv_freq = ROPE_BASE ** (-2.0 * jnp.arange(rot_dim // 2, dtype=F32) / rot_dim)
    angles = positions.astype(F32)[:, None, :] * inv_freq[:, None]
    return jnp.cos(angles), jnp.sin(angles)


def wide(column, lanes):
    return jnp.concatenate([column] * (lanes // column.shape[1]), axis=1)


def scores_of(query, keys, scale, mask):
    scores = lax.dot_general(query, keys, (((1,), (1,)), ((), ())), preferred_element_type=F32) * scale
    return scores if mask is None else jnp.where(mask, scores, NEG_BIG)


def lane_sum(values, lanes):
    return functools.reduce(jnp.add, [values[:, n:n + lanes] for n in range(0, values.shape[1], lanes)])


def lane_max(values, lanes):
    return functools.reduce(jnp.maximum, [values[:, n:n + lanes] for n in range(0, values.shape[1], lanes)])


def ahead(heads, scores):
    coming = scores(0)
    for h in range(heads):
        now = coming
        if h + 1 < heads:
            coming = scores(h + 1)
        yield h, now


def first_step(heads, scale, q_of, k_of, v_of, m_scr, l_scr, o_scr, mask):
    lanes = o_scr.shape[2]
    for h, scores in ahead(heads, lambda h: scores_of(q_of(h), k_of(h), scale, mask)):
        peak = jnp.maximum(jnp.max(lane_max(scores, lanes), axis=1, keepdims=True), EMPTY)
        peak = jnp.broadcast_to(peak, m_scr.shape[1:])
        probs = jnp.exp2(scores - wide(peak, scores.shape[1]))
        m_scr[h] = peak
        l_scr[h] = lane_sum(probs, lanes)
        o_scr[h] = jnp.dot(probs.astype(BF16), v_of(h), preferred_element_type=F32)


def block_step(heads, scale, q_of, k_of, v_of, m_scr, l_scr, o_scr, mask):
    lanes = o_scr.shape[2]
    for h, scores in ahead(heads, lambda h: scores_of(q_of(h), k_of(h), scale, mask)):
        m_old = m_scr[h]
        m_new = jnp.maximum(m_old, jnp.max(lane_max(scores, lanes), axis=1, keepdims=True))
        probs = jnp.exp2(scores - wide(m_new, scores.shape[1]))
        shrink = jnp.exp2(m_old - m_new)
        l_scr[h] = l_scr[h] * shrink + lane_sum(probs, lanes)
        m_scr[h] = m_new
        o_scr[h] = o_scr[h] * shrink + jnp.dot(probs.astype(BF16), v_of(h), preferred_element_type=F32)


def piece_weights(heads, stats, head_dim):
    peak = functools.reduce(jnp.maximum, [s[:heads] for s in stats])
    weights = [jnp.exp2(s[:heads] - peak) for s in stats]
    total = functools.reduce(jnp.add, [s[heads:2 * heads] * w for s, w in zip(stats, weights)])
    return peak, weights, total


def as_columns(parts, head_dim):
    count = sum(p.shape[0] for p in parts)
    return jnp.concatenate(parts + [jnp.zeros((head_dim - count, parts[0].shape[1]), F32)], axis=0).T


def layer_kernel(tp_size, heads, lengths, hidden, cos_all, sin_all, k_cache, v_cache, w_qkv, w_up, w_down, w_out,
                 gain1, bias1, gain2, bias2, small,
                 out_ref, y_box, core_box, last_box, pk, qb, ob,
                 acc, from_left, from_right, up, down, proj, mine, x_big, tab_buf, kv, ob_far, m_scr, l_scr, o_scr, st, sbox,
                 stage, land,
                 up_sem, down_sem, proj_sem, xb_sem, tab_sem, pk_sem, mine_sem, kv_sem, q_sem, x_sem, o_sem,
                 qs_sem, qr_sem, fs_sem, fr_sem, ns_sem, nr_sem, ys_sem, yr_sem,
                 fss_sem, fsr_sem, nss_sem, nsr_sem, yss_sem, ysr_sem,
                 left_sem, right_sem, y_sem, core_sem, last_sem, send_sem, stage_sem, land_sem):
    z = lax.axis_index("tp")
    j = lax.axis_index("cp")
    y, c = lax.div(j, 2), lax.rem(j, 2)
    across, mate, corner = (1 - y) * 2 + c, y * 2 + (1 - c), (1 - y) * 2 + (1 - c)
    chunk_len, d_model = acc.shape
    head_dim = o_scr.shape[2]
    span = heads * head_dim
    slots = k_cache.shape[2]
    tokens = chunk_len // CHUNKS
    block = chunk_len // BLOCKS
    half = chunk_len // HALVES
    tile = chunk_len // TILES
    pairs = CHUNKS // 2
    per_block = pairs // BLOCKS
    width = up.shape[2]
    last = tp_size - 1
    root_a, root_b = (tp_size - 1) // 2, tp_size // 2
    rot_dim = head_dim // ROTARY_SHARE
    half_rot = rot_dim // 2
    scale = head_dim ** -0.5 * LOG2E
    own_at, sent_at, kept_at, q_at = 0, span, 2 * span, 3 * span
    extra_at = 3 * span + SLICES * width
    per_half = BLOCKS // HALVES
    waited = per_half * SLICES

    def rows_of(n, size):
        return pl.ds(pl.multiple_of(n * size, size), size)

    def weight_copies(f):
        cols = pl.ds(f * width, width)
        return (pltpu.make_async_copy(w_up.at[:, cols], up.at[f], up_sem.at[f]),
                pltpu.make_async_copy(w_down.at[cols, :], down.at[f], down_sem.at[f]))

    def row_of(n):
        return across * (1 - n) + j * n

    def big_x(i):
        return pltpu.make_async_copy(
            hidden.at[row_of(lax.div(i, TILES)), rows_of(lax.rem(i, TILES), tile), :], x_big.at[lax.rem(i, 2)], xb_sem.at[lax.rem(i, 2)])

    def cache_copies(row, slot):
        return (pltpu.make_async_copy(k_cache.at[row], kv.at[slot, 0], kv_sem.at[slot, 0]),
                pltpu.make_async_copy(v_cache.at[row], kv.at[slot, 1], kv_sem.at[slot, 1]))

    def start(copies):
        for copy in copies:
            copy.start()

    def wait(copies):
        for copy in copies:
            copy.wait()

    qkv_copies = [pltpu.make_async_copy(w_qkv.at[:, pl.ds(s * width, width)], up.at[s], up_sem.at[s]) for s in range(3)]
    tab_copies = [pltpu.make_async_copy(ref.at[row], tab_buf.at[n, p], tab_sem.at[n, p])
                  for n, row in enumerate((across, j)) for p, ref in enumerate((cos_all, sin_all))]
    proj_copy = pltpu.make_async_copy(w_out, proj, proj_sem)
    big_x(0).start()
    start(qkv_copies)
    start(tab_copies)
    start(cache_copies(corner, 0))
    start(cache_copies(across, 1))
    proj_copy.start()

    barrier = pltpu.get_barrier_semaphore()
    pl.semaphore_signal(barrier, inc=1, device_id={"cp": across}, device_id_type=MESH)
    pl.semaphore_signal(barrier, inc=1, device_id={"cp": mate}, device_id_type=MESH)

    @pl.when(z > 0)
    def _():
        pl.semaphore_signal(barrier, inc=1, device_id={"tp": z - 1}, device_id_type=MESH)

    @pl.when(z < last)
    def _():
        pl.semaphore_signal(barrier, inc=1, device_id={"tp": z + 1}, device_id_type=MESH)

    inside = jnp.logical_and(z > 0, z < last)

    @pl.when(inside)
    def _():
        pl.semaphore_wait(barrier, 4)

    @pl.when(jnp.logical_not(inside))
    def _():
        pl.semaphore_wait(barrier, 3)

    def to_core(src, dst, send, arrive):
        return pltpu.make_async_remote_copy(
            src_ref=src, dst_ref=dst, send_sem=send, recv_sem=arrive, device_id={"cp": mate}, device_id_type=MESH)

    def to_y(src, dst, send, arrive):
        return pltpu.make_async_remote_copy(
            src_ref=src, dst_ref=dst, send_sem=send, recv_sem=arrive, device_id={"cp": across}, device_id_type=MESH)


    def staged(t, part):
        return acc.at[rows_of(t, tile), pl.ds(part * span, span)]

    def sent_tile(n, t):
        return [to_core(staged(t, p), qb.at[n, rows_of(t, tile), pl.ds(p * span, span)], qs_sem.at[n, t, p], qr_sem.at[n, t, p])
                for p in range(3)]

    def sent_off(n, t):
        for copy in sent_tile(n, t):
            copy.wait_send()

    def project(n, t, place):
        i = n * TILES + t

        @pl.when(i + 1 < 2 * TILES)
        def _():
            big_x(i + 1).start()

        big_x(i).wait()
        if n == 1:
            sent_off(0, t)
        normed = layer_norm(x_big[lax.rem(i, 2)], gain1[...], bias1[...])
        cos_part, sin_part = tab_buf[n, 0, :, rows_of(t, tile)], tab_buf[n, 1, :, rows_of(t, tile)]
        tab = jnp.concatenate([cos_part, cos_part, -sin_part, sin_part] * (head_dim // (4 * half_rot)), axis=0).T
        lane = lax.broadcasted_iota(jnp.int32, tab.shape, 1)
        cos_tab = jnp.where(lane < rot_dim, tab, 1.0)
        sin_tab = jnp.where(lane < rot_dim, pltpu.roll(tab, head_dim - rot_dim, 1), 0.0)

        def rotate(values):
            long = values.astype(F32)
            other = jnp.where(lane < half_rot, pltpu.roll(long, head_dim - half_rot, 1), pltpu.roll(long, half_rot, 1))
            return (long * cos_tab + other * sin_tab).astype(BF16)

        for p, product in ahead(3, lambda p: jnp.dot(normed, up[p], preferred_element_type=F32)):
            some = (product + small[:, p * span:(p + 1) * span]).astype(BF16)
            for g in range(heads):
                group = p * heads + g
                values = some[:, g * head_dim:(g + 1) * head_dim]
                if group % 3 < 2:
                    values = rotate(values)
                place[:, group * head_dim:(group + 1) * head_dim] = values
                staged(t, p)[:, g * head_dim:(g + 1) * head_dim] = values.astype(F32)
        start(sent_tile(n, t))

    def arrived_tiles(n):
        for t in range(TILES):
            for copy in sent_tile(n, t):
                copy.wait_recv()

    def query_copies(n):
        return [pltpu.make_async_copy(qb.at[n, :, pl.ds(3 * h * head_dim, head_dim)],
                                      acc.at[:, pl.ds(q_at + h * head_dim, head_dim)], q_sem.at[h]) for h in range(heads)]

    per_slice = width // tile

    def far_place(t):
        return down.at[lax.div(t, per_slice), rows_of(lax.rem(t, per_slice), tile), pl.ds(0, 3 * span)]

    def mine_out(t):
        return pltpu.make_async_copy(mine.at[t], pk.at[1, rows_of(t, tile), :], mine_sem.at[t])

    wait(qkv_copies)
    wait(tab_copies)

    @pl.loop(0, TILES)
    def _(t):
        project(0, t, far_place(t))

    pack_copies = [pltpu.make_async_copy(far_place(t), pk.at[0, rows_of(t, tile), :], pk_sem.at[t]) for t in range(TILES)]
    start(pack_copies)

    @pl.loop(0, TILES)
    def _(t):
        @pl.when(t == TILES // 2)
        def _():
            arrived_tiles(0)
            start(query_copies(0))

        project(1, t, mine.at[t])
        mine_out(t).start()

    for f in range(SLICES):
        weight_copies(f)[0].start()


    def attend(row, slot, query, e):
        valid = jnp.clip(lengths[row] - j * slots, 0, slots)
        mask = lax.broadcasted_iota(jnp.int32, (half, slots), 1) < valid
        first_step(heads, scale, lambda h: query(e, h), lambda h: kv[slot, 0, h], lambda h: kv[slot, 1, h],
                   m_scr, l_scr, o_scr, mask)

    def attend_own(e):
        def own_block(b, mask):
            def part(p):
                return lambda h: mine[b, :, (3 * h + p) * head_dim:(3 * h + p + 1) * head_dim]

            block_step(heads, scale, lambda h: held_mine(e, h), part(1), part(2), m_scr, l_scr, o_scr, mask)

        @pl.loop(0, e)
        def _(b):
            own_block(b, None)

        shape = (half, half)
        own_block(e, lax.broadcasted_iota(jnp.int32, shape, 0) >= lax.broadcasted_iota(jnp.int32, shape, 1))

    def keep(e, at, kind):
        lane = lax.broadcasted_iota(jnp.int32, (half, head_dim), 1)
        stats = jnp.zeros((half, head_dim), F32)
        for h in range(heads):
            stats = jnp.where(lane == h, m_scr[h], stats)
            stats = jnp.where(lane == heads + h, jnp.sum(l_scr[h], axis=1, keepdims=True), stats)
            acc[rows_of(e, half), at + h * head_dim:at + (h + 1) * head_dim] = o_scr[h]
        st[kind, :, rows_of(e, half)] = stats.T[:8]

    def held_far(e, h):
        return far_place(e)[:, 3 * h * head_dim:(3 * h + 1) * head_dim]

    def held_mine(e, h):
        return mine[e, :, 3 * h * head_dim:(3 * h + 1) * head_dim]

    def taken(e, h):
        return acc[rows_of(e, half), q_at + h * head_dim:q_at + (h + 1) * head_dim].astype(BF16)

    def far_piece(e):
        return to_core(acc.at[rows_of(e, half), pl.ds(sent_at, span)], ob_far.at[rows_of(e, half), :], fs_sem.at[e], fr_sem.at[e])

    def near_piece(e):
        return to_core(acc.at[rows_of(e, half), pl.ds(sent_at, span)], ob.at[0, rows_of(e, half), :], ns_sem.at[e], nr_sem.at[e])

    def y_piece(e):
        return to_y(acc.at[rows_of(e, half), pl.ds(kept_at, span)], ob.at[1, rows_of(e, half), :], ys_sem.at[e], yr_sem.at[e])

    def far_stats(e):
        return to_core(st.at[0, :, rows_of(e, half)], sbox.at[0, :, rows_of(e, half)], fss_sem.at[e], fsr_sem.at[e])

    def near_stats(e):
        return to_core(st.at[2, :, rows_of(e, half)], sbox.at[1, :, rows_of(e, half)], nss_sem.at[e], nsr_sem.at[e])

    def y_stats(e):
        return to_y(st.at[1, :, rows_of(e, half)], sbox.at[2, :, rows_of(e, half)], yss_sem.at[e], ysr_sem.at[e])

    wait(query_copies(0))
    wait(cache_copies(corner, 0))
    wait(cache_copies(across, 1))

    @pl.loop(0, HALVES)
    def _(e):
        sent_off(1, e)
        attend(corner, 0, taken, e)
        keep(e, sent_at, 0)
        far_stats(e).start()
        far_piece(e).start()

        @pl.when(e == HALVES - 1)
        def _():
            start(cache_copies(mate, 0))
            arrived_tiles(1)
            start(query_copies(1))

        attend(across, 1, held_far, e)
        keep(e, kept_at, 1)

        far_stats(e).wait_recv()
        far_piece(e).wait_recv()
        rows = rows_of(e, half)
        peak, weights, total = piece_weights(heads, [st[1, :, rows], sbox[0, :, rows]], head_dim)
        columns = as_columns(weights, head_dim)
        for h in range(heads):
            at = kept_at + h * head_dim
            acc[rows, at:at + head_dim] = (acc[rows, at:at + head_dim] * columns[:, h:h + 1]
                                           + ob_far[rows, h * head_dim:(h + 1) * head_dim] * columns[:, heads + h:heads + h + 1])
        st[1, :heads, rows] = peak
        st[1, heads:2 * heads, rows] = total
        y_stats(e).start()
        y_piece(e).start()

    start(cache_copies(j, 1))
    wait(pack_copies)
    for f in range(SLICES):
        weight_copies(f)[1].start()
    for e in range(HALVES):
        far_stats(e).wait_send()
        far_piece(e).wait_send()
    wait(query_copies(1))
    wait(cache_copies(mate, 0))


    def near(e, phase):
        @pl.when(phase == 5)
        def _():
            attend(mate, 0, taken, e)
            keep(e, sent_at, 2)
            near_stats(e).start()
            near_piece(e).start()

            @pl.when(e == 0)
            def _():
                wait(cache_copies(j, 1))

        @pl.when(phase == 6)
        def _():
            attend(j, 1, held_mine, e)

        @pl.when(phase == 7)
        def _():
            attend_own(e)
            keep(e, own_at, 3)

            @pl.when(e == 0)
            def _():
                proj_copy.wait()

    def block_copies(b):
        rows = rows_of(b, block)
        slot = lax.rem(b, 2)
        return [pltpu.make_async_copy(hidden.at[j, rows, :], x_big.at[slot, pl.ds(0, block), :], x_sem.at[slot])] + [
            pltpu.make_async_copy(ob.at[n, rows, :], ob_far.at[rows_of(2 * slot + n, block), :], o_sem.at[slot, n]) for n in range(2)]

    def fetch(b):
        @pl.when(lax.rem(b, per_half) == 0)
        def _():
            e = lax.div(b, per_half)
            near_stats(e).wait_recv()
            near_piece(e).wait_recv()
            y_stats(e).wait_recv()
            y_piece(e).wait_recv()

        start(block_copies(b))

    def begin(b):
        slot = lax.rem(b, 2)
        rows = rows_of(b, block)

        wait(block_copies(b))

        @pl.when(lax.rem(b, per_half) == 0)
        def _():
            e = lax.div(b, per_half)
            for copy in (near_stats(e), near_piece(e), y_stats(e), y_piece(e)):
                copy.wait_send()

        _, weights, total = piece_weights(heads, [st[3, :, rows], sbox[1, :, rows], sbox[2, :, rows]], head_dim)
        columns = as_columns([w / total for w in weights], head_dim)
        for h in range(heads):
            cols = slice(h * head_dim, (h + 1) * head_dim)
            pieces = [acc[rows, own_at + h * head_dim:own_at + (h + 1) * head_dim]]
            pieces += [ob_far[rows_of(2 * slot + n, block), cols] for n in range(2)]
            context = functools.reduce(
                jnp.add, [o * columns[:, n * heads + h:n * heads + h + 1] for n, o in enumerate(pieces)])
            x_big[1, block:2 * block, cols] = context.astype(BF16)
        x = x_big[slot, :block, :]
        x_big[0, block:2 * block, :] = layer_norm(x, gain2[...], bias2[...])
        acc[rows, :] = jnp.dot(x_big[1, block:2 * block, :span], proj[...], preferred_element_type=F32)

        @pl.when(z == 0)
        def _():
            acc[rows, :] += x.astype(F32) + small[:, extra_at:]

    def slice_of(b, f):
        rows = rows_of(b, block)

        @pl.when(b == 0)
        def _():
            wait(weight_copies(f))

        b_up = small[:, pl.ds(pl.multiple_of(3 * span + f * width, width), width)]
        wide_h = jnp.dot(x_big[0, block:2 * block, :], up[f], preferred_element_type=F32) + b_up
        act = (0.5 * wide_h * (1.0 + lax.erf(wide_h * math.sqrt(0.5)))).astype(BF16)
        acc[rows, :] += jnp.dot(act, down[f], preferred_element_type=F32)


    def at(ref, k):
        return ref.at[pl.ds(pl.multiple_of(k * tokens, tokens), tokens), :]

    def remote(src, dst, k, which, arrive, device):
        return pltpu.make_async_remote_copy(
            src_ref=at(src, k), dst_ref=at(dst, k), send_sem=send_sem.at[which], recv_sem=arrive.at[k],
            device_id=device, device_id_type=MESH,
        )

    def send_right(src, k):
        remote(src, from_left, k, 0, left_sem, {"tp": z + 1}).start()

    def send_left(src, k):
        remote(src, from_right, k, 1, right_sem, {"tp": z - 1}).start()

    def arrived(ref, sem, k):
        remote(ref, ref, k, 0, sem, {"cp": j}).wait_recv()

    def drained(ref, which):
        pltpu.make_async_copy(ref, ref, send_sem.at[which]).wait()

    def emit(stream, values, k, row):
        slot = lax.rem(k, STAGES)

        def copy():
            return pltpu.make_async_copy(stage.at[stream, slot], at(out_ref.at[row], k), stage_sem.at[stream, slot])

        @pl.when(k >= STAGES)
        def _():
            copy().wait()

        stage[stream, slot] = values.astype(BF16)
        copy().start()

    def chunk(ref, k):
        return ref[pl.ds(pl.multiple_of(k * tokens, tokens), tokens), :]

    def finish(src, k):
        remote(src, y_box, k, 2, y_sem, {"cp": across}).start()
        remote(src, core_box, k, 3, core_sem, {"cp": mate}).start()
        emit(0, chunk(src, k), k, j)

    def landing(n, box, k):
        slot = lax.rem(k, STAGES)
        return pltpu.make_async_copy(at(box, k), land.at[n, slot], land_sem.at[n, slot])

    def gathered(i):
        def lagged(lag, act):
            @pl.when(jnp.logical_and(i >= lag, i < pairs + lag))
            def _():
                for n in range(2):
                    act((i - lag) * 2 + n)

        def core(k):
            arrived(core_box, core_sem, k)
            landing(0, core_box, k).start()

        def core_out(k):
            landing(0, core_box, k).wait()
            emit(1, land[0, lax.rem(k, STAGES)], k, mate)

        def side(k):
            arrived(y_box, y_sem, k)
            remote(y_box, last_box, k, 4, last_sem, {"cp": mate}).start()
            landing(2, y_box, k).start()

        def side_out(k):
            landing(2, y_box, k).wait()
            emit(2, land[2, lax.rem(k, STAGES)], k, across)

        def final(k):
            arrived(last_box, last_sem, k)
            landing(1, last_box, k).start()

        def final_out(k):
            landing(1, last_box, k).wait()
            emit(3, land[1, lax.rem(k, STAGES)], k, corner)

        lagged(LAG_CORE + 1, core_out)
        lagged(LAG_Y + 1, side_out)
        lagged(LAG_LAST + 1, final_out)
        lagged(LAG_CORE, core)
        lagged(LAG_Y, side)
        lagged(LAG_LAST, final)

    def add(k, *others):
        rows = pl.ds(pl.multiple_of(k * tokens, tokens), tokens)
        total = acc[rows, :]
        for other in others:
            total = total + other[rows, :]
        acc[rows, :] = total

    def when(cond, act, *args):
        @pl.when(cond)
        def _():
            act(*args)

    def end(i, first):
        inbox, sem = (from_right, right_sem) if first else (from_left, left_sem)
        near_bit = 0 if first else 1

        def got(k):
            arrived(inbox, sem, k)
            finish(inbox, k)

        when(jnp.logical_and(i >= 0, i < pairs), lambda: got(2 * i + near_bit))
        when(jnp.logical_and(i >= LAG_BACK, i < pairs + LAG_BACK), lambda: got(2 * (i - LAG_BACK) + 1 - near_bit))

    def inner(i, left_side):
        mine = 0 if left_side else 1
        if left_side:
            (outer, outer_sem, to_outer), (inward, inward_sem, to_inner) = (
                (from_left, left_sem, send_left), (from_right, right_sem, send_right))
        else:
            (outer, outer_sem, to_outer), (inward, inward_sem, to_inner) = (
                (from_right, right_sem, send_right), (from_left, left_sem, send_left))

        def early(p):
            passed = 2 * p + 1 - mine
            arrived(outer, outer_sem, passed)
            add(passed, outer)
            to_inner(acc, passed)

        def near(p):
            rooted = 2 * p + mine
            arrived(outer, outer_sem, rooted)
            arrived(inward, inward_sem, rooted)
            add(rooted, from_left, from_right)
            to_outer(acc, rooted)
            to_inner(acc, rooted)
            finish(acc, rooted)

        def far(p):
            k = 2 * p + 1 - mine
            arrived(inward, inward_sem, k)
            to_outer(inward, k)
            finish(inward, k)

        when(jnp.logical_and(i + LAG_AHEAD >= 0, i + LAG_AHEAD < pairs), early, i + LAG_AHEAD)
        when(jnp.logical_and(i >= 0, i < pairs), near, i)
        when(jnp.logical_and(i >= LAG_BACK, i < pairs + LAG_BACK), far, i - LAG_BACK)

    lead = SLICES + LAG_START

    @pl.loop(0, waited + lead + pairs + LAG_LAST + 2)
    def _(step):
        s = step - waited

        @pl.when(step < HALVES * waited)
        def _():
            near(lax.div(step, waited), lax.rem(step, waited))

        @pl.when(step == waited - 2)
        def _():
            fetch(0)

        @pl.when(jnp.logical_and(s >= 0, s < BLOCKS * SLICES))
        def _():
            b, f = lax.div(s, SLICES), lax.rem(s, SLICES)
            when(f == 0, begin, b)
            when(jnp.logical_and(f == SLICES - 1, b + 1 < BLOCKS), fetch, b + 1)
            slice_of(b, f)

            def push(send, swapped):
                @pl.loop(0, 2 * per_block)
                def _(n):
                    send(acc, b * 2 * per_block + (n + 1 - 2 * lax.rem(n, 2) if swapped else n))

            when(jnp.logical_and(f == SLICES - 1, z == 0), push, send_right, True)
            when(jnp.logical_and(f == SLICES - 1, z == last), push, send_left, False)

        i = s - lead
        when(z == 0, end, i, True)
        when(z == root_a, inner, i, True)
        when(z == root_b, inner, i, False)
        when(z == last, end, i, False)
        gathered(i)

    @pl.when(z < last)
    def _():
        drained(acc, 0)

    @pl.when(z > 0)
    def _():
        drained(acc, 1)

    for which in (2, 3, 4):
        drained(acc, which)
    for t in range(TILES):
        mine_out(t).wait()
    for stream in range(4):
        for slot in range(STAGES):
            pltpu.make_async_copy(stage.at[stream, slot], at(out_ref.at[0], 0), stage_sem.at[stream, slot]).wait()


def run_layer(lengths, hidden_in, tables, k_block, v_block, w_qkv, w_up, w_down, w_out, norms, small, tp_size):
    num_rows, chunk_len, d_model = hidden_in.shape
    heads, slots, head_dim = k_block.shape[1:]
    span = heads * head_dim
    width = w_up.shape[1] // SLICES
    tokens = chunk_len // CHUNKS
    block = chunk_len // BLOCKS
    half = chunk_len // HALVES
    tile = chunk_len // TILES
    dma = pltpu.SemaphoreType.DMA
    buffer = pltpu.VMEM((chunk_len, d_model), F32)
    box = jax.ShapeDtypeStruct((chunk_len, d_model), F32)
    hbm = pl.BlockSpec(memory_space=pl.ANY)
    vmem = pl.BlockSpec(memory_space=pltpu.VMEM)
    out, _, _, _, pk, qb, _ = pl.pallas_call(
        functools.partial(layer_kernel, tp_size, heads),
        in_specs=[pl.BlockSpec(memory_space=pltpu.SMEM)] + [hbm] * 9 + [vmem] * 5,
        out_specs=[hbm] * 7,
        out_shape=[
            jax.ShapeDtypeStruct((num_rows, chunk_len, d_model), BF16), box, box, box,
            jax.ShapeDtypeStruct((2, chunk_len, 3 * span), BF16),
            jax.ShapeDtypeStruct((2, chunk_len, 3 * span), F32),
            jax.ShapeDtypeStruct((2, chunk_len, span), F32),
        ],
        scratch_shapes=[buffer] * 3
        + [
            pltpu.VMEM((SLICES, d_model, width), BF16),
            pltpu.VMEM((SLICES, width, d_model), BF16),
            pltpu.VMEM((span, d_model), BF16),
            pltpu.VMEM((TILES, tile, 3 * span), BF16),
            pltpu.VMEM((2, tile, d_model), BF16),
            pltpu.VMEM((2, 2) + tables[0].shape[1:], F32),
            pltpu.VMEM((2, 2, heads, slots, head_dim), BF16),
            pltpu.VMEM((chunk_len, span), F32),
            pltpu.VMEM((heads, half, head_dim), F32),
            pltpu.VMEM((heads, half, head_dim), F32),
            pltpu.VMEM((heads, half, head_dim), F32),
            pltpu.VMEM((4, 8, chunk_len), F32),
            pltpu.VMEM((3, 8, chunk_len), F32),
            pltpu.VMEM((4, STAGES, tokens, d_model), BF16),
            pltpu.VMEM((3, STAGES, tokens, d_model), F32),
        ]
        + [dma((SLICES,)), dma((SLICES,)), dma, dma((2,)), dma((2, 2)), dma((TILES,)), dma((TILES,)), dma((2, 2)), dma((heads,)),
           dma((2,)), dma((2, 2))]
        + [dma((2, TILES, 3))] * 2
        + [dma((HALVES,))] * 12
        + [dma((CHUNKS,))] * 5
        + [dma((5,)), dma((4, STAGES)), dma((3, STAGES))],
        compiler_params=pltpu.CompilerParams(collective_id=0, has_side_effects=True, vmem_limit_bytes=LAYER_LIMIT),
        cost_estimate=pl.CostEstimate(flops=100_000_000_000, bytes_accessed=chunk_len * d_model * 16, transcendentals=0),
        name="layer",
    )(lengths, hidden_in, *tables, k_block, v_block, w_qkv, w_up, w_down, w_out, *norms, small)
    return out, pk, qb


def finish_kernel(heads, meta, in_ref, pk, qb, out_ref, k_ref, v_ref, buf, low, high, in_sem, out_sem, low_sem, high_sem, kv_sem):
    pieces = in_sem.shape[1]
    tile = buf.shape[1] // pieces
    head_dim = k_ref.shape[3]
    places = [(b, pl.ds(t * tile, tile), t) for b in range(buf.shape[0]) for t in range(pieces)]
    inward = [pltpu.make_async_copy(in_ref.at[b, rows], buf.at[b, rows], in_sem.at[b, t]) for b, rows, t in places]
    outward = [pltpu.make_async_copy(buf.at[b, rows], out_ref.at[b, rows], out_sem.at[b, t]) for b, rows, t in places]
    both = 2 * head_dim

    def taken(src, dst, sem):
        return [[pltpu.make_async_copy(src.at[n, :, pl.ds((3 * h + 1) * head_dim, both)], dst.at[n, :, pl.ds(h * both, both)], sem.at[n, h])
                 for h in range(heads)] for n in range(2)]

    lows, highs = taken(pk, low, low_sem), taken(qb, high, high_sem)
    stored = []

    def store(n, h, row):
        for p, ref in enumerate((k_ref, v_ref)):
            cols = pl.ds(h * both + p * head_dim, head_dim)
            copy = pltpu.make_async_copy(low.at[n, :, cols], ref.at[row, h], kv_sem.at[n, h, p])
            copy.start()
            stored.append(copy)

    for copy in highs[0] + highs[1] + lows[0] + lows[1] + inward:
        copy.start()
    j = meta[0]
    for n in range(2):
        for h in range(heads):
            lows[n][h].wait()
            store(n, h, j ^ (2 - 2 * n))
    for n in range(2):
        for h in range(heads):
            highs[n][h].wait()
            cols = slice(h * both, (h + 1) * both)
            low[2 + n, :, cols] = high[n, :, cols].astype(BF16)
            store(2 + n, h, j ^ (3 - 2 * n))
    for one, other in zip(inward, outward):
        one.wait()
        other.start()
    for copy in outward + stored:
        copy.wait()


def finish(meta, out, pk, qb, heads, head_dim):
    rows, chunk_len, _ = out.shape
    span = 2 * heads * head_dim
    hbm = pl.BlockSpec(memory_space=pl.ANY)
    cache = jax.ShapeDtypeStruct((rows, heads, chunk_len, head_dim), BF16)
    dma = pltpu.SemaphoreType.DMA
    return pl.pallas_call(
        functools.partial(finish_kernel, heads),
        in_specs=[pl.BlockSpec(memory_space=pltpu.SMEM)] + [hbm] * 3,
        out_specs=[hbm] * 3,
        out_shape=[jax.ShapeDtypeStruct(out.shape, out.dtype), cache, cache],
        scratch_shapes=[
            pltpu.VMEM(out.shape, out.dtype), pltpu.VMEM((4, chunk_len, span), BF16), pltpu.VMEM((2, chunk_len, span), F32),
            dma((rows, 4)), dma((rows, 4)), dma((2, heads)), dma((2, heads)), dma((4, heads, 2)),
        ],
        compiler_params=pltpu.CompilerParams(vmem_limit_bytes=VMEM_LIMIT),
        name="finish",
    )(meta, out, pk, qb)


def solution(mesh):
    in_specs = (P("dp", None, None), P("dp"), P("dp", "tp", "cp", None), P("dp", "tp", "cp", None), P(), P(), P(), P(), P(None, "tp"), P("tp"), P("tp", None), P(), P(None, "tp"), P("tp"), P("tp", None), P())
    out_specs = (P("dp", None, None), P("dp", "tp", None, None), P("dp", "tp", None, None))
    tp_size = mesh.shape["tp"]

    def local_layer(hidden_in, lengths, k_block, v_block, ln1_gain, ln1_bias, ln2_gain, ln2_bias, w_qkv, b_qkv, w_out, b_out, w_up, b_up, w_down, b_down):
        num_rows, chunk_len, d_model = hidden_in.shape
        heads, block_len, head_dim = k_block.shape[1:]
        tables = rope_tables(lengths, chunk_len, head_dim)
        norms = [p[None] for p in (ln1_gain, ln1_bias, ln2_gain, ln2_bias)]
        parts = [(b_qkv, 0), (b_up, b_qkv.shape[0]), (b_out, b_qkv.shape[0] + b_up.shape[0]), (b_down, b_qkv.shape[0] + b_up.shape[0])]
        total = b_qkv.shape[0] + b_up.shape[0] + d_model
        small = functools.reduce(jnp.add, [jnp.pad(p[None].astype(F32), ((0, 0), (at, total - at - p.shape[0]))) for p, at in parts])
        out, pk, qb = run_layer(lengths, hidden_in, tables, k_block, v_block, w_qkv, w_up, w_down, w_out, norms, small, tp_size)
        return tuple(finish(lax.axis_index("cp")[None], out, pk, qb, heads, head_dim))

    return jax.shard_map(local_layer, mesh=mesh, in_specs=in_specs, out_specs=out_specs, check_vma=False)
```

```python
import functools
import math

import jax
import jax.numpy as jnp
from jax import lax
from jax.experimental import pallas as pl
from jax.experimental.pallas import tpu as pltpu
from jax.sharding import PartitionSpec as P

EPSILON = 1e-5
NEG_BIG = -1e30
ROTARY_SHARE = 4
ROPE_BASE = 10000.0
LOG2E = math.log2(math.e)
MESH = pl.DeviceIdType.MESH
F32 = jnp.float32
BF16 = jnp.bfloat16
VMEM_LIMIT = 60 * 1024 * 1024
LAYER_LIMIT = 67_043_328
EMPTY = -1e29
CHUNKS = 64
STAGES = 4
BLOCKS = 8
SLICES = 4
TILES = 4
HALVES = 4
LAG_START = 2
LAG_AHEAD = 1
LAG_BACK = 1
LAG_CORE = 2
LAG_Y = 5
LAG_LAST = 6


def layer_norm(values_in, gain_vec, bias_vec):
    x_f32 = values_in.astype(F32)
    row_mean = jnp.mean(x_f32, axis=-1, keepdims=True)
    centered = x_f32 - row_mean
    variance = jnp.mean(centered * centered, axis=-1, keepdims=True)
    return (centered * lax.rsqrt(variance + EPSILON) * gain_vec + bias_vec).astype(BF16)


def rope_tables(lengths, chunk_len, head_dim):
    rot_dim = head_dim // ROTARY_SHARE
    shape = (lengths.shape[0], rot_dim // 2, chunk_len)
    positions = lengths[:, None, None] + lax.broadcasted_iota(jnp.int32, shape, 2)
    inv_freq = ROPE_BASE ** (-2.0 * jnp.arange(rot_dim // 2, dtype=F32) / rot_dim)
    angles = positions.astype(F32) * inv_freq[:, None]
    return jnp.cos(angles), jnp.sin(angles)


def wide(column, lanes):
    return jnp.concatenate([column] * (lanes // column.shape[1]), axis=1)


def scores_of(query, keys, scale, mask):
    scores = lax.dot_general(query, keys, (((1,), (1,)), ((), ())), preferred_element_type=F32) * scale
    return scores if mask is None else jnp.where(mask, scores, NEG_BIG)


def lane_sum(values, lanes):
    return functools.reduce(jnp.add, [values[:, n:n + lanes] for n in range(0, values.shape[1], lanes)])


def lane_max(values, lanes):
    return functools.reduce(jnp.maximum, [values[:, n:n + lanes] for n in range(0, values.shape[1], lanes)])


def ahead(heads, scores):
    coming = scores(0)
    for h in range(heads):
        now = coming
        if h + 1 < heads:
            coming = scores(h + 1)
        yield h, now


def first_step(heads, scale, q_of, k_of, v_of, m_scr, l_scr, o_scr, mask):
    lanes = o_scr.shape[2]
    for h, scores in ahead(heads, lambda h: scores_of(q_of(h), k_of(h), scale, mask)):
        peak = jnp.maximum(jnp.max(lane_max(scores, lanes), axis=1, keepdims=True), EMPTY)
        peak = jnp.broadcast_to(peak, m_scr.shape[1:])
        probs = jnp.exp2(scores - wide(peak, scores.shape[1]))
        m_scr[h] = peak
        l_scr[h] = lane_sum(probs, lanes)
        o_scr[h] = jnp.dot(probs.astype(BF16), v_of(h), preferred_element_type=F32)


def block_step(heads, scale, q_of, k_of, v_of, m_scr, l_scr, o_scr, mask):
    lanes = o_scr.shape[2]
    for h, scores in ahead(heads, lambda h: scores_of(q_of(h), k_of(h), scale, mask)):
        m_old = m_scr[h]
        m_new = jnp.maximum(m_old, jnp.max(lane_max(scores, lanes), axis=1, keepdims=True))
        probs = jnp.exp2(scores - wide(m_new, scores.shape[1]))
        shrink = jnp.exp2(m_old - m_new)
        l_scr[h] = l_scr[h] * shrink + lane_sum(probs, lanes)
        m_scr[h] = m_new
        o_scr[h] = o_scr[h] * shrink + jnp.dot(probs.astype(BF16), v_of(h), preferred_element_type=F32)


def piece_weights(heads, stats, head_dim):
    peak = functools.reduce(jnp.maximum, [s[:heads] for s in stats])
    weights = [jnp.exp2(s[:heads] - peak) for s in stats]
    total = functools.reduce(jnp.add, [s[heads:2 * heads] * w for s, w in zip(stats, weights)])
    return peak, weights, total


def as_columns(parts, head_dim):
    count = sum(p.shape[0] for p in parts)
    return jnp.concatenate(parts + [jnp.zeros((head_dim - count, parts[0].shape[1]), F32)], axis=0).T


def layer_kernel(tp_size, heads, lengths, hidden, cos_all, sin_all, k_cache, v_cache, w_qkv, w_up, w_down, w_out,
                 gain1, bias1, gain2, bias2, small,
                 out_ref, y_box, core_box, last_box, pk, qb, ob,
                 acc, from_left, from_right, up, down, proj, mine, x_big, tab_buf, kv, ob_far, m_scr, l_scr, o_scr, st, sbox,
                 stage, land,
                 up_sem, down_sem, proj_sem, xb_sem, tab_sem, pk_sem, mine_sem, kv_sem, q_sem, x_sem, o_sem,
                 qs_sem, qr_sem, fs_sem, fr_sem, ns_sem, nr_sem, ys_sem, yr_sem,
                 fss_sem, fsr_sem, nss_sem, nsr_sem, yss_sem, ysr_sem,
                 left_sem, right_sem, y_sem, core_sem, last_sem, send_sem, stage_sem, land_sem):
    z = lax.axis_index("tp")
    j = lax.axis_index("cp")
    y, c = lax.div(j, 2), lax.rem(j, 2)
    across, mate, corner = (1 - y) * 2 + c, y * 2 + (1 - c), (1 - y) * 2 + (1 - c)
    chunk_len, d_model = acc.shape
    head_dim = o_scr.shape[2]
    span = heads * head_dim
    slots = k_cache.shape[2]
    tokens = chunk_len // CHUNKS
    block = chunk_len // BLOCKS
    half = chunk_len // HALVES
    tile = chunk_len // TILES
    pairs = CHUNKS // 2
    per_block = pairs // BLOCKS
    width = up.shape[2]
    last = tp_size - 1
    root_a, root_b = (tp_size - 1) // 2, tp_size // 2
    rot_dim = head_dim // ROTARY_SHARE
    half_rot = rot_dim // 2
    scale = head_dim ** -0.5 * LOG2E
    own_at, sent_at, kept_at, q_at = 0, span, 2 * span, 3 * span
    extra_at = 3 * span + SLICES * width
    per_half = BLOCKS // HALVES
    waited = per_half * SLICES

    def rows_of(n, size):
        return pl.ds(pl.multiple_of(n * size, size), size)

    def weight_copies(f):
        cols = pl.ds(f * width, width)
        return (pltpu.make_async_copy(w_up.at[:, cols], up.at[f], up_sem.at[f]),
                pltpu.make_async_copy(w_down.at[cols, :], down.at[f], down_sem.at[f]))

    def row_of(n):
        return across * (1 - n) + j * n

    def big_x(i):
        return pltpu.make_async_copy(
            hidden.at[row_of(lax.div(i, TILES)), rows_of(lax.rem(i, TILES), tile), :], x_big.at[lax.rem(i, 2)], xb_sem.at[lax.rem(i, 2)])

    def cache_copies(row, slot):
        return (pltpu.make_async_copy(k_cache.at[row], kv.at[slot, 0], kv_sem.at[slot, 0]),
                pltpu.make_async_copy(v_cache.at[row], kv.at[slot, 1], kv_sem.at[slot, 1]))

    def start(copies):
        for copy in copies:
            copy.start()

    def wait(copies):
        for copy in copies:
            copy.wait()

    qkv_copies = [pltpu.make_async_copy(w_qkv.at[:, pl.ds(s * width, width)], up.at[s], up_sem.at[s]) for s in range(3)]
    tab_copies = [pltpu.make_async_copy(ref.at[row], tab_buf.at[n, p], tab_sem.at[n, p])
                  for n, row in enumerate((across, j)) for p, ref in enumerate((cos_all, sin_all))]
    proj_copy = pltpu.make_async_copy(w_out, proj, proj_sem)
    big_x(0).start()
    start(qkv_copies)
    start(tab_copies)
    start(cache_copies(corner, 0))
    start(cache_copies(across, 1))
    proj_copy.start()

    barrier = pltpu.get_barrier_semaphore()
    pl.semaphore_signal(barrier, inc=1, device_id={"cp": across}, device_id_type=MESH)
    pl.semaphore_signal(barrier, inc=1, device_id={"cp": mate}, device_id_type=MESH)

    @pl.when(z > 0)
    def _():
        pl.semaphore_signal(barrier, inc=1, device_id={"tp": z - 1}, device_id_type=MESH)

    @pl.when(z < last)
    def _():
        pl.semaphore_signal(barrier, inc=1, device_id={"tp": z + 1}, device_id_type=MESH)

    inside = jnp.logical_and(z > 0, z < last)

    @pl.when(inside)
    def _():
        pl.semaphore_wait(barrier, 4)

    @pl.when(jnp.logical_not(inside))
    def _():
        pl.semaphore_wait(barrier, 3)

    def to_core(src, dst, send, arrive):
        return pltpu.make_async_remote_copy(
            src_ref=src, dst_ref=dst, send_sem=send, recv_sem=arrive, device_id={"cp": mate}, device_id_type=MESH)

    def to_y(src, dst, send, arrive):
        return pltpu.make_async_remote_copy(
            src_ref=src, dst_ref=dst, send_sem=send, recv_sem=arrive, device_id={"cp": across}, device_id_type=MESH)


    def staged(n, t, part):
        return acc.at[rows_of(t, tile), pl.ds((q_at if n == 1 and part == 2 else part * span), span)]

    def sent_tile(n, t):
        return [to_core(staged(n, t, p), qb.at[n, rows_of(t, tile), pl.ds(p * span, span)], qs_sem.at[n, t, p], qr_sem.at[n, t, p])
                for p in range(3)]

    def sent_off(n, t):
        for copy in sent_tile(n, t):
            copy.wait_send()

    def project(n, t, place):
        i = n * TILES + t

        @pl.when(i + 1 < 2 * TILES)
        def _():
            big_x(i + 1).start()

        big_x(i).wait()
        normed = layer_norm(x_big[lax.rem(i, 2)], gain1[...], bias1[...])
        cos_part, sin_part = tab_buf[n, 0, :, rows_of(t, tile)], tab_buf[n, 1, :, rows_of(t, tile)]
        tab = jnp.concatenate([cos_part, cos_part, -sin_part, sin_part] * (head_dim // (4 * half_rot)), axis=0).T
        lane = lax.broadcasted_iota(jnp.int32, tab.shape, 1)
        cos_tab = jnp.where(lane < rot_dim, tab, 1.0)
        sin_tab = jnp.where(lane < rot_dim, pltpu.roll(tab, head_dim - rot_dim, 1), 0.0)

        def rotate(values):
            long = values.astype(F32)
            other = jnp.where(lane < half_rot, pltpu.roll(long, head_dim - half_rot, 1), pltpu.roll(long, half_rot, 1))
            return (long * cos_tab + other * sin_tab).astype(BF16)

        for p, product in ahead(3, lambda p: jnp.dot(normed, up[p], preferred_element_type=F32)):
            some = (product + small[:, p * span:(p + 1) * span]).astype(BF16)
            for g in range(heads):
                group = p * heads + g
                values = some[:, g * head_dim:(g + 1) * head_dim]
                if group % 3 < 2:
                    values = rotate(values)
                place[:, group * head_dim:(group + 1) * head_dim] = values
                staged(n, t, p)[:, g * head_dim:(g + 1) * head_dim] = values.astype(F32)
        start(sent_tile(n, t))

    def query_copies(n, t):
        rows = rows_of(t, tile)
        return [pltpu.make_async_copy(qb.at[n, rows, pl.ds(3 * h * head_dim, head_dim)],
                                      acc.at[rows, pl.ds(q_at + h * head_dim, head_dim)], q_sem.at[h]) for h in range(heads)]

    def fetch_queries(n, t):
        for copy in sent_tile(n, t):
            copy.wait_recv()
        start(query_copies(n, t))

    per_slice = width // tile

    def far_place(t):
        return down.at[lax.div(t, per_slice), rows_of(lax.rem(t, per_slice), tile), pl.ds(0, 3 * span)]

    def mine_out(t):
        return pltpu.make_async_copy(mine.at[t], pk.at[1, rows_of(t, tile), :], mine_sem.at[t])

    wait(qkv_copies)
    wait(tab_copies)


    def attend(row, slot, query, e):
        valid = jnp.clip(lengths[row] - j * slots, 0, slots)
        mask = lax.broadcasted_iota(jnp.int32, (half, slots), 1) < valid
        first_step(heads, scale, lambda h: query(e, h), lambda h: kv[slot, 0, h], lambda h: kv[slot, 1, h],
                   m_scr, l_scr, o_scr, mask)

    def attend_own(e):
        def own_block(b, mask):
            def part(p):
                return lambda h: mine[b, :, (3 * h + p) * head_dim:(3 * h + p + 1) * head_dim]

            block_step(heads, scale, lambda h: held_mine(e, h), part(1), part(2), m_scr, l_scr, o_scr, mask)

        @pl.loop(0, e)
        def _(b):
            own_block(b, None)

        shape = (half, half)
        own_block(e, lax.broadcasted_iota(jnp.int32, shape, 0) >= lax.broadcasted_iota(jnp.int32, shape, 1))

    def keep(e, at, kind):
        lane = lax.broadcasted_iota(jnp.int32, (half, head_dim), 1)
        stats = jnp.zeros((half, head_dim), F32)
        for h in range(heads):
            stats = jnp.where(lane == h, m_scr[h], stats)
            stats = jnp.where(lane == heads + h, jnp.sum(l_scr[h], axis=1, keepdims=True), stats)
            acc[rows_of(e, half), at + h * head_dim:at + (h + 1) * head_dim] = o_scr[h]
        st[kind, :, rows_of(e, half)] = stats.T[:8]

    def held_far(e, h):
        return far_place(e)[:, 3 * h * head_dim:(3 * h + 1) * head_dim]

    def held_mine(e, h):
        return mine[e, :, 3 * h * head_dim:(3 * h + 1) * head_dim]

    def taken(e, h):
        return acc[rows_of(e, half), q_at + h * head_dim:q_at + (h + 1) * head_dim].astype(BF16)

    def far_piece(e):
        return to_core(acc.at[rows_of(e, half), pl.ds(sent_at, span)], ob_far.at[rows_of(e, half), :], fs_sem.at[e], fr_sem.at[e])

    def near_piece(e):
        return to_core(acc.at[rows_of(e, half), pl.ds(sent_at, span)], ob.at[0, rows_of(e, half), :], ns_sem.at[e], nr_sem.at[e])

    def y_piece(e):
        return to_y(acc.at[rows_of(e, half), pl.ds(kept_at, span)], ob.at[1, rows_of(e, half), :], ys_sem.at[e], yr_sem.at[e])

    def far_stats(e):
        return to_core(st.at[0, :, rows_of(e, half)], sbox.at[0, :, rows_of(e, half)], fss_sem.at[e], fsr_sem.at[e])

    def near_stats(e):
        return to_core(st.at[2, :, rows_of(e, half)], sbox.at[1, :, rows_of(e, half)], nss_sem.at[e], nsr_sem.at[e])

    def y_stats(e):
        return to_y(st.at[1, :, rows_of(e, half)], sbox.at[2, :, rows_of(e, half)], yss_sem.at[e], ysr_sem.at[e])

    def far_attend(e):
        fetch_queries(0, e)
        sent_off(0, e)
        attend(across, 1, held_far, e)
        keep(e, kept_at, 1)
        wait(query_copies(0, e))
        attend(corner, 0, taken, e)
        keep(e, sent_at, 0)
        far_stats(e).start()
        far_piece(e).start()

    def far_join(e):
        far_stats(e).wait_recv()
        far_piece(e).wait_recv()
        rows = rows_of(e, half)
        peak, weights, total = piece_weights(heads, [st[1, :, rows], sbox[0, :, rows]], head_dim)
        columns = as_columns(weights, head_dim)
        for h in range(heads):
            at = kept_at + h * head_dim
            acc[rows, at:at + head_dim] = (acc[rows, at:at + head_dim] * columns[:, h:h + 1]
                                           + ob_far[rows, h * head_dim:(h + 1) * head_dim] * columns[:, heads + h:heads + h + 1])
        st[1, :heads, rows] = peak
        st[1, heads:2 * heads, rows] = total
        y_stats(e).start()
        y_piece(e).start()

    @pl.loop(0, TILES + 2)
    def _(t):
        @pl.when(t < TILES)
        def _():
            project(0, t, far_place(t))

        @pl.when(t == 1)
        def _():
            wait(cache_copies(corner, 0))
            wait(cache_copies(across, 1))

        @pl.when(t >= 2)
        def _():
            far_join(t - 2)

        @pl.when(jnp.logical_and(t >= 1, t <= TILES))
        def _():
            far_attend(t - 1)

    start(cache_copies(mate, 0))
    start(cache_copies(j, 1))
    pack_copies = [pltpu.make_async_copy(far_place(t), pk.at[0, rows_of(t, tile), :], pk_sem.at[t]) for t in range(TILES)]
    start(pack_copies)
    for e in range(HALVES):
        far_stats(e).wait_send()
        far_piece(e).wait_send()

    @pl.loop(0, TILES)
    def _(t):
        @pl.when(t == 2)
        def _():
            sent_off(1, 0)
            fetch_queries(1, 0)

        project(1, t, mine.at[t])
        mine_out(t).start()

    wait(pack_copies)
    for f in range(SLICES):
        start(weight_copies(f))
    wait(cache_copies(mate, 0))


    def near(e, phase):
        @pl.when(jnp.logical_and(phase == 4, e > 0))
        def _():
            sent_off(1, e)
            fetch_queries(1, e)

        @pl.when(phase == 5)
        def _():
            wait(query_copies(1, e))
            attend(mate, 0, taken, e)
            keep(e, sent_at, 2)
            near_stats(e).start()
            near_piece(e).start()

            @pl.when(e == 0)
            def _():
                wait(cache_copies(j, 1))

        @pl.when(phase == 6)
        def _():
            attend(j, 1, held_mine, e)

        @pl.when(phase == 7)
        def _():
            attend_own(e)
            keep(e, own_at, 3)

            @pl.when(e == 0)
            def _():
                proj_copy.wait()

    def block_copies(b):
        rows = rows_of(b, block)
        slot = lax.rem(b, 2)
        return [pltpu.make_async_copy(hidden.at[j, rows, :], x_big.at[slot, pl.ds(0, block), :], x_sem.at[slot])] + [
            pltpu.make_async_copy(ob.at[n, rows, :], ob_far.at[rows_of(2 * slot + n, block), :], o_sem.at[slot, n]) for n in range(2)]

    def fetch(b):
        @pl.when(lax.rem(b, per_half) == 0)
        def _():
            e = lax.div(b, per_half)
            near_stats(e).wait_recv()
            near_piece(e).wait_recv()
            y_stats(e).wait_recv()
            y_piece(e).wait_recv()

        start(block_copies(b))

    def begin(b):
        slot = lax.rem(b, 2)
        rows = rows_of(b, block)

        wait(block_copies(b))

        @pl.when(lax.rem(b, per_half) == 0)
        def _():
            e = lax.div(b, per_half)
            for copy in (near_stats(e), near_piece(e), y_stats(e), y_piece(e)):
                copy.wait_send()

        _, weights, total = piece_weights(heads, [st[3, :, rows], sbox[1, :, rows], sbox[2, :, rows]], head_dim)
        columns = as_columns([w / total for w in weights], head_dim)
        for h in range(heads):
            cols = slice(h * head_dim, (h + 1) * head_dim)
            pieces = [acc[rows, own_at + h * head_dim:own_at + (h + 1) * head_dim]]
            pieces += [ob_far[rows_of(2 * slot + n, block), cols] for n in range(2)]
            context = functools.reduce(
                jnp.add, [o * columns[:, n * heads + h:n * heads + h + 1] for n, o in enumerate(pieces)])
            x_big[1, block:2 * block, cols] = context.astype(BF16)
        x = x_big[slot, :block, :]
        x_big[0, block:2 * block, :] = layer_norm(x, gain2[...], bias2[...])
        acc[rows, :] = jnp.dot(x_big[1, block:2 * block, :span], proj[...], preferred_element_type=F32)

        @pl.when(z == 0)
        def _():
            acc[rows, :] += x.astype(F32) + small[:, extra_at:]

    def slice_of(b, f):
        rows = rows_of(b, block)

        @pl.when(b == 0)
        def _():
            wait(weight_copies(f))

        b_up = small[:, pl.ds(pl.multiple_of(3 * span + f * width, width), width)]
        wide_h = jnp.dot(x_big[0, block:2 * block, :], up[f], preferred_element_type=F32) + b_up
        act = (0.5 * wide_h * (1.0 + lax.erf(wide_h * math.sqrt(0.5)))).astype(BF16)
        acc[rows, :] += jnp.dot(act, down[f], preferred_element_type=F32)


    def at(ref, k):
        return ref.at[pl.ds(pl.multiple_of(k * tokens, tokens), tokens), :]

    def remote(src, dst, k, which, arrive, device):
        return pltpu.make_async_remote_copy(
            src_ref=at(src, k), dst_ref=at(dst, k), send_sem=send_sem.at[which], recv_sem=arrive.at[k],
            device_id=device, device_id_type=MESH,
        )

    def send_right(src, k):
        remote(src, from_left, k, 0, left_sem, {"tp": z + 1}).start()

    def send_left(src, k):
        remote(src, from_right, k, 1, right_sem, {"tp": z - 1}).start()

    def arrived(ref, sem, k):
        remote(ref, ref, k, 0, sem, {"cp": j}).wait_recv()

    def drained(ref, which):
        pltpu.make_async_copy(ref, ref, send_sem.at[which]).wait()

    def emit(stream, values, k, row):
        slot = lax.rem(k, STAGES)

        def copy():
            return pltpu.make_async_copy(stage.at[stream, slot], at(out_ref.at[row], k), stage_sem.at[stream, slot])

        @pl.when(k >= STAGES)
        def _():
            copy().wait()

        stage[stream, slot] = values.astype(BF16)
        copy().start()

    def chunk(ref, k):
        return ref[pl.ds(pl.multiple_of(k * tokens, tokens), tokens), :]

    def finish(src, k):
        remote(src, y_box, k, 2, y_sem, {"cp": across}).start()
        remote(src, core_box, k, 3, core_sem, {"cp": mate}).start()
        emit(0, chunk(src, k), k, j)

    def landing(n, box, k):
        slot = lax.rem(k, STAGES)
        return pltpu.make_async_copy(at(box, k), land.at[n, slot], land_sem.at[n, slot])

    def gathered(i):
        def lagged(lag, act):
            @pl.when(jnp.logical_and(i >= lag, i < pairs + lag))
            def _():
                for n in range(2):
                    act((i - lag) * 2 + n)

        def core(k):
            arrived(core_box, core_sem, k)
            landing(0, core_box, k).start()

        def core_out(k):
            landing(0, core_box, k).wait()
            emit(1, land[0, lax.rem(k, STAGES)], k, mate)

        def side(k):
            arrived(y_box, y_sem, k)
            remote(y_box, last_box, k, 4, last_sem, {"cp": mate}).start()
            landing(2, y_box, k).start()

        def side_out(k):
            landing(2, y_box, k).wait()
            emit(2, land[2, lax.rem(k, STAGES)], k, across)

        def final(k):
            arrived(last_box, last_sem, k)
            landing(1, last_box, k).start()

        def final_out(k):
            landing(1, last_box, k).wait()
            emit(3, land[1, lax.rem(k, STAGES)], k, corner)

        lagged(LAG_CORE + 1, core_out)
        lagged(LAG_Y + 1, side_out)
        lagged(LAG_LAST + 1, final_out)
        lagged(LAG_CORE, core)
        lagged(LAG_Y, side)
        lagged(LAG_LAST, final)

    def add(k, *others):
        rows = pl.ds(pl.multiple_of(k * tokens, tokens), tokens)
        total = acc[rows, :]
        for other in others:
            total = total + other[rows, :]
        acc[rows, :] = total

    def when(cond, act, *args):
        @pl.when(cond)
        def _():
            act(*args)

    def end(i, first):
        inbox, sem = (from_right, right_sem) if first else (from_left, left_sem)
        near_bit = 0 if first else 1

        def got(k):
            arrived(inbox, sem, k)
            finish(inbox, k)

        when(jnp.logical_and(i >= 0, i < pairs), lambda: got(2 * i + near_bit))
        when(jnp.logical_and(i >= LAG_BACK, i < pairs + LAG_BACK), lambda: got(2 * (i - LAG_BACK) + 1 - near_bit))

    def inner(i, left_side):
        mine = 0 if left_side else 1
        if left_side:
            (outer, outer_sem, to_outer), (inward, inward_sem, to_inner) = (
                (from_left, left_sem, send_left), (from_right, right_sem, send_right))
        else:
            (outer, outer_sem, to_outer), (inward, inward_sem, to_inner) = (
                (from_right, right_sem, send_right), (from_left, left_sem, send_left))

        def early(p):
            passed = 2 * p + 1 - mine
            arrived(outer, outer_sem, passed)
            add(passed, outer)
            to_inner(acc, passed)

        def near(p):
            rooted = 2 * p + mine
            arrived(outer, outer_sem, rooted)
            arrived(inward, inward_sem, rooted)
            add(rooted, from_left, from_right)
            to_outer(acc, rooted)
            to_inner(acc, rooted)
            finish(acc, rooted)

        def far(p):
            k = 2 * p + 1 - mine
            arrived(inward, inward_sem, k)
            to_outer(inward, k)
            finish(inward, k)

        when(jnp.logical_and(i + LAG_AHEAD >= 0, i + LAG_AHEAD < pairs), early, i + LAG_AHEAD)
        when(jnp.logical_and(i >= 0, i < pairs), near, i)
        when(jnp.logical_and(i >= LAG_BACK, i < pairs + LAG_BACK), far, i - LAG_BACK)

    lead = SLICES + LAG_START

    @pl.loop(0, waited + lead + pairs + LAG_LAST + 2)
    def _(step):
        s = step - waited

        @pl.when(step < HALVES * waited)
        def _():
            near(lax.div(step, waited), lax.rem(step, waited))

        @pl.when(step == waited - 2)
        def _():
            fetch(0)

        @pl.when(jnp.logical_and(s >= 0, s < BLOCKS * SLICES))
        def _():
            b, f = lax.div(s, SLICES), lax.rem(s, SLICES)
            when(f == 0, begin, b)
            when(jnp.logical_and(f == SLICES - 1, b + 1 < BLOCKS), fetch, b + 1)
            slice_of(b, f)

            def push(send, swapped):
                @pl.loop(0, 2 * per_block)
                def _(n):
                    send(acc, b * 2 * per_block + (n + 1 - 2 * lax.rem(n, 2) if swapped else n))

            when(jnp.logical_and(f == SLICES - 1, z == 0), push, send_right, True)
            when(jnp.logical_and(f == SLICES - 1, z == last), push, send_left, False)

        i = s - lead
        when(z == 0, end, i, True)
        when(z == root_a, inner, i, True)
        when(z == root_b, inner, i, False)
        when(z == last, end, i, False)
        gathered(i)

    @pl.when(z < last)
    def _():
        drained(acc, 0)

    @pl.when(z > 0)
    def _():
        drained(acc, 1)

    for which in (2, 3, 4):
        drained(acc, which)
    for t in range(TILES):
        mine_out(t).wait()
    for stream in range(4):
        for slot in range(STAGES):
            pltpu.make_async_copy(stage.at[stream, slot], at(out_ref.at[0], 0), stage_sem.at[stream, slot]).wait()


def run_layer(lengths, hidden_in, tables, k_block, v_block, w_qkv, w_up, w_down, w_out, norms, small, tp_size):
    num_rows, chunk_len, d_model = hidden_in.shape
    heads, slots, head_dim = k_block.shape[1:]
    span = heads * head_dim
    width = w_up.shape[1] // SLICES
    tokens = chunk_len // CHUNKS
    block = chunk_len // BLOCKS
    half = chunk_len // HALVES
    tile = chunk_len // TILES
    dma = pltpu.SemaphoreType.DMA
    buffer = pltpu.VMEM((chunk_len, d_model), F32)
    box = jax.ShapeDtypeStruct((chunk_len, d_model), F32)
    hbm = pl.BlockSpec(memory_space=pl.ANY)
    vmem = pl.BlockSpec(memory_space=pltpu.VMEM)
    out, _, _, _, pk, qb, _ = pl.pallas_call(
        functools.partial(layer_kernel, tp_size, heads),
        in_specs=[pl.BlockSpec(memory_space=pltpu.SMEM)] + [hbm] * 9 + [vmem] * 5,
        out_specs=[hbm] * 7,
        out_shape=[
            jax.ShapeDtypeStruct((num_rows, chunk_len, d_model), BF16), box, box, box,
            jax.ShapeDtypeStruct((2, chunk_len, 3 * span), BF16),
            jax.ShapeDtypeStruct((2, chunk_len, 3 * span), F32),
            jax.ShapeDtypeStruct((2, chunk_len, span), F32),
        ],
        scratch_shapes=[buffer] * 3
        + [
            pltpu.VMEM((SLICES, d_model, width), BF16),
            pltpu.VMEM((SLICES, width, d_model), BF16),
            pltpu.VMEM((span, d_model), BF16),
            pltpu.VMEM((TILES, tile, 3 * span), BF16),
            pltpu.VMEM((2, tile, d_model), BF16),
            pltpu.VMEM((2, 2) + tables[0].shape[1:], F32),
            pltpu.VMEM((2, 2, heads, slots, head_dim), BF16),
            pltpu.VMEM((chunk_len, span), F32),
            pltpu.VMEM((heads, half, head_dim), F32),
            pltpu.VMEM((heads, half, head_dim), F32),
            pltpu.VMEM((heads, half, head_dim), F32),
            pltpu.VMEM((4, 8, chunk_len), F32),
            pltpu.VMEM((3, 8, chunk_len), F32),
            pltpu.VMEM((4, STAGES, tokens, d_model), BF16),
            pltpu.VMEM((3, STAGES, tokens, d_model), F32),
        ]
        + [dma((SLICES,)), dma((SLICES,)), dma, dma((2,)), dma((2, 2)), dma((TILES,)), dma((TILES,)), dma((2, 2)), dma((heads,)),
           dma((2,)), dma((2, 2))]
        + [dma((2, TILES, 3))] * 2
        + [dma((HALVES,))] * 12
        + [dma((CHUNKS,))] * 5
        + [dma((5,)), dma((4, STAGES)), dma((3, STAGES))],
        compiler_params=pltpu.CompilerParams(collective_id=0, has_side_effects=True, vmem_limit_bytes=LAYER_LIMIT),
        cost_estimate=pl.CostEstimate(flops=100_000_000_000, bytes_accessed=chunk_len * d_model * 16, transcendentals=0),
        name="layer",
    )(lengths, hidden_in, *tables, k_block, v_block, w_qkv, w_up, w_down, w_out, *norms, small[None])
    return out, pk, qb


def finish_kernel(heads, meta, in_ref, pk, qb, out_ref, k_ref, v_ref, buf, low, high, in_sem, out_sem, low_sem, high_sem, kv_sem):
    pieces = in_sem.shape[1]
    tile = buf.shape[1] // pieces
    head_dim = k_ref.shape[3]
    places = [(b, pl.ds(t * tile, tile), t) for b in range(buf.shape[0]) for t in range(pieces)]
    inward = [pltpu.make_async_copy(in_ref.at[b, rows], buf.at[b, rows], in_sem.at[b, t]) for b, rows, t in places]
    outward = [pltpu.make_async_copy(buf.at[b, rows], out_ref.at[b, rows], out_sem.at[b, t]) for b, rows, t in places]
    both = 2 * head_dim

    def taken(src, dst, sem):
        return [[pltpu.make_async_copy(src.at[n, :, pl.ds((3 * h + 1) * head_dim, both)], dst.at[n, :, pl.ds(h * both, both)], sem.at[n, h])
                 for h in range(heads)] for n in range(2)]

    lows, highs = taken(pk, low, low_sem), taken(qb, high, high_sem)
    stored = []

    def store(n, h, row):
        for p, ref in enumerate((k_ref, v_ref)):
            cols = pl.ds(h * both + p * head_dim, head_dim)
            copy = pltpu.make_async_copy(low.at[n, :, cols], ref.at[row, h], kv_sem.at[n, h, p])
            copy.start()
            stored.append(copy)

    for copy in highs[0] + highs[1] + lows[0] + lows[1] + inward:
        copy.start()
    j = meta[0]
    for n in range(2):
        for h in range(heads):
            lows[n][h].wait()
            store(n, h, j ^ (2 - 2 * n))
    for n in range(2):
        for h in range(heads):
            highs[n][h].wait()
            cols = slice(h * both, (h + 1) * both)
            low[2 + n, :, cols] = high[n, :, cols].astype(BF16)
            store(2 + n, h, j ^ (3 - 2 * n))
    for one, other in zip(inward, outward):
        one.wait()
        other.start()
    for copy in outward + stored:
        copy.wait()


def finish(meta, out, pk, qb, heads, head_dim):
    rows, chunk_len, _ = out.shape
    span = 2 * heads * head_dim
    hbm = pl.BlockSpec(memory_space=pl.ANY)
    cache = jax.ShapeDtypeStruct((rows, heads, chunk_len, head_dim), BF16)
    dma = pltpu.SemaphoreType.DMA
    return pl.pallas_call(
        functools.partial(finish_kernel, heads),
        in_specs=[pl.BlockSpec(memory_space=pltpu.SMEM)] + [hbm] * 3,
        out_specs=[hbm] * 3,
        out_shape=[jax.ShapeDtypeStruct(out.shape, out.dtype), cache, cache],
        scratch_shapes=[
            pltpu.VMEM(out.shape, out.dtype), pltpu.VMEM((4, chunk_len, span), BF16), pltpu.VMEM((2, chunk_len, span), F32),
            dma((rows, 4)), dma((rows, 4)), dma((2, heads)), dma((2, heads)), dma((4, heads, 2)),
        ],
        compiler_params=pltpu.CompilerParams(vmem_limit_bytes=VMEM_LIMIT),
        name="finish",
    )(meta, out, pk, qb)


def solution(mesh):
    in_specs = (P("dp", None, None), P("dp"), P("dp", "tp", "cp", None), P("dp", "tp", "cp", None), P(), P(), P(), P(), P(None, "tp"), P("tp"), P("tp", None), P(), P(None, "tp"), P("tp"), P("tp", None), P())
    out_specs = (P("dp", None, None), P("dp", "tp", None, None), P("dp", "tp", None, None))
    tp_size = mesh.shape["tp"]

    def local_layer(hidden_in, lengths, k_block, v_block, ln1_gain, ln1_bias, ln2_gain, ln2_bias, w_qkv, b_qkv, w_out, b_out, w_up, b_up, w_down, b_down):
        num_rows, chunk_len, d_model = hidden_in.shape
        heads, block_len, head_dim = k_block.shape[1:]
        tables = rope_tables(lengths, chunk_len, head_dim)
        norms = [p[None] for p in (ln1_gain, ln1_bias, ln2_gain, ln2_bias)]
        parts = [(b_qkv, 0), (b_up, b_qkv.shape[0]), (b_out, b_qkv.shape[0] + b_up.shape[0]), (b_down, b_qkv.shape[0] + b_up.shape[0])]
        total = b_qkv.shape[0] + b_up.shape[0] + d_model
        small = functools.reduce(jnp.add, [jnp.pad(p.astype(F32), (at, total - at - p.shape[0])) for p, at in parts])
        out, pk, qb = run_layer(lengths, hidden_in, tables, k_block, v_block, w_qkv, w_up, w_down, w_out, norms, small, tp_size)
        return tuple(finish(lax.axis_index("cp")[None], out, pk, qb, heads, head_dim))

    return jax.shard_map(local_layer, mesh=mesh, in_specs=in_specs, out_specs=out_specs, check_vma=False)
```

```python
import functools
import math

import jax
import jax.numpy as jnp
from jax import lax
from jax.experimental import pallas as pl
from jax.experimental.pallas import tpu as pltpu
from jax.sharding import PartitionSpec as P

EPSILON = 1e-5
NEG_BIG = -1e30
ROTARY_SHARE = 4
ROPE_BASE = 10000.0
LOG2E = math.log2(math.e)
MESH = pl.DeviceIdType.MESH
F32 = jnp.float32
BF16 = jnp.bfloat16
VMEM_LIMIT = 60 * 1024 * 1024
LAYER_LIMIT = 67_043_328
EMPTY = -1e29
CHUNKS = 64
STAGES = 4
BLOCKS = 8
SLICES = 4
TILES = 4
HALVES = 4
LAG_START = 2
LAG_AHEAD = 1
LAG_BACK = 1
LAG_CORE = 3
LAG_Y = 9
LAG_LAST = 11


def layer_norm(values_in, gain_vec, bias_vec):
    x_f32 = values_in.astype(F32)
    row_mean = jnp.mean(x_f32, axis=-1, keepdims=True)
    centered = x_f32 - row_mean
    variance = jnp.mean(centered * centered, axis=-1, keepdims=True)
    return (centered * lax.rsqrt(variance + EPSILON) * gain_vec + bias_vec).astype(BF16)


def rope_tables(lengths, chunk_len, head_dim):
    rot_dim = head_dim // ROTARY_SHARE
    shape = (lengths.shape[0], rot_dim // 2, chunk_len)
    positions = lengths[:, None, None] + lax.broadcasted_iota(jnp.int32, shape, 2)
    inv_freq = ROPE_BASE ** (-2.0 * jnp.arange(rot_dim // 2, dtype=F32) / rot_dim)
    angles = positions.astype(F32) * inv_freq[:, None]
    return jnp.cos(angles), jnp.sin(angles)


def wide(column, lanes):
    return jnp.concatenate([column] * (lanes // column.shape[1]), axis=1)


def scores_of(query, keys, scale, mask):
    scores = lax.dot_general(query, keys, (((1,), (1,)), ((), ())), preferred_element_type=F32) * scale
    return scores if mask is None else jnp.where(mask, scores, NEG_BIG)


def lane_sum(values, lanes):
    return functools.reduce(jnp.add, [values[:, n:n + lanes] for n in range(0, values.shape[1], lanes)])


def lane_max(values, lanes):
    return functools.reduce(jnp.maximum, [values[:, n:n + lanes] for n in range(0, values.shape[1], lanes)])


def ahead(heads, scores):
    coming = scores(0)
    for h in range(heads):
        now = coming
        if h + 1 < heads:
            coming = scores(h + 1)
        yield h, now


def first_step(heads, scale, q_of, k_of, v_of, m_scr, l_scr, o_scr, mask):
    lanes = o_scr.shape[2]
    for h, scores in ahead(heads, lambda h: scores_of(q_of(h), k_of(h), scale, mask)):
        peak = jnp.maximum(jnp.max(lane_max(scores, lanes), axis=1, keepdims=True), EMPTY)
        peak = jnp.broadcast_to(peak, m_scr.shape[1:])
        probs = jnp.exp2(scores - wide(peak, scores.shape[1]))
        m_scr[h] = peak
        l_scr[h] = lane_sum(probs, lanes)
        o_scr[h] = jnp.dot(probs.astype(BF16), v_of(h), preferred_element_type=F32)


def block_step(heads, scale, q_of, k_of, v_of, m_scr, l_scr, o_scr, mask):
    lanes = o_scr.shape[2]
    for h, scores in ahead(heads, lambda h: scores_of(q_of(h), k_of(h), scale, mask)):
        m_old = m_scr[h]
        m_new = jnp.maximum(m_old, jnp.max(lane_max(scores, lanes), axis=1, keepdims=True))
        probs = jnp.exp2(scores - wide(m_new, scores.shape[1]))
        shrink = jnp.exp2(m_old - m_new)
        l_scr[h] = l_scr[h] * shrink + lane_sum(probs, lanes)
        m_scr[h] = m_new
        o_scr[h] = o_scr[h] * shrink + jnp.dot(probs.astype(BF16), v_of(h), preferred_element_type=F32)


def piece_weights(heads, stats, head_dim):
    peak = functools.reduce(jnp.maximum, [s[:heads] for s in stats])
    weights = [jnp.exp2(s[:heads] - peak) for s in stats]
    total = functools.reduce(jnp.add, [s[heads:2 * heads] * w for s, w in zip(stats, weights)])
    return peak, weights, total


def as_columns(parts, head_dim):
    count = sum(p.shape[0] for p in parts)
    return jnp.concatenate(parts + [jnp.zeros((head_dim - count, parts[0].shape[1]), F32)], axis=0).T


def layer_kernel(tp_size, heads, lengths, hidden, cos_all, sin_all, k_cache, v_cache, w_qkv, w_up, w_down, w_out,
                 gain1, bias1, gain2, bias2, small,
                 out_ref, y_box, core_box, last_box, pk, qb, ob,
                 acc, from_left, from_right, up, down, proj, mine, x_big, tab_buf, kv, ob_far, m_scr, l_scr, o_scr, st, sbox,
                 stage, land,
                 up_sem, down_sem, proj_sem, xb_sem, tab_sem, pk_sem, mine_sem, kv_sem, q_sem, x_sem, o_sem,
                 qs_sem, qr_sem, fs_sem, fr_sem, ns_sem, nr_sem, ys_sem, yr_sem,
                 fss_sem, fsr_sem, nss_sem, nsr_sem, yss_sem, ysr_sem,
                 left_sem, right_sem, y_sem, core_sem, last_sem, send_sem, stage_sem, land_sem):
    z = lax.axis_index("tp")
    j = lax.axis_index("cp")
    y, c = lax.div(j, 2), lax.rem(j, 2)
    across, mate, corner = (1 - y) * 2 + c, y * 2 + (1 - c), (1 - y) * 2 + (1 - c)
    chunk_len, d_model = acc.shape
    head_dim = o_scr.shape[2]
    span = heads * head_dim
    slots = k_cache.shape[2]
    tokens = chunk_len // CHUNKS
    block = chunk_len // BLOCKS
    half = chunk_len // HALVES
    tile = chunk_len // TILES
    pairs = CHUNKS // 2
    per_block = pairs // BLOCKS
    width = up.shape[2]
    last = tp_size - 1
    root_a, root_b = (tp_size - 1) // 2, tp_size // 2
    rot_dim = head_dim // ROTARY_SHARE
    half_rot = rot_dim // 2
    scale = head_dim ** -0.5 * LOG2E
    own_at, sent_at, kept_at, q_at = 0, span, 2 * span, 3 * span
    extra_at = 3 * span + SLICES * width
    per_half = BLOCKS // HALVES
    waited = per_half * SLICES

    def rows_of(n, size):
        return pl.ds(pl.multiple_of(n * size, size), size)

    def weight_copies(f):
        cols = pl.ds(f * width, width)
        return (pltpu.make_async_copy(w_up.at[:, cols], up.at[f], up_sem.at[f]),
                pltpu.make_async_copy(w_down.at[cols, :], down.at[f], down_sem.at[f]))

    def row_of(n):
        return across * (1 - n) + j * n

    def big_x(i):
        return pltpu.make_async_copy(
            hidden.at[row_of(lax.div(i, TILES)), rows_of(lax.rem(i, TILES), tile), :], x_big.at[lax.rem(i, 2)], xb_sem.at[lax.rem(i, 2)])

    def cache_copies(row, slot):
        return (pltpu.make_async_copy(k_cache.at[row], kv.at[slot, 0], kv_sem.at[slot, 0]),
                pltpu.make_async_copy(v_cache.at[row], kv.at[slot, 1], kv_sem.at[slot, 1]))

    def start(copies):
        for copy in copies:
            copy.start()

    def wait(copies):
        for copy in copies:
            copy.wait()

    qkv_copies = [pltpu.make_async_copy(w_qkv.at[:, pl.ds(s * width, width)], up.at[s], up_sem.at[s]) for s in range(3)]
    tab_copies = [pltpu.make_async_copy(ref.at[row], tab_buf.at[n, p], tab_sem.at[n, p])
                  for n, row in enumerate((across, j)) for p, ref in enumerate((cos_all, sin_all))]
    proj_copy = pltpu.make_async_copy(w_out, proj, proj_sem)
    big_x(0).start()
    start(qkv_copies)
    start(tab_copies)
    start(cache_copies(corner, 0))
    start(cache_copies(across, 1))
    proj_copy.start()

    barrier = pltpu.get_barrier_semaphore()
    pl.semaphore_signal(barrier, inc=1, device_id={"cp": across}, device_id_type=MESH)
    pl.semaphore_signal(barrier, inc=1, device_id={"cp": mate}, device_id_type=MESH)

    @pl.when(z > 0)
    def _():
        pl.semaphore_signal(barrier, inc=1, device_id={"tp": z - 1}, device_id_type=MESH)

    @pl.when(z < last)
    def _():
        pl.semaphore_signal(barrier, inc=1, device_id={"tp": z + 1}, device_id_type=MESH)

    inside = jnp.logical_and(z > 0, z < last)

    @pl.when(inside)
    def _():
        pl.semaphore_wait(barrier, 4)

    @pl.when(jnp.logical_not(inside))
    def _():
        pl.semaphore_wait(barrier, 3)

    def to_core(src, dst, send, arrive):
        return pltpu.make_async_remote_copy(
            src_ref=src, dst_ref=dst, send_sem=send, recv_sem=arrive, device_id={"cp": mate}, device_id_type=MESH)

    def to_y(src, dst, send, arrive):
        return pltpu.make_async_remote_copy(
            src_ref=src, dst_ref=dst, send_sem=send, recv_sem=arrive, device_id={"cp": across}, device_id_type=MESH)


    def staged(n, t, part):
        return acc.at[rows_of(t, tile), pl.ds((q_at if n == 1 and part == 2 else part * span), span)]

    def sent_tile(n, t):
        return [to_core(staged(n, t, p), qb.at[n, rows_of(t, tile), pl.ds(p * span, span)], qs_sem.at[n, t, p], qr_sem.at[n, t, p])
                for p in range(3)]

    def sent_off(n, t):
        for copy in sent_tile(n, t):
            copy.wait_send()

    def project(n, t, place):
        i = n * TILES + t

        @pl.when(i + 1 < 2 * TILES)
        def _():
            big_x(i + 1).start()

        big_x(i).wait()
        normed = layer_norm(x_big[lax.rem(i, 2)], gain1[...], bias1[...])
        cos_part, sin_part = tab_buf[n, 0, :, rows_of(t, tile)], tab_buf[n, 1, :, rows_of(t, tile)]
        tab = jnp.concatenate([cos_part, cos_part, -sin_part, sin_part] * (head_dim // (4 * half_rot)), axis=0).T
        lane = lax.broadcasted_iota(jnp.int32, tab.shape, 1)
        cos_tab = jnp.where(lane < rot_dim, tab, 1.0)
        sin_tab = jnp.where(lane < rot_dim, pltpu.roll(tab, head_dim - rot_dim, 1), 0.0)

        def rotate(values):
            long = values.astype(F32)
            other = jnp.where(lane < half_rot, pltpu.roll(long, head_dim - half_rot, 1), pltpu.roll(long, half_rot, 1))
            return (long * cos_tab + other * sin_tab).astype(BF16)

        for p, product in ahead(3, lambda p: jnp.dot(normed, up[p], preferred_element_type=F32)):
            some = (product + small[:, p * span:(p + 1) * span]).astype(BF16)
            for g in range(heads):
                group = p * heads + g
                values = some[:, g * head_dim:(g + 1) * head_dim]
                if group % 3 < 2:
                    values = rotate(values)
                place[:, group * head_dim:(group + 1) * head_dim] = values
                staged(n, t, p)[:, g * head_dim:(g + 1) * head_dim] = values.astype(F32)
        start(sent_tile(n, t))

    def query_copies(n, t):
        rows = rows_of(t, tile)
        return [pltpu.make_async_copy(qb.at[n, rows, pl.ds(3 * h * head_dim, head_dim)],
                                      acc.at[rows, pl.ds(q_at + h * head_dim, head_dim)], q_sem.at[h]) for h in range(heads)]

    def fetch_queries(n, t):
        for copy in sent_tile(n, t):
            copy.wait_recv()
        start(query_copies(n, t))

    per_slice = width // tile

    def far_place(t):
        return down.at[lax.div(t, per_slice), rows_of(lax.rem(t, per_slice), tile), pl.ds(0, 3 * span)]

    def mine_out(t):
        return pltpu.make_async_copy(mine.at[t], pk.at[1, rows_of(t, tile), :], mine_sem.at[t])

    wait(qkv_copies)
    wait(tab_copies)


    def attend(row, slot, query, e):
        valid = jnp.clip(lengths[row] - j * slots, 0, slots)
        mask = lax.broadcasted_iota(jnp.int32, (half, slots), 1) < valid
        first_step(heads, scale, lambda h: query(e, h), lambda h: kv[slot, 0, h], lambda h: kv[slot, 1, h],
                   m_scr, l_scr, o_scr, mask)

    def attend_own(e):
        def own_block(b, mask):
            def part(p):
                return lambda h: mine[b, :, (3 * h + p) * head_dim:(3 * h + p + 1) * head_dim]

            block_step(heads, scale, lambda h: held_mine(e, h), part(1), part(2), m_scr, l_scr, o_scr, mask)

        @pl.loop(0, e)
        def _(b):
            own_block(b, None)

        shape = (half, half)
        own_block(e, lax.broadcasted_iota(jnp.int32, shape, 0) >= lax.broadcasted_iota(jnp.int32, shape, 1))

    def keep(e, at, kind):
        lane = lax.broadcasted_iota(jnp.int32, (half, head_dim), 1)
        stats = jnp.zeros((half, head_dim), F32)
        for h in range(heads):
            stats = jnp.where(lane == h, m_scr[h], stats)
            stats = jnp.where(lane == heads + h, jnp.sum(l_scr[h], axis=1, keepdims=True), stats)
            acc[rows_of(e, half), at + h * head_dim:at + (h + 1) * head_dim] = o_scr[h]
        st[kind, :, rows_of(e, half)] = stats.T[:8]

    def held_far(e, h):
        return far_place(e)[:, 3 * h * head_dim:(3 * h + 1) * head_dim]

    def held_mine(e, h):
        return mine[e, :, 3 * h * head_dim:(3 * h + 1) * head_dim]

    def taken(e, h):
        return acc[rows_of(e, half), q_at + h * head_dim:q_at + (h + 1) * head_dim].astype(BF16)

    def far_piece(e):
        return to_core(acc.at[rows_of(e, half), pl.ds(sent_at, span)], ob_far.at[rows_of(e, half), :], fs_sem.at[e], fr_sem.at[e])

    def near_piece(e):
        return to_core(acc.at[rows_of(e, half), pl.ds(sent_at, span)], ob.at[0, rows_of(e, half), :], ns_sem.at[e], nr_sem.at[e])

    def y_piece(e):
        return to_y(acc.at[rows_of(e, half), pl.ds(kept_at, span)], ob.at[1, rows_of(e, half), :], ys_sem.at[e], yr_sem.at[e])

    def far_stats(e):
        return to_core(st.at[0, :, rows_of(e, half)], sbox.at[0, :, rows_of(e, half)], fss_sem.at[e], fsr_sem.at[e])

    def near_stats(e):
        return to_core(st.at[2, :, rows_of(e, half)], sbox.at[1, :, rows_of(e, half)], nss_sem.at[e], nsr_sem.at[e])

    def y_stats(e):
        return to_y(st.at[1, :, rows_of(e, half)], sbox.at[2, :, rows_of(e, half)], yss_sem.at[e], ysr_sem.at[e])

    def far_attend(e):
        fetch_queries(0, e)
        sent_off(0, e)
        attend(across, 1, held_far, e)
        keep(e, kept_at, 1)
        wait(query_copies(0, e))
        attend(corner, 0, taken, e)
        keep(e, sent_at, 0)
        far_stats(e).start()
        far_piece(e).start()

    def far_join(e):
        far_stats(e).wait_recv()
        far_piece(e).wait_recv()
        rows = rows_of(e, half)
        peak, weights, total = piece_weights(heads, [st[1, :, rows], sbox[0, :, rows]], head_dim)
        columns = as_columns(weights, head_dim)
        for h in range(heads):
            at = kept_at + h * head_dim
            acc[rows, at:at + head_dim] = (acc[rows, at:at + head_dim] * columns[:, h:h + 1]
                                           + ob_far[rows, h * head_dim:(h + 1) * head_dim] * columns[:, heads + h:heads + h + 1])
        st[1, :heads, rows] = peak
        st[1, heads:2 * heads, rows] = total
        y_stats(e).start()
        y_piece(e).start()

    @pl.loop(0, TILES + 2)
    def _(t):
        @pl.when(t < TILES)
        def _():
            project(0, t, far_place(t))

        @pl.when(t == 1)
        def _():
            wait(cache_copies(corner, 0))
            wait(cache_copies(across, 1))

        @pl.when(t >= 2)
        def _():
            far_join(t - 2)

        @pl.when(jnp.logical_and(t >= 1, t <= TILES))
        def _():
            far_attend(t - 1)

    start(cache_copies(mate, 0))
    start(cache_copies(j, 1))
    pack_copies = [pltpu.make_async_copy(far_place(t), pk.at[0, rows_of(t, tile), :], pk_sem.at[t]) for t in range(TILES)]
    start(pack_copies)
    for e in range(HALVES):
        far_stats(e).wait_send()
        far_piece(e).wait_send()

    @pl.loop(0, TILES)
    def _(t):
        @pl.when(t == 2)
        def _():
            sent_off(1, 0)
            fetch_queries(1, 0)

        project(1, t, mine.at[t])
        mine_out(t).start()

    wait(pack_copies)
    for f in range(SLICES):
        start(weight_copies(f))
    wait(cache_copies(mate, 0))


    def near(e, phase):
        @pl.when(jnp.logical_and(phase == 4, e > 0))
        def _():
            sent_off(1, e)
            fetch_queries(1, e)

        @pl.when(phase == 5)
        def _():
            wait(query_copies(1, e))
            attend(mate, 0, taken, e)
            keep(e, sent_at, 2)
            near_stats(e).start()
            near_piece(e).start()

            @pl.when(e == 0)
            def _():
                wait(cache_copies(j, 1))

        @pl.when(phase == 6)
        def _():
            attend(j, 1, held_mine, e)

        @pl.when(phase == 7)
        def _():
            attend_own(e)
            keep(e, own_at, 3)

            @pl.when(e == 0)
            def _():
                proj_copy.wait()

    def block_copies(b):
        rows = rows_of(b, block)
        slot = lax.rem(b, 2)
        return [pltpu.make_async_copy(hidden.at[j, rows, :], x_big.at[slot, pl.ds(0, block), :], x_sem.at[slot])] + [
            pltpu.make_async_copy(ob.at[n, rows, :], ob_far.at[rows_of(2 * slot + n, block), :], o_sem.at[slot, n]) for n in range(2)]

    def fetch(b):
        @pl.when(lax.rem(b, per_half) == 0)
        def _():
            e = lax.div(b, per_half)
            near_stats(e).wait_recv()
            near_piece(e).wait_recv()
            y_stats(e).wait_recv()
            y_piece(e).wait_recv()

        start(block_copies(b))

    def begin(b):
        slot = lax.rem(b, 2)
        rows = rows_of(b, block)

        wait(block_copies(b))

        @pl.when(lax.rem(b, per_half) == 0)
        def _():
            e = lax.div(b, per_half)
            for copy in (near_stats(e), near_piece(e), y_stats(e), y_piece(e)):
                copy.wait_send()

        _, weights, total = piece_weights(heads, [st[3, :, rows], sbox[1, :, rows], sbox[2, :, rows]], head_dim)
        columns = as_columns([w / total for w in weights], head_dim)
        for h in range(heads):
            cols = slice(h * head_dim, (h + 1) * head_dim)
            pieces = [acc[rows, own_at + h * head_dim:own_at + (h + 1) * head_dim]]
            pieces += [ob_far[rows_of(2 * slot + n, block), cols] for n in range(2)]
            context = functools.reduce(
                jnp.add, [o * columns[:, n * heads + h:n * heads + h + 1] for n, o in enumerate(pieces)])
            x_big[1, block:2 * block, cols] = context.astype(BF16)
        x = x_big[slot, :block, :]
        x_big[0, block:2 * block, :] = layer_norm(x, gain2[...], bias2[...])
        acc[rows, :] = jnp.dot(x_big[1, block:2 * block, :span], proj[...], preferred_element_type=F32)

        @pl.when(z == 0)
        def _():
            acc[rows, :] += x.astype(F32) + small[:, extra_at:]

    def slice_of(b, f):
        rows = rows_of(b, block)

        @pl.when(b == 0)
        def _():
            wait(weight_copies(f))

        b_up = small[:, pl.ds(pl.multiple_of(3 * span + f * width, width), width)]
        wide_h = jnp.dot(x_big[0, block:2 * block, :], up[f], preferred_element_type=F32) + b_up
        act = (0.5 * wide_h * (1.0 + lax.erf(wide_h * math.sqrt(0.5)))).astype(BF16)
        acc[rows, :] += jnp.dot(act, down[f], preferred_element_type=F32)


    def at(ref, k):
        return ref.at[pl.ds(pl.multiple_of(k * tokens, tokens), tokens), :]

    def remote(src, dst, k, which, arrive, device):
        return pltpu.make_async_remote_copy(
            src_ref=at(src, k), dst_ref=at(dst, k), send_sem=send_sem.at[which], recv_sem=arrive.at[k],
            device_id=device, device_id_type=MESH,
        )

    def send_right(src, k):
        remote(src, from_left, k, 0, left_sem, {"tp": z + 1}).start()

    def send_left(src, k):
        remote(src, from_right, k, 1, right_sem, {"tp": z - 1}).start()

    def arrived(ref, sem, k):
        remote(ref, ref, k, 0, sem, {"cp": j}).wait_recv()

    def drained(ref, which):
        pltpu.make_async_copy(ref, ref, send_sem.at[which]).wait()

    def emit(stream, values, k, row):
        slot = lax.rem(k, STAGES)

        def copy():
            return pltpu.make_async_copy(stage.at[stream, slot], at(out_ref.at[row], k), stage_sem.at[stream, slot])

        @pl.when(k >= STAGES)
        def _():
            copy().wait()

        stage[stream, slot] = values.astype(BF16)
        copy().start()

    def chunk(ref, k):
        return ref[pl.ds(pl.multiple_of(k * tokens, tokens), tokens), :]

    def finish(src, k):
        remote(src, y_box, k, 2, y_sem, {"cp": across}).start()
        remote(src, core_box, k, 3, core_sem, {"cp": mate}).start()
        emit(0, chunk(src, k), k, j)

    def landing(n, box, k):
        slot = lax.rem(k, STAGES)
        return pltpu.make_async_copy(at(box, k), land.at[n, slot], land_sem.at[n, slot])

    def gathered(i):
        def lagged(lag, act):
            @pl.when(jnp.logical_and(i >= lag, i < pairs + lag))
            def _():
                for n in range(2):
                    act((i - lag) * 2 + n)

        def core(k):
            arrived(core_box, core_sem, k)
            landing(0, core_box, k).start()

        def core_out(k):
            landing(0, core_box, k).wait()
            emit(1, land[0, lax.rem(k, STAGES)], k, mate)

        def side(k):
            arrived(y_box, y_sem, k)
            remote(y_box, last_box, k, 4, last_sem, {"cp": mate}).start()
            landing(2, y_box, k).start()

        def side_out(k):
            landing(2, y_box, k).wait()
            emit(2, land[2, lax.rem(k, STAGES)], k, across)

        def final(k):
            arrived(last_box, last_sem, k)
            landing(1, last_box, k).start()

        def final_out(k):
            landing(1, last_box, k).wait()
            emit(3, land[1, lax.rem(k, STAGES)], k, corner)

        lagged(LAG_CORE + 1, core_out)
        lagged(LAG_Y + 1, side_out)
        lagged(LAG_LAST + 1, final_out)
        lagged(LAG_CORE, core)
        lagged(LAG_Y, side)
        lagged(LAG_LAST, final)

    def add(k, *others):
        rows = pl.ds(pl.multiple_of(k * tokens, tokens), tokens)
        total = acc[rows, :]
        for other in others:
            total = total + other[rows, :]
        acc[rows, :] = total

    def when(cond, act, *args):
        @pl.when(cond)
        def _():
            act(*args)

    def end(i, first):
        inbox, sem = (from_right, right_sem) if first else (from_left, left_sem)
        near_bit = 0 if first else 1

        def got(k):
            arrived(inbox, sem, k)
            finish(inbox, k)

        when(jnp.logical_and(i >= 0, i < pairs), lambda: got(2 * i + near_bit))
        when(jnp.logical_and(i >= LAG_BACK, i < pairs + LAG_BACK), lambda: got(2 * (i - LAG_BACK) + 1 - near_bit))

    def inner(i, left_side):
        mine = 0 if left_side else 1
        if left_side:
            (outer, outer_sem, to_outer), (inward, inward_sem, to_inner) = (
                (from_left, left_sem, send_left), (from_right, right_sem, send_right))
        else:
            (outer, outer_sem, to_outer), (inward, inward_sem, to_inner) = (
                (from_right, right_sem, send_right), (from_left, left_sem, send_left))

        def early(p):
            passed = 2 * p + 1 - mine
            arrived(outer, outer_sem, passed)
            add(passed, outer)
            to_inner(acc, passed)

        def near(p):
            rooted = 2 * p + mine
            arrived(outer, outer_sem, rooted)
            arrived(inward, inward_sem, rooted)
            add(rooted, from_left, from_right)
            to_outer(acc, rooted)
            to_inner(acc, rooted)
            finish(acc, rooted)

        def far(p):
            k = 2 * p + 1 - mine
            arrived(inward, inward_sem, k)
            to_outer(inward, k)
            finish(inward, k)

        when(jnp.logical_and(i + LAG_AHEAD >= 0, i + LAG_AHEAD < pairs), early, i + LAG_AHEAD)
        when(jnp.logical_and(i >= 0, i < pairs), near, i)
        when(jnp.logical_and(i >= LAG_BACK, i < pairs + LAG_BACK), far, i - LAG_BACK)

    lead = SLICES + LAG_START

    @pl.loop(0, waited + lead + pairs + LAG_LAST + 2)
    def _(step):
        s = step - waited

        @pl.when(step < HALVES * waited)
        def _():
            near(lax.div(step, waited), lax.rem(step, waited))

        @pl.when(step == waited - 2)
        def _():
            fetch(0)

        @pl.when(jnp.logical_and(s >= 0, s < BLOCKS * SLICES))
        def _():
            b, f = lax.div(s, SLICES), lax.rem(s, SLICES)
            when(f == 0, begin, b)
            when(jnp.logical_and(f == SLICES - 1, b + 1 < BLOCKS), fetch, b + 1)
            slice_of(b, f)

            def push(send, swapped):
                @pl.loop(0, 2 * per_block)
                def _(n):
                    send(acc, b * 2 * per_block + (n + 1 - 2 * lax.rem(n, 2) if swapped else n))

            when(jnp.logical_and(f == SLICES - 1, z == 0), push, send_right, True)
            when(jnp.logical_and(f == SLICES - 1, z == last), push, send_left, False)

        i = s - lead
        when(z == 0, end, i, True)
        when(z == root_a, inner, i, True)
        when(z == root_b, inner, i, False)
        when(z == last, end, i, False)
        gathered(i)

    @pl.when(z < last)
    def _():
        drained(acc, 0)

    @pl.when(z > 0)
    def _():
        drained(acc, 1)

    for which in (2, 3, 4):
        drained(acc, which)
    for t in range(TILES):
        mine_out(t).wait()
    for stream in range(4):
        for slot in range(STAGES):
            pltpu.make_async_copy(stage.at[stream, slot], at(out_ref.at[0], 0), stage_sem.at[stream, slot]).wait()


def run_layer(lengths, hidden_in, tables, k_block, v_block, w_qkv, w_up, w_down, w_out, norms, small, tp_size):
    num_rows, chunk_len, d_model = hidden_in.shape
    heads, slots, head_dim = k_block.shape[1:]
    span = heads * head_dim
    width = w_up.shape[1] // SLICES
    tokens = chunk_len // CHUNKS
    block = chunk_len // BLOCKS
    half = chunk_len // HALVES
    tile = chunk_len // TILES
    dma = pltpu.SemaphoreType.DMA
    buffer = pltpu.VMEM((chunk_len, d_model), F32)
    box = jax.ShapeDtypeStruct((chunk_len, d_model), F32)
    hbm = pl.BlockSpec(memory_space=pl.ANY)
    vmem = pl.BlockSpec(memory_space=pltpu.VMEM)
    out, _, _, _, pk, qb, _ = pl.pallas_call(
        functools.partial(layer_kernel, tp_size, heads),
        in_specs=[pl.BlockSpec(memory_space=pltpu.SMEM)] + [hbm] * 9 + [vmem] * 5,
        out_specs=[hbm] * 7,
        out_shape=[
            jax.ShapeDtypeStruct((num_rows, chunk_len, d_model), BF16), box, box, box,
            jax.ShapeDtypeStruct((2, chunk_len, 3 * span), BF16),
            jax.ShapeDtypeStruct((2, chunk_len, 3 * span), F32),
            jax.ShapeDtypeStruct((2, chunk_len, span), F32),
        ],
        scratch_shapes=[buffer] * 3
        + [
            pltpu.VMEM((SLICES, d_model, width), BF16),
            pltpu.VMEM((SLICES, width, d_model), BF16),
            pltpu.VMEM((span, d_model), BF16),
            pltpu.VMEM((TILES, tile, 3 * span), BF16),
            pltpu.VMEM((2, tile, d_model), BF16),
            pltpu.VMEM((2, 2) + tables[0].shape[1:], F32),
            pltpu.VMEM((2, 2, heads, slots, head_dim), BF16),
            pltpu.VMEM((chunk_len, span), F32),
            pltpu.VMEM((heads, half, head_dim), F32),
            pltpu.VMEM((heads, half, head_dim), F32),
            pltpu.VMEM((heads, half, head_dim), F32),
            pltpu.VMEM((4, 8, chunk_len), F32),
            pltpu.VMEM((3, 8, chunk_len), F32),
            pltpu.VMEM((4, STAGES, tokens, d_model), BF16),
            pltpu.VMEM((3, STAGES, tokens, d_model), F32),
        ]
        + [dma((SLICES,)), dma((SLICES,)), dma, dma((2,)), dma((2, 2)), dma((TILES,)), dma((TILES,)), dma((2, 2)), dma((heads,)),
           dma((2,)), dma((2, 2))]
        + [dma((2, TILES, 3))] * 2
        + [dma((HALVES,))] * 12
        + [dma((CHUNKS,))] * 5
        + [dma((5,)), dma((4, STAGES)), dma((3, STAGES))],
        compiler_params=pltpu.CompilerParams(collective_id=0, has_side_effects=True, vmem_limit_bytes=LAYER_LIMIT),
        cost_estimate=pl.CostEstimate(flops=100_000_000_000, bytes_accessed=chunk_len * d_model * 16, transcendentals=0),
        name="layer",
    )(lengths, hidden_in, *tables, k_block, v_block, w_qkv, w_up, w_down, w_out, *norms, small[None])
    return out, pk, qb


def finish_kernel(heads, meta, in_ref, pk, qb, out_ref, k_ref, v_ref, buf, low, high, in_sem, out_sem, low_sem, high_sem, kv_sem):
    pieces = in_sem.shape[1]
    tile = buf.shape[1] // pieces
    head_dim = k_ref.shape[3]
    places = [(b, pl.ds(t * tile, tile), t) for b in range(buf.shape[0]) for t in range(pieces)]
    inward = [pltpu.make_async_copy(in_ref.at[b, rows], buf.at[b, rows], in_sem.at[b, t]) for b, rows, t in places]
    outward = [pltpu.make_async_copy(buf.at[b, rows], out_ref.at[b, rows], out_sem.at[b, t]) for b, rows, t in places]
    both = 2 * head_dim

    def taken(src, dst, sem):
        return [[pltpu.make_async_copy(src.at[n, :, pl.ds((3 * h + 1) * head_dim, both)], dst.at[n, :, pl.ds(h * both, both)], sem.at[n, h])
                 for h in range(heads)] for n in range(2)]

    lows, highs = taken(pk, low, low_sem), taken(qb, high, high_sem)
    stored = []

    def store(n, h, row):
        for p, ref in enumerate((k_ref, v_ref)):
            cols = pl.ds(h * both + p * head_dim, head_dim)
            copy = pltpu.make_async_copy(low.at[n, :, cols], ref.at[row, h], kv_sem.at[n, h, p])
            copy.start()
            stored.append(copy)

    for copy in highs[0] + highs[1] + lows[0] + lows[1] + inward:
        copy.start()
    j = meta[0]
    for n in range(2):
        for h in range(heads):
            lows[n][h].wait()
            store(n, h, j ^ (2 - 2 * n))
    for n in range(2):
        for h in range(heads):
            highs[n][h].wait()
            cols = slice(h * both, (h + 1) * both)
            low[2 + n, :, cols] = high[n, :, cols].astype(BF16)
            store(2 + n, h, j ^ (3 - 2 * n))
    for one, other in zip(inward, outward):
        one.wait()
        other.start()
    for copy in outward + stored:
        copy.wait()


def finish(meta, out, pk, qb, heads, head_dim):
    rows, chunk_len, _ = out.shape
    span = 2 * heads * head_dim
    hbm = pl.BlockSpec(memory_space=pl.ANY)
    cache = jax.ShapeDtypeStruct((rows, heads, chunk_len, head_dim), BF16)
    dma = pltpu.SemaphoreType.DMA
    return pl.pallas_call(
        functools.partial(finish_kernel, heads),
        in_specs=[pl.BlockSpec(memory_space=pltpu.SMEM)] + [hbm] * 3,
        out_specs=[hbm] * 3,
        out_shape=[jax.ShapeDtypeStruct(out.shape, out.dtype), cache, cache],
        scratch_shapes=[
            pltpu.VMEM(out.shape, out.dtype), pltpu.VMEM((4, chunk_len, span), BF16), pltpu.VMEM((2, chunk_len, span), F32),
            dma((rows, 4)), dma((rows, 4)), dma((2, heads)), dma((2, heads)), dma((4, heads, 2)),
        ],
        compiler_params=pltpu.CompilerParams(vmem_limit_bytes=VMEM_LIMIT),
        name="finish",
    )(meta, out, pk, qb)


def solution(mesh):
    in_specs = (P("dp", None, None), P("dp"), P("dp", "tp", "cp", None), P("dp", "tp", "cp", None), P(), P(), P(), P(), P(None, "tp"), P("tp"), P("tp", None), P(), P(None, "tp"), P("tp"), P("tp", None), P())
    out_specs = (P("dp", None, None), P("dp", "tp", None, None), P("dp", "tp", None, None))
    tp_size = mesh.shape["tp"]

    def local_layer(hidden_in, lengths, k_block, v_block, ln1_gain, ln1_bias, ln2_gain, ln2_bias, w_qkv, b_qkv, w_out, b_out, w_up, b_up, w_down, b_down):
        num_rows, chunk_len, d_model = hidden_in.shape
        heads, block_len, head_dim = k_block.shape[1:]
        tables = rope_tables(lengths, chunk_len, head_dim)
        norms = [p[None] for p in (ln1_gain, ln1_bias, ln2_gain, ln2_bias)]
        parts = [(b_qkv, 0), (b_up, b_qkv.shape[0]), (b_out, b_qkv.shape[0] + b_up.shape[0]), (b_down, b_qkv.shape[0] + b_up.shape[0])]
        total = b_qkv.shape[0] + b_up.shape[0] + d_model
        small = functools.reduce(jnp.add, [jnp.pad(p.astype(F32), (at, total - at - p.shape[0])) for p, at in parts])
        out, pk, qb = run_layer(lengths, hidden_in, tables, k_block, v_block, w_qkv, w_up, w_down, w_out, norms, small, tp_size)
        return tuple(finish(lax.axis_index("cp")[None], out, pk, qb, heads, head_dim))

    return jax.shard_map(local_layer, mesh=mesh, in_specs=in_specs, out_specs=out_specs, check_vma=False)
```
